128 devices in a mesh: prompts: 1, model: 16 (over z, y), resp: 8 (over x, core).
Axes of the slice: x: 4, y: 4, z: 4, core: 2. Of those that a mesh axis runs over, the one named last changes fastest.
Arguments:
- x_prompt: bfloat16 [1024, 4096], P(('prompts', 'resp'))
- x_resp: bfloat16 [8, 1024, 4096], P(('prompts', 'resp'))
- targets: int32 [8, 1024], P(('prompts', 'resp'))
- resp_lens: int32 [8], P(('prompts', 'resp'))
- attn_gain: float32 [2, 4096], replicated
- w_query: bfloat16 [2, 4096, 32, 128], P(None, None, 'model')
- w_key: bfloat16 [2, 4096, 32, 128], P(None, None, 'model')
- w_value: bfloat16 [2, 4096, 32, 128], P(None, None, 'model')
- w_out: bfloat16 [2, 32, 128, 4096], P(None, 'model')
- mlp_gain: float32 [2, 4096], replicated
- w_gate: bfloat16 [2, 4096, 11008], P(None, None, 'model')
- w_up: bfloat16 [2, 4096, 11008], P(None, None, 'model')
- w_down: bfloat16 [2, 11008, 4096], P(None, 'model')
- final_gain: float32 [4096], replicated
- w_vocab: bfloat16 [4096, 32768], P(None, 'model')
Outputs:
- output: float32 [8, 1024], P(('prompts', 'resp'))
All inputs are finite; a program needn't handle non-finite values.
Results may differ from the reference program's by a relative error of at most 0.002451.
Values are sent between devices in bfloat16 or wider.
A program may use at most 1 GiB of HBM per device.

```python
import jax
import jax.numpy as jnp
from jax import lax

MODEL_DIM = 4096
NUM_HEADS = 32
KV_HEADS = 32
HEAD_DIM = 128
FFN_DIM = 11008
VOCAB_SIZE = 32768
GROUP_SIZE = 8
PROMPT_ROWS = 128
RESP_LEN = 1024
LAYERS = 2
PROMPT_LEN = GROUP_SIZE * PROMPT_ROWS
EPS = 1e-6
ROPE_BASE = 10000.0


def rms_norm(acts_in, gain_vec):
    acts_f = acts_in.astype(jnp.float32)
    inv_rms = lax.rsqrt(jnp.mean(acts_f * acts_f, axis=-1, keepdims=True) + EPS)
    return (acts_f * inv_rms * gain_vec).astype(jnp.bfloat16)


def rotary(projected, positions):
    half_dim = projected.shape[-1] // 2
    frequency = ROPE_BASE ** (-jnp.arange(half_dim, dtype=jnp.float32) / half_dim)
    angles = positions.astype(jnp.float32)[..., None] * frequency
    cos_part = jnp.cos(angles)[..., None, :]
    sin_part = jnp.sin(angles)[..., None, :]
    lower_half = projected[..., :half_dim]
    upper_half = projected[..., half_dim:]
    return jnp.concatenate([lower_half * cos_part - upper_half * sin_part, upper_half * cos_part + lower_half * sin_part], axis=-1)


def attend(queries, keys, values, query_pos, key_pos):
    tokens = queries.shape[0]
    grouped = queries.reshape(tokens, KV_HEADS, NUM_HEADS // KV_HEADS, HEAD_DIM).astype(jnp.float32)
    scores = jnp.einsum('tkrd,skd->krts', grouped, keys.astype(jnp.float32)) * (HEAD_DIM ** -0.5)
    visible = key_pos[None, :] <= query_pos[:, None]
    scores = jnp.where(visible, scores, -jnp.inf)
    row_max = jnp.max(scores, axis=-1, keepdims=True)
    exp_scores = jnp.exp(scores - row_max)
    row_sum = jnp.moveaxis(jnp.sum(exp_scores, axis=-1), -1, 0)
    mixed = jnp.einsum('krts,skd->tkrd', exp_scores.astype(jnp.bfloat16).astype(jnp.float32), values.astype(jnp.float32))
    return (mixed / row_sum[..., None]).reshape(tokens, NUM_HEADS * HEAD_DIM).astype(jnp.bfloat16)


def setup_inputs(seed: int = 0, part: int = 0) -> dict:
    root_keys = jax.random.split(jax.random.key(seed), 2)
    part_keys = jax.random.split(jax.random.fold_in(root_keys[0], part), 7)
    shared_keys = jax.random.split(root_keys[1], 11)

    def normal_weight(key_in, shape, scale):
        return (jax.random.normal(key_in, shape, jnp.float32) * scale).astype(jnp.bfloat16)

    def gain_draw(key_in, shape):
        return jax.random.uniform(key_in, shape, jnp.float32, 0.25, 1.75)

    topics = jax.random.normal(part_keys[0], (4, 1, MODEL_DIM), jnp.float32)
    prompt_noise = jax.random.normal(part_keys[1], (4, PROMPT_LEN // 4, MODEL_DIM), jnp.float32)
    x_prompt = (0.6 * topics + 0.3 * prompt_noise).reshape(PROMPT_LEN, MODEL_DIM).astype(jnp.bfloat16)
    resp_topics = jax.random.normal(part_keys[2], (GROUP_SIZE, 1, MODEL_DIM), jnp.float32)
    resp_noise = jax.random.normal(part_keys[3], (GROUP_SIZE, RESP_LEN, MODEL_DIM), jnp.float32)
    x_resp = (0.6 * resp_topics + 0.3 * resp_noise).astype(jnp.bfloat16)
    targets = jax.random.randint(part_keys[4], (GROUP_SIZE, RESP_LEN), 0, VOCAB_SIZE, dtype=jnp.int32)
    targets = targets.at[0, 0].set(0).at[0, 1].set(VOCAB_SIZE - 1)
    drawn_lens = jax.random.randint(part_keys[5], (GROUP_SIZE,), RESP_LEN // 8, RESP_LEN + 1, dtype=jnp.int32)
    full_slot = jax.random.randint(part_keys[6], (), 0, GROUP_SIZE, dtype=jnp.int32)
    resp_lens = jnp.where(jnp.arange(GROUP_SIZE) == full_slot, RESP_LEN, drawn_lens).astype(jnp.int32)
    return {
        'x_prompt': x_prompt,
        'x_resp': x_resp,
        'targets': targets,
        'resp_lens': resp_lens,
        'attn_gain': gain_draw(shared_keys[0], (LAYERS, MODEL_DIM)),
        'w_query': normal_weight(shared_keys[1], (LAYERS, MODEL_DIM, NUM_HEADS, HEAD_DIM), MODEL_DIM ** -0.5),
        'w_key': normal_weight(shared_keys[2], (LAYERS, MODEL_DIM, KV_HEADS, HEAD_DIM), MODEL_DIM ** -0.5),
        'w_value': normal_weight(shared_keys[3], (LAYERS, MODEL_DIM, KV_HEADS, HEAD_DIM), MODEL_DIM ** -0.5),
        'w_out': normal_weight(shared_keys[4], (LAYERS, NUM_HEADS, HEAD_DIM, MODEL_DIM), (NUM_HEADS * HEAD_DIM) ** -0.5),
        'mlp_gain': gain_draw(shared_keys[5], (LAYERS, MODEL_DIM)),
        'w_gate': normal_weight(shared_keys[6], (LAYERS, MODEL_DIM, FFN_DIM), MODEL_DIM ** -0.5),
        'w_up': normal_weight(shared_keys[7], (LAYERS, MODEL_DIM, FFN_DIM), MODEL_DIM ** -0.5),
        'w_down': normal_weight(shared_keys[8], (LAYERS, FFN_DIM, MODEL_DIM), FFN_DIM ** -0.5),
        'final_gain': gain_draw(shared_keys[9], (MODEL_DIM,)),
        'w_vocab': normal_weight(shared_keys[10], (MODEL_DIM, VOCAB_SIZE), 2.0 * MODEL_DIM ** -0.5),
    }


def reference(x_prompt, x_resp, targets, resp_lens, attn_gain, w_query, w_key, w_value, w_out, mlp_gain, w_gate, w_up, w_down, final_gain, w_vocab):
    prompt_pos = jnp.arange(PROMPT_LEN)
    resp_pos = PROMPT_LEN + jnp.arange(RESP_LEN)
    key_pos = jnp.concatenate([prompt_pos, resp_pos])

    def project(hidden, weight, heads):
        flat = jnp.dot(hidden, weight.reshape(MODEL_DIM, heads * HEAD_DIM), preferred_element_type=jnp.float32)
        return flat.reshape(hidden.shape[0], heads, HEAD_DIM)

    def key_value(hidden, layer_idx, positions):
        keys = rotary(project(hidden, w_key[layer_idx], KV_HEADS), positions).astype(jnp.bfloat16)
        values = project(hidden, w_value[layer_idx], KV_HEADS).astype(jnp.bfloat16)
        return keys, values

    def query_proj(hidden, layer_idx, positions):
        return rotary(project(hidden, w_query[layer_idx], NUM_HEADS), positions).astype(jnp.bfloat16)

    def finish(residual, mixed, layer_idx):
        attn_out = jnp.dot(mixed, w_out[layer_idx].reshape(NUM_HEADS * HEAD_DIM, MODEL_DIM), preferred_element_type=jnp.float32)
        residual = (residual.astype(jnp.float32) + attn_out).astype(jnp.bfloat16)
        hidden = rms_norm(residual, mlp_gain[layer_idx])
        gate = jnp.dot(hidden, w_gate[layer_idx], preferred_element_type=jnp.float32)
        up_proj = jnp.dot(hidden, w_up[layer_idx], preferred_element_type=jnp.float32)
        inner = (jax.nn.silu(gate) * up_proj).astype(jnp.bfloat16)
        down_out = jnp.dot(inner, w_down[layer_idx], preferred_element_type=jnp.float32)
        return (residual.astype(jnp.float32) + down_out).astype(jnp.bfloat16)

    residual = x_prompt
    prompt_cache = []
    for layer_idx in range(LAYERS):
        hidden = rms_norm(residual, attn_gain[layer_idx])
        keys, values = key_value(hidden, layer_idx, prompt_pos)
        prompt_cache.append((keys, values))
        if layer_idx < LAYERS - 1:
            blocks = query_proj(hidden, layer_idx, prompt_pos).reshape(GROUP_SIZE, PROMPT_ROWS, NUM_HEADS, HEAD_DIM)
            block_pos = prompt_pos.reshape(GROUP_SIZE, PROMPT_ROWS)
            mixed = lax.map(lambda block_args: attend(block_args[0], keys, values, block_args[1], prompt_pos), (blocks, block_pos))
            residual = finish(residual, mixed.reshape(PROMPT_LEN, NUM_HEADS * HEAD_DIM), layer_idx)

    def one_response(resp_args):
        residual_r, target_row, length = resp_args
        for layer_idx in range(LAYERS):
            hidden = rms_norm(residual_r, attn_gain[layer_idx])
            keys, values = key_value(hidden, layer_idx, resp_pos)
            queries = query_proj(hidden, layer_idx, resp_pos)
            all_keys = jnp.concatenate([prompt_cache[layer_idx][0], keys], axis=0)
            all_values = jnp.concatenate([prompt_cache[layer_idx][1], values], axis=0)
            mixed = attend(queries, all_keys, all_values, resp_pos, key_pos)
            residual_r = finish(residual_r, mixed, layer_idx)
        logits = jnp.dot(rms_norm(residual_r, final_gain), w_vocab, preferred_element_type=jnp.float32)
        picked = jnp.take_along_axis(logits, target_row[:, None], axis=-1)[:, 0]
        log_probs = picked - jax.nn.logsumexp(logits, axis=-1)
        return jnp.where(jnp.arange(RESP_LEN) < length, log_probs, 0.0)

    return lax.map(one_response, (x_resp, targets, resp_lens))
```

```python
import jax
import jax.numpy as jnp
from jax import lax
from jax.sharding import PartitionSpec as P

EPS = 1e-6
ROPE_BASE = 10000.0


def rms_norm(acts_in, gain_vec):
    acts_f = acts_in.astype(jnp.float32)
    inv_rms = lax.rsqrt(jnp.mean(acts_f * acts_f, axis=-1, keepdims=True) + EPS)
    return (acts_f * inv_rms * gain_vec).astype(jnp.bfloat16)


def rope_tables(positions, half_dim):
    frequency = ROPE_BASE ** (-jnp.arange(half_dim, dtype=jnp.float32) / half_dim)
    angles = positions.astype(jnp.float32)[..., None] * frequency
    return jnp.cos(angles)[..., None, :], jnp.sin(angles)[..., None, :]


def rotary(projected, tables):
    cos_part, sin_part = tables
    half_dim = projected.shape[-1] // 2
    lower_half = projected[..., :half_dim]
    upper_half = projected[..., half_dim:]
    return jnp.concatenate([lower_half * cos_part - upper_half * sin_part, upper_half * cos_part + lower_half * sin_part], axis=-1)


def attend(queries, keys, values, query_pos, key_pos):
    head_dim = queries.shape[-1]
    scores = jnp.einsum('the,she->hts', queries, keys, preferred_element_type=jnp.float32) * (head_dim ** -0.5)
    visible = (key_pos[None, :] <= query_pos[:, None])[None]
    scores = jnp.where(visible, scores, -jnp.inf)
    row_max = jnp.max(scores, axis=-1, keepdims=True)
    exp_scores = jnp.exp(scores - row_max)
    row_sum = jnp.moveaxis(jnp.sum(exp_scores, axis=-1), -1, 0)
    mixed = jnp.einsum('hts,she->the', exp_scores.astype(jnp.bfloat16), values, preferred_element_type=jnp.float32)
    return (mixed / row_sum[..., None]).astype(jnp.bfloat16)


def solution(mesh):
    groups = mesh.shape['resp']
    shards = mesh.shape['model']
    row_axes = ('prompts', 'resp')
    head_spec = P(None, None, 'model', None)
    in_specs = (P(row_axes, None), P(row_axes, None, None), P(row_axes, None), P(row_axes), P(None, None), head_spec, head_spec, head_spec, P(None, 'model', None, None), P(None, None), P(None, None, 'model'), P(None, None, 'model'), P(None, 'model', None), P(None), P(None, 'model'))

    def device_step(x_prompt, x_resp, targets, resp_lens, attn_gain, w_query, w_key, w_value, w_out, mlp_gain, w_gate, w_up, w_down, final_gain, w_vocab):
        prompt_rows = x_prompt.shape[0]
        resp_len = x_resp.shape[1]
        width = x_resp.shape[2]
        prompt_len = prompt_rows * groups
        num_layers = w_query.shape[0]
        part_p, part_r = prompt_rows // shards, resp_len // shards
        me = lax.axis_index('model')
        resp_pos = prompt_len + jnp.arange(resp_len)
        prompt_pos = lax.axis_index('resp') * prompt_rows + jnp.arange(prompt_rows)
        mine = lambda rows, n: lax.dynamic_slice_in_dim(rows, me * n, n, 0)
        residual = jnp.concatenate([mine(x_prompt, part_p), mine(x_resp[0], part_r)], axis=0)
        hidden = jnp.concatenate([x_prompt.reshape(shards, part_p, width), x_resp[0].reshape(shards, part_r, width)], axis=1).reshape(-1, width)
        hidden = rms_norm(hidden, attn_gain[0])
        tok_pos = jnp.concatenate([prompt_pos.reshape(shards, part_p), resp_pos.reshape(shards, part_r)], axis=1).reshape(-1)
        key_pos = jnp.concatenate([jnp.arange(prompt_len), resp_pos])

        def reduce_rows(part):
            return lax.psum_scatter(part, 'model', scatter_dimension=0, tiled=True)

        def gather_rows(rows):
            return lax.all_gather(rows, 'model', axis=0, tiled=True)

        def split(rows):
            cut = rows.reshape((shards, part_p + part_r) + rows.shape[1:])
            return cut[:, :part_p].reshape((prompt_rows,) + rows.shape[1:]), cut[:, part_p:].reshape((resp_len,) + rows.shape[1:])

        for layer_idx in range(num_layers):
            tables = rope_tables(tok_pos, w_key.shape[-1] // 2)
            keys = rotary(jnp.einsum('td,dhe->the', hidden, w_key[layer_idx], preferred_element_type=jnp.float32), tables).astype(jnp.bfloat16)
            values = jnp.einsum('td,dhe->the', hidden, w_value[layer_idx], preferred_element_type=jnp.float32).astype(jnp.bfloat16)
            key_p, key_r = split(keys)
            val_p, val_r = split(values)
            both = lax.all_gather(jnp.concatenate([key_p, val_p], axis=1), 'resp', axis=0, tiled=True)
            heads = keys.shape[1]
            all_keys = jnp.concatenate([both[:, :heads], key_r], axis=0)
            all_values = jnp.concatenate([both[:, heads:], val_r], axis=0)
            query_pos = tok_pos
            if layer_idx == num_layers - 1:
                residual = residual[part_p:]
                hidden = split(hidden)[1]
                query_pos = resp_pos
                tables = rope_tables(query_pos, w_key.shape[-1] // 2)
            queries = rotary(jnp.einsum('td,dhe->the', hidden, w_query[layer_idx], preferred_element_type=jnp.float32), tables).astype(jnp.bfloat16)
            mixed = attend(queries, all_keys, all_values, query_pos, key_pos)
            attn_part = jnp.einsum('the,hed->td', mixed, w_out[layer_idx], preferred_element_type=jnp.float32)
            residual = (residual.astype(jnp.float32) + reduce_rows(attn_part)).astype(jnp.bfloat16)
            hidden = gather_rows(rms_norm(residual, mlp_gain[layer_idx]))
            gate = jnp.dot(hidden, w_gate[layer_idx], preferred_element_type=jnp.float32)
            up_proj = jnp.dot(hidden, w_up[layer_idx], preferred_element_type=jnp.float32)
            inner = (jax.nn.silu(gate) * up_proj).astype(jnp.bfloat16)
            down_part = jnp.dot(inner, w_down[layer_idx], preferred_element_type=jnp.float32)
            residual = (residual.astype(jnp.float32) + reduce_rows(down_part)).astype(jnp.bfloat16)
            next_gain = attn_gain[layer_idx + 1] if layer_idx < num_layers - 1 else final_gain
            hidden = gather_rows(rms_norm(residual, next_gain))
        logits = jnp.dot(hidden, w_vocab, preferred_element_type=jnp.float32)
        vocab_local = logits.shape[-1]
        vocab_ids = me * vocab_local + jnp.arange(vocab_local)
        row_max = jnp.max(logits, axis=-1)
        exp_total = jnp.sum(jnp.exp(logits - row_max[:, None]), axis=-1)
        picked = jnp.sum(jnp.where(vocab_ids[None, :] == targets[0][:, None], logits, 0.0), axis=-1)
        stats = lax.all_gather(jnp.stack([row_max, exp_total, picked]), 'model', axis=0)
        top = jnp.max(stats[:, 0], axis=0)
        total = jnp.sum(stats[:, 1] * jnp.exp(stats[:, 0] - top), axis=0)
        log_probs = jnp.sum(stats[:, 2], axis=0) - top - jnp.log(total)
        log_probs = jnp.where(jnp.arange(resp_len) < resp_lens[0], log_probs, 0.0)
        return log_probs[None, :]

    return jax.shard_map(device_step, mesh=mesh, in_specs=in_specs, out_specs=P(row_axes, None), check_vma=False)
```

```python
import functools

import jax
import jax.numpy as jnp
from jax import lax
from jax.experimental import pallas as pl
from jax.experimental.pallas import tpu as pltpu

MESH = pl.DeviceIdType.MESH
F32 = jnp.float32
BF16 = jnp.bfloat16
EPS = 1e-6
N_KINDS = 24


def block_of(color, first, second):
    return 4 * second + first if color == 0 else 4 * first + second


class Torus:
    def __init__(self, refs, send_sem, recv_sem):
        self.st2, self.sb, self.r1, self.r2a, self.r2b, self.r3, self.r4, self.xg = refs
        self.send_sem, self.recv_sem = send_sem, recv_sem
        me = lax.axis_index("model")
        z, y = me // 4, me % 4
        self.place = ((y, z), (z, y))
        plus = lambda v, d: (v + d + 4) % 4
        self.plus = plus
        along_y = (z * 4 + plus(y, 1), z * 4 + plus(y, -1))
        along_z = (plus(z, 1) * 4 + y, plus(z, -1) * 4 + y)
        self.near = ((along_y, along_z), (along_z, along_y))
        self.all_near = along_y + along_z

    def barrier(self):
        sem = pltpu.get_barrier_semaphore()
        for device in self.all_near:
            pl.semaphore_signal(sem, inc=1, device_id={"model": device}, device_id_type=MESH)
        pl.semaphore_wait(sem, 4)

    def copy(self, kind, c, q, src, dst, device):
        return pltpu.make_async_remote_copy(
            src_ref=src, dst_ref=dst, send_sem=self.send_sem.at[c, q, kind], recv_sem=self.recv_sem.at[c, q, kind],
            device_id={"model": device}, device_id_type=MESH)

    def outgoing(self, kind, c, q):
        (p, s), plus = self.place[q], self.plus
        (right_p, left_p), (right_s, left_s) = self.near[q]
        st2, sb, r1, r2a, r2b, r3, r4, xg = (ref.at[c, q] for ref in (self.st2, self.sb, self.r1, self.r2a, self.r2b, self.r3, self.r4, self.xg))
        lo, hi = pl.ds(0, 2), pl.ds(2, 2)
        src, dst, device = {
            0: lambda: (st2.at[lo], r1.at[0], right_p),
            1: lambda: (st2.at[hi], r1.at[1], left_p),
            2: lambda: (sb.at[0], r2a.at[hi], right_p),
            3: lambda: (sb.at[1], r2b.at[lo], left_p),
            4: lambda: (r1.at[0], r2a.at[lo], right_p),
            5: lambda: (r1.at[1], r2b.at[hi], left_p),
            6: lambda: (r2a.at[plus(s, 2), 0], r3.at[0], right_s),
            7: lambda: (r2a.at[plus(s, 2), 1], r3.at[1], left_s),
            8: lambda: (r2a.at[plus(s, 1), 1], r4.at[0, 1], right_s),
            9: lambda: (r2a.at[plus(s, -1), 0], r4.at[1, 0], left_s),
            10: lambda: (r3.at[0], r4.at[0, 0], right_s),
            11: lambda: (r3.at[1], r4.at[1, 1], left_s),
            12: lambda: (xg.at[p, s, 0], xg.at[p, s, 0], right_s),
            13: lambda: (xg.at[p, s, 1], xg.at[p, s, 1], left_s),
            14: lambda: (xg.at[p, s, 1], xg.at[p, s, 1], right_s),
            15: lambda: (xg.at[p, s, 0], xg.at[p, s, 0], left_s),
            16: lambda: (xg.at[p, plus(s, -1), 0], xg.at[p, plus(s, -1), 0], right_s),
            17: lambda: (xg.at[p, plus(s, 1), 1], xg.at[p, plus(s, 1), 1], left_s),
            18: lambda: (xg.at[p, lo], xg.at[p, lo], right_p),
            19: lambda: (xg.at[p, hi], xg.at[p, hi], left_p),
            20: lambda: (xg.at[p, hi], xg.at[p, hi], right_p),
            21: lambda: (xg.at[p, lo], xg.at[p, lo], left_p),
            22: lambda: (xg.at[plus(p, -1), lo], xg.at[plus(p, -1), lo], right_p),
            23: lambda: (xg.at[plus(p, 1), hi], xg.at[plus(p, 1), hi], left_p),
        }[kind]()
        return self.copy(kind, c, q, src, dst, device)

    def incoming(self, kind, c, q):
        (p, s), plus = self.place[q], self.plus
        r1, r2a, r2b, r3, r4, xg = (ref.at[c, q] for ref in (self.r1, self.r2a, self.r2b, self.r3, self.r4, self.xg))
        lo, hi = pl.ds(0, 2), pl.ds(2, 2)
        (right_p, left_p), (right_s, left_s) = self.near[q]
        dst = {
            0: lambda: r1.at[0], 1: lambda: r1.at[1],
            2: lambda: r2a.at[hi], 3: lambda: r2b.at[lo], 4: lambda: r2a.at[lo], 5: lambda: r2b.at[hi],
            6: lambda: r3.at[0], 7: lambda: r3.at[1],
            8: lambda: r4.at[0, 1], 9: lambda: r4.at[1, 0], 10: lambda: r4.at[0, 0], 11: lambda: r4.at[1, 1],
            12: lambda: xg.at[p, plus(s, -1), 0], 13: lambda: xg.at[p, plus(s, 1), 1],
            14: lambda: xg.at[p, plus(s, -1), 1], 15: lambda: xg.at[p, plus(s, 1), 0],
            16: lambda: xg.at[p, plus(s, 2), 0], 17: lambda: xg.at[p, plus(s, 2), 1],
            18: lambda: xg.at[plus(p, -1), lo], 19: lambda: xg.at[plus(p, 1), hi],
            20: lambda: xg.at[plus(p, -1), hi], 21: lambda: xg.at[plus(p, 1), lo],
            22: lambda: xg.at[plus(p, 2), lo], 23: lambda: xg.at[plus(p, 2), hi],
        }[kind]()
        return self.copy(kind, c, q, dst, dst, right_p)

    def send(self, c, q, *kinds):
        for kind in kinds:
            self.outgoing(kind, c, q).start()

    def sent(self, c, q, *kinds):
        for kind in kinds:
            self.outgoing(kind, c, q).wait_send()

    def arrived(self, c, q, *kinds):
        for kind in kinds:
            self.incoming(kind, c, q).wait_recv()


def store_block(ref, value):
    ref[0] = value[:, :128]
    ref[1] = value[:, 128:]


def add_block(ref, value):
    ref[0] += value[:, :128]
    ref[1] += value[:, 128:]


def product(lhs, w_ref, color, first, second):
    start = pl.multiple_of(block_of(color, first, second) * 256, 256)
    return jnp.dot(lhs, w_ref[:, pl.ds(start, 256)], preferred_element_type=F32)


def stage_head(net, c, q, lhs, w_ref):
    (p, s), plus = net.place[q], net.plus
    for k in range(4):
        store_block(net.st2.at[c, q, k], product(lhs, w_ref, q, plus(p, 2), k))
    net.send(c, q, 0, 1)
    for k in range(2):
        store_block(net.sb.at[c, q, 0, k], product(lhs, w_ref, q, plus(p, 1), 2 + k))
        store_block(net.sb.at[c, q, 1, k], product(lhs, w_ref, q, plus(p, -1), k))
    net.send(c, q, 2, 3)


def stage_rest(net, chunks, lhs_of, w_ref, finish):
    plus = net.plus

    def over_chunks(body):
        @pl.loop(0, chunks)
        def _(c):
            for q in range(2):
                body(c, q)

    def relay_first(c, q):
        p, s = net.place[q]
        lhs = lhs_of(c, q)
        net.arrived(c, q, 0)
        for k in range(2):
            add_block(net.r1.at[c, q, 0, k], product(lhs, w_ref, q, plus(p, 1), k))
        net.send(c, q, 4)
        net.arrived(c, q, 1)
        for k in range(2):
            add_block(net.r1.at[c, q, 1, k], product(lhs, w_ref, q, plus(p, -1), 2 + k))
        net.send(c, q, 5)

    def own_first(c, q):
        p, s = net.place[q]
        lhs = lhs_of(c, q)
        net.arrived(c, q, 2, 3, 4, 5)
        for k in range(4):
            part = product(lhs, w_ref, q, p, k)
            net.r2a[c, q, k, 0] += net.r2b[c, q, k, 0] + part[:, :128]
            net.r2a[c, q, k, 1] += net.r2b[c, q, k, 1] + part[:, 128:]
        net.send(c, q, 6, 7, 8, 9)
        net.sent(c, q, 0, 1)

    def relay_second(c, q):
        p, s = net.place[q]
        net.arrived(c, q, 6)
        net.r3[c, q, 0] += net.r2a[c, q, plus(s, 1), 0]
        net.send(c, q, 10)
        net.arrived(c, q, 7)
        net.r3[c, q, 1] += net.r2a[c, q, plus(s, -1), 1]
        net.send(c, q, 11)

    def own_second(c, q):
        p, s = net.place[q]
        net.sent(c, q, 2, 3, 4, 5)
        net.arrived(c, q, 8, 9, 10, 11)
        for half in range(2):
            total = net.r2a[c, q, s, half] + net.r4[c, q, 0, half] + net.r4[c, q, 1, half]
            finish(c, q, half, total)
        net.send(c, q, 12, 13, 14, 15)

    def forward_first(c, q):
        net.sent(c, q, 6, 7, 8, 9, 10, 11)
        net.arrived(c, q, 12)
        net.send(c, q, 16)
        net.arrived(c, q, 13)
        net.send(c, q, 17)

    def send_second(c, q):
        net.arrived(c, q, 14, 15, 16, 17)
        net.send(c, q, 18, 19, 20, 21)

    def forward_second(c, q):
        net.arrived(c, q, 18)
        net.send(c, q, 22)
        net.arrived(c, q, 19)
        net.send(c, q, 23)

    for body in (relay_first, own_first, relay_second, own_second, forward_first, send_second, forward_second):
        over_chunks(body)


def stage_tail(net, c, q):
    net.arrived(c, q, 20, 21, 22, 23)
    net.sent(c, q, 12, 13, 14, 15, 16, 17, 18, 19, 20, 21, 22, 23)


def normed(net, c, q, gain_ref):
    rows = net.xg.shape[-2]
    tile = 16 if rows % 16 == 0 else 8

    @pl.loop(0, rows // tile)
    def _(i):
        span = pl.ds(pl.multiple_of(i * tile, tile), tile)
        acts = [net.xg[c, q, first, second, half, span].astype(F32) for first in range(4) for second in range(4) for half in range(2)]
        squares = functools.reduce(jnp.add, [v * v for v in acts])
        inv = lax.rsqrt(jnp.sum(squares, axis=-1, keepdims=True) * (1.0 / (128 * len(acts))) + EPS)
        for k, v in enumerate(acts):
            net.xg[c, q, k // 8, (k // 2) % 4, k % 2, span] = (v * inv * gain_ref[q, pl.ds(k, 1)]).astype(BF16)


def rows_of(net, c, q):
    parts = []
    for block in range(16):
        first, second = (block % 4, block // 4) if q == 0 else (block // 4, block % 4)
        parts += [net.xg[c, q, first, second, 0], net.xg[c, q, first, second, 1]]
    return jnp.concatenate(parts, axis=1)


def mega_kernel(chunks, a_ref, res_ref, gain_ref, next_gain_ref, w_out_hbm, w_gate_hbm, w_up_hbm, w_down_hbm,
                h_hbm, new_res_ref,
                w_out, w_gate, w_up, w_down, inner, res2, st2, sb, r1, r2a, r2b, r3, r4, xg,
                w_sem, out_sem, send_sem, recv_sem):
    loads = [pltpu.make_async_copy(src, dst, w_sem.at[i]) for i, (src, dst) in enumerate(
        ((w_out_hbm, w_out), (w_gate_hbm, w_gate), (w_up_hbm, w_up), (w_down_hbm, w_down)))]
    for load in loads:
        load.start()
    net = Torus((st2, sb, r1, r2a, r2b, r3, r4, xg), send_sem, recv_sem)
    net.barrier()
    loads[0].wait()

    @pl.loop(0, chunks)
    def _(c):
        for q in range(2):
            stage_head(net, c, q, a_ref[c, q], w_out)

    def finish_attention(c, q, half, total):
        p, s = net.place[q]
        value = (res_ref[c, q, half].astype(F32) + total).astype(BF16)
        res2[c, q, half] = value
        xg[c, q, p, s, half] = value

    stage_rest(net, chunks, lambda c, q: a_ref[c, q], w_out, finish_attention)
    for load in loads[1:]:
        load.wait()

    @pl.loop(0, chunks)
    def _(c):
        for q in range(2):
            stage_tail(net, c, q)
            normed(net, c, q, gain_ref)
            rows = rows_of(net, c, q)
            gate = lax.dot_general(rows, w_gate[...], (((1,), (1,)), ((), ())), preferred_element_type=F32)
            up = lax.dot_general(rows, w_up[...], (((1,), (1,)), ((), ())), preferred_element_type=F32)
            inner[c, q] = (jax.nn.silu(gate) * up).astype(BF16)
            stage_head(net, c, q, inner[c, q], w_down)

    def finish_mlp(c, q, half, total):
        p, s = net.place[q]
        value = (res2[c, q, half].astype(F32) + total).astype(BF16)
        new_res_ref[c, q, half] = value
        xg[c, q, p, s, half] = value

    stage_rest(net, chunks, lambda c, q: inner[c, q], w_down, finish_mlp)

    def out_copy(c, q):
        return pltpu.make_async_copy(xg.at[c, q], h_hbm.at[c, q], out_sem.at[c, q])

    @pl.loop(0, chunks)
    def _(c):
        for q in range(2):
            stage_tail(net, c, q)
            normed(net, c, q, next_gain_ref)
            out_copy(c, q).start()

    @pl.loop(0, chunks)
    def _(c):
        for q in range(2):
            out_copy(c, q).wait()


def mega(a, res, gain, next_gain, w_out, w_gate_t, w_up_t, w_down, collective_id):
    chunks, _, rows, depth = a.shape
    hidden = w_gate_t.shape[0]
    width = w_out.shape[1]
    per = (chunks, 2)
    vmem = pl.BlockSpec(memory_space=pltpu.VMEM)
    hbm = pl.BlockSpec(memory_space=pl.ANY)

    def by_color(g):
        grid = g.reshape(4, 4, 2, 128)
        return jnp.stack([grid.transpose(1, 0, 2, 3), grid]).reshape(2, 32, 128)

    return pl.pallas_call(
        functools.partial(mega_kernel, chunks),
        out_shape=(jax.ShapeDtypeStruct(per + (4, 4, 2, rows, 128), BF16), jax.ShapeDtypeStruct(per + (2, rows, 128), BF16)),
        in_specs=[vmem] * 4 + [hbm] * 4,
        out_specs=(hbm, vmem),
        scratch_shapes=[
            pltpu.VMEM((depth, width), BF16),
            pltpu.VMEM((hidden, width), BF16),
            pltpu.VMEM((hidden, width), BF16),
            pltpu.VMEM((hidden, width), BF16),
            pltpu.VMEM(per + (rows, hidden), BF16),
            pltpu.VMEM(per + (2, rows, 128), BF16),
            pltpu.VMEM(per + (4, 2, rows, 128), F32),
            pltpu.VMEM(per + (2, 2, 2, rows, 128), F32),
            pltpu.VMEM(per + (2, 2, 2, rows, 128), F32),
            pltpu.VMEM(per + (4, 2, rows, 128), F32),
            pltpu.VMEM(per + (4, 2, rows, 128), F32),
            pltpu.VMEM(per + (2, rows, 128), F32),
            pltpu.VMEM(per + (2, 2, rows, 128), F32),
            pltpu.VMEM(per + (4, 4, 2, rows, 128), BF16),
            pltpu.SemaphoreType.DMA((4,)),
            pltpu.SemaphoreType.DMA(per),
            pltpu.SemaphoreType.DMA(per + (N_KINDS,)),
            pltpu.SemaphoreType.DMA(per + (N_KINDS,)),
        ],
        compiler_params=pltpu.CompilerParams(collective_id=collective_id, has_side_effects=True, vmem_limit_bytes=67_000_000),
        name=f"mega{collective_id}",
    )(a, res, by_color(gain), by_color(next_gain), w_out, w_gate_t, w_up_t, w_down)


from jax.sharding import PartitionSpec as P

ROPE_BASE = 10000.0


def rms_norm(acts_in, gain_vec):
    acts_f = acts_in.astype(F32)
    inv_rms = lax.rsqrt(jnp.mean(acts_f * acts_f, axis=-1, keepdims=True) + EPS)
    return (acts_f * inv_rms * gain_vec).astype(BF16)


def rope_tables(positions, half_dim):
    frequency = ROPE_BASE ** (-jnp.arange(half_dim, dtype=F32) / half_dim)
    angles = positions.astype(F32)[..., None] * frequency
    return jnp.cos(angles)[..., None, :], jnp.sin(angles)[..., None, :]


def rotary(projected, tables):
    cos_part, sin_part = tables
    half_dim = projected.shape[-1] // 2
    lower_half = projected[..., :half_dim]
    upper_half = projected[..., half_dim:]
    return jnp.concatenate([lower_half * cos_part - upper_half * sin_part, upper_half * cos_part + lower_half * sin_part], axis=-1)


def attend(queries, keys, values, query_pos, key_pos):
    head_dim = queries.shape[-1]
    scores = jnp.einsum('the,she->hts', queries, keys, preferred_element_type=F32) * (head_dim ** -0.5)
    visible = (key_pos[None, :] <= query_pos[:, None])[None]
    scores = jnp.where(visible, scores, -jnp.inf)
    row_max = jnp.max(scores, axis=-1, keepdims=True)
    exp_scores = jnp.exp(scores - row_max)
    row_sum = jnp.moveaxis(jnp.sum(exp_scores, axis=-1), -1, 0)
    mixed = jnp.einsum('hts,she->the', exp_scores.astype(BF16), values, preferred_element_type=F32)
    return (mixed / row_sum[..., None]).astype(BF16)


def solution(mesh):
    groups = mesh.shape['resp']
    row_axes = ('prompts', 'resp')
    head_spec = P(None, None, 'model', None)
    in_specs = (P(row_axes, None), P(row_axes, None, None), P(row_axes, None), P(row_axes), P(None, None), head_spec, head_spec, head_spec, P(None, 'model', None, None), P(None, None), P(None, None, 'model'), P(None, None, 'model'), P(None, 'model', None), P(None), P(None, 'model'))
    chunks = 4

    def device_step(x_prompt, x_resp, targets, resp_lens, attn_gain, w_query, w_key, w_value, w_out, mlp_gain, w_gate, w_up, w_down, final_gain, w_vocab):
        prompt_rows = x_prompt.shape[0]
        resp_len, width = x_resp.shape[1:]
        prompt_len = prompt_rows * groups
        num_layers, _, heads, head_dim = w_query.shape
        me = lax.axis_index('model')
        resp_pos = prompt_len + jnp.arange(resp_len)
        tok_pos = jnp.concatenate([lax.axis_index('resp') * prompt_rows + jnp.arange(prompt_rows), resp_pos])
        key_pos = jnp.concatenate([jnp.arange(prompt_len), resp_pos])
        rows = jnp.concatenate([x_prompt, x_resp[0]], axis=0)
        residual = lax.dynamic_slice_in_dim(rows, me * 256, 256, 1)
        hidden = rms_norm(rows, attn_gain[0])
        gate_t, up_t = jnp.swapaxes(w_gate, 1, 2), jnp.swapaxes(w_up, 1, 2)

        for layer_idx in range(num_layers):
            tables = rope_tables(tok_pos, head_dim // 2)
            keys = rotary(jnp.einsum('td,dhe->the', hidden, w_key[layer_idx], preferred_element_type=F32), tables).astype(BF16)
            values = jnp.einsum('td,dhe->the', hidden, w_value[layer_idx], preferred_element_type=F32).astype(BF16)
            both = lax.all_gather(jnp.concatenate([keys[:prompt_rows], values[:prompt_rows]], axis=1), 'resp', axis=0, tiled=True)
            all_keys = jnp.concatenate([both[:, :heads], keys[prompt_rows:]], axis=0)
            all_values = jnp.concatenate([both[:, heads:], values[prompt_rows:]], axis=0)
            query_pos = tok_pos
            last = layer_idx == num_layers - 1
            if last:
                residual = residual[prompt_rows:]
                hidden = hidden[prompt_rows:]
                query_pos = resp_pos
                tables = rope_tables(query_pos, head_dim // 2)
            queries = rotary(jnp.einsum('td,dhe->the', hidden, w_query[layer_idx], preferred_element_type=F32), tables).astype(BF16)
            mixed = attend(queries, all_keys, all_values, query_pos, key_pos)
            count = residual.shape[0]
            part = count // (2 * chunks)
            gathered, new_res = mega(
                mixed.reshape(chunks, 2, part, heads * head_dim),
                residual.reshape(chunks, 2, part, 2, 128).transpose(0, 1, 3, 2, 4),
                mlp_gain[layer_idx], final_gain if last else attn_gain[layer_idx + 1],
                w_out[layer_idx].reshape(heads * head_dim, width), gate_t[layer_idx], up_t[layer_idx], w_down[layer_idx], layer_idx)
            residual = new_res.transpose(0, 1, 3, 2, 4).reshape(count, 256)
            first = gathered[:, 0].transpose(0, 4, 2, 1, 3, 5).reshape(chunks, part, width)
            second = gathered[:, 1].transpose(0, 4, 1, 2, 3, 5).reshape(chunks, part, width)
            hidden = jnp.stack([first, second], axis=1).reshape(count, width)
        logits = jnp.dot(hidden, w_vocab, preferred_element_type=F32)
        vocab_local = logits.shape[-1]
        vocab_ids = me * vocab_local + jnp.arange(vocab_local)
        row_max = jnp.max(logits, axis=-1)
        exp_total = jnp.sum(jnp.exp(logits - row_max[:, None]), axis=-1)
        picked = jnp.sum(jnp.where(vocab_ids[None, :] == targets[0][:, None], logits, 0.0), axis=-1)
        stats = lax.all_gather(jnp.stack([row_max, exp_total, picked]), 'model', axis=0)
        top = jnp.max(stats[:, 0], axis=0)
        total = jnp.sum(stats[:, 1] * jnp.exp(stats[:, 0] - top), axis=0)
        log_probs = jnp.sum(stats[:, 2], axis=0) - top - jnp.log(total)
        log_probs = jnp.where(jnp.arange(resp_len) < resp_lens[0], log_probs, 0.0)
        return log_probs[None, :]

    return jax.shard_map(device_step, mesh=mesh, in_specs=in_specs, out_specs=P(row_axes, None), check_vma=False)
```

```python
import functools

import jax
import jax.numpy as jnp
from jax import lax
from jax.experimental import pallas as pl
from jax.experimental.pallas import tpu as pltpu
from jax.sharding import PartitionSpec as P

MESH = pl.DeviceIdType.MESH
F32 = jnp.float32
BF16 = jnp.bfloat16
EPS = 1e-6
LANES = 128
PAIR = 2
RING = 4
COLUMNS = PAIR * LANES
SHARDS = RING * RING
BOTH = range(PAIR)
VMEM_BYTES = 67_000_000
VMEM = pl.BlockSpec(memory_space=pltpu.VMEM)
ANY = pl.BlockSpec(memory_space=pl.ANY)
DMA = pltpu.SemaphoreType.DMA
KINDS = range(RING * 3)
SUM_FAR, SUM_NEAR, SUM_RELAY, SUM2_FAR, SUM2_NEAR, SUM2_RELAY, TAKE_OWN, TAKE_REST, TAKE_RELAY, TAKE2_OWN, TAKE2_REST, TAKE2_RELAY = KINDS


def block_of(color, first, second):
    return RING * first + second if color else RING * second + first


def pair(index):
    return pl.ds(PAIR * index, PAIR)


class Torus:
    def __init__(self, refs, send_sem, recv_sem):
        self.refs = refs
        self.far, self.near, self.relayed, self.sums, self.relayed2, self.sums2, self.rows = refs
        self.send_sem, self.recv_sem = send_sem, recv_sem
        me = lax.axis_index("model")
        z, y = me // RING, me % RING
        self.place = ((y, z), (z, y))
        along_y = [z * RING + self.step(y, way) for way in (1, -1)]
        along_z = [self.step(z, way) * RING + y for way in (1, -1)]
        self.neighbors = ((along_y, along_z), (along_z, along_y))

    def step(self, place, by):
        return (place + by + RING) % RING

    def barrier(self):
        sem = pltpu.get_barrier_semaphore()
        for ring in self.neighbors[0]:
            for device in ring:
                pl.semaphore_signal(sem, device_id={"model": device}, device_id_type=MESH)
        pl.semaphore_wait(sem, RING)

    def ends(self, kind, c, q, d):
        (p, s), way, other = self.place[q], 1 - PAIR * d, 1 - d
        far, near, relayed, sums, relayed2, sums2, rows = (ref.at[c, q] for ref in self.refs)
        own = sums.at[0]
        back_s, back_p = self.step(s, -way), self.step(p, -way)
        return {
            SUM_FAR: lambda: (far.at[pair(d)], relayed.at[d], relayed.at[d]),
            SUM_NEAR: lambda: (near.at[d], sums.at[d, pair(other)], sums.at[d, pair(other)]),
            SUM_RELAY: lambda: (relayed.at[d], sums.at[d, pair(d)], sums.at[d, pair(d)]),
            SUM2_FAR: lambda: (own.at[self.step(s, PAIR), d], relayed2.at[d], relayed2.at[d]),
            SUM2_NEAR: lambda: (own.at[self.step(s, way), other], sums2.at[d, other], sums2.at[d, other]),
            SUM2_RELAY: lambda: (relayed2.at[d], sums2.at[d, d], sums2.at[d, d]),
            TAKE_OWN: lambda: (rows.at[p, s, d], rows.at[p, s, d], rows.at[p, back_s, d]),
            TAKE_REST: lambda: (rows.at[p, s, other], rows.at[p, s, other], rows.at[p, back_s, other]),
            TAKE_RELAY: lambda: (rows.at[p, back_s, d], rows.at[p, back_s, d], rows.at[p, self.step(s, PAIR), d]),
            TAKE2_OWN: lambda: (rows.at[p, pair(d)], rows.at[p, pair(d)], rows.at[back_p, pair(d)]),
            TAKE2_REST: lambda: (rows.at[p, pair(other)], rows.at[p, pair(other)], rows.at[back_p, pair(other)]),
            TAKE2_RELAY: lambda: (rows.at[back_p, pair(d)], rows.at[back_p, pair(d)], rows.at[self.step(p, PAIR), pair(d)]),
        }[kind]()

    def copy(self, kind, c, q, d, src, dst):
        second_ring = kind in (SUM2_FAR, SUM2_NEAR, SUM2_RELAY, TAKE_OWN, TAKE_REST, TAKE_RELAY)
        return pltpu.make_async_remote_copy(
            src_ref=src, dst_ref=dst, send_sem=self.send_sem.at[c, q, d, kind], recv_sem=self.recv_sem.at[c, q, d, kind],
            device_id={"model": self.neighbors[q][second_ring][d]}, device_id_type=MESH)

    def send(self, c, q, d, kind):
        src, dst, _ = self.ends(kind, c, q, d)
        self.copy(kind, c, q, d, src, dst).start()

    def sent(self, c, q, *kinds):
        for kind in kinds:
            for d in BOTH:
                src, dst, _ = self.ends(kind, c, q, d)
                self.copy(kind, c, q, d, src, dst).wait_send()

    def arrived(self, c, q, d, *kinds):
        for kind in kinds:
            _, _, here = self.ends(kind, c, q, d)
            self.copy(kind, c, q, d, here, here).wait_recv()


def halves(value):
    return value[:, :LANES], value[:, LANES:]


def store_block(ref, value):
    for half, part in enumerate(halves(value)):
        ref[half] = part


def add_block(ref, value):
    for half, part in enumerate(halves(value)):
        ref[half] += part


def product(lhs, w_ref, color, first, second):
    start = pl.multiple_of(block_of(color, first, second) * COLUMNS, COLUMNS)
    return jnp.dot(lhs, w_ref[:, pl.ds(start, COLUMNS)], preferred_element_type=F32)


def stage_head(net, c, q, lhs, w_ref):
    p = net.place[q][0]
    for k in range(RING):
        store_block(net.far.at[c, q, k], product(lhs, w_ref, q, net.step(p, PAIR), k))
    for d in BOTH:
        net.send(c, q, d, SUM_FAR)
    for d in BOTH:
        for k in BOTH:
            store_block(net.near.at[c, q, d, k], product(lhs, w_ref, q, net.step(p, 1 - PAIR * d), PAIR * (1 - d) + k))
        net.send(c, q, d, SUM_NEAR)


def stage_rest(net, chunks, lhs_of, w_ref, finish):
    def relay_first(c, q):
        lhs = lhs_of(c, q)
        for d in BOTH:
            net.arrived(c, q, d, SUM_FAR)
            for k in BOTH:
                add_block(net.relayed.at[c, q, d, k], product(lhs, w_ref, q, net.step(net.place[q][0], 1 - PAIR * d), PAIR * d + k))
            net.send(c, q, d, SUM_RELAY)

    def own_first(c, q):
        lhs = lhs_of(c, q)
        for d in BOTH:
            net.arrived(c, q, d, SUM_NEAR, SUM_RELAY)
        for k in range(RING):
            for half, part in enumerate(halves(product(lhs, w_ref, q, net.place[q][0], k))):
                net.sums[c, q, 0, k, half] += net.sums[c, q, 1, k, half] + part
        for d in BOTH:
            net.send(c, q, d, SUM2_FAR)
        for d in BOTH:
            net.send(c, q, d, SUM2_NEAR)
        net.sent(c, q, SUM_FAR)

    def relay_second(c, q):
        for d in BOTH:
            net.arrived(c, q, d, SUM2_FAR)
            net.relayed2[c, q, d] += net.sums[c, q, 0, net.step(net.place[q][1], 1 - PAIR * d), d]
            net.send(c, q, d, SUM2_RELAY)

    def own_second(c, q):
        net.sent(c, q, SUM_NEAR, SUM_RELAY)
        for d in BOTH:
            net.arrived(c, q, d, SUM2_NEAR, SUM2_RELAY)
        for half in BOTH:
            finish(c, q, half, net.sums[c, q, 0, net.place[q][1], half] + net.sums2[c, q, 0, half] + net.sums2[c, q, 1, half])
        for d in BOTH:
            net.send(c, q, d, TAKE_OWN)
        for d in BOTH:
            net.send(c, q, d, TAKE_REST)

    def forward_first(c, q):
        net.sent(c, q, SUM2_FAR, SUM2_NEAR, SUM2_RELAY)
        for d in BOTH:
            net.arrived(c, q, d, TAKE_OWN)
            net.send(c, q, d, TAKE_RELAY)

    def send_second(c, q):
        for d in BOTH:
            net.arrived(c, q, d, TAKE_REST, TAKE_RELAY)
        for d in BOTH:
            net.send(c, q, d, TAKE2_OWN)
        for d in BOTH:
            net.send(c, q, d, TAKE2_REST)

    def forward_second(c, q):
        for d in BOTH:
            net.arrived(c, q, d, TAKE2_OWN)
            net.send(c, q, d, TAKE2_RELAY)

    for body in (relay_first, own_first, relay_second, own_second, forward_first, send_second, forward_second):
        @pl.loop(0, chunks)
        def _(c):
            for q in BOTH:
                body(c, q)


def stage_tail(net, c, q):
    for d in BOTH:
        net.arrived(c, q, d, TAKE2_REST, TAKE2_RELAY)
    net.sent(c, q, TAKE_OWN, TAKE_REST, TAKE_RELAY, TAKE2_OWN, TAKE2_REST, TAKE2_RELAY)


def normed(net, c, q, gain_ref):
    rows = net.rows.shape[-PAIR]
    tile = PAIR * 8 if rows % (PAIR * 8) == 0 else 8
    spots = [(first, second, half) for first in range(RING) for second in range(RING) for half in BOTH]

    @pl.loop(0, rows // tile)
    def _(i):
        span = pl.ds(pl.multiple_of(i * tile, tile), tile)
        acts = [net.rows[(c, q) + spot + (span,)].astype(F32) for spot in spots]
        squares = functools.reduce(jnp.add, [v * v for v in acts])
        inv = lax.rsqrt(jnp.sum(squares, axis=-1, keepdims=True) / (LANES * len(acts)) + EPS)
        for k, (spot, v) in enumerate(zip(spots, acts)):
            net.rows[(c, q) + spot + (span,)] = (v * inv * gain_ref[q, pl.ds(k, 1)]).astype(BF16)


def rows_of(net, c, q):
    parts = []
    for upper in range(RING):
        for lower in range(RING):
            first, second = (upper, lower) if q else (lower, upper)
            parts += [net.rows[c, q, first, second, half] for half in BOTH]
    return jnp.concatenate(parts, axis=1)


def times_transposed(lhs, rhs):
    return lax.dot_general(lhs, rhs, (((1,), (1,)), ((), ())), preferred_element_type=F32)


def mega_kernel(chunks, a_ref, res_ref, gain_ref, next_gain_ref, w_out_hbm, w_gate_hbm, w_up_hbm, w_down_hbm,
                h_hbm, new_res_ref,
                w_out, w_gate, w_up, w_down, inner, middle,
                far, near, relayed, sums, relayed2, sums2, rows, w_sem, out_sem, send_sem, recv_sem):
    loads = [pltpu.make_async_copy(src, dst, w_sem.at[i]) for i, (src, dst) in enumerate(
        ((w_out_hbm, w_out), (w_gate_hbm, w_gate), (w_up_hbm, w_up), (w_down_hbm, w_down)))]
    for load in loads:
        load.start()
    net = Torus((far, near, relayed, sums, relayed2, sums2, rows), send_sem, recv_sem)
    net.barrier()
    loads[0].wait()

    @pl.loop(0, chunks)
    def _(c):
        for q in BOTH:
            stage_head(net, c, q, a_ref[c, q], w_out)

    def finish_with(old_ref, new_ref):
        def finish(c, q, half, total):
            value = (old_ref[c, q, half].astype(F32) + total).astype(BF16)
            new_ref[c, q, half] = value
            rows[(c, q) + net.place[q] + (half,)] = value
        return finish

    stage_rest(net, chunks, lambda c, q: a_ref[c, q], w_out, finish_with(res_ref, middle))
    for load in loads[1:]:
        load.wait()

    @pl.loop(0, chunks)
    def _(c):
        for q in BOTH:
            stage_tail(net, c, q)
            normed(net, c, q, gain_ref)
            hidden = rows_of(net, c, q)
            inner[c, q] = (jax.nn.silu(times_transposed(hidden, w_gate[...])) * times_transposed(hidden, w_up[...])).astype(BF16)
            stage_head(net, c, q, inner[c, q], w_down)

    stage_rest(net, chunks, lambda c, q: inner[c, q], w_down, finish_with(middle, new_res_ref))

    def out_copies(c, q):
        if q:
            return [pltpu.make_async_copy(rows.at[c, q], h_hbm.at[c, q], out_sem.at[c, q, 0])]
        return [pltpu.make_async_copy(rows.at[c, q, k], h_hbm.at[c, q, :, k], out_sem.at[c, q, k]) for k in range(RING)]

    @pl.loop(0, chunks)
    def _(c):
        for q in BOTH:
            stage_tail(net, c, q)
            normed(net, c, q, next_gain_ref)
            for copy in out_copies(c, q):
                copy.start()

    @pl.loop(0, chunks)
    def _(c):
        for q in BOTH:
            for copy in out_copies(c, q):
                copy.wait()


def mega(a, res, gain, next_gain, w_out, w_gate_t, w_up_t, w_down, collective_id):
    chunks, _, rows, depth = a.shape
    hidden, width = w_gate_t.shape
    per = (chunks, PAIR)
    tile = (rows, LANES)

    def by_color(g):
        grid = g.reshape(RING, RING, PAIR, LANES)
        return jnp.stack([jnp.swapaxes(grid, 0, 1), grid]).reshape(PAIR, PAIR * SHARDS, LANES)

    sem = DMA(per + (PAIR, len(KINDS)))
    return pl.pallas_call(
        functools.partial(mega_kernel, chunks),
        out_shape=(jax.ShapeDtypeStruct(per + (RING, RING, PAIR) + tile, BF16), jax.ShapeDtypeStruct(per + (PAIR,) + tile, BF16)),
        in_specs=[VMEM] * 4 + [ANY] * 4,
        out_specs=(ANY, VMEM),
        scratch_shapes=[
            pltpu.VMEM((depth, width), BF16),
            *[pltpu.VMEM((hidden, width), BF16) for _ in range(3)],
            pltpu.VMEM(per + (rows, hidden), BF16),
            pltpu.VMEM(per + (PAIR,) + tile, BF16),
            pltpu.VMEM(per + (RING, PAIR) + tile, F32),
            pltpu.VMEM(per + (PAIR, PAIR, PAIR) + tile, F32),
            pltpu.VMEM(per + (PAIR, PAIR, PAIR) + tile, F32),
            pltpu.VMEM(per + (PAIR, RING, PAIR) + tile, F32),
            pltpu.VMEM(per + (PAIR,) + tile, F32),
            pltpu.VMEM(per + (PAIR, PAIR) + tile, F32),
            pltpu.VMEM(per + (RING, RING, PAIR) + tile, BF16),
            DMA((RING,)), DMA(per + (RING,)), sem, sem,
        ],
        compiler_params=pltpu.CompilerParams(collective_id=collective_id, has_side_effects=True, vmem_limit_bytes=VMEM_BYTES),
        name=f"mega{collective_id}",
    )(a, res, by_color(gain), by_color(next_gain), w_out, w_gate_t, w_up_t, w_down)


PEERS = 8
TILE = 128
Q_TILE = 256
LOG2E = 1.4426950408889634


class Exchange:
    def __init__(self):
        self.me = lax.axis_index("resp")
        self.others = [(self.me + k) % PEERS for k in range(1, PEERS)]

    def barrier(self):
        sem = pltpu.get_barrier_semaphore()
        for device in self.others:
            pl.semaphore_signal(sem, inc=1, device_id={"resp": device}, device_id_type=MESH)
        pl.semaphore_wait(sem, PEERS - 1)

    def copy(self, src, dst, send_sem, recv_sem, device):
        return pltpu.make_async_remote_copy(src_ref=src, dst_ref=dst, send_sem=send_sem, recv_sem=recv_sem,
                                            device_id={"resp": device}, device_id_type=MESH)

    def scatter(self, src_of, dst, send_sem, recv_sem):
        for device in self.others:
            self.copy(src_of(device), dst, send_sem.at[device], recv_sem.at[self.me], device).start()

    def collected(self, dst_of, recv_sem):
        for device in self.others:
            self.copy(dst_of(device), dst_of(device), recv_sem.at[device], recv_sem.at[device], device).wait_recv()

    def sent(self, src_of, send_sem, recv_sem):
        for device in self.others:
            self.copy(src_of(device), src_of(device), send_sem.at[device], recv_sem.at[device], device).wait_send()


def deal(rows):
    out = lax.broadcasted_iota(jnp.int32, (rows, rows), 0)
    src = lax.broadcasted_iota(jnp.int32, (rows, rows), 1)
    per = rows // PEERS
    return jnp.where(src == (out % per) * PEERS + out // per, 1.0, 0.0).astype(BF16)


def undeal(rows):
    out = lax.broadcasted_iota(jnp.int32, (rows, rows), 0)
    src = lax.broadcasted_iota(jnp.int32, (rows, rows), 1)
    per = rows // PEERS
    return jnp.where(src == (out % PEERS) * per + out // PEERS, 1.0, 0.0).astype(BF16)


def rope(value, cos, sin):
    heads = [value[:, :128], value[:, 128:]]
    return jnp.concatenate([v * cos + pltpu.roll(v, 64, 1) * sin for v in heads], axis=1)


def norm_tile(x_ref, out_ref, gain_ref):
    for i in range(x_ref.shape[0] // 16):
        v = x_ref[pl.ds(16 * i, 16), :].astype(F32)
        inv = lax.rsqrt(jnp.mean(v * v, axis=-1, keepdims=True) + EPS)
        out_ref[pl.ds(16 * i, 16), :] = (v * inv * gain_ref[...]).astype(BF16)


def softmax_mix(q, pieces):
    factor = LOG2E * 128 ** -0.5
    outs = []
    for h in range(2):
        lanes = slice(128 * h, 128 * h + 128)
        scores = []
        for keys, _, mask in pieces:
            s = lax.dot_general(q[:, lanes], keys[:, lanes], (((1,), (1,)), ((), ())), preferred_element_type=F32)
            scores.append(s if mask is None else jnp.where(mask, s, -jnp.inf))
        top = functools.reduce(jnp.maximum, [jnp.max(s, axis=-1, keepdims=True) for s in scores])
        probs = [jnp.exp2((s - top) * factor) for s in scores]
        total = functools.reduce(jnp.add, [jnp.sum(p, axis=-1, keepdims=True) for p in probs])
        mixed = functools.reduce(jnp.add, [jnp.dot(p.astype(BF16), values[:, lanes], preferred_element_type=F32) for p, (_, values, _) in zip(probs, pieces)])
        outs.append(mixed / total)
    return jnp.concatenate(outs, axis=1).astype(BF16)


def attend_response(t, q, kp, vp, k_own, v_own):
    row = lax.broadcasted_iota(jnp.int32, (Q_TILE, Q_TILE), 0)
    col = lax.broadcasted_iota(jnp.int32, (Q_TILE, Q_TILE), 1)
    pieces = [(kp[...].reshape(PEERS * TILE, 256), vp[...].reshape(PEERS * TILE, 256), None)]
    if t:
        pieces.append((k_own[:t * Q_TILE], v_own[:t * Q_TILE], None))
    span = slice(t * Q_TILE, (t + 1) * Q_TILE)
    pieces.append((k_own[span], v_own[span], col <= row))
    return softmax_mix(q, pieces)


def deal_mixed(net, t, mixed, stage, out, send_sem, recv_sem):
    dealt = jnp.dot(deal(Q_TILE), mixed, preferred_element_type=F32).astype(BF16)
    stage[t] = dealt.reshape(PEERS, Q_TILE // PEERS, 256)
    net.scatter(lambda d: stage.at[t, d], out.at[net.me, t], send_sem.at[t], recv_sem.at[t])
    out[net.me, t] = stage[t, net.me]


def first_attention_kernel(xp_hbm, xr_hbm, wq_hbm, wk_hbm, wv_hbm, gain_ref, cos_ref, sin_ref, info_ref,
                           mixed_out, res_out, info_out, mixed_prompt,
                           xs, w, hidden, q_s, k_s, v_s, kp, vp, mixed_stage, res_stage,
                           x_sem, w_sem, kv_send, kv_recv, mix_send, mix_recv, res_send, res_recv, info_send, info_recv):
    net = Exchange()
    me = net.me
    column = pl.multiple_of(lax.axis_index("model") * 256, 256)

    def load(t):
        src = xp_hbm if isinstance(t, int) and t == 0 else xr_hbm.at[pl.ds(pl.multiple_of((t - 1) * TILE, TILE), TILE)]
        return pltpu.make_async_copy(src, xs.at[t], x_sem.at[t])

    load(0).start()
    weights = [pltpu.make_async_copy(src, w.at[:, pl.ds(256 * i, 256)], w_sem.at[i]) for i, src in enumerate((wq_hbm, wk_hbm, wv_hbm))]
    for copy in weights:
        copy.start()
    for t in range(1, 9):
        load(t).start()
    net.barrier()
    net.scatter(lambda d: info_ref.at[d], info_out.at[me], info_send, info_recv)
    info_out[me] = info_ref[me]

    def project(t):
        span = pl.ds(pl.multiple_of(t * TILE, TILE), TILE)
        qkv = jnp.dot(hidden[t % 2], w[...], preferred_element_type=F32)
        cos, sin = cos_ref[span], sin_ref[span]
        return span, rope(qkv[:, :256], cos, sin).astype(BF16), rope(qkv[:, 256:512], cos, sin).astype(BF16), qkv[:, 512:].astype(BF16)

    load(0).wait()
    norm_tile(xs.at[0], hidden.at[0], gain_ref)
    load(1).wait()
    for copy in weights:
        copy.wait()
    norm_tile(xs.at[1], hidden.at[1], gain_ref)
    span, q, k, v = project(0)
    q_s[span] = q
    kp[me] = k
    vp[me] = v
    net.scatter(lambda d: kp.at[me], kp.at[me], kv_send.at[0], kv_recv.at[0])
    net.scatter(lambda d: vp.at[me], vp.at[me], kv_send.at[1], kv_recv.at[1])
    spread = deal(TILE)

    @pl.loop(1, 9)
    def _(t):
        later = jnp.minimum(t + 1, 8)

        @pl.when(t < 8)
        def _():
            load(t + 1).wait()

        span, q, k, v = project(t)
        norm_tile(xs.at[later], hidden.at[(t + 1) % 2], gain_ref)
        q_s[span] = q
        own = pl.ds(pl.multiple_of((t - 1) * TILE, TILE), TILE)
        k_s[own] = k
        v_s[own] = v
        dealt = jnp.dot(spread, xs[t, :, pl.ds(column, 256)], preferred_element_type=F32).astype(BF16)
        res_stage[:, t - 1] = dealt.reshape(PEERS, TILE // PEERS, 256)

    net.scatter(lambda d: res_stage.at[d], res_out.at[me], res_send, res_recv)
    res_out[me] = res_stage[me]
    net.collected(lambda d: kp.at[d], kv_recv.at[0])
    net.collected(lambda d: vp.at[d], kv_recv.at[1])
    for t in range(4):
        mixed = attend_response(t, q_s[pl.ds(TILE + t * Q_TILE, Q_TILE)], kp, vp, k_s, v_s)
        deal_mixed(net, t, mixed, mixed_stage, mixed_out, mix_send, mix_recv)
    row = lax.broadcasted_iota(jnp.int32, (TILE, PEERS * TILE), 0) + me * TILE
    col = lax.broadcasted_iota(jnp.int32, (TILE, PEERS * TILE), 1)
    mixed_prompt[...] = softmax_mix(q_s[pl.ds(0, TILE)], [(kp[...].reshape(PEERS * TILE, 256), vp[...].reshape(PEERS * TILE, 256), col <= row)])
    finish_exchange(net, mixed_stage, mixed_out, mix_send, mix_recv)
    net.collected(lambda d: res_out.at[d], res_recv)
    net.sent(lambda d: res_stage.at[d], res_send, res_recv)
    net.collected(lambda d: info_out.at[d], info_recv)
    net.sent(lambda d: info_ref.at[d], info_send, info_recv)
    for i, ref in enumerate((kp, vp)):
        net.sent(lambda d: ref.at[me], kv_send.at[i], kv_recv.at[i])


def finish_exchange(net, stage, out, send_sem, recv_sem):
    for t in range(4):
        net.collected(lambda d: out.at[d, t], recv_sem.at[t])
        net.sent(lambda d: stage.at[t, d], send_sem.at[t], recv_sem.at[t])


def first_attention(x_prompt, x_resp, w_query, w_key, w_value, gain, cos, sin, info, collective_id):
    rows = TILE + x_resp.shape[0]
    width = x_resp.shape[1]
    return pl.pallas_call(
        first_attention_kernel,
        out_shape=(jax.ShapeDtypeStruct((PEERS, 4, 32, 256), BF16), jax.ShapeDtypeStruct((PEERS, 8, 16, 256), BF16),
                   jax.ShapeDtypeStruct((PEERS, 8, 128), jnp.int32), jax.ShapeDtypeStruct((TILE, 256), BF16)),
        in_specs=[ANY] * 5 + [VMEM] * 4,
        out_specs=(VMEM,) * 4,
        scratch_shapes=[
            pltpu.VMEM((9, TILE, width), BF16), pltpu.VMEM((width, 768), BF16), pltpu.VMEM((2, TILE, width), BF16),
            pltpu.VMEM((rows, 256), BF16), pltpu.VMEM((rows - TILE, 256), BF16), pltpu.VMEM((rows - TILE, 256), BF16),
            pltpu.VMEM((PEERS, TILE, 256), BF16), pltpu.VMEM((PEERS, TILE, 256), BF16),
            pltpu.VMEM((4, PEERS, 32, 256), BF16), pltpu.VMEM((PEERS, 8, 16, 256), BF16),
            DMA((9,)), DMA((3,)), DMA((2, PEERS)), DMA((2, PEERS)), DMA((4, PEERS)), DMA((4, PEERS)),
            DMA((PEERS,)), DMA((PEERS,)), DMA((PEERS,)), DMA((PEERS,)),
        ],
        compiler_params=pltpu.CompilerParams(collective_id=collective_id, has_side_effects=True, vmem_limit_bytes=VMEM_BYTES),
        name="first_attention",
    )(x_prompt, x_resp, w_query, w_key, w_value, gain.reshape(1, width), cos, sin, info)


def second_attention_kernel(qkv_ref, kv_prompt_ref, mixed_out, qkv_in, k_s, v_s, kp, vp, mixed_stage,
                            kv_send, kv_recv, qkv_send, qkv_recv, mix_send, mix_recv):
    net = Exchange()
    me = net.me
    net.barrier()
    for i, ref in enumerate((kp, vp)):
        net.scatter(lambda d: kv_prompt_ref.at[i], ref.at[me], kv_send.at[i], kv_recv.at[i])
        ref[me] = kv_prompt_ref[i]
    for t in range(4):
        net.scatter(lambda d: qkv_ref.at[t, d], qkv_in.at[t, me], qkv_send.at[t], qkv_recv.at[t])
        qkv_in[t, me] = qkv_ref[t, me]
    net.collected(lambda d: kp.at[d], kv_recv.at[0])
    net.collected(lambda d: vp.at[d], kv_recv.at[1])
    for t in range(4):
        net.collected(lambda d: qkv_in.at[t, d], qkv_recv.at[t])
        rows = jnp.dot(undeal(Q_TILE), qkv_in[t].reshape(Q_TILE, 768), preferred_element_type=F32).astype(BF16)
        k_s[pl.ds(t * Q_TILE, Q_TILE)] = rows[:, 256:512]
        v_s[pl.ds(t * Q_TILE, Q_TILE)] = rows[:, 512:]
        mixed = attend_response(t, rows[:, :256], kp, vp, k_s, v_s)
        deal_mixed(net, t, mixed, mixed_stage, mixed_out, mix_send, mix_recv)
    finish_exchange(net, mixed_stage, mixed_out, mix_send, mix_recv)
    for t in range(4):
        net.sent(lambda d: qkv_ref.at[t, d], qkv_send.at[t], qkv_recv.at[t])
    for i in range(2):
        net.sent(lambda d: kv_prompt_ref.at[i], kv_send.at[i], kv_recv.at[i])


def second_attention(qkv, kv_prompt, collective_id):
    return pl.pallas_call(
        second_attention_kernel,
        out_shape=jax.ShapeDtypeStruct((PEERS, 4, 32, 256), BF16),
        in_specs=[VMEM] * 2,
        out_specs=VMEM,
        scratch_shapes=[
            pltpu.VMEM((4, PEERS, 32, 768), BF16), pltpu.VMEM((1024, 256), BF16), pltpu.VMEM((1024, 256), BF16),
            pltpu.VMEM((PEERS, TILE, 256), BF16), pltpu.VMEM((PEERS, TILE, 256), BF16), pltpu.VMEM((4, PEERS, 32, 256), BF16),
            DMA((2, PEERS)), DMA((2, PEERS)), DMA((4, PEERS)), DMA((4, PEERS)), DMA((4, PEERS)), DMA((4, PEERS)),
        ],
        compiler_params=pltpu.CompilerParams(collective_id=collective_id, has_side_effects=True, vmem_limit_bytes=VMEM_BYTES),
        name="second_attention",
    )(qkv, kv_prompt)


def project_kernel(h_ref, wq_ref, wk_ref, wv_ref, cos_ref, sin_ref, out_ref):
    rows = jnp.concatenate([h_ref[0, 0, b // 4, b % 4, half] for b in range(16) for half in range(2)], axis=1)
    cos, sin = cos_ref[...], sin_ref[...]
    out_ref[:, :256] = rope(jnp.dot(rows, wq_ref[...], preferred_element_type=F32), cos, sin).astype(BF16)
    out_ref[:, 256:512] = rope(jnp.dot(rows, wk_ref[...], preferred_element_type=F32), cos, sin).astype(BF16)
    out_ref[:, 512:] = jnp.dot(rows, wv_ref[...], preferred_element_type=F32).astype(BF16)


def project(h, w_query, w_key, w_value, cos, sin):
    chunks, _, _, _, _, part, _ = h.shape
    width = w_query.shape[0]
    whole = pl.BlockSpec((width, 256), lambda i: (0, 0), pipeline_mode=pl.Buffered(1))
    table = pl.BlockSpec((part, 128), lambda i: (i, 0))
    return pl.pallas_call(
        project_kernel,
        grid=(2 * chunks,),
        out_shape=jax.ShapeDtypeStruct((2 * chunks * part, 768), BF16),
        in_specs=[pl.BlockSpec((1, 1, 4, 4, 2, part, 128), lambda i: (i // 2, i % 2, 0, 0, 0, 0, 0)), whole, whole, whole, table, table],
        out_specs=pl.BlockSpec((part, 768), lambda i: (i, 0)),
        compiler_params=pltpu.CompilerParams(vmem_limit_bytes=VMEM_BYTES),
        cost_estimate=pl.CostEstimate(flops=2 * 2 * chunks * part * width * 768, bytes_accessed=width * 768 * 2, transcendentals=0),
        name="project",
    )(h, w_query, w_key, w_value, cos, sin)


def head_kernel(h_ref, w_ref, target_ref, out_ref):
    rows = jnp.concatenate([h_ref[0, 0, b // 4, b % 4, half] for b in range(16) for half in range(2)], axis=1)
    logits = jnp.dot(rows, w_ref[...], preferred_element_type=F32)
    top = jnp.max(logits, axis=-1, keepdims=True)
    total = jnp.sum(jnp.exp(logits - top), axis=-1, keepdims=True)
    ids = lax.broadcasted_iota(jnp.int32, logits.shape, 1)
    picked = jnp.sum(jnp.where(ids == target_ref[:, :1], logits, 0.0), axis=-1, keepdims=True)
    lane = lax.broadcasted_iota(jnp.int32, out_ref.shape, 1)
    out_ref[...] = jnp.where(lane == 0, top, jnp.where(lane == 1, total, picked))


def head(h, w_vocab, local_targets):
    chunks, _, _, _, _, part, _ = h.shape
    width, vocab = w_vocab.shape
    return pl.pallas_call(
        head_kernel,
        grid=(2 * chunks,),
        out_shape=jax.ShapeDtypeStruct((2 * chunks * part, 128), F32),
        in_specs=[pl.BlockSpec((1, 1, 4, 4, 2, part, 128), lambda i: (i // 2, i % 2, 0, 0, 0, 0, 0)),
                  pl.BlockSpec((width, vocab), lambda i: (0, 0), pipeline_mode=pl.Buffered(1)),
                  pl.BlockSpec((part, 128), lambda i: (i, 0))],
        out_specs=pl.BlockSpec((part, 128), lambda i: (i, 0)),
        compiler_params=pltpu.CompilerParams(vmem_limit_bytes=VMEM_BYTES),
        cost_estimate=pl.CostEstimate(flops=2 * 2 * chunks * part * width * vocab, bytes_accessed=width * vocab * 2, transcendentals=0),
        name="head",
    )(h, w_vocab, local_targets)


def combine_kernel(shards, stats_ref, out_ref, every, stat_send, stat_recv, row_send, row_recv):
    me, home = lax.axis_index("model"), lax.axis_index("resp")
    sem = pltpu.get_barrier_semaphore()
    models = [(me + k) % shards for k in range(1, shards)]
    homes = [(home + k) % PEERS for k in range(1, PEERS)]
    for device in models:
        pl.semaphore_signal(sem, inc=1, device_id={"model": device}, device_id_type=MESH)
    for device in homes:
        pl.semaphore_signal(sem, inc=1, device_id={"resp": device}, device_id_type=MESH)
    pl.semaphore_wait(sem, shards + PEERS - 2)

    def stat_copy(src, dst, send, recv, device):
        return pltpu.make_async_remote_copy(src_ref=src, dst_ref=dst, send_sem=send, recv_sem=recv, device_id={"model": device}, device_id_type=MESH)

    def row_copy(src, dst, send, recv, device):
        return pltpu.make_async_remote_copy(src_ref=src, dst_ref=dst, send_sem=send, recv_sem=recv, device_id={"resp": device}, device_id_type=MESH)

    for device in models:
        stat_copy(stats_ref, every.at[me], stat_send.at[device], stat_recv.at[me], device).start()
    every[me] = stats_ref[...]
    for device in models:
        stat_copy(every.at[device], every.at[device], stat_send.at[device], stat_recv.at[device], device).wait_recv()
    tops = [every[k, 0] for k in range(shards)]
    top = functools.reduce(jnp.maximum, tops)
    total = functools.reduce(jnp.add, [every[k, 1] * jnp.exp(tops[k] - top) for k in range(shards)])
    picked = functools.reduce(jnp.add, [every[k, 2] for k in range(shards)])
    out_ref[home] = picked - top - jnp.log(total)
    for device in homes:
        row_copy(out_ref.at[home], out_ref.at[home], row_send.at[device], row_recv.at[home], device).start()
    for device in homes:
        row_copy(out_ref.at[device], out_ref.at[device], row_send.at[device], row_recv.at[device], device).wait_recv()
    for device in models:
        stat_copy(stats_ref, stats_ref, stat_send.at[device], stat_recv.at[device], device).wait_send()
    for device in homes:
        row_copy(out_ref.at[home], out_ref.at[home], row_send.at[device], row_recv.at[device], device).wait_send()


def combine(stats, shards, collective_id):
    return pl.pallas_call(
        functools.partial(combine_kernel, shards),
        out_shape=jax.ShapeDtypeStruct((PEERS, 8, 128), F32),
        in_specs=[VMEM],
        out_specs=VMEM,
        scratch_shapes=[pltpu.VMEM((shards, 3, 8, 128), F32), DMA((shards,)), DMA((shards,)), DMA((PEERS,)), DMA((PEERS,))],
        compiler_params=pltpu.CompilerParams(collective_id=collective_id, has_side_effects=True),
        name="combine",
    )(stats)


ROPE_BASE = 10000.0
VARIANTS = (576, 640, 704, 768, 1024)
CHUNKS = 4


def rope_tables(positions):
    frequency = ROPE_BASE ** (-jnp.arange(64, dtype=F32) / 64)
    angles = positions.astype(F32)[:, None] * frequency
    cos, sin = jnp.cos(angles), jnp.sin(angles)
    return jnp.concatenate([cos, cos], axis=1), jnp.concatenate([-sin, sin], axis=1)


def to_blocks(rows, chunks):
    count = rows.shape[0]
    return rows.reshape(chunks, 2, count // (2 * chunks), 2, 128).transpose(0, 1, 3, 2, 4)


def from_blocks(blocks):
    chunks, _, _, part, _ = blocks.shape
    return blocks.transpose(0, 1, 3, 2, 4).reshape(2 * chunks * part, 256)


def solution(mesh):
    groups = mesh.shape['resp']
    shards = mesh.shape['model']
    row_axes = ('prompts', 'resp')
    head_spec = P(None, None, 'model', None)
    in_specs = (P(row_axes, None), P(row_axes, None, None), P(row_axes, None), P(row_axes), P(None, None), head_spec, head_spec, head_spec, P(None, 'model', None, None), P(None, None), P(None, None, 'model'), P(None, None, 'model'), P(None, 'model', None), P(None), P(None, 'model'))

    def device_step(x_prompt, x_resp, targets, resp_lens, attn_gain, w_query, w_key, w_value, w_out, mlp_gain, w_gate, w_up, w_down, final_gain, w_vocab):
        prompt_rows = x_prompt.shape[0]
        resp_len, width = x_resp.shape[1:]
        prompt_len = prompt_rows * groups
        num_layers, _, heads, head_dim = w_query.shape
        me = lax.axis_index('model')
        home = lax.axis_index('resp')
        per = resp_len // groups
        gate_t, up_t = jnp.swapaxes(w_gate, 1, 2), jnp.swapaxes(w_up, 1, 2)
        flat = lambda w, l: w[l].reshape(width, heads * head_dim)
        prompt_pos = home * prompt_rows + jnp.arange(prompt_rows)

        cos, sin = rope_tables(jnp.concatenate([prompt_pos, prompt_len + jnp.arange(resp_len)]))
        info = jnp.concatenate([
            targets[0].reshape(per, groups).T[:, None, :],
            jnp.broadcast_to(resp_lens[0], (groups, 7, per)).astype(jnp.int32)], axis=1)
        mixed, res, infos, mixed_prompt = first_attention(
            x_prompt, x_resp[0], flat(w_query, 0), flat(w_key, 0), flat(w_value, 0), attn_gain[0], cos, sin, info, 0)
        lens = infos[:, 1, 0]
        need = (lens + groups - 1) // groups
        ends = jnp.cumsum(need)
        starts = ends - need
        res_prompt = lax.dynamic_slice_in_dim(x_prompt, me * 256, 256, 1)

        def places(size):
            slot = jnp.arange(size)
            which = jnp.sum((slot[:, None] >= ends[None, :]).astype(jnp.int32), axis=1)
            begin = jnp.sum(jnp.where(which[:, None] == jnp.arange(groups), starts, 0), axis=1)
            return which, slot - begin, slot < ends[-1]

        def layer_first(size, ident):
            def run(operands):
                mixed, res, mixed_prompt, res_prompt = operands
                chunks = CHUNKS
                which, row, real = places(size)
                source = jnp.where(real, which * per + row, -1)
                pick = (source[:, None] == jnp.arange(groups * per)[None, :]).astype(BF16)
                both = jnp.dot(pick, jnp.concatenate([mixed.reshape(groups * per, 256), res.reshape(groups * per, 256)], axis=1), preferred_element_type=F32).astype(BF16)
                rows = jnp.concatenate([jnp.concatenate([mixed_prompt, res_prompt], axis=1), both], axis=0)
                count = prompt_rows + size
                gathered, new_res = mega(
                    rows[:, :256].reshape(chunks, 2, count // (2 * chunks), 256), to_blocks(rows[:, 256:], chunks), mlp_gain[0], attn_gain[1],
                    w_out[0].reshape(heads * head_dim, width), gate_t[0], up_t[0], w_down[0], ident)
                cos, sin = rope_tables(jnp.concatenate([prompt_pos, prompt_len + groups * row + home]))
                qkv = project(gathered, flat(w_query, 1), flat(w_key, 1), flat(w_value, 1), cos, sin)
                back = jnp.where(real, (row // 32) * 256 + which * 32 + row % 32, -1)
                place = (jnp.arange(groups * per)[:, None] == back[None, :]).astype(BF16)
                home_rows = jnp.dot(place, qkv[prompt_rows:], preferred_element_type=F32).astype(BF16)
                kv_prompt = jnp.stack([qkv[:prompt_rows, 256:512], qkv[:prompt_rows, 512:]])
                kept = from_blocks(new_res)[prompt_rows:]
                return home_rows.reshape(4, groups, 32, 768), kv_prompt, jnp.pad(kept, ((0, resp_len - size), (0, 0)))
            return run

        def layer_second(size, ident):
            def run(operands):
                mixed, kept = operands
                chunks = CHUNKS
                which, row, real = places(size)
                source = jnp.where(real, which * per + row, -1)
                chosen = source[:, None] == jnp.arange(groups * per)[None, :]
                rows = jnp.dot(chosen.astype(BF16), mixed.reshape(groups * per, 256), preferred_element_type=F32).astype(BF16)
                gathered, _ = mega(
                    rows.reshape(chunks, 2, size // (2 * chunks), 256), to_blocks(kept[:size], chunks), mlp_gain[1], final_gain,
                    w_out[1].reshape(heads * head_dim, width), gate_t[1], up_t[1], w_down[1], ident)
                wanted = jnp.sum(jnp.where(chosen, infos[:, 0, :].reshape(1, groups * per), 0), axis=1)
                local = jnp.broadcast_to((wanted - me * w_vocab.shape[1])[:, None], (size, 128))
                stats = head(gathered, w_vocab, local)[:, :3].T
                return jnp.pad(stats, ((0, 0), (0, resp_len - size)))
            return run

        total = ends[-1]
        index = sum((total > size).astype(jnp.int32) for size in VARIANTS[:-1]) if len(VARIANTS) > 1 else 0

        def choose(makers, operands):
            if len(makers) == 1:
                return makers[0](operands)
            return lax.switch(index, makers, operands)

        qkv, kv_prompt, kept = choose([layer_first(s, 4 + i) for i, s in enumerate(VARIANTS)], (mixed, res, mixed_prompt, res_prompt))
        mixed = second_attention(qkv, kv_prompt, 1)
        stats = choose([layer_second(s, 4 + len(VARIANTS) + i) for i, s in enumerate(VARIANTS)], (mixed, kept))
        found = combine(stats.reshape(3, groups, per), shards, 2).reshape(groups, resp_len)
        start = jnp.sum(jnp.where(jnp.arange(groups) == home, starts, 0))
        mine = lax.dynamic_slice(jnp.pad(found, ((0, 0), (0, per))), (0, start), (groups, per))
        log_probs = jnp.where(jnp.arange(resp_len) < resp_lens[0], mine.T.reshape(resp_len), 0.0)
        return log_probs[None, :]

    return jax.shard_map(device_step, mesh=mesh, in_specs=in_specs, out_specs=P(row_axes, None), check_vma=False)
```

```python
import functools

import jax
import jax.numpy as jnp
from jax import lax
from jax.experimental import pallas as pl
from jax.experimental.pallas import tpu as pltpu
from jax.sharding import PartitionSpec as P

MESH = pl.DeviceIdType.MESH
F32 = jnp.float32
BF16 = jnp.bfloat16
EPS = 1e-6
LANES = 128
PAIR = 2
RING = 4
COLUMNS = PAIR * LANES
SHARDS = RING * RING
BOTH = range(PAIR)
VMEM_BYTES = 67_000_000
LATE_ROWS = 640
LOGITS = 512
GROUP = 2
LAG = 4
VMEM = pl.BlockSpec(memory_space=pltpu.VMEM)
ANY = pl.BlockSpec(memory_space=pl.ANY)
DMA = pltpu.SemaphoreType.DMA
KINDS = range(RING * 3)
SUM_FAR, SUM_NEAR, SUM_RELAY, SUM2_FAR, SUM2_NEAR, SUM2_RELAY, TAKE_OWN, TAKE_REST, TAKE_RELAY, TAKE2_OWN, TAKE2_REST, TAKE2_RELAY = KINDS


def block_of(color, first, second):
    return RING * first + second if color else RING * second + first


def pair(index):
    return pl.ds(PAIR * index, PAIR)


class Torus:
    def __init__(self, refs, send_sem, recv_sem):
        self.refs = refs
        self.far, self.near, self.relayed, self.sums, self.relayed2, self.sums2, self.rows = refs
        self.send_sem, self.recv_sem = send_sem, recv_sem
        me = lax.axis_index("model")
        z, y = me // RING, me % RING
        self.place = ((y, z), (z, y))
        along_y = [z * RING + self.step(y, way) for way in (1, -1)]
        along_z = [self.step(z, way) * RING + y for way in (1, -1)]
        self.neighbors = ((along_y, along_z), (along_z, along_y))

    def step(self, place, by):
        return (place + by + RING) % RING

    def barrier(self):
        sem = pltpu.get_barrier_semaphore()
        for ring in self.neighbors[0]:
            for device in ring:
                pl.semaphore_signal(sem, device_id={"model": device}, device_id_type=MESH)
        pl.semaphore_wait(sem, RING)

    def ends(self, kind, c, q, d):
        (p, s), way, other = self.place[q], 1 - PAIR * d, 1 - d
        far, near, relayed, sums, relayed2, sums2, rows = (ref.at[c, q] for ref in self.refs)
        own = sums.at[0]
        back_s, back_p = self.step(s, -way), self.step(p, -way)
        return {
            SUM_FAR: lambda: (far.at[pair(d)], relayed.at[d], relayed.at[d]),
            SUM_NEAR: lambda: (near.at[d], sums.at[d, pair(other)], sums.at[d, pair(other)]),
            SUM_RELAY: lambda: (relayed.at[d], sums.at[d, pair(d)], sums.at[d, pair(d)]),
            SUM2_FAR: lambda: (own.at[self.step(s, PAIR), d], relayed2.at[d], relayed2.at[d]),
            SUM2_NEAR: lambda: (own.at[self.step(s, way), other], sums2.at[d, other], sums2.at[d, other]),
            SUM2_RELAY: lambda: (relayed2.at[d], sums2.at[d, d], sums2.at[d, d]),
            TAKE_OWN: lambda: (rows.at[p, s, d], rows.at[p, s, d], rows.at[p, back_s, d]),
            TAKE_REST: lambda: (rows.at[p, s, other], rows.at[p, s, other], rows.at[p, back_s, other]),
            TAKE_RELAY: lambda: (rows.at[p, back_s, d], rows.at[p, back_s, d], rows.at[p, self.step(s, PAIR), d]),
            TAKE2_OWN: lambda: (rows.at[p, pair(d)], rows.at[p, pair(d)], rows.at[back_p, pair(d)]),
            TAKE2_REST: lambda: (rows.at[p, pair(other)], rows.at[p, pair(other)], rows.at[back_p, pair(other)]),
            TAKE2_RELAY: lambda: (rows.at[back_p, pair(d)], rows.at[back_p, pair(d)], rows.at[self.step(p, PAIR), pair(d)]),
        }[kind]()

    def copy(self, kind, c, q, d, src, dst):
        second_ring = kind in (SUM2_FAR, SUM2_NEAR, SUM2_RELAY, TAKE_OWN, TAKE_REST, TAKE_RELAY)
        return pltpu.make_async_remote_copy(
            src_ref=src, dst_ref=dst, send_sem=self.send_sem.at[c, q, d, kind], recv_sem=self.recv_sem.at[c, q, d, kind],
            device_id={"model": self.neighbors[q][second_ring][d]}, device_id_type=MESH)

    def send(self, c, q, d, kind):
        src, dst, _ = self.ends(kind, c, q, d)
        self.copy(kind, c, q, d, src, dst).start()

    def sent(self, c, q, *kinds):
        for kind in kinds:
            for d in BOTH:
                src, dst, _ = self.ends(kind, c, q, d)
                self.copy(kind, c, q, d, src, dst).wait_send()

    def arrived(self, c, q, d, *kinds):
        for kind in kinds:
            _, _, here = self.ends(kind, c, q, d)
            self.copy(kind, c, q, d, here, here).wait_recv()


def halves(value):
    return value[:, :LANES], value[:, LANES:]


def store_block(ref, value):
    for half, part in enumerate(halves(value)):
        ref[half] = part


def add_block(ref, value):
    for half, part in enumerate(halves(value)):
        ref[half] += part


class Stage:
    def __init__(self, net, lhs_of, w_ref, finish):
        self.net, self.lhs_of, self.w_ref, self.finish = net, lhs_of, w_ref, finish

    def product(self, lhs, color, first, second):
        start = pl.multiple_of(block_of(color, first, second) * COLUMNS, COLUMNS)
        return jnp.dot(lhs, self.w_ref[:, pl.ds(start, COLUMNS)], preferred_element_type=F32)

    def begin(self, c, q):
        net, p, lhs = self.net, self.net.place[q][0], self.lhs_of(c, q)
        for k in range(RING):
            store_block(net.far.at[c, q, k], self.product(lhs, q, net.step(p, PAIR), k))
        for d in BOTH:
            net.send(c, q, d, SUM_FAR)
        for d in BOTH:
            for k in BOTH:
                store_block(net.near.at[c, q, d, k], self.product(lhs, q, net.step(p, 1 - PAIR * d), PAIR * (1 - d) + k))
            net.send(c, q, d, SUM_NEAR)

    def relay_sum(self, c, q):
        net, p, lhs = self.net, self.net.place[q][0], self.lhs_of(c, q)
        for d in BOTH:
            net.arrived(c, q, d, SUM_FAR)
            for k in BOTH:
                add_block(net.relayed.at[c, q, d, k], self.product(lhs, q, net.step(p, 1 - PAIR * d), PAIR * d + k))
            net.send(c, q, d, SUM_RELAY)

    def begin_second(self, c, q):
        net, lhs = self.net, self.lhs_of(c, q)
        for d in BOTH:
            net.arrived(c, q, d, SUM_NEAR, SUM_RELAY)
        for k in range(RING):
            for half, part in enumerate(halves(self.product(lhs, q, net.place[q][0], k))):
                net.sums[c, q, 0, k, half] += net.sums[c, q, 1, k, half] + part
        for kind in (SUM2_FAR, SUM2_NEAR):
            for d in BOTH:
                net.send(c, q, d, kind)
        net.sent(c, q, SUM_FAR)

    def relay_second(self, c, q):
        net = self.net
        for d in BOTH:
            net.arrived(c, q, d, SUM2_FAR)
            net.relayed2[c, q, d] += net.sums[c, q, 0, net.step(net.place[q][1], 1 - PAIR * d), d]
            net.send(c, q, d, SUM2_RELAY)

    def finish_sum(self, c, q):
        net = self.net
        net.sent(c, q, SUM_NEAR, SUM_RELAY)
        for d in BOTH:
            net.arrived(c, q, d, SUM2_NEAR, SUM2_RELAY)
        for half in BOTH:
            self.finish(c, q, half, net.sums[c, q, 0, net.place[q][1], half] + net.sums2[c, q, 0, half] + net.sums2[c, q, 1, half])
        for kind in (TAKE_OWN, TAKE_REST):
            for d in BOTH:
                net.send(c, q, d, kind)

    def relay_rows(self, c, q):
        net = self.net
        net.sent(c, q, SUM2_FAR, SUM2_NEAR, SUM2_RELAY)
        for d in BOTH:
            net.arrived(c, q, d, TAKE_OWN)
            net.send(c, q, d, TAKE_RELAY)

    def take_second(self, c, q):
        net = self.net
        for d in BOTH:
            net.arrived(c, q, d, TAKE_REST, TAKE_RELAY)
        for kind in (TAKE2_OWN, TAKE2_REST):
            for d in BOTH:
                net.send(c, q, d, kind)

    def relay_last(self, c, q):
        net = self.net
        for d in BOTH:
            net.arrived(c, q, d, TAKE2_OWN)
            net.send(c, q, d, TAKE2_RELAY)

    def complete(self, c, q):
        net = self.net
        for d in BOTH:
            net.arrived(c, q, d, TAKE2_REST, TAKE2_RELAY)
        net.sent(c, q, TAKE_OWN, TAKE_REST, TAKE_RELAY, TAKE2_OWN, TAKE2_REST, TAKE2_RELAY)

    def middle(self):
        return [self.relay_sum, self.begin_second, self.relay_second, self.finish_sum, self.relay_rows, self.take_second, self.relay_last]


def normed(net, c, q, gain_ref):
    rows = net.rows.shape[-PAIR]
    tile = PAIR * 8 if rows % (PAIR * 8) == 0 else 8
    spots = [(first, second, half) for first in range(RING) for second in range(RING) for half in BOTH]

    @pl.loop(0, rows // tile)
    def _(i):
        span = pl.ds(pl.multiple_of(i * tile, tile), tile)
        acts = [net.rows[(c, q) + spot + (span,)].astype(F32) for spot in spots]
        squares = functools.reduce(jnp.add, [v * v for v in acts])
        inv = lax.rsqrt(jnp.sum(squares, axis=-1, keepdims=True) / (LANES * len(acts)) + EPS)
        for k, (spot, v) in enumerate(zip(spots, acts)):
            net.rows[(c, q) + spot + (span,)] = (v * inv * gain_ref[q, pl.ds(k, 1)]).astype(BF16)


def rows_of(net, c, q):
    parts = []
    for upper in range(RING):
        for lower in range(RING):
            first, second = (upper, lower) if q else (lower, upper)
            parts += [net.rows[c, q, first, second, half] for half in BOTH]
    return jnp.concatenate(parts, axis=1)


def times_transposed(lhs, rhs):
    return lax.dot_general(lhs, rhs, (((1,), (1,)), ((), ())), preferred_element_type=F32)


def late_plan(width, count):
    plan, start = [], 0
    for buffer in BOTH:
        for slot in range(width // count):
            size = min(LATE_ROWS, width - start)
            if size:
                plan.append((buffer, slot * count, start, size))
            start += size
    return plan, width - start


def rope(value, cos, sin):
    return jnp.concatenate([v * cos + pltpu.roll(v, LANES // PAIR, 1) * sin for v in halves(value)], axis=1)


def put_projected(product, cos_ref, sin_ref, out_ref, c, q):
    for k in range(3):
        value = product(k * COLUMNS, COLUMNS)
        if k < PAIR:
            value = rope(value, cos_ref[c, q], sin_ref[c, q])
        out_ref[c, q, :, pl.ds(k * COLUMNS, COLUMNS)] = value.astype(BF16)


def put_statistics(product, count, target_ref, out_ref, c, q):
    top = total = picked = None
    for k in range(count // LOGITS):
        logits = product(k * LOGITS, LOGITS)
        here = jnp.max(logits, axis=-1, keepdims=True)
        ids = lax.broadcasted_iota(jnp.int32, logits.shape, 1) + k * LOGITS
        found = jnp.sum(jnp.where(ids == target_ref[c, q, :, :1], logits, 0.0), axis=-1, keepdims=True)
        if k:
            both = jnp.maximum(top, here)
            total = total * jnp.exp(top - both) + jnp.sum(jnp.exp(logits - both), axis=-1, keepdims=True)
            top, picked = both, picked + found
        else:
            top, total, picked = here, jnp.sum(jnp.exp(logits - here), axis=-1, keepdims=True), found
    lane = lax.broadcasted_iota(jnp.int32, out_ref.shape[PAIR:], 1)
    out_ref[c, q] = jnp.where(lane == 0, top, jnp.where(lane == 1, total, picked))


def mega_kernel(chunks, layer, last, a_ref, res_ref, gain_ref, next_gain_ref, *args):
    side_refs, args = args[:PAIR - last], args[PAIR - last:]
    (w_out_hbm, w_gate_hbm, w_up_hbm, w_down_hbm, late_hbm, out_ref, new_res_ref,
     w_out, w_gate, w_up, w_down, late_rest, inner, middle,
     far, near, relayed, sums, relayed2, sums2, rows, w_sem, late_sem, send_sem, recv_sem) = args
    loads = [pltpu.make_async_copy(src.at[layer], dst, w_sem.at[i]) for i, (src, dst) in enumerate(
        ((w_out_hbm, w_out), (w_gate_hbm, w_gate), (w_up_hbm, w_up), (w_down_hbm, w_down)))]
    for load in loads:
        load.start()
    width, count = late_hbm.shape
    plan, left = late_plan(width, count)
    late = [(late_hbm.at[pl.ds(start, size)], (w_gate, w_up)[buffer].at[pl.ds(0, size), pl.ds(lane, count)]) for buffer, lane, start, size in plan]
    if left:
        late.append((late_hbm.at[pl.ds(width - left, left)], late_rest))
    late_loads = [pltpu.make_async_copy(src, dst, late_sem.at[i]) for i, (src, dst) in enumerate(late)]
    net = Torus((far, near, relayed, sums, relayed2, sums2, rows), send_sem, recv_sem)
    net.barrier()
    loads[0].wait()

    def finish_with(old_ref, new_ref):
        def finish(c, q, half, total):
            value = (old_ref[c, q, half].astype(F32) + total).astype(BF16)
            new_ref[c, q, half] = value
            rows[(c, q) + net.place[q] + (half,)] = value
        return finish

    first = Stage(net, lambda c, q: a_ref[c, q], w_out, finish_with(res_ref, middle))
    second = Stage(net, lambda c, q: inner[c, q], w_down, finish_with(middle, new_res_ref))

    def mlp(c, q):
        first.complete(c, q)
        normed(net, c, q, gain_ref)
        hidden = rows_of(net, c, q)
        inner[c, q] = (jax.nn.silu(times_transposed(hidden, w_gate[...])) * times_transposed(hidden, w_up[...])).astype(BF16)
        second.begin(c, q)

    def after(c, q):
        second.complete(c, q)
        normed(net, c, q, next_gain_ref)
        hidden = rows_of(net, c, q)

        def product(lane, size):
            parts = [jnp.dot(hidden[:, start:start + rows_here], (w_gate, w_up)[buffer][pl.ds(0, rows_here), pl.ds(at + lane, size)], preferred_element_type=F32)
                     for buffer, at, start, rows_here in plan]
            if left:
                parts.append(jnp.dot(hidden[:, width - left:], late_rest[:, pl.ds(lane, size)], preferred_element_type=F32))
            return functools.reduce(jnp.add, parts)

        if last:
            put_statistics(product, count, *side_refs, out_ref, c, q)
        else:
            put_projected(product, *side_refs, out_ref, c, q)

    steps = [first.begin, *first.middle(), mlp, *second.middle(), after]
    groups = [(at, min(at + GROUP, chunks)) for at in range(0, chunks, GROUP)]
    final = len(groups) - 1

    def run(step, group):
        if step == mlp and group == 0:
            for load in loads[1:]:
                load.wait()
        if step == after and group == 0:
            for load in late_loads:
                load.wait()

        @pl.loop(*groups[group])
        def _(c):
            for q in BOTH:
                step(c, q)

        if step == mlp and group == final:
            for load in late_loads:
                load.start()

    for slot in range(len(steps) + LAG * final):
        for group in range(len(groups)):
            if 0 <= slot - LAG * group < len(steps):
                run(steps[slot - LAG * group], group)


def mega(a, res, gain, next_gain, sides, w_out, w_gate_t, w_up_t, w_down, late, layer, collective_id):
    chunks, _, rows, depth = a.shape
    _, hidden, width = w_gate_t.shape
    per = (chunks, PAIR)
    tile = (rows, LANES)
    last = len(sides) == 1
    count = late.shape[1]
    _, left = late_plan(width, count)

    def by_color(g):
        grid = g.reshape(RING, RING, PAIR, LANES)
        return jnp.stack([jnp.swapaxes(grid, 0, 1), grid]).reshape(PAIR, PAIR * SHARDS, LANES)

    sem = DMA(per + (PAIR, len(KINDS)))
    out = jax.ShapeDtypeStruct(per + tile, F32) if last else jax.ShapeDtypeStruct(per + (rows, count), BF16)
    return pl.pallas_call(
        functools.partial(mega_kernel, chunks, layer, last),
        out_shape=(out, jax.ShapeDtypeStruct(per + (PAIR,) + tile, BF16)),
        in_specs=[VMEM] * (4 + len(sides)) + [ANY] * 5,
        out_specs=(VMEM, VMEM),
        scratch_shapes=[
            pltpu.VMEM((depth, width), BF16),
            *[pltpu.VMEM((hidden, width), BF16) for _ in range(3)],
            pltpu.VMEM((left or 8, count), BF16),
            pltpu.VMEM(per + (rows, hidden), BF16),
            pltpu.VMEM(per + (PAIR,) + tile, BF16),
            pltpu.VMEM(per + (RING, PAIR) + tile, F32),
            pltpu.VMEM(per + (PAIR, PAIR, PAIR) + tile, F32),
            pltpu.VMEM(per + (PAIR, PAIR, PAIR) + tile, F32),
            pltpu.VMEM(per + (PAIR, RING, PAIR) + tile, F32),
            pltpu.VMEM(per + (PAIR,) + tile, F32),
            pltpu.VMEM(per + (PAIR, PAIR) + tile, F32),
            pltpu.VMEM(per + (RING, RING, PAIR) + tile, BF16),
            DMA((RING,)), DMA((SHARDS,)), sem, sem,
        ],
        compiler_params=pltpu.CompilerParams(collective_id=collective_id, has_side_effects=True, vmem_limit_bytes=VMEM_BYTES),
        name=f"mega{collective_id}",
    )(a, res, by_color(gain), by_color(next_gain), *sides, w_out, w_gate_t, w_up_t, w_down, late)


PEERS = 8
TILE = 128
Q_TILE = 256
LOG2E = 1.4426950408889634
HELD = pltpu.VMEM((PEERS, PAIR, TILE, COLUMNS), BF16)
GATHER_SEMS = [DMA((PAIR, 3)), DMA((PAIR, 3)), DMA((RING,)), DMA((RING,))]


class Exchange:
    def __init__(self):
        self.me = lax.axis_index("resp")
        self.others = [(self.me + k) % PEERS for k in range(1, PEERS)]

    def barrier(self):
        sem = pltpu.get_barrier_semaphore()
        for device in self.others:
            pl.semaphore_signal(sem, inc=1, device_id={"resp": device}, device_id_type=MESH)
        pl.semaphore_wait(sem, PEERS - 1)

    def copy(self, src, dst, send_sem, recv_sem, device):
        return pltpu.make_async_remote_copy(src_ref=src, dst_ref=dst, send_sem=send_sem, recv_sem=recv_sem,
                                            device_id={"resp": device}, device_id_type=MESH)

    def scatter(self, src_of, dst, send_sem, recv_sem):
        for device in self.others:
            self.copy(src_of(device), dst, send_sem.at[device], recv_sem.at[self.me], device).start()

    def collected(self, dst_of, recv_sem):
        for device in self.others:
            self.copy(dst_of(device), dst_of(device), recv_sem.at[device], recv_sem.at[device], device).wait_recv()

    def sent(self, src_of, send_sem, recv_sem):
        for device in self.others:
            self.copy(src_of(device), src_of(device), send_sem.at[device], recv_sem.at[device], device).wait_send()


class PromptGather:
    def __init__(self, net, held, ring_send, ring_recv, near_send, near_recv):
        self.net, self.held = net, held
        self.ring_sems, self.near_sems = (ring_send, ring_recv), (near_send, near_recv)
        x, core = net.me // PAIR, net.me % PAIR
        self.at = lambda by, here: (x + by + RING) % RING * PAIR + (core if here else 1 - core)

    def ring_copy(self, d, kind, ref):
        return self.net.copy(ref, ref, self.ring_sems[0].at[d, kind], self.ring_sems[1].at[d, kind], self.at(1 - PAIR * d, True))

    def near_copy(self, kind, ref):
        return self.net.copy(ref, ref, self.near_sems[0].at[kind], self.near_sems[1].at[kind], self.at(0, False))

    def sources(self, here):
        return [self.at(by, here) for by in (0, -1, 1, PAIR)]

    def start(self):
        own = self.held.at[self.net.me]
        for kind in BOTH:
            for d in BOTH:
                self.ring_copy(d, kind, own.at[1 - d if kind else d]).start()
        self.near_copy(0, own).start()

    def relay(self):
        for d in BOTH:
            ref = self.held.at[self.at(PAIR * d - 1, True), d]
            self.ring_copy(d, 0, ref).wait_recv()
            self.ring_copy(d, PAIR, ref).start()

    def share(self):
        for d in BOTH:
            device = self.at(PAIR * d - 1, True)
            self.ring_copy(d, 1, self.held.at[device, 1 - d]).wait_recv()
            self.near_copy(1 + d, self.held.at[device]).start()
        far = self.held.at[self.at(PAIR, True)]
        for d in BOTH:
            self.ring_copy(d, PAIR, far.at[d]).wait_recv()
        self.near_copy(3, far).start()

    def collect(self):
        for kind, device in enumerate(self.sources(False)):
            self.near_copy(kind, self.held.at[device]).wait_recv()

    def finish(self):
        for kind in range(3):
            for d in BOTH:
                self.ring_copy(d, kind, self.held.at[self.net.me, d]).wait_send()
        for kind in range(RING):
            self.near_copy(kind, self.held.at[self.net.me]).wait_send()


def deal(rows):
    out = lax.broadcasted_iota(jnp.int32, (rows, rows), 0)
    src = lax.broadcasted_iota(jnp.int32, (rows, rows), 1)
    per = rows // PEERS
    return jnp.where(src == (out % per) * PEERS + out // per, 1.0, 0.0).astype(BF16)


def undeal(rows):
    out = lax.broadcasted_iota(jnp.int32, (rows, rows), 0)
    src = lax.broadcasted_iota(jnp.int32, (rows, rows), 1)
    per = rows // PEERS
    return jnp.where(src == (out % PEERS) * per + out // PEERS, 1.0, 0.0).astype(BF16)


def norm_tile(x_ref, out_ref, gain_ref):
    for i in range(x_ref.shape[0] // 16):
        v = x_ref[pl.ds(16 * i, 16), :].astype(F32)
        inv = lax.rsqrt(jnp.mean(v * v, axis=-1, keepdims=True) + EPS)
        out_ref[pl.ds(16 * i, 16), :] = (v * inv * gain_ref[...]).astype(BF16)


def softmax_mix(q, pieces):
    factor = LOG2E * 128 ** -0.5
    outs = []
    for h in range(2):
        lanes = slice(128 * h, 128 * h + 128)
        scores = []
        for keys, _, mask in pieces:
            s = lax.dot_general(q[:, lanes], keys[:, lanes], (((1,), (1,)), ((), ())), preferred_element_type=F32)
            scores.append(s if mask is None else jnp.where(mask, s, -jnp.inf))
        top = functools.reduce(jnp.maximum, [jnp.max(s, axis=-1, keepdims=True) for s in scores])
        probs = [jnp.exp2((s - top) * factor) for s in scores]
        total = functools.reduce(jnp.add, [jnp.sum(p, axis=-1, keepdims=True) for p in probs])
        mixed = functools.reduce(jnp.add, [jnp.dot(p.astype(BF16), values[:, lanes], preferred_element_type=F32) for p, (_, values, _) in zip(probs, pieces)])
        outs.append(mixed / total)
    return jnp.concatenate(outs, axis=1).astype(BF16)


def prompt_rows_of(held, which):
    return held[:, which].reshape(PEERS * TILE, COLUMNS)


def attend_response(t, q, held, k_own, v_own):
    row = lax.broadcasted_iota(jnp.int32, (Q_TILE, Q_TILE), 0)
    col = lax.broadcasted_iota(jnp.int32, (Q_TILE, Q_TILE), 1)
    pieces = [(prompt_rows_of(held, 0), prompt_rows_of(held, 1), None)]
    if t:
        pieces.append((k_own[:t * Q_TILE], v_own[:t * Q_TILE], None))
    span = slice(t * Q_TILE, (t + 1) * Q_TILE)
    pieces.append((k_own[span], v_own[span], col <= row))
    return softmax_mix(q, pieces)


def deal_mixed(net, t, mixed, stage, out, send_sem, recv_sem):
    dealt = jnp.dot(deal(Q_TILE), mixed, preferred_element_type=F32).astype(BF16)
    stage[t] = dealt.reshape(PEERS, Q_TILE // PEERS, COLUMNS)
    net.scatter(lambda d: stage.at[t, d], out.at[net.me, t], send_sem.at[t], recv_sem.at[t])
    out[net.me, t] = stage[t, net.me]


def first_attention_kernel(xp_hbm, xr_hbm, wq_hbm, wk_hbm, wv_hbm, gain_ref, cos_ref, sin_ref, info_ref,
                           mixed_out, res_out, info_out, prompt_out,
                           xs, w, hidden, q_s, k_s, v_s, held, mixed_stage, res_stage,
                           x_sem, w_sem, ring_send, ring_recv, near_send, near_recv, mix_send, mix_recv, res_send, res_recv, info_send, info_recv):
    net = Exchange()
    prompt = PromptGather(net, held, ring_send, ring_recv, near_send, near_recv)
    me = net.me
    column = pl.multiple_of(lax.axis_index("model") * COLUMNS, COLUMNS)

    def load(t):
        src = xp_hbm if isinstance(t, int) and t == 0 else xr_hbm.at[pl.ds(pl.multiple_of((t - 1) * TILE, TILE), TILE)]
        return pltpu.make_async_copy(src, xs.at[t], x_sem.at[t])

    load(0).start()
    weights = [pltpu.make_async_copy(src, w.at[:, pl.ds(COLUMNS * i, COLUMNS)], w_sem.at[i]) for i, src in enumerate((wq_hbm, wk_hbm, wv_hbm))]
    for copy in weights:
        copy.start()
    for t in range(1, 9):
        load(t).start()
    net.barrier()
    net.scatter(lambda d: info_ref.at[d], info_out.at[me], info_send, info_recv)
    info_out[me] = info_ref[me]

    def project(t):
        span = pl.ds(pl.multiple_of(t * TILE, TILE), TILE)
        qkv = jnp.dot(hidden[t % 2], w[...], preferred_element_type=F32)
        cos, sin = cos_ref[span], sin_ref[span]
        return span, rope(qkv[:, :COLUMNS], cos, sin).astype(BF16), rope(qkv[:, COLUMNS:512], cos, sin).astype(BF16), qkv[:, 512:].astype(BF16)

    load(0).wait()
    norm_tile(xs.at[0], hidden.at[0], gain_ref)
    load(1).wait()
    for copy in weights:
        copy.wait()
    norm_tile(xs.at[1], hidden.at[1], gain_ref)
    span, q, k, v = project(0)
    q_s[span] = q
    held[me, 0] = k
    held[me, 1] = v
    prompt.start()
    spread = deal(TILE)

    @pl.loop(1, 9)
    def _(t):
        later = jnp.minimum(t + 1, 8)

        @pl.when(t < 8)
        def _():
            load(t + 1).wait()

        span, q, k, v = project(t)
        norm_tile(xs.at[later], hidden.at[(t + 1) % 2], gain_ref)
        q_s[span] = q
        own = pl.ds(pl.multiple_of((t - 1) * TILE, TILE), TILE)
        k_s[own] = k
        v_s[own] = v
        dealt = jnp.dot(spread, xs[t, :, pl.ds(column, COLUMNS)], preferred_element_type=F32).astype(BF16)
        res_stage[:, t - 1] = dealt.reshape(PEERS, TILE // PEERS, COLUMNS)
        pl.when(t == 3)(prompt.relay)
        pl.when(t == 5)(prompt.share)

    net.scatter(lambda d: res_stage.at[d], res_out.at[me], res_send, res_recv)
    res_out[me] = res_stage[me]
    prompt.collect()
    for t in range(RING):
        mixed = attend_response(t, q_s[pl.ds(TILE + t * Q_TILE, Q_TILE)], held, k_s, v_s)
        deal_mixed(net, t, mixed, mixed_stage, mixed_out, mix_send, mix_recv)
    row = lax.broadcasted_iota(jnp.int32, (TILE, PEERS * TILE), 0) + me * TILE
    col = lax.broadcasted_iota(jnp.int32, (TILE, PEERS * TILE), 1)
    prompt_out[:, :COLUMNS] = softmax_mix(q_s[pl.ds(0, TILE)], [(prompt_rows_of(held, 0), prompt_rows_of(held, 1), col <= row)])
    prompt_out[:, COLUMNS:] = xs[0, :, pl.ds(column, COLUMNS)]
    finish_exchange(net, mixed_stage, mixed_out, mix_send, mix_recv)
    net.collected(lambda d: res_out.at[d], res_recv)
    net.sent(lambda d: res_stage.at[d], res_send, res_recv)
    net.collected(lambda d: info_out.at[d], info_recv)
    net.sent(lambda d: info_ref.at[d], info_send, info_recv)
    prompt.finish()


def finish_exchange(net, stage, out, send_sem, recv_sem):
    for t in range(RING):
        net.collected(lambda d: out.at[d, t], recv_sem.at[t])
        net.sent(lambda d: stage.at[t, d], send_sem.at[t], recv_sem.at[t])


def first_attention(x_prompt, x_resp, w_query, w_key, w_value, gain, cos, sin, info, collective_id):
    rows = TILE + x_resp.shape[0]
    width = x_resp.shape[1]
    return pl.pallas_call(
        first_attention_kernel,
        out_shape=(jax.ShapeDtypeStruct((PEERS, RING, 32, COLUMNS), BF16), jax.ShapeDtypeStruct((PEERS, 8, 16, COLUMNS), BF16),
                   jax.ShapeDtypeStruct((PEERS, 8, 128), jnp.int32), jax.ShapeDtypeStruct((TILE, PAIR * COLUMNS), BF16)),
        in_specs=[ANY] * 5 + [VMEM] * 4,
        out_specs=(VMEM,) * 4,
        scratch_shapes=[
            pltpu.VMEM((9, TILE, width), BF16), pltpu.VMEM((width, 768), BF16), pltpu.VMEM((2, TILE, width), BF16),
            pltpu.VMEM((rows, COLUMNS), BF16), pltpu.VMEM((rows - TILE, COLUMNS), BF16), pltpu.VMEM((rows - TILE, COLUMNS), BF16),
            HELD, pltpu.VMEM((RING, PEERS, 32, COLUMNS), BF16), pltpu.VMEM((PEERS, 8, 16, COLUMNS), BF16),
            DMA((9,)), DMA((3,)), *GATHER_SEMS, DMA((RING, PEERS)), DMA((RING, PEERS)), *[DMA((PEERS,)) for _ in range(RING)],
        ],
        compiler_params=pltpu.CompilerParams(collective_id=collective_id, has_side_effects=True, vmem_limit_bytes=VMEM_BYTES),
        name="first_attention",
    )(x_prompt, x_resp, w_query, w_key, w_value, gain.reshape(1, width), cos, sin, info)


def second_attention_kernel(qkv_ref, kv_prompt_ref, mixed_out, qkv_in, k_s, v_s, held, mixed_stage,
                            ring_send, ring_recv, near_send, near_recv, qkv_send, qkv_recv, mix_send, mix_recv):
    net = Exchange()
    me = net.me
    prompt = PromptGather(net, held, ring_send, ring_recv, near_send, near_recv)
    held[me] = kv_prompt_ref[...]
    net.barrier()
    prompt.start()

    def send_rows(t):
        net.scatter(lambda d: qkv_ref.at[t, d], qkv_in.at[t, me], qkv_send.at[t], qkv_recv.at[t])
        qkv_in[t, me] = qkv_ref[t, me]

    send_rows(0)
    prompt.relay()
    prompt.share()
    for t in range(1, RING):
        send_rows(t)
    prompt.collect()
    for t in range(RING):
        net.collected(lambda d: qkv_in.at[t, d], qkv_recv.at[t])
        rows = jnp.dot(undeal(Q_TILE), qkv_in[t].reshape(Q_TILE, 3 * COLUMNS), preferred_element_type=F32).astype(BF16)
        k_s[pl.ds(t * Q_TILE, Q_TILE)] = rows[:, COLUMNS:PAIR * COLUMNS]
        v_s[pl.ds(t * Q_TILE, Q_TILE)] = rows[:, PAIR * COLUMNS:]
        mixed = attend_response(t, rows[:, :COLUMNS], held, k_s, v_s)
        deal_mixed(net, t, mixed, mixed_stage, mixed_out, mix_send, mix_recv)
    finish_exchange(net, mixed_stage, mixed_out, mix_send, mix_recv)
    for t in range(RING):
        net.sent(lambda d: qkv_ref.at[t, d], qkv_send.at[t], qkv_recv.at[t])
    prompt.finish()


def second_attention(qkv, kv_prompt, collective_id):
    rows = RING * Q_TILE
    return pl.pallas_call(
        second_attention_kernel,
        out_shape=jax.ShapeDtypeStruct((PEERS, RING, 32, COLUMNS), BF16),
        in_specs=[VMEM, VMEM],
        out_specs=VMEM,
        scratch_shapes=[
            pltpu.VMEM((RING, PEERS, 32, 3 * COLUMNS), BF16), pltpu.VMEM((rows, COLUMNS), BF16), pltpu.VMEM((rows, COLUMNS), BF16),
            HELD, pltpu.VMEM((RING, PEERS, 32, COLUMNS), BF16), *GATHER_SEMS, *[DMA((RING, PEERS)) for _ in range(RING)],
        ],
        compiler_params=pltpu.CompilerParams(collective_id=collective_id, has_side_effects=True, vmem_limit_bytes=VMEM_BYTES),
        name=f"second_attention{collective_id}",
    )(qkv, kv_prompt)


def combine_kernel(shards, stats_ref, out_ref, every, stat_send, stat_recv, row_send, row_recv):
    me, home = lax.axis_index("model"), lax.axis_index("resp")
    sem = pltpu.get_barrier_semaphore()
    models = [(me + k) % shards for k in range(1, shards)]
    homes = [(home + k) % PEERS for k in range(1, PEERS)]
    for device in models:
        pl.semaphore_signal(sem, inc=1, device_id={"model": device}, device_id_type=MESH)
    for device in homes:
        pl.semaphore_signal(sem, inc=1, device_id={"resp": device}, device_id_type=MESH)
    pl.semaphore_wait(sem, shards + PEERS - 2)

    def stat_copy(src, dst, send, recv, device):
        return pltpu.make_async_remote_copy(src_ref=src, dst_ref=dst, send_sem=send, recv_sem=recv, device_id={"model": device}, device_id_type=MESH)

    def row_copy(src, dst, send, recv, device):
        return pltpu.make_async_remote_copy(src_ref=src, dst_ref=dst, send_sem=send, recv_sem=recv, device_id={"resp": device}, device_id_type=MESH)

    for device in models:
        stat_copy(stats_ref, every.at[me], stat_send.at[device], stat_recv.at[me], device).start()
    every[me] = stats_ref[...]
    for device in models:
        stat_copy(every.at[device], every.at[device], stat_send.at[device], stat_recv.at[device], device).wait_recv()
    tops = [every[k, 0] for k in range(shards)]
    top = functools.reduce(jnp.maximum, tops)
    total = functools.reduce(jnp.add, [every[k, 1] * jnp.exp(tops[k] - top) for k in range(shards)])
    picked = functools.reduce(jnp.add, [every[k, 2] for k in range(shards)])
    out_ref[home] = picked - top - jnp.log(total)
    for device in homes:
        row_copy(out_ref.at[home], out_ref.at[home], row_send.at[device], row_recv.at[home], device).start()
    for device in homes:
        row_copy(out_ref.at[device], out_ref.at[device], row_send.at[device], row_recv.at[device], device).wait_recv()
    for device in models:
        stat_copy(stats_ref, stats_ref, stat_send.at[device], stat_recv.at[device], device).wait_send()
    for device in homes:
        row_copy(out_ref.at[home], out_ref.at[home], row_send.at[device], row_recv.at[device], device).wait_send()


def combine(stats, shards, collective_id):
    return pl.pallas_call(
        functools.partial(combine_kernel, shards),
        out_shape=jax.ShapeDtypeStruct((PEERS, 8, 128), F32),
        in_specs=[VMEM],
        out_specs=VMEM,
        scratch_shapes=[pltpu.VMEM((shards, 3, 8, 128), F32), DMA((shards,)), DMA((shards,)), DMA((PEERS,)), DMA((PEERS,))],
        compiler_params=pltpu.CompilerParams(collective_id=collective_id, has_side_effects=True),
        name=f"combine{collective_id}",
    )(stats)


ROPE_BASE = 10000.0
VARIANTS = (704, 1024)
CHUNKS = 4


def rope_tables(positions):
    half = LANES // PAIR
    frequency = ROPE_BASE ** (-jnp.arange(half, dtype=F32) / half)
    angles = positions.astype(F32)[:, None] * frequency
    cos, sin = jnp.cos(angles), jnp.sin(angles)
    return jnp.concatenate([cos, cos], axis=1), jnp.concatenate([-sin, sin], axis=1)


def by_chunk(rows):
    return rows.reshape(CHUNKS, PAIR, rows.shape[0] // (CHUNKS * PAIR), rows.shape[1])


def to_blocks(rows):
    grid = by_chunk(rows)
    return jnp.swapaxes(grid.reshape(grid.shape[:3] + (PAIR, LANES)), 2, 3)


def from_blocks(blocks):
    return jnp.swapaxes(blocks, 2, 3).reshape(-1, COLUMNS)


def solution(mesh):
    groups = mesh.shape['resp']
    shards = mesh.shape['model']
    row_axes = ('prompts', 'resp')
    head_spec = P(None, None, 'model', None)
    in_specs = (P(row_axes, None), P(row_axes, None, None), P(row_axes, None), P(row_axes), P(None, None), head_spec, head_spec, head_spec, P(None, 'model', None, None), P(None, None), P(None, None, 'model'), P(None, None, 'model'), P(None, 'model', None), P(None), P(None, 'model'))

    def device_step(x_prompt, x_resp, targets, resp_lens, attn_gain, w_query, w_key, w_value, w_out, mlp_gain, w_gate, w_up, w_down, final_gain, w_vocab):
        prompt_rows = x_prompt.shape[0]
        resp_len, width = x_resp.shape[1:]
        prompt_len = prompt_rows * groups
        me = lax.axis_index('model')
        home = lax.axis_index('resp')
        per = resp_len // groups
        gate_t, up_t = jnp.swapaxes(w_gate, 1, 2), jnp.swapaxes(w_up, 1, 2)
        out_flat = w_out.reshape(w_out.shape[0], COLUMNS, width)
        flat = lambda w, layer: w[layer].reshape(width, COLUMNS)
        project_next = jnp.concatenate([flat(w, 1) for w in (w_query, w_key, w_value)], axis=1)
        prompt_pos = home * prompt_rows + jnp.arange(prompt_rows)

        cos, sin = rope_tables(jnp.concatenate([prompt_pos, prompt_len + jnp.arange(resp_len)]))
        info = jnp.concatenate([
            targets[0].reshape(per, groups).T[:, None, :],
            jnp.broadcast_to(resp_lens[0], (groups, groups - 1, per)).astype(jnp.int32)], axis=1)
        mixed, res, infos, prompt = first_attention(
            x_prompt, x_resp[0], flat(w_query, 0), flat(w_key, 0), flat(w_value, 0), attn_gain[0], cos, sin, info, 0)
        lens = infos[:, 1, 0]
        need = (lens + groups - 1) // groups
        ends = jnp.sum(jnp.where(jnp.arange(groups)[:, None] >= jnp.arange(groups), need, 0), axis=1)
        starts = ends - need
        dealt = groups * per

        def finish_with(size, ident):
            def run(operands):
                mixed, res, prompt = operands
                slot = jnp.arange(size)
                which = jnp.sum((slot[:, None] >= ends).astype(jnp.int32), axis=1)
                row = slot - jnp.sum(jnp.where(which[:, None] == jnp.arange(groups), starts, 0), axis=1)
                real = slot < ends[-1]
                chosen = jnp.where(real, which * per + row, -1)[:, None] == jnp.arange(dealt)
                pick = chosen.astype(BF16)

                def pack(rows):
                    return jnp.dot(pick, rows, preferred_element_type=F32).astype(BF16)

                kept = pack(jnp.concatenate([mixed.reshape(dealt, COLUMNS), res.reshape(dealt, COLUMNS)], axis=1))
                rows = jnp.concatenate([prompt, kept], axis=0)
                tables = rope_tables(jnp.concatenate([prompt_pos, prompt_len + groups * row + home]))
                qkv, new_res = mega(
                    by_chunk(rows[:, :COLUMNS]), to_blocks(rows[:, COLUMNS:]), mlp_gain[0], attn_gain[1], [by_chunk(t) for t in tables],
                    out_flat, gate_t, up_t, w_down, project_next, 0, ident)
                qkv = qkv.reshape(prompt_rows + size, 3 * COLUMNS)
                part = per // RING
                back = jnp.where(real, (row // part) * (groups * part) + which * part + row % part, -1)
                place = (jnp.arange(dealt)[:, None] == back).astype(BF16)
                home_rows = jnp.dot(place, qkv[prompt_rows:], preferred_element_type=F32).astype(BF16)
                kv_prompt = jnp.stack([qkv[:prompt_rows, COLUMNS:PAIR * COLUMNS], qkv[:prompt_rows, PAIR * COLUMNS:]])
                mixed = second_attention(home_rows.reshape(RING, groups, part, 3 * COLUMNS), kv_prompt, ident + 1)
                wanted = jnp.sum(jnp.where(chosen, infos[:, 0, :].reshape(dealt), 0), axis=1) - me * w_vocab.shape[1]
                stats, _ = mega(
                    by_chunk(pack(mixed.reshape(dealt, COLUMNS))), to_blocks(from_blocks(new_res)[prompt_rows:]), mlp_gain[1], final_gain,
                    [by_chunk(jnp.broadcast_to(wanted[:, None], (size, LANES)))], out_flat, gate_t, up_t, w_down, w_vocab, 1, ident + PAIR)
                stats = jnp.pad(stats.reshape(size, LANES)[:, :3].T, ((0, 0), (0, dealt - size)))
                found = combine(stats.reshape(3, groups, per), shards, ident + 3).reshape(groups, dealt)
                start = jnp.sum(jnp.where(jnp.arange(groups) == home, starts, 0))
                mine = lax.dynamic_slice(jnp.pad(found, ((0, 0), (0, per))), (0, start), (groups, per))
                return mine.T.reshape(resp_len)
            return run

        index = sum((ends[-1] > size).astype(jnp.int32) for size in VARIANTS[:-1])
        log_probs = lax.switch(index, [finish_with(size, 1 + RING * i) for i, size in enumerate(VARIANTS)], (mixed, res, prompt))
        log_probs = jnp.where(jnp.arange(resp_len) < resp_lens[0], log_probs, 0.0)
        return log_probs[None, :]

    return jax.shard_map(device_step, mesh=mesh, in_specs=in_specs, out_specs=P(row_axes, None), check_vma=False)
```

```python
import functools

import jax
import jax.numpy as jnp
from jax import lax
from jax.experimental import pallas as pl
from jax.experimental.pallas import tpu as pltpu
from jax.sharding import PartitionSpec as P

MESH = pl.DeviceIdType.MESH
F32 = jnp.float32
BF16 = jnp.bfloat16
EPS = 1e-6
LANES = 128
PAIR = 2
RING = 4
COLUMNS = PAIR * LANES
SHARDS = RING * RING
BOTH = range(PAIR)
VMEM_BYTES = 67_000_000
LATE_ROWS = 640
LOGITS = 512
VMEM = pl.BlockSpec(memory_space=pltpu.VMEM)
ANY = pl.BlockSpec(memory_space=pl.ANY)
DMA = pltpu.SemaphoreType.DMA
KINDS = range(RING * 3)
SUM_FAR, SUM_NEAR, SUM_RELAY, SUM2_FAR, SUM2_NEAR, SUM2_RELAY, TAKE_OWN, TAKE_REST, TAKE_RELAY, TAKE2_OWN, TAKE2_REST, TAKE2_RELAY = KINDS


def block_of(color, first, second):
    return RING * first + second if color else RING * second + first


def pair(index):
    return pl.ds(PAIR * index, PAIR)


class Torus:
    def __init__(self, refs, send_sem, recv_sem):
        self.refs = refs
        self.far, self.near, self.relayed, self.sums, self.relayed2, self.sums2, self.rows = refs
        self.send_sem, self.recv_sem = send_sem, recv_sem
        me = lax.axis_index("model")
        z, y = me // RING, me % RING
        self.place = ((y, z), (z, y))
        along_y = [z * RING + self.step(y, way) for way in (1, -1)]
        along_z = [self.step(z, way) * RING + y for way in (1, -1)]
        self.neighbors = ((along_y, along_z), (along_z, along_y))

    def step(self, place, by):
        return (place + by + RING) % RING

    def barrier(self):
        sem = pltpu.get_barrier_semaphore()
        for ring in self.neighbors[0]:
            for device in ring:
                pl.semaphore_signal(sem, device_id={"model": device}, device_id_type=MESH)
        pl.semaphore_wait(sem, RING)

    def ends(self, kind, c, q, d):
        (p, s), way, other = self.place[q], 1 - PAIR * d, 1 - d
        far, near, relayed, sums, relayed2, sums2, rows = (ref.at[c, q] for ref in self.refs)
        own = sums.at[0]
        back_s, back_p = self.step(s, -way), self.step(p, -way)
        return {
            SUM_FAR: lambda: (far.at[pair(d)], relayed.at[d], relayed.at[d]),
            SUM_NEAR: lambda: (near.at[d], sums.at[d, pair(other)], sums.at[d, pair(other)]),
            SUM_RELAY: lambda: (relayed.at[d], sums.at[d, pair(d)], sums.at[d, pair(d)]),
            SUM2_FAR: lambda: (own.at[self.step(s, PAIR), d], relayed2.at[d], relayed2.at[d]),
            SUM2_NEAR: lambda: (own.at[self.step(s, way), other], sums2.at[d, other], sums2.at[d, other]),
            SUM2_RELAY: lambda: (relayed2.at[d], sums2.at[d, d], sums2.at[d, d]),
            TAKE_OWN: lambda: (rows.at[p, s, d], rows.at[p, s, d], rows.at[p, back_s, d]),
            TAKE_REST: lambda: (rows.at[p, s, other], rows.at[p, s, other], rows.at[p, back_s, other]),
            TAKE_RELAY: lambda: (rows.at[p, back_s, d], rows.at[p, back_s, d], rows.at[p, self.step(s, PAIR), d]),
            TAKE2_OWN: lambda: (rows.at[p, pair(d)], rows.at[p, pair(d)], rows.at[back_p, pair(d)]),
            TAKE2_REST: lambda: (rows.at[p, pair(other)], rows.at[p, pair(other)], rows.at[back_p, pair(other)]),
            TAKE2_RELAY: lambda: (rows.at[back_p, pair(d)], rows.at[back_p, pair(d)], rows.at[self.step(p, PAIR), pair(d)]),
        }[kind]()

    def copy(self, kind, c, q, d, src, dst):
        second_ring = kind in (SUM2_FAR, SUM2_NEAR, SUM2_RELAY, TAKE_OWN, TAKE_REST, TAKE_RELAY)
        return pltpu.make_async_remote_copy(
            src_ref=src, dst_ref=dst, send_sem=self.send_sem.at[c, q, d, kind], recv_sem=self.recv_sem.at[c, q, d, kind],
            device_id={"model": self.neighbors[q][second_ring][d]}, device_id_type=MESH)

    def send(self, c, q, d, kind):
        src, dst, _ = self.ends(kind, c, q, d)
        self.copy(kind, c, q, d, src, dst).start()

    def sent(self, c, q, *kinds):
        for kind in kinds:
            for d in BOTH:
                src, dst, _ = self.ends(kind, c, q, d)
                self.copy(kind, c, q, d, src, dst).wait_send()

    def arrived(self, c, q, d, *kinds):
        for kind in kinds:
            _, _, here = self.ends(kind, c, q, d)
            self.copy(kind, c, q, d, here, here).wait_recv()


def halves(value):
    return value[:, :LANES], value[:, LANES:]


def store_block(ref, value):
    for half, part in enumerate(halves(value)):
        ref[half] = part


def add_block(ref, value):
    for half, part in enumerate(halves(value)):
        ref[half] += part


class Stage:
    def __init__(self, net, lhs_of, w_ref, finish):
        self.net, self.lhs_of, self.w_ref, self.finish = net, lhs_of, w_ref, finish

    def product(self, lhs, color, first, second):
        start = pl.multiple_of(block_of(color, first, second) * COLUMNS, COLUMNS)
        return jnp.dot(lhs, self.w_ref[:, pl.ds(start, COLUMNS)], preferred_element_type=F32)

    def begin(self, c, q):
        net, p, lhs = self.net, self.net.place[q][0], self.lhs_of(c, q)
        for k in range(RING):
            store_block(net.far.at[c, q, k], self.product(lhs, q, net.step(p, PAIR), k))
        for d in BOTH:
            net.send(c, q, d, SUM_FAR)
        for d in BOTH:
            for k in BOTH:
                store_block(net.near.at[c, q, d, k], self.product(lhs, q, net.step(p, 1 - PAIR * d), PAIR * (1 - d) + k))
            net.send(c, q, d, SUM_NEAR)

    def relay_sum(self, c, q):
        net, p, lhs = self.net, self.net.place[q][0], self.lhs_of(c, q)
        for d in BOTH:
            net.arrived(c, q, d, SUM_FAR)
            for k in BOTH:
                add_block(net.relayed.at[c, q, d, k], self.product(lhs, q, net.step(p, 1 - PAIR * d), PAIR * d + k))
            net.send(c, q, d, SUM_RELAY)

    def begin_second(self, c, q):
        net, lhs = self.net, self.lhs_of(c, q)
        for d in BOTH:
            net.arrived(c, q, d, SUM_NEAR, SUM_RELAY)
        for k in range(RING):
            for half, part in enumerate(halves(self.product(lhs, q, net.place[q][0], k))):
                net.sums[c, q, 0, k, half] += net.sums[c, q, 1, k, half] + part
        for kind in (SUM2_FAR, SUM2_NEAR):
            for d in BOTH:
                net.send(c, q, d, kind)
        net.sent(c, q, SUM_FAR)

    def relay_second(self, c, q):
        net = self.net
        for d in BOTH:
            net.arrived(c, q, d, SUM2_FAR)
            net.relayed2[c, q, d] += net.sums[c, q, 0, net.step(net.place[q][1], 1 - PAIR * d), d]
            net.send(c, q, d, SUM2_RELAY)

    def finish_sum(self, c, q):
        net = self.net
        net.sent(c, q, SUM_NEAR, SUM_RELAY)
        for d in BOTH:
            net.arrived(c, q, d, SUM2_NEAR, SUM2_RELAY)
        for half in BOTH:
            self.finish(c, q, half, net.sums[c, q, 0, net.place[q][1], half] + net.sums2[c, q, 0, half] + net.sums2[c, q, 1, half])
        for kind in (TAKE_OWN, TAKE_REST):
            for d in BOTH:
                net.send(c, q, d, kind)

    def relay_rows(self, c, q):
        net = self.net
        net.sent(c, q, SUM2_FAR, SUM2_NEAR, SUM2_RELAY)
        for d in BOTH:
            net.arrived(c, q, d, TAKE_OWN)
            net.send(c, q, d, TAKE_RELAY)

    def take_second(self, c, q):
        net = self.net
        for d in BOTH:
            net.arrived(c, q, d, TAKE_REST, TAKE_RELAY)
        for kind in (TAKE2_OWN, TAKE2_REST):
            for d in BOTH:
                net.send(c, q, d, kind)

    def relay_last(self, c, q):
        net = self.net
        for d in BOTH:
            net.arrived(c, q, d, TAKE2_OWN)
            net.send(c, q, d, TAKE2_RELAY)

    def complete(self, c, q):
        net = self.net
        for d in BOTH:
            net.arrived(c, q, d, TAKE2_REST, TAKE2_RELAY)
        net.sent(c, q, TAKE_OWN, TAKE_REST, TAKE_RELAY, TAKE2_OWN, TAKE2_REST, TAKE2_RELAY)

    def middle(self):
        return [self.relay_sum, self.begin_second, self.relay_second, self.finish_sum, self.relay_rows, self.take_second, self.relay_last]


def normed(net, c, q, gain_ref):
    rows = net.rows.shape[-PAIR]
    tile = PAIR * 8 if rows % (PAIR * 8) == 0 else 8
    spots = [(first, second, half) for first in range(RING) for second in range(RING) for half in BOTH]

    @pl.loop(0, rows // tile)
    def _(i):
        span = pl.ds(pl.multiple_of(i * tile, tile), tile)
        acts = [net.rows[(c, q) + spot + (span,)].astype(F32) for spot in spots]
        squares = functools.reduce(jnp.add, [v * v for v in acts])
        inv = lax.rsqrt(jnp.sum(squares, axis=-1, keepdims=True) / (LANES * len(acts)) + EPS)
        for k, (spot, v) in enumerate(zip(spots, acts)):
            net.rows[(c, q) + spot + (span,)] = (v * inv * gain_ref[q, pl.ds(k, 1)]).astype(BF16)


def rows_of(net, c, q):
    parts = []
    for upper in range(RING):
        for lower in range(RING):
            first, second = (upper, lower) if q else (lower, upper)
            parts += [net.rows[c, q, first, second, half] for half in BOTH]
    return jnp.concatenate(parts, axis=1)


def times_transposed(lhs, rhs):
    return lax.dot_general(lhs, rhs, (((1,), (1,)), ((), ())), preferred_element_type=F32)


def late_plan(width, count):
    plan, start = [], 0
    for buffer in BOTH:
        for slot in range(width // count):
            size = min(LATE_ROWS, width - start)
            if size:
                plan.append((buffer, slot * count, start, size))
            start += size
    return plan, width - start


def rope(value, cos, sin):
    return jnp.concatenate([v * cos + pltpu.roll(v, LANES // PAIR, 1) * sin for v in halves(value)], axis=1)


def put_projected(product, cos_ref, sin_ref, out_ref, c):
    for k in range(3):
        value = product(k * COLUMNS, COLUMNS)
        if k < PAIR:
            value = rope(value, cos_ref[c], sin_ref[c])
        out_ref[c, :, pl.ds(k * COLUMNS, COLUMNS)] = value.astype(BF16)


def put_statistics(product, count, target_ref, out_ref, c):
    top = total = picked = None
    for k in range(count // LOGITS):
        logits = product(k * LOGITS, LOGITS)
        here = jnp.max(logits, axis=-1, keepdims=True)
        ids = lax.broadcasted_iota(jnp.int32, logits.shape, 1) + k * LOGITS
        found = jnp.sum(jnp.where(ids == target_ref[c, :, :1], logits, 0.0), axis=-1, keepdims=True)
        if k:
            both = jnp.maximum(top, here)
            total = total * jnp.exp(top - both) + jnp.sum(jnp.exp(logits - both), axis=-1, keepdims=True)
            top, picked = both, picked + found
        else:
            top, total, picked = here, jnp.sum(jnp.exp(logits - here), axis=-1, keepdims=True), found
    lane = lax.broadcasted_iota(jnp.int32, out_ref.shape[1:], 1)
    out_ref[c] = jnp.where(lane == 0, top, jnp.where(lane == 1, total, picked))


def mega_kernel(chunks, layer, last, a_ref, res_ref, gain_ref, next_gain_ref, *args):
    side_refs, args = args[:PAIR - last], args[PAIR - last:]
    (w_out_hbm, w_gate_hbm, w_up_hbm, w_down_hbm, late_hbm, out_ref, new_res_ref,
     w_out, w_gate, w_up, w_down, late_rest, inner, middle,
     far, near, relayed, sums, relayed2, sums2, rows, w_sem, late_sem, send_sem, recv_sem) = args
    loads = [pltpu.make_async_copy(src.at[layer], dst, w_sem.at[i]) for i, (src, dst) in enumerate(
        ((w_out_hbm, w_out), (w_gate_hbm, w_gate), (w_up_hbm, w_up), (w_down_hbm, w_down)))]
    for load in loads:
        load.start()
    width, count = late_hbm.shape
    plan, left = late_plan(width, count)
    late = [(late_hbm.at[pl.ds(start, size)], (w_gate, w_up)[buffer].at[pl.ds(0, size), pl.ds(lane, count)]) for buffer, lane, start, size in plan]
    if left:
        late.append((late_hbm.at[pl.ds(width - left, left)], late_rest))
    late_loads = [pltpu.make_async_copy(src, dst, late_sem.at[i]) for i, (src, dst) in enumerate(late)]
    net = Torus((far, near, relayed, sums, relayed2, sums2, rows), send_sem, recv_sem)
    net.barrier()
    loads[0].wait()

    def finish_with(old_ref, new_ref):
        def finish(c, q, half, total):
            value = (old_ref[c, q, half].astype(F32) + total).astype(BF16)
            new_ref[c, q, half] = value
            rows[(c, q) + net.place[q] + (half,)] = value
        return finish

    first = Stage(net, lambda c, q: a_ref[c, q], w_out, finish_with(res_ref, middle))
    second = Stage(net, lambda c, q: inner[c, q], w_down, finish_with(middle, new_res_ref))

    def hidden_of(c, stage, gain):
        for q in BOTH:
            stage.complete(c, q)
            normed(net, c, q, gain)
        return jnp.concatenate([rows_of(net, c, q) for q in BOTH], axis=0)

    def mlp(c):
        hidden = hidden_of(c, first, gain_ref)
        value = (jax.nn.silu(times_transposed(hidden, w_gate[...])) * times_transposed(hidden, w_up[...])).astype(BF16)
        inner[c] = value.reshape(inner.shape[1:])
        for q in BOTH:
            second.begin(c, q)

    def after(c):
        hidden = hidden_of(c, second, next_gain_ref)

        def product(lane, size):
            parts = [jnp.dot(hidden[:, start:start + rows_here], (w_gate, w_up)[buffer][pl.ds(0, rows_here), pl.ds(at + lane, size)], preferred_element_type=F32)
                     for buffer, at, start, rows_here in plan]
            if left:
                parts.append(jnp.dot(hidden[:, width - left:], late_rest[:, pl.ds(lane, size)], preferred_element_type=F32))
            return functools.reduce(jnp.add, parts)

        if last:
            put_statistics(product, count, *side_refs, out_ref, c)
        else:
            put_projected(product, *side_refs, out_ref, c)

    def on_both(step):
        def run(c):
            for q in BOTH:
                step(c, q)
        return run

    steps = [on_both(first.begin), *map(on_both, first.middle()), mlp, *map(on_both, second.middle()), after]
    at_mlp = steps.index(mlp)

    @pl.loop(0, len(steps) + chunks - 1)
    def _(slot):
        @pl.when(slot == at_mlp)
        def _():
            for load in loads[1:]:
                load.wait()

        @pl.when(slot == len(steps) - 1)
        def _():
            for load in late_loads:
                load.wait()

        for k, step in reversed(list(enumerate(steps))):
            @pl.when(slot >= k)
            def _():
                @pl.when(slot < k + chunks)
                def _():
                    step(slot - k)

        @pl.when(slot == at_mlp + chunks - 1)
        def _():
            for load in late_loads:
                load.start()


def mega(a, res, gain, next_gain, sides, w_out, w_gate_t, w_up_t, w_down, late, layer, collective_id):
    chunks, _, rows, depth = a.shape
    _, hidden, width = w_gate_t.shape
    per = (chunks, PAIR)
    tile = (rows, LANES)
    last = len(sides) == 1
    count = late.shape[1]
    _, left = late_plan(width, count)

    def by_color(g):
        grid = g.reshape(RING, RING, PAIR, LANES)
        return jnp.stack([jnp.swapaxes(grid, 0, 1), grid]).reshape(PAIR, PAIR * SHARDS, LANES)

    sem = DMA(per + (PAIR, len(KINDS)))
    out = jax.ShapeDtypeStruct((chunks, PAIR * rows, LANES if last else count), F32 if last else BF16)
    return pl.pallas_call(
        functools.partial(mega_kernel, chunks, layer, last),
        out_shape=(out, jax.ShapeDtypeStruct(per + (PAIR,) + tile, BF16)),
        in_specs=[VMEM] * (4 + len(sides)) + [ANY] * 5,
        out_specs=(VMEM, VMEM),
        scratch_shapes=[
            pltpu.VMEM((depth, width), BF16),
            *[pltpu.VMEM((hidden, width), BF16) for _ in range(3)],
            pltpu.VMEM((left or 8, count), BF16),
            pltpu.VMEM(per + (rows, hidden), BF16),
            pltpu.VMEM(per + (PAIR,) + tile, BF16),
            pltpu.VMEM(per + (RING, PAIR) + tile, F32),
            pltpu.VMEM(per + (PAIR, PAIR, PAIR) + tile, F32),
            pltpu.VMEM(per + (PAIR, PAIR, PAIR) + tile, F32),
            pltpu.VMEM(per + (PAIR, RING, PAIR) + tile, F32),
            pltpu.VMEM(per + (PAIR,) + tile, F32),
            pltpu.VMEM(per + (PAIR, PAIR) + tile, F32),
            pltpu.VMEM(per + (RING, RING, PAIR) + tile, BF16),
            DMA((RING,)), DMA((SHARDS,)), sem, sem,
        ],
        compiler_params=pltpu.CompilerParams(collective_id=collective_id, has_side_effects=True, vmem_limit_bytes=VMEM_BYTES),
        name=f"mega{collective_id}",
    )(a, res, by_color(gain), by_color(next_gain), *sides, w_out, w_gate_t, w_up_t, w_down, late)


PEERS = 8
TILE = 128
Q_TILE = 256
LOG2E = 1.4426950408889634
HELD = pltpu.VMEM((PEERS, PAIR, TILE, COLUMNS), BF16)
GATHER_SEMS = [DMA((PAIR, 3)), DMA((PAIR, 3)), DMA((RING,)), DMA((RING,))]


class Exchange:
    def __init__(self):
        self.me = lax.axis_index("resp")
        self.others = [(self.me + k) % PEERS for k in range(1, PEERS)]

    def barrier(self):
        sem = pltpu.get_barrier_semaphore()
        for device in self.others:
            pl.semaphore_signal(sem, inc=1, device_id={"resp": device}, device_id_type=MESH)
        pl.semaphore_wait(sem, PEERS - 1)

    def copy(self, src, dst, send_sem, recv_sem, device):
        return pltpu.make_async_remote_copy(src_ref=src, dst_ref=dst, send_sem=send_sem, recv_sem=recv_sem,
                                            device_id={"resp": device}, device_id_type=MESH)

    def scatter(self, src_of, dst, send_sem, recv_sem):
        for device in self.others:
            self.copy(src_of(device), dst, send_sem.at[device], recv_sem.at[self.me], device).start()

    def collected(self, dst_of, recv_sem):
        for device in self.others:
            self.copy(dst_of(device), dst_of(device), recv_sem.at[device], recv_sem.at[device], device).wait_recv()

    def sent(self, src_of, send_sem, recv_sem):
        for device in self.others:
            self.copy(src_of(device), src_of(device), send_sem.at[device], recv_sem.at[device], device).wait_send()


class PromptGather:
    def __init__(self, net, held, ring_send, ring_recv, near_send, near_recv):
        self.net, self.held = net, held
        self.ring_sems, self.near_sems = (ring_send, ring_recv), (near_send, near_recv)
        x, core = net.me // PAIR, net.me % PAIR
        self.at = lambda by, here: (x + by + RING) % RING * PAIR + (core if here else 1 - core)

    def ring_copy(self, d, kind, ref):
        return self.net.copy(ref, ref, self.ring_sems[0].at[d, kind], self.ring_sems[1].at[d, kind], self.at(1 - PAIR * d, True))

    def near_copy(self, kind, ref):
        return self.net.copy(ref, ref, self.near_sems[0].at[kind], self.near_sems[1].at[kind], self.at(0, False))

    def sources(self, here):
        return [self.at(by, here) for by in (0, -1, 1, PAIR)]

    def start(self):
        own = self.held.at[self.net.me]
        for kind in BOTH:
            for d in BOTH:
                self.ring_copy(d, kind, own.at[1 - d if kind else d]).start()
        self.near_copy(0, own).start()

    def relay(self):
        for d in BOTH:
            ref = self.held.at[self.at(PAIR * d - 1, True), d]
            self.ring_copy(d, 0, ref).wait_recv()
            self.ring_copy(d, PAIR, ref).start()

    def share(self):
        for d in BOTH:
            device = self.at(PAIR * d - 1, True)
            self.ring_copy(d, 1, self.held.at[device, 1 - d]).wait_recv()
            self.near_copy(1 + d, self.held.at[device]).start()
        far = self.held.at[self.at(PAIR, True)]
        for d in BOTH:
            self.ring_copy(d, PAIR, far.at[d]).wait_recv()
        self.near_copy(3, far).start()

    def collect(self):
        for kind, device in enumerate(self.sources(False)):
            self.near_copy(kind, self.held.at[device]).wait_recv()

    def finish(self):
        for kind in range(3):
            for d in BOTH:
                self.ring_copy(d, kind, self.held.at[self.net.me, d]).wait_send()
        for kind in range(RING):
            self.near_copy(kind, self.held.at[self.net.me]).wait_send()


def deal(rows):
    out = lax.broadcasted_iota(jnp.int32, (rows, rows), 0)
    src = lax.broadcasted_iota(jnp.int32, (rows, rows), 1)
    per = rows // PEERS
    return jnp.where(src == (out % per) * PEERS + out // per, 1.0, 0.0).astype(BF16)


def undeal(rows):
    out = lax.broadcasted_iota(jnp.int32, (rows, rows), 0)
    src = lax.broadcasted_iota(jnp.int32, (rows, rows), 1)
    per = rows // PEERS
    return jnp.where(src == (out % PEERS) * per + out // PEERS, 1.0, 0.0).astype(BF16)


def norm_tile(x_ref, out_ref, gain_ref):
    for i in range(x_ref.shape[0] // 16):
        v = x_ref[pl.ds(16 * i, 16), :].astype(F32)
        inv = lax.rsqrt(jnp.mean(v * v, axis=-1, keepdims=True) + EPS)
        out_ref[pl.ds(16 * i, 16), :] = (v * inv * gain_ref[...]).astype(BF16)


def softmax_mix(q, pieces):
    factor = LOG2E * 128 ** -0.5
    outs = []
    for h in range(2):
        lanes = slice(128 * h, 128 * h + 128)
        scores = []
        for keys, _, mask in pieces:
            s = lax.dot_general(q[:, lanes], keys[:, lanes], (((1,), (1,)), ((), ())), preferred_element_type=F32)
            scores.append(s if mask is None else jnp.where(mask, s, -jnp.inf))
        top = functools.reduce(jnp.maximum, [jnp.max(s, axis=-1, keepdims=True) for s in scores])
        probs = [jnp.exp2((s - top) * factor) for s in scores]
        total = functools.reduce(jnp.add, [jnp.sum(p, axis=-1, keepdims=True) for p in probs])
        mixed = functools.reduce(jnp.add, [jnp.dot(p.astype(BF16), values[:, lanes], preferred_element_type=F32) for p, (_, values, _) in zip(probs, pieces)])
        outs.append(mixed / total)
    return jnp.concatenate(outs, axis=1).astype(BF16)


def prompt_rows_of(held, which):
    return held[:, which].reshape(PEERS * TILE, COLUMNS)


def attend_response(t, q, held, k_own, v_own):
    row = lax.broadcasted_iota(jnp.int32, (Q_TILE, Q_TILE), 0)
    col = lax.broadcasted_iota(jnp.int32, (Q_TILE, Q_TILE), 1)
    pieces = [(prompt_rows_of(held, 0), prompt_rows_of(held, 1), None)]
    if t:
        pieces.append((k_own[:t * Q_TILE], v_own[:t * Q_TILE], None))
    span = slice(t * Q_TILE, (t + 1) * Q_TILE)
    pieces.append((k_own[span], v_own[span], col <= row))
    return softmax_mix(q, pieces)


def deal_mixed(net, t, mixed, stage, out, send_sem, recv_sem):
    dealt = jnp.dot(deal(Q_TILE), mixed, preferred_element_type=F32).astype(BF16)
    stage[t] = dealt.reshape(PEERS, Q_TILE // PEERS, COLUMNS)
    net.scatter(lambda d: stage.at[t, d], out.at[net.me, t], send_sem.at[t], recv_sem.at[t])
    out[net.me, t] = stage[t, net.me]


def first_attention_kernel(xp_hbm, xr_hbm, wq_hbm, wk_hbm, wv_hbm, gain_ref, cos_ref, sin_ref, info_ref,
                           mixed_out, res_out, info_out, prompt_out,
                           xs, w, even, odd, q_s, k_s, v_s, held, mixed_stage, res_stage,
                           x_sem, w_sem, ring_send, ring_recv, near_send, near_recv, mix_send, mix_recv, res_send, res_recv, info_send, info_recv):
    net = Exchange()
    prompt = PromptGather(net, held, ring_send, ring_recv, near_send, near_recv)
    me = net.me
    column = pl.multiple_of(lax.axis_index("model") * COLUMNS, COLUMNS)

    def load(t):
        src = xp_hbm if isinstance(t, int) and t == 0 else xr_hbm.at[pl.ds(pl.multiple_of((t - 1) * TILE, TILE), TILE)]
        return pltpu.make_async_copy(src, xs.at[t], x_sem.at[t])

    load(0).start()
    weights = [pltpu.make_async_copy(src, w.at[:, pl.ds(COLUMNS * i, COLUMNS)], w_sem.at[i]) for i, src in enumerate((wq_hbm, wk_hbm, wv_hbm))]
    for copy in weights:
        copy.start()
    for t in range(1, 9):
        load(t).start()
    net.barrier()
    net.scatter(lambda d: info_ref.at[d], info_out.at[me], info_send, info_recv)
    info_out[me] = info_ref[me]

    def project(t, hidden):
        span = pl.ds(pl.multiple_of(t * TILE, TILE), TILE)
        qkv = jnp.dot(hidden[...], w[...], preferred_element_type=F32)
        cos, sin = cos_ref[span], sin_ref[span]
        return span, rope(qkv[:, :COLUMNS], cos, sin).astype(BF16), rope(qkv[:, COLUMNS:512], cos, sin).astype(BF16), qkv[:, 512:].astype(BF16)

    load(0).wait()
    norm_tile(xs.at[0], even, gain_ref)
    for copy in weights:
        copy.wait()
    load(1).wait()
    span, q, k, v = project(0, even)
    norm_tile(xs.at[1], odd, gain_ref)
    q_s[span] = q
    held[me, 0] = k
    held[me, 1] = v
    prompt.start()
    spread = deal(TILE)

    def response_tile(t, here, there):
        span, q, k, v = project(t, here)
        norm_tile(xs.at[jnp.minimum(t + 1, 8)], there, gain_ref)
        q_s[span] = q
        own = pl.ds(pl.multiple_of((t - 1) * TILE, TILE), TILE)
        k_s[own] = k
        v_s[own] = v
        dealt = jnp.dot(spread, xs[t, :, pl.ds(column, COLUMNS)], preferred_element_type=F32).astype(BF16)
        res_stage[:, t - 1] = dealt.reshape(PEERS, TILE // PEERS, COLUMNS)

    @pl.loop(0, RING)
    def _(i):
        load(PAIR * i + PAIR).wait()
        response_tile(PAIR * i + 1, odd, even)

        @pl.when(i < RING - 1)
        def _():
            load(PAIR * i + 3).wait()

        response_tile(PAIR * i + PAIR, even, odd)
        pl.when(i == 1)(prompt.relay)
        pl.when(i == PAIR)(prompt.share)

    net.scatter(lambda d: res_stage.at[d], res_out.at[me], res_send, res_recv)
    res_out[me] = res_stage[me]
    prompt.collect()
    for t in range(RING):
        mixed = attend_response(t, q_s[pl.ds(TILE + t * Q_TILE, Q_TILE)], held, k_s, v_s)
        deal_mixed(net, t, mixed, mixed_stage, mixed_out, mix_send, mix_recv)
    row = lax.broadcasted_iota(jnp.int32, (TILE, PEERS * TILE), 0) + me * TILE
    col = lax.broadcasted_iota(jnp.int32, (TILE, PEERS * TILE), 1)
    prompt_out[:, :COLUMNS] = softmax_mix(q_s[pl.ds(0, TILE)], [(prompt_rows_of(held, 0), prompt_rows_of(held, 1), col <= row)])
    prompt_out[:, COLUMNS:] = xs[0, :, pl.ds(column, COLUMNS)]
    finish_exchange(net, mixed_stage, mixed_out, mix_send, mix_recv)
    net.collected(lambda d: res_out.at[d], res_recv)
    net.sent(lambda d: res_stage.at[d], res_send, res_recv)
    net.collected(lambda d: info_out.at[d], info_recv)
    net.sent(lambda d: info_ref.at[d], info_send, info_recv)
    prompt.finish()


def finish_exchange(net, stage, out, send_sem, recv_sem):
    for t in range(RING):
        net.collected(lambda d: out.at[d, t], recv_sem.at[t])
        net.sent(lambda d: stage.at[t, d], send_sem.at[t], recv_sem.at[t])


def first_attention(x_prompt, x_resp, w_query, w_key, w_value, gain, cos, sin, info, collective_id):
    rows = TILE + x_resp.shape[0]
    width = x_resp.shape[1]
    return pl.pallas_call(
        first_attention_kernel,
        out_shape=(jax.ShapeDtypeStruct((PEERS, RING, 32, COLUMNS), BF16), jax.ShapeDtypeStruct((PEERS, 8, 16, COLUMNS), BF16),
                   jax.ShapeDtypeStruct((PEERS, 8, 128), jnp.int32), jax.ShapeDtypeStruct((TILE, PAIR * COLUMNS), BF16)),
        in_specs=[ANY] * 5 + [VMEM] * 4,
        out_specs=(VMEM,) * 4,
        scratch_shapes=[
            pltpu.VMEM((9, TILE, width), BF16), pltpu.VMEM((width, 3 * COLUMNS), BF16), pltpu.VMEM((TILE, width), BF16), pltpu.VMEM((TILE, width), BF16),
            pltpu.VMEM((rows, COLUMNS), BF16), pltpu.VMEM((rows - TILE, COLUMNS), BF16), pltpu.VMEM((rows - TILE, COLUMNS), BF16),
            HELD, pltpu.VMEM((RING, PEERS, 32, COLUMNS), BF16), pltpu.VMEM((PEERS, 8, 16, COLUMNS), BF16),
            DMA((9,)), DMA((3,)), *GATHER_SEMS, DMA((RING, PEERS)), DMA((RING, PEERS)), *[DMA((PEERS,)) for _ in range(RING)],
        ],
        compiler_params=pltpu.CompilerParams(collective_id=collective_id, has_side_effects=True, vmem_limit_bytes=VMEM_BYTES),
        name="first_attention",
    )(x_prompt, x_resp, w_query, w_key, w_value, gain.reshape(1, width), cos, sin, info)


def second_attention_kernel(qkv_ref, kv_prompt_ref, mixed_out, qkv_in, k_s, v_s, held, mixed_stage,
                            ring_send, ring_recv, near_send, near_recv, qkv_send, qkv_recv, mix_send, mix_recv):
    net = Exchange()
    me = net.me
    prompt = PromptGather(net, held, ring_send, ring_recv, near_send, near_recv)
    held[me] = kv_prompt_ref[...]
    net.barrier()
    prompt.start()

    def send_rows(t):
        net.scatter(lambda d: qkv_ref.at[t, d], qkv_in.at[t, me], qkv_send.at[t], qkv_recv.at[t])
        qkv_in[t, me] = qkv_ref[t, me]

    send_rows(0)
    prompt.relay()
    prompt.share()
    for t in range(1, RING):
        send_rows(t)
    prompt.collect()
    for t in range(RING):
        net.collected(lambda d: qkv_in.at[t, d], qkv_recv.at[t])
        rows = jnp.dot(undeal(Q_TILE), qkv_in[t].reshape(Q_TILE, 3 * COLUMNS), preferred_element_type=F32).astype(BF16)
        k_s[pl.ds(t * Q_TILE, Q_TILE)] = rows[:, COLUMNS:PAIR * COLUMNS]
        v_s[pl.ds(t * Q_TILE, Q_TILE)] = rows[:, PAIR * COLUMNS:]
        mixed = attend_response(t, rows[:, :COLUMNS], held, k_s, v_s)
        deal_mixed(net, t, mixed, mixed_stage, mixed_out, mix_send, mix_recv)
    finish_exchange(net, mixed_stage, mixed_out, mix_send, mix_recv)
    for t in range(RING):
        net.sent(lambda d: qkv_ref.at[t, d], qkv_send.at[t], qkv_recv.at[t])
    prompt.finish()


def second_attention(qkv, kv_prompt, collective_id):
    rows = RING * Q_TILE
    return pl.pallas_call(
        second_attention_kernel,
        out_shape=jax.ShapeDtypeStruct((PEERS, RING, 32, COLUMNS), BF16),
        in_specs=[VMEM, VMEM],
        out_specs=VMEM,
        scratch_shapes=[
            pltpu.VMEM((RING, PEERS, 32, 3 * COLUMNS), BF16), pltpu.VMEM((rows, COLUMNS), BF16), pltpu.VMEM((rows, COLUMNS), BF16),
            HELD, pltpu.VMEM((RING, PEERS, 32, COLUMNS), BF16), *GATHER_SEMS, *[DMA((RING, PEERS)) for _ in range(RING)],
        ],
        compiler_params=pltpu.CompilerParams(collective_id=collective_id, has_side_effects=True, vmem_limit_bytes=VMEM_BYTES),
        name=f"second_attention{collective_id}",
    )(qkv, kv_prompt)


def combine_kernel(shards, stats_ref, out_ref, every, stat_send, stat_recv, row_send, row_recv):
    me, home = lax.axis_index("model"), lax.axis_index("resp")
    sem = pltpu.get_barrier_semaphore()
    models = [(me + k) % shards for k in range(1, shards)]
    homes = [(home + k) % PEERS for k in range(1, PEERS)]
    for device in models:
        pl.semaphore_signal(sem, inc=1, device_id={"model": device}, device_id_type=MESH)
    for device in homes:
        pl.semaphore_signal(sem, inc=1, device_id={"resp": device}, device_id_type=MESH)
    pl.semaphore_wait(sem, shards + PEERS - 2)

    def stat_copy(src, dst, send, recv, device):
        return pltpu.make_async_remote_copy(src_ref=src, dst_ref=dst, send_sem=send, recv_sem=recv, device_id={"model": device}, device_id_type=MESH)

    def row_copy(src, dst, send, recv, device):
        return pltpu.make_async_remote_copy(src_ref=src, dst_ref=dst, send_sem=send, recv_sem=recv, device_id={"resp": device}, device_id_type=MESH)

    for device in models:
        stat_copy(stats_ref, every.at[me], stat_send.at[device], stat_recv.at[me], device).start()
    every[me] = stats_ref[...]
    for device in models:
        stat_copy(every.at[device], every.at[device], stat_send.at[device], stat_recv.at[device], device).wait_recv()
    tops = [every[k, 0] for k in range(shards)]
    top = functools.reduce(jnp.maximum, tops)
    total = functools.reduce(jnp.add, [every[k, 1] * jnp.exp(tops[k] - top) for k in range(shards)])
    picked = functools.reduce(jnp.add, [every[k, 2] for k in range(shards)])
    out_ref[home] = picked - top - jnp.log(total)
    for device in homes:
        row_copy(out_ref.at[home], out_ref.at[home], row_send.at[device], row_recv.at[home], device).start()
    for device in homes:
        row_copy(out_ref.at[device], out_ref.at[device], row_send.at[device], row_recv.at[device], device).wait_recv()
    for device in models:
        stat_copy(stats_ref, stats_ref, stat_send.at[device], stat_recv.at[device], device).wait_send()
    for device in homes:
        row_copy(out_ref.at[home], out_ref.at[home], row_send.at[device], row_recv.at[device], device).wait_send()


def combine(stats, shards, collective_id):
    return pl.pallas_call(
        functools.partial(combine_kernel, shards),
        out_shape=jax.ShapeDtypeStruct((PEERS, 8, 128), F32),
        in_specs=[VMEM],
        out_specs=VMEM,
        scratch_shapes=[pltpu.VMEM((shards, 3, 8, 128), F32), DMA((shards,)), DMA((shards,)), DMA((PEERS,)), DMA((PEERS,))],
        compiler_params=pltpu.CompilerParams(collective_id=collective_id, has_side_effects=True),
        name=f"combine{collective_id}",
    )(stats)


ROPE_BASE = 10000.0
VARIANTS = (768, 1024)
CHUNKS = 4


def rope_tables(positions):
    half = LANES // PAIR
    frequency = ROPE_BASE ** (-jnp.arange(half, dtype=F32) / half)
    angles = positions.astype(F32)[:, None] * frequency
    cos, sin = jnp.cos(angles), jnp.sin(angles)
    return jnp.concatenate([cos, cos], axis=1), jnp.concatenate([-sin, sin], axis=1)


def by_chunk(rows):
    return rows.reshape(CHUNKS, PAIR, rows.shape[0] // (CHUNKS * PAIR), rows.shape[1])


def side(rows):
    return rows.reshape(CHUNKS, -1, LANES)


def to_blocks(rows):
    grid = by_chunk(rows)
    return jnp.swapaxes(grid.reshape(grid.shape[:3] + (PAIR, LANES)), 2, 3)


def from_blocks(blocks):
    return jnp.swapaxes(blocks, 2, 3).reshape(-1, COLUMNS)


def solution(mesh):
    groups = mesh.shape['resp']
    shards = mesh.shape['model']
    row_axes = ('prompts', 'resp')
    head_spec = P(None, None, 'model', None)
    in_specs = (P(row_axes, None), P(row_axes, None, None), P(row_axes, None), P(row_axes), P(None, None), head_spec, head_spec, head_spec, P(None, 'model', None, None), P(None, None), P(None, None, 'model'), P(None, None, 'model'), P(None, 'model', None), P(None), P(None, 'model'))

    def device_step(x_prompt, x_resp, targets, resp_lens, attn_gain, w_query, w_key, w_value, w_out, mlp_gain, w_gate, w_up, w_down, final_gain, w_vocab):
        prompt_rows = x_prompt.shape[0]
        resp_len, width = x_resp.shape[1:]
        prompt_len = prompt_rows * groups
        me = lax.axis_index('model')
        home = lax.axis_index('resp')
        per = resp_len // groups
        gate_t, up_t = jnp.swapaxes(w_gate, 1, 2), jnp.swapaxes(w_up, 1, 2)
        out_flat = w_out.reshape(w_out.shape[0], COLUMNS, width)
        flat = lambda w, layer: w[layer].reshape(width, COLUMNS)
        project_next = jnp.concatenate([flat(w, 1) for w in (w_query, w_key, w_value)], axis=1)
        prompt_pos = home * prompt_rows + jnp.arange(prompt_rows)

        cos, sin = rope_tables(jnp.concatenate([prompt_pos, prompt_len + jnp.arange(resp_len)]))
        info = jnp.concatenate([
            targets[0].reshape(per, groups).T[:, None, :],
            jnp.broadcast_to(resp_lens[0], (groups, groups - 1, per)).astype(jnp.int32)], axis=1)
        mixed, res, infos, prompt = first_attention(
            x_prompt, x_resp[0], flat(w_query, 0), flat(w_key, 0), flat(w_value, 0), attn_gain[0], cos, sin, info, 0)
        lens = infos[:, 1, 0]
        need = (lens + groups - 1) // groups
        ends = jnp.sum(jnp.where(jnp.arange(groups)[:, None] >= jnp.arange(groups), need, 0), axis=1)
        starts = ends - need
        dealt = groups * per

        def finish_with(size, ident):
            def run(operands):
                mixed, res, prompt = operands
                slot = jnp.arange(size)
                which = jnp.sum((slot[:, None] >= ends).astype(jnp.int32), axis=1)
                row = slot - jnp.sum(jnp.where(which[:, None] == jnp.arange(groups), starts, 0), axis=1)
                real = slot < ends[-1]
                chosen = jnp.where(real, which * per + row, -1)[:, None] == jnp.arange(dealt)
                pick = chosen.astype(BF16)

                def pack(rows):
                    return jnp.dot(pick, rows, preferred_element_type=F32).astype(BF16)

                kept = pack(jnp.concatenate([mixed.reshape(dealt, COLUMNS), res.reshape(dealt, COLUMNS)], axis=1))
                rows = jnp.concatenate([prompt, kept], axis=0)
                tables = rope_tables(jnp.concatenate([prompt_pos, prompt_len + groups * row + home]))
                qkv, new_res = mega(
                    by_chunk(rows[:, :COLUMNS]), to_blocks(rows[:, COLUMNS:]), mlp_gain[0], attn_gain[1], [side(t) for t in tables],
                    out_flat, gate_t, up_t, w_down, project_next, 0, ident)
                qkv = qkv.reshape(prompt_rows + size, 3 * COLUMNS)
                part = per // RING
                back = jnp.where(real, (row // part) * (groups * part) + which * part + row % part, -1)
                place = (jnp.arange(dealt)[:, None] == back).astype(BF16)
                home_rows = jnp.dot(place, qkv[prompt_rows:], preferred_element_type=F32).astype(BF16)
                kv_prompt = jnp.stack([qkv[:prompt_rows, COLUMNS:PAIR * COLUMNS], qkv[:prompt_rows, PAIR * COLUMNS:]])
                mixed = second_attention(home_rows.reshape(RING, groups, part, 3 * COLUMNS), kv_prompt, ident + 1)
                wanted = jnp.sum(jnp.where(chosen, infos[:, 0, :].reshape(dealt), 0), axis=1) - me * w_vocab.shape[1]
                stats, _ = mega(
                    by_chunk(pack(mixed.reshape(dealt, COLUMNS))), to_blocks(from_blocks(new_res)[prompt_rows:]), mlp_gain[1], final_gain,
                    [side(jnp.broadcast_to(wanted[:, None], (size, LANES)))], out_flat, gate_t, up_t, w_down, w_vocab, 1, ident + PAIR)
                stats = jnp.pad(stats.reshape(size, LANES)[:, :3].T, ((0, 0), (0, dealt - size)))
                found = combine(stats.reshape(3, groups, per), shards, ident + 3).reshape(groups, dealt)
                start = jnp.sum(jnp.where(jnp.arange(groups) == home, starts, 0))
                mine = lax.dynamic_slice(jnp.pad(found, ((0, 0), (0, per))), (0, start), (groups, per))
                return mine.T.reshape(resp_len)
            return run

        index = sum((ends[-1] > size).astype(jnp.int32) for size in VARIANTS[:-1])
        log_probs = lax.switch(index, [finish_with(size, 1 + RING * i) for i, size in enumerate(VARIANTS)], (mixed, res, prompt))
        log_probs = jnp.where(jnp.arange(resp_len) < resp_lens[0], log_probs, 0.0)
        return log_probs[None, :]

    return jax.shard_map(device_step, mesh=mesh, in_specs=in_specs, out_specs=P(row_axes, None), check_vma=False)
```

```python
import functools

import jax
import jax.numpy as jnp
from jax import lax
from jax.experimental import pallas as pl
from jax.experimental.pallas import tpu as pltpu
from jax.sharding import PartitionSpec as P

MESH = pl.DeviceIdType.MESH
F32 = jnp.float32
BF16 = jnp.bfloat16
EPS = 1e-6
LANES = 128
PAIR = 2
RING = 4
COLUMNS = PAIR * LANES
SHARDS = RING * RING
PEERS = 8
BOTH = range(PAIR)
VMEM_BYTES = 67_000_000
LATE_ROWS = 640
LOGITS = 512
VMEM = pl.BlockSpec(memory_space=pltpu.VMEM)
ANY = pl.BlockSpec(memory_space=pl.ANY)
DMA = pltpu.SemaphoreType.DMA
KINDS = range(RING * 3)
SUM_FAR, SUM_NEAR, SUM_RELAY, SUM2_FAR, SUM2_NEAR, SUM2_RELAY, TAKE_OWN, TAKE_REST, TAKE_RELAY, TAKE2_OWN, TAKE2_REST, TAKE2_RELAY = KINDS


def block_of(color, first, second):
    return RING * first + second if color else RING * second + first


def pair(index):
    return pl.ds(PAIR * index, PAIR)


class Torus:
    def __init__(self, refs, send_sem, recv_sem):
        self.refs = refs
        self.far, self.near, self.relayed, self.sums, self.relayed2, self.sums2, self.rows = refs
        self.send_sem, self.recv_sem = send_sem, recv_sem
        me = lax.axis_index("model")
        z, y = me // RING, me % RING
        self.place = ((y, z), (z, y))
        along_y = [z * RING + self.step(y, way) for way in (1, -1)]
        along_z = [self.step(z, way) * RING + y for way in (1, -1)]
        self.neighbors = ((along_y, along_z), (along_z, along_y))

    def step(self, place, by):
        return (place + by + RING) % RING

    def barrier(self):
        sem = pltpu.get_barrier_semaphore()
        for ring in self.neighbors[0]:
            for device in ring:
                pl.semaphore_signal(sem, device_id={"model": device}, device_id_type=MESH)
        pl.semaphore_wait(sem, RING)

    def ends(self, kind, c, q, d):
        (p, s), way, other = self.place[q], 1 - PAIR * d, 1 - d
        far, near, relayed, sums, relayed2, sums2, rows = (ref.at[c, q] for ref in self.refs)
        own = sums.at[0]
        back_s, back_p = self.step(s, -way), self.step(p, -way)
        return {
            SUM_FAR: lambda: (far.at[pair(d)], relayed.at[d], relayed.at[d]),
            SUM_NEAR: lambda: (near.at[d], sums.at[d, pair(other)], sums.at[d, pair(other)]),
            SUM_RELAY: lambda: (relayed.at[d], sums.at[d, pair(d)], sums.at[d, pair(d)]),
            SUM2_FAR: lambda: (own.at[self.step(s, PAIR), d], relayed2.at[d], relayed2.at[d]),
            SUM2_NEAR: lambda: (own.at[self.step(s, way), other], sums2.at[d, other], sums2.at[d, other]),
            SUM2_RELAY: lambda: (relayed2.at[d], sums2.at[d, d], sums2.at[d, d]),
            TAKE_OWN: lambda: (rows.at[p, s, d], rows.at[p, s, d], rows.at[p, back_s, d]),
            TAKE_REST: lambda: (rows.at[p, s, other], rows.at[p, s, other], rows.at[p, back_s, other]),
            TAKE_RELAY: lambda: (rows.at[p, back_s, d], rows.at[p, back_s, d], rows.at[p, self.step(s, PAIR), d]),
            TAKE2_OWN: lambda: (rows.at[p, pair(d)], rows.at[p, pair(d)], rows.at[back_p, pair(d)]),
            TAKE2_REST: lambda: (rows.at[p, pair(other)], rows.at[p, pair(other)], rows.at[back_p, pair(other)]),
            TAKE2_RELAY: lambda: (rows.at[back_p, pair(d)], rows.at[back_p, pair(d)], rows.at[self.step(p, PAIR), pair(d)]),
        }[kind]()

    def copy(self, kind, c, q, d, src, dst):
        second_ring = kind in (SUM2_FAR, SUM2_NEAR, SUM2_RELAY, TAKE_OWN, TAKE_REST, TAKE_RELAY)
        return pltpu.make_async_remote_copy(
            src_ref=src, dst_ref=dst, send_sem=self.send_sem.at[c, q, d, kind], recv_sem=self.recv_sem.at[c, q, d, kind],
            device_id={"model": self.neighbors[q][second_ring][d]}, device_id_type=MESH)

    def send(self, c, q, d, kind):
        src, dst, _ = self.ends(kind, c, q, d)
        self.copy(kind, c, q, d, src, dst).start()

    def sent(self, c, q, *kinds):
        for kind in kinds:
            for d in BOTH:
                src, dst, _ = self.ends(kind, c, q, d)
                self.copy(kind, c, q, d, src, dst).wait_send()

    def arrived(self, c, q, d, *kinds):
        for kind in kinds:
            _, _, here = self.ends(kind, c, q, d)
            self.copy(kind, c, q, d, here, here).wait_recv()


def halves(value):
    return value[:, :LANES], value[:, LANES:]


def store_block(ref, value):
    for half, part in enumerate(halves(value)):
        ref[half] = part


def add_block(ref, value):
    for half, part in enumerate(halves(value)):
        ref[half] += part


class Stage:
    def __init__(self, net, lhs_of, w_ref, finish):
        self.net, self.lhs_of, self.w_ref, self.finish = net, lhs_of, w_ref, finish

    def product(self, lhs, color, first, second):
        start = pl.multiple_of(block_of(color, first, second) * COLUMNS, COLUMNS)
        return jnp.dot(lhs, self.w_ref[:, pl.ds(start, COLUMNS)], preferred_element_type=F32)

    def begin(self, c, q):
        net, p, lhs = self.net, self.net.place[q][0], self.lhs_of(c, q)
        for k in range(RING):
            store_block(net.far.at[c, q, k], self.product(lhs, q, net.step(p, PAIR), k))
        for d in BOTH:
            net.send(c, q, d, SUM_FAR)
        for d in BOTH:
            for k in BOTH:
                store_block(net.near.at[c, q, d, k], self.product(lhs, q, net.step(p, 1 - PAIR * d), PAIR * (1 - d) + k))
            net.send(c, q, d, SUM_NEAR)

    def relay_sum(self, c, q):
        net, p, lhs = self.net, self.net.place[q][0], self.lhs_of(c, q)
        for d in BOTH:
            net.arrived(c, q, d, SUM_FAR)
            for k in BOTH:
                add_block(net.relayed.at[c, q, d, k], self.product(lhs, q, net.step(p, 1 - PAIR * d), PAIR * d + k))
            net.send(c, q, d, SUM_RELAY)

    def begin_second(self, c, q):
        net, lhs = self.net, self.lhs_of(c, q)
        for d in BOTH:
            net.arrived(c, q, d, SUM_NEAR, SUM_RELAY)
        for k in range(RING):
            for half, part in enumerate(halves(self.product(lhs, q, net.place[q][0], k))):
                net.sums[c, q, 0, k, half] += net.sums[c, q, 1, k, half] + part
        for kind in (SUM2_FAR, SUM2_NEAR):
            for d in BOTH:
                net.send(c, q, d, kind)
        net.sent(c, q, SUM_FAR)

    def relay_second(self, c, q):
        net = self.net
        for d in BOTH:
            net.arrived(c, q, d, SUM2_FAR)
            net.relayed2[c, q, d] += net.sums[c, q, 0, net.step(net.place[q][1], 1 - PAIR * d), d]
            net.send(c, q, d, SUM2_RELAY)

    def finish_sum(self, c, q):
        net = self.net
        net.sent(c, q, SUM_NEAR, SUM_RELAY)
        for d in BOTH:
            net.arrived(c, q, d, SUM2_NEAR, SUM2_RELAY)
        for half in BOTH:
            self.finish(c, q, half, net.sums[c, q, 0, net.place[q][1], half] + net.sums2[c, q, 0, half] + net.sums2[c, q, 1, half])
        for kind in (TAKE_OWN, TAKE_REST):
            for d in BOTH:
                net.send(c, q, d, kind)

    def relay_rows(self, c, q):
        net = self.net
        net.sent(c, q, SUM2_FAR, SUM2_NEAR, SUM2_RELAY)
        for d in BOTH:
            net.arrived(c, q, d, TAKE_OWN)
            net.send(c, q, d, TAKE_RELAY)

    def take_second(self, c, q):
        net = self.net
        for d in BOTH:
            net.arrived(c, q, d, TAKE_REST, TAKE_RELAY)
        for kind in (TAKE2_OWN, TAKE2_REST):
            for d in BOTH:
                net.send(c, q, d, kind)

    def relay_last(self, c, q):
        net = self.net
        for d in BOTH:
            net.arrived(c, q, d, TAKE2_OWN)
            net.send(c, q, d, TAKE2_RELAY)

    def complete(self, c, q):
        net = self.net
        for d in BOTH:
            net.arrived(c, q, d, TAKE2_REST, TAKE2_RELAY)
        net.sent(c, q, TAKE_OWN, TAKE_REST, TAKE_RELAY, TAKE2_OWN, TAKE2_REST, TAKE2_RELAY)

    def middle(self):
        return [self.relay_sum, self.begin_second, self.relay_second, self.finish_sum, self.relay_rows, self.take_second, self.relay_last]


def normed(net, c, q, gain_ref):
    rows = net.rows.shape[-PAIR]
    tile = PAIR * 8 if rows % (PAIR * 8) == 0 else 8
    spots = [(first, second, half) for first in range(RING) for second in range(RING) for half in BOTH]

    @pl.loop(0, rows // tile)
    def _(i):
        span = pl.ds(pl.multiple_of(i * tile, tile), tile)
        acts = [net.rows[(c, q) + spot + (span,)].astype(F32) for spot in spots]
        squares = functools.reduce(jnp.add, [v * v for v in acts])
        inv = lax.rsqrt(jnp.sum(squares, axis=-1, keepdims=True) / (LANES * len(acts)) + EPS)
        for k, (spot, v) in enumerate(zip(spots, acts)):
            net.rows[(c, q) + spot + (span,)] = (v * inv * gain_ref[q, pl.ds(k, 1)]).astype(BF16)


def rows_of(net, c, q):
    parts = []
    for upper in range(RING):
        for lower in range(RING):
            first, second = (upper, lower) if q else (lower, upper)
            parts += [net.rows[c, q, first, second, half] for half in BOTH]
    return jnp.concatenate(parts, axis=1)


def times_transposed(lhs, rhs):
    return lax.dot_general(lhs, rhs, (((1,), (1,)), ((), ())), preferred_element_type=F32)


def late_plan(width, count):
    plan, start = [], 0
    for buffer in BOTH:
        for slot in range(width // count):
            size = min(LATE_ROWS, width - start)
            if size:
                plan.append((buffer, slot * count, start, size))
            start += size
    return plan, width - start


def rope(value, cos, sin):
    return jnp.concatenate([v * cos + pltpu.roll(v, LANES // PAIR, 1) * sin for v in halves(value)], axis=1)


def put_projected(product, cos_ref, sin_ref, out_ref, c):
    for k in range(3):
        value = product(k * COLUMNS, COLUMNS)
        if k < PAIR:
            value = rope(value, cos_ref[c], sin_ref[c])
        out_ref[c, :, pl.ds(k * COLUMNS, COLUMNS)] = value.astype(BF16)


def statistics(product, count, target):
    top = total = picked = None
    for k in range(count // LOGITS):
        logits = product(k * LOGITS, LOGITS)
        here = jnp.max(logits, axis=-1, keepdims=True)
        ids = lax.broadcasted_iota(jnp.int32, logits.shape, 1) + k * LOGITS
        found = jnp.sum(jnp.where(ids == target, logits, 0.0), axis=-1, keepdims=True)
        if k:
            both = jnp.maximum(top, here)
            total = total * jnp.exp(top - both) + jnp.sum(jnp.exp(logits - both), axis=-1, keepdims=True)
            top, picked = both, picked + found
        else:
            top, total, picked = here, jnp.sum(jnp.exp(logits - here), axis=-1, keepdims=True), found
    lane = lax.broadcasted_iota(jnp.int32, (LANES, LANES), 1)
    return jnp.where(lane == 0, top, jnp.where(lane == 1, total, picked)).T[:PEERS]


def mega_kernel(chunks, layer, last, gain_ref, next_gain_ref, ids_ref, dealt_ref, old_ref, *args):
    if last:
        side_refs, args = (), args
    else:
        side_refs, args = args[:3], args[3:]
    w_out_hbm, w_gate_hbm, w_up_hbm, w_down_hbm, late_hbm, out_ref, *args = args
    if not last:
        new_res_ref, *args = args
    (w_out, w_gate, w_up, w_down, late_rest, acts, res, inner, middle,
     far, near, relayed, sums, relayed2, sums2, rows, w_sem, late_sem, send_sem, recv_sem) = args
    loads = [pltpu.make_async_copy(src.at[layer], dst, w_sem.at[i]) for i, (src, dst) in enumerate(
        ((w_out_hbm, w_out), (w_gate_hbm, w_gate), (w_up_hbm, w_up), (w_down_hbm, w_down)))]
    for load in loads:
        load.start()
    width, count = late_hbm.shape
    plan, left = late_plan(width, count)
    late = [(late_hbm.at[pl.ds(start, size)], (w_gate, w_up)[buffer].at[pl.ds(0, size), pl.ds(lane, count)]) for buffer, lane, start, size in plan]
    if left:
        late.append((late_hbm.at[pl.ds(width - left, left)], late_rest))
    late_loads = [pltpu.make_async_copy(src, dst, late_sem.at[i]) for i, (src, dst) in enumerate(late)]
    net = Torus((far, near, relayed, sums, relayed2, sums2, rows), send_sem, recv_sem)
    net.barrier()
    loads[0].wait()
    if last:
        new_res_ref = middle

    def picked(ids, ref):
        chosen = (ids == lax.broadcasted_iota(jnp.int32, (LANES, PEERS * LANES), 1)).astype(BF16)
        return jnp.dot(chosen, ref[...], preferred_element_type=F32).astype(BF16)

    def put(c, mixed, columns):
        for q in BOTH:
            span = slice(q * acts.shape[PAIR], (q + 1) * acts.shape[PAIR])
            acts[c, q] = mixed[span]
            for half, part in enumerate(halves(columns) if columns is not None else ()):
                res[c, q, half] = part[span]

    def begin(c):
        if last:
            put(c, picked(ids_ref[c, :, :1], dealt_ref), None)
        else:
            @pl.when(c == 0)
            def _():
                put(c, side_refs[PAIR][:, :COLUMNS], side_refs[PAIR][:, COLUMNS:])

            @pl.when(c > 0)
            def _():
                ids = ids_ref[c - 1, :, :1]
                put(c, picked(ids, dealt_ref), picked(ids, old_ref))
        for q in BOTH:
            first.begin(c, q)

    def finish_with(old_ref, new_ref, skip=0):
        def finish(c, q, half, total):
            value = (old_ref[c + skip, q, half].astype(F32) + total).astype(BF16)
            new_ref[c, q, half] = value
            rows[(c, q) + net.place[q] + (half,)] = value
        return finish

    first = Stage(net, lambda c, q: acts[c, q], w_out, finish_with(old_ref if last else res, middle, last))
    second = Stage(net, lambda c, q: inner[c, q], w_down, finish_with(middle, new_res_ref))

    def hidden_of(c, stage, gain):
        for q in BOTH:
            stage.complete(c, q)
            normed(net, c, q, gain)
        return jnp.concatenate([rows_of(net, c, q) for q in BOTH], axis=0)

    def mlp(c):
        hidden = hidden_of(c, first, gain_ref)
        value = (jax.nn.silu(times_transposed(hidden, w_gate[...])) * times_transposed(hidden, w_up[...])).astype(BF16)
        inner[c] = value.reshape(inner.shape[1:])
        for q in BOTH:
            second.begin(c, q)

    def after(c):
        hidden = hidden_of(c, second, next_gain_ref)

        def product(lane, size):
            parts = [jnp.dot(hidden[:, start:start + rows_here], (w_gate, w_up)[buffer][pl.ds(0, rows_here), pl.ds(at + lane, size)], preferred_element_type=F32)
                     for buffer, at, start, rows_here in plan]
            if left:
                parts.append(jnp.dot(hidden[:, width - left:], late_rest[:, pl.ds(lane, size)], preferred_element_type=F32))
            return functools.reduce(jnp.add, parts)

        if last:
            out_ref[c] = statistics(product, count, ids_ref[c, :, 1:PAIR])
        else:
            put_projected(product, *side_refs[:PAIR], out_ref, c)

    def on_both(step):
        def run(c):
            for q in BOTH:
                step(c, q)
        return run

    steps = [begin, *map(on_both, first.middle()), mlp, *map(on_both, second.middle())]
    at_mlp = steps.index(mlp)
    steps += [None] * max(0, at_mlp + chunks - len(steps)) + [after]

    @pl.loop(0, len(steps) + chunks - 1)
    def _(slot):
        @pl.when(slot == at_mlp)
        def _():
            for load in loads[1:]:
                load.wait()

        @pl.when(slot == len(steps) - 1)
        def _():
            for load in late_loads:
                load.wait()

        for k, step in reversed(list(enumerate(steps))):
            if step is None:
                continue

            @pl.when(slot >= k)
            def _():
                @pl.when(slot < k + chunks)
                def _():
                    step(slot - k)

        @pl.when(slot == at_mlp + chunks - 1)
        def _():
            for load in late_loads:
                load.start()


def mega(gain, next_gain, ids, dealt, old, sides, w_out, w_gate_t, w_up_t, w_down, late, layer, collective_id):
    last = not sides
    chunks = ids.shape[0] + (not last)
    _, depth, width = w_out.shape
    hidden = w_gate_t.shape[1]
    rows = LANES // PAIR
    per = (chunks, PAIR)
    tile = (rows, LANES)
    count = late.shape[1]
    _, left = late_plan(width, count)

    def by_color(g):
        grid = g.reshape(RING, RING, PAIR, LANES)
        return jnp.stack([jnp.swapaxes(grid, 0, 1), grid]).reshape(PAIR, PAIR * SHARDS, LANES)

    sem = DMA(per + (PAIR, len(KINDS)))
    out = jax.ShapeDtypeStruct((chunks, PEERS, LANES), F32) if last else (
        jax.ShapeDtypeStruct((chunks, LANES, count), BF16), jax.ShapeDtypeStruct(per + (PAIR,) + tile, BF16))
    return pl.pallas_call(
        functools.partial(mega_kernel, chunks, layer, last),
        out_shape=out,
        in_specs=[VMEM] * (5 + len(sides)) + [ANY] * 5,
        out_specs=VMEM if last else (VMEM, VMEM),
        scratch_shapes=[
            pltpu.VMEM((depth, width), BF16),
            *[pltpu.VMEM((hidden, width), BF16) for _ in range(3)],
            pltpu.VMEM((left or 8, count), BF16),
            pltpu.VMEM(per + (rows, depth), BF16),
            pltpu.VMEM(per + (PAIR,) + (tile if not last else (8, LANES)), BF16),
            pltpu.VMEM(per + (rows, hidden), BF16),
            pltpu.VMEM(per + (PAIR,) + tile, BF16),
            pltpu.VMEM(per + (RING, PAIR) + tile, F32),
            pltpu.VMEM(per + (PAIR, PAIR, PAIR) + tile, F32),
            pltpu.VMEM(per + (PAIR, PAIR, PAIR) + tile, F32),
            pltpu.VMEM(per + (PAIR, RING, PAIR) + tile, F32),
            pltpu.VMEM(per + (PAIR,) + tile, F32),
            pltpu.VMEM(per + (PAIR, PAIR) + tile, F32),
            pltpu.VMEM(per + (RING, RING, PAIR) + tile, BF16),
            DMA((RING,)), DMA((SHARDS,)), sem, sem,
        ],
        compiler_params=pltpu.CompilerParams(collective_id=collective_id, has_side_effects=True, vmem_limit_bytes=VMEM_BYTES),
        name=f"mega{collective_id}",
    )(by_color(gain), by_color(next_gain), ids, dealt, old, *sides, w_out, w_gate_t, w_up_t, w_down, late)


TILE = 128
Q_TILE = 256
LOG2E = 1.4426950408889634
HELD = pltpu.VMEM((PEERS, PAIR, TILE, COLUMNS), BF16)
GATHER_SEMS = [DMA((PAIR, 3)), DMA((PAIR, 3)), DMA((RING,)), DMA((RING,))]


class Exchange:
    def __init__(self):
        self.me = lax.axis_index("resp")
        self.others = [(self.me + k) % PEERS for k in range(1, PEERS)]

    def barrier(self):
        sem = pltpu.get_barrier_semaphore()
        for device in self.others:
            pl.semaphore_signal(sem, inc=1, device_id={"resp": device}, device_id_type=MESH)
        pl.semaphore_wait(sem, PEERS - 1)

    def copy(self, src, dst, send_sem, recv_sem, device):
        return pltpu.make_async_remote_copy(src_ref=src, dst_ref=dst, send_sem=send_sem, recv_sem=recv_sem,
                                            device_id={"resp": device}, device_id_type=MESH)

    def scatter(self, src_of, dst, send_sem, recv_sem):
        for device in self.others:
            self.copy(src_of(device), dst, send_sem.at[device], recv_sem.at[self.me], device).start()

    def collected(self, dst_of, recv_sem):
        for device in self.others:
            self.copy(dst_of(device), dst_of(device), recv_sem.at[device], recv_sem.at[device], device).wait_recv()

    def sent(self, src_of, send_sem, recv_sem):
        for device in self.others:
            self.copy(src_of(device), src_of(device), send_sem.at[device], recv_sem.at[device], device).wait_send()


def router_scratch(tiles, unit):
    return [pltpu.VMEM((tiles, PAIR) + unit, BF16), DMA((tiles, PEERS)), DMA((tiles, PEERS)), DMA((tiles, PAIR)), DMA((tiles, PAIR))]


class Router:
    def __init__(self, net, tiles, src_of, dst_of, scratch):
        self.net, self.tiles, self.src_of, self.dst_of = net, tiles, src_of, dst_of
        self.held, self.send_sem, self.recv_sem, self.relay_send, self.relay_recv = scratch
        x, self.core = net.me // PAIR, net.me % PAIR
        self.at = lambda by, core: (x + by + RING) % RING * PAIR + core
        self.way = 1 - PAIR * self.core
        self.close = [self.at(0, 1 - self.core)] + [self.at(by, core) for core in BOTH for by in (1, -1)]
        self.distant = [self.at(PAIR, core) for core in BOTH]

    def send(self, t):
        for device in self.close:
            self.net.copy(self.src_of(t, device), self.dst_of(t, self.net.me), self.send_sem.at[t, device], self.recv_sem.at[t, self.net.me], device).start()
        for core, device in enumerate(self.distant):
            self.net.copy(self.src_of(t, device), self.held.at[t, self.core], self.send_sem.at[t, device], self.relay_recv.at[t, self.core], self.at(1 - PAIR * core, core)).start()

    def relay_copy(self, t, core):
        source = self.at(-self.way, core)
        ref = self.held.at[t, core]
        return self.net.copy(ref, self.dst_of(t, source), self.relay_send.at[t, core], self.recv_sem.at[t, source], self.at(self.way, self.core))

    def relay(self, t):
        for core in BOTH:
            ref = self.held.at[t, core]
            self.net.copy(ref, ref, self.relay_send.at[t, core], self.relay_recv.at[t, core], self.net.me).wait_recv()
            self.relay_copy(t, core).start()

    def collect(self, t):
        for device in self.close + self.distant:
            ref = self.dst_of(t, device)
            self.net.copy(ref, ref, self.send_sem.at[t, device], self.recv_sem.at[t, device], device).wait_recv()

    def finish(self):
        for t in range(self.tiles):
            for device in self.close + self.distant:
                ref = self.src_of(t, device)
                self.net.copy(ref, ref, self.send_sem.at[t, device], self.recv_sem.at[t, device], device).wait_send()
            for core in BOTH:
                self.relay_copy(t, core).wait_send()


class PromptGather:
    def __init__(self, net, held, ring_send, ring_recv, near_send, near_recv):
        self.net, self.held = net, held
        self.ring_sems, self.near_sems = (ring_send, ring_recv), (near_send, near_recv)
        x, core = net.me // PAIR, net.me % PAIR
        self.at = lambda by, here: (x + by + RING) % RING * PAIR + (core if here else 1 - core)

    def ring_copy(self, d, kind, ref):
        return self.net.copy(ref, ref, self.ring_sems[0].at[d, kind], self.ring_sems[1].at[d, kind], self.at(1 - PAIR * d, True))

    def near_copy(self, kind, ref):
        return self.net.copy(ref, ref, self.near_sems[0].at[kind], self.near_sems[1].at[kind], self.at(0, False))

    def sources(self, here):
        return [self.at(by, here) for by in (0, -1, 1, PAIR)]

    def start(self):
        own = self.held.at[self.net.me]
        for kind in BOTH:
            for d in BOTH:
                self.ring_copy(d, kind, own.at[1 - d if kind else d]).start()
        self.near_copy(0, own).start()

    def relay(self):
        for d in BOTH:
            ref = self.held.at[self.at(PAIR * d - 1, True), d]
            self.ring_copy(d, 0, ref).wait_recv()
            self.ring_copy(d, PAIR, ref).start()

    def share(self):
        for d in BOTH:
            device = self.at(PAIR * d - 1, True)
            self.ring_copy(d, 1, self.held.at[device, 1 - d]).wait_recv()
            self.near_copy(1 + d, self.held.at[device]).start()
        far = self.held.at[self.at(PAIR, True)]
        for d in BOTH:
            self.ring_copy(d, PAIR, far.at[d]).wait_recv()
        self.near_copy(3, far).start()

    def collect(self):
        for kind, device in enumerate(self.sources(False)):
            self.near_copy(kind, self.held.at[device]).wait_recv()

    def finish(self):
        for kind in range(3):
            for d in BOTH:
                self.ring_copy(d, kind, self.held.at[self.net.me, d]).wait_send()
        for kind in range(RING):
            self.near_copy(kind, self.held.at[self.net.me]).wait_send()


def deal(rows):
    out = lax.broadcasted_iota(jnp.int32, (rows, rows), 0)
    src = lax.broadcasted_iota(jnp.int32, (rows, rows), 1)
    per = rows // PEERS
    return jnp.where(src == (out % per) * PEERS + out // per, 1.0, 0.0).astype(BF16)


def undeal(rows):
    out = lax.broadcasted_iota(jnp.int32, (rows, rows), 0)
    src = lax.broadcasted_iota(jnp.int32, (rows, rows), 1)
    per = rows // PEERS
    return jnp.where(src == (out % PEERS) * per + out // PEERS, 1.0, 0.0).astype(BF16)


def norm_tile(x_ref, out_ref, gain_ref):
    for i in range(x_ref.shape[0] // 16):
        v = x_ref[pl.ds(16 * i, 16), :].astype(F32)
        inv = lax.rsqrt(jnp.mean(v * v, axis=-1, keepdims=True) + EPS)
        out_ref[pl.ds(16 * i, 16), :] = (v * inv * gain_ref[...]).astype(BF16)


def softmax_mix(q, pieces):
    factor = LOG2E * 128 ** -0.5
    outs = []
    for h in range(2):
        lanes = slice(128 * h, 128 * h + 128)
        scores = []
        for keys, _, mask in pieces:
            s = lax.dot_general(q[:, lanes], keys[:, lanes], (((1,), (1,)), ((), ())), preferred_element_type=F32)
            scores.append(s if mask is None else jnp.where(mask, s, -jnp.inf))
        top = functools.reduce(jnp.maximum, [jnp.max(s, axis=-1, keepdims=True) for s in scores])
        probs = [jnp.exp2((s - top) * factor) for s in scores]
        total = functools.reduce(jnp.add, [jnp.sum(p, axis=-1, keepdims=True) for p in probs])
        mixed = functools.reduce(jnp.add, [jnp.dot(p.astype(BF16), values[:, lanes], preferred_element_type=F32) for p, (_, values, _) in zip(probs, pieces)])
        outs.append(mixed / total)
    return jnp.concatenate(outs, axis=1).astype(BF16)


def prompt_rows_of(held, which):
    return held[:, which].reshape(PEERS * TILE, COLUMNS)


def attend_response(t, q, held, k_own, v_own):
    row = lax.broadcasted_iota(jnp.int32, (Q_TILE, Q_TILE), 0)
    col = lax.broadcasted_iota(jnp.int32, (Q_TILE, Q_TILE), 1)
    pieces = [(prompt_rows_of(held, 0), prompt_rows_of(held, 1), None)]
    if t:
        pieces.append((k_own[:t * Q_TILE], v_own[:t * Q_TILE], None))
    span = slice(t * Q_TILE, (t + 1) * Q_TILE)
    pieces.append((k_own[span], v_own[span], col <= row))
    return softmax_mix(q, pieces)


def deal_mixed(router, t, mixed, stage, out):
    dealt = jnp.dot(deal(Q_TILE), mixed, preferred_element_type=F32).astype(BF16)
    stage[t] = dealt.reshape(PEERS, Q_TILE // PEERS, COLUMNS)
    router.send(t)
    out[router.net.me, t] = stage[t, router.net.me]
    if t:
        router.relay(t - 1)


def collect_mixed(router):
    router.relay(router.tiles - 1)
    for t in range(router.tiles):
        router.collect(t)


def first_attention_kernel(xp_hbm, xr_hbm, wq_hbm, wk_hbm, wv_hbm, gain_ref, cos_ref, sin_ref, info_ref,
                           mixed_out, res_out, info_out, prompt_out,
                           xs, w, even, odd, q_s, k_s, v_s, held, mixed_stage, res_stage,
                           x_sem, w_sem, ring_send, ring_recv, near_send, near_recv, info_send, info_recv, *routes):
    net = Exchange()
    mixed_router = Router(net, RING, lambda t, d: mixed_stage.at[t, d], lambda t, d: mixed_out.at[d, t], routes[:5])
    res_router = Router(net, 1, lambda t, d: res_stage.at[d], lambda t, d: res_out.at[d], routes[5:])
    prompt = PromptGather(net, held, ring_send, ring_recv, near_send, near_recv)
    me = net.me
    column = pl.multiple_of(lax.axis_index("model") * COLUMNS, COLUMNS)

    def load(t):
        src = xp_hbm if isinstance(t, int) and t == 0 else xr_hbm.at[pl.ds(pl.multiple_of((t - 1) * TILE, TILE), TILE)]
        return pltpu.make_async_copy(src, xs.at[t], x_sem.at[t])

    load(0).start()
    weights = [pltpu.make_async_copy(src, w.at[:, pl.ds(COLUMNS * i, COLUMNS)], w_sem.at[i]) for i, src in enumerate((wq_hbm, wk_hbm, wv_hbm))]
    for copy in weights:
        copy.start()
    for t in range(1, 9):
        load(t).start()
    net.barrier()
    net.scatter(lambda d: info_ref.at[d], info_out.at[me], info_send, info_recv)
    info_out[me] = info_ref[me]

    def project(t, hidden):
        span = pl.ds(pl.multiple_of(t * TILE, TILE), TILE)
        qkv = jnp.dot(hidden[...], w[...], preferred_element_type=F32)
        cos, sin = cos_ref[span], sin_ref[span]
        return span, rope(qkv[:, :COLUMNS], cos, sin).astype(BF16), rope(qkv[:, COLUMNS:512], cos, sin).astype(BF16), qkv[:, 512:].astype(BF16)

    load(0).wait()
    norm_tile(xs.at[0], even, gain_ref)
    for t in range(1, 9):
        load(t).wait()
    spread = deal(TILE)

    @pl.loop(1, 9)
    def _(t):
        dealt = jnp.dot(spread, xs[t, :, pl.ds(column, COLUMNS)], preferred_element_type=F32).astype(BF16)
        res_stage[:, t - 1] = dealt.reshape(PEERS, TILE // PEERS, COLUMNS)

    res_router.send(0)
    res_out[me] = res_stage[me]
    for copy in weights:
        copy.wait()
    span, q, k, v = project(0, even)
    norm_tile(xs.at[1], odd, gain_ref)
    q_s[span] = q
    held[me, 0] = k
    held[me, 1] = v
    prompt.start()

    def response_tile(t, here, there):
        span, q, k, v = project(t, here)
        norm_tile(xs.at[jnp.minimum(t + 1, 8)], there, gain_ref)
        q_s[span] = q
        own = pl.ds(pl.multiple_of((t - 1) * TILE, TILE), TILE)
        k_s[own] = k
        v_s[own] = v

    @pl.loop(0, RING)
    def _(i):
        response_tile(PAIR * i + 1, odd, even)
        response_tile(PAIR * i + PAIR, even, odd)
        pl.when(i == 0)(prompt.relay)
        pl.when(i == 1)(prompt.share)
        pl.when(i == PAIR)(lambda: res_router.relay(0))

    prompt.collect()
    for t in range(RING):
        mixed = attend_response(t, q_s[pl.ds(TILE + t * Q_TILE, Q_TILE)], held, k_s, v_s)
        deal_mixed(mixed_router, t, mixed, mixed_stage, mixed_out)
    row = lax.broadcasted_iota(jnp.int32, (TILE, PEERS * TILE), 0) + me * TILE
    col = lax.broadcasted_iota(jnp.int32, (TILE, PEERS * TILE), 1)
    prompt_out[:, :COLUMNS] = softmax_mix(q_s[pl.ds(0, TILE)], [(prompt_rows_of(held, 0), prompt_rows_of(held, 1), col <= row)])
    prompt_out[:, COLUMNS:] = xs[0, :, pl.ds(column, COLUMNS)]
    collect_mixed(mixed_router)
    res_router.collect(0)
    for router in (mixed_router, res_router):
        router.finish()
    net.collected(lambda d: info_out.at[d], info_recv)
    net.sent(lambda d: info_ref.at[d], info_send, info_recv)
    prompt.finish()


def first_attention(x_prompt, x_resp, w_query, w_key, w_value, gain, cos, sin, info, collective_id):
    rows = TILE + x_resp.shape[0]
    width = x_resp.shape[1]
    return pl.pallas_call(
        first_attention_kernel,
        out_shape=(jax.ShapeDtypeStruct((PEERS, RING, 32, COLUMNS), BF16), jax.ShapeDtypeStruct((PEERS, 8, 16, COLUMNS), BF16),
                   jax.ShapeDtypeStruct((PEERS, 8, 128), jnp.int32), jax.ShapeDtypeStruct((TILE, PAIR * COLUMNS), BF16)),
        in_specs=[ANY] * 5 + [VMEM] * 4,
        out_specs=(VMEM,) * 4,
        scratch_shapes=[
            pltpu.VMEM((9, TILE, width), BF16), pltpu.VMEM((width, 3 * COLUMNS), BF16), pltpu.VMEM((TILE, width), BF16), pltpu.VMEM((TILE, width), BF16),
            pltpu.VMEM((rows, COLUMNS), BF16), pltpu.VMEM((rows - TILE, COLUMNS), BF16), pltpu.VMEM((rows - TILE, COLUMNS), BF16),
            HELD, pltpu.VMEM((RING, PEERS, 32, COLUMNS), BF16), pltpu.VMEM((PEERS, 8, 16, COLUMNS), BF16),
            DMA((9,)), DMA((3,)), *GATHER_SEMS, DMA((PEERS,)), DMA((PEERS,)),
            *router_scratch(RING, (32, COLUMNS)), *router_scratch(1, (8, 16, COLUMNS)),
        ],
        compiler_params=pltpu.CompilerParams(collective_id=collective_id, has_side_effects=True, vmem_limit_bytes=VMEM_BYTES),
        name="first_attention",
    )(x_prompt, x_resp, w_query, w_key, w_value, gain.reshape(1, width), cos, sin, info)


def second_attention_kernel(qkv_ref, back_ref, mixed_out, stage, qkv_in, k_s, v_s, held, mixed_stage,
                            ring_send, ring_recv, near_send, near_recv, *routes):
    net = Exchange()
    me = net.me
    prompt = PromptGather(net, held, ring_send, ring_recv, near_send, near_recv)
    router = Router(net, RING, lambda t, d: stage.at[t, d], lambda t, d: qkv_in.at[t, d], routes[:5])
    mixed_router = Router(net, RING, lambda t, d: mixed_stage.at[t, d], lambda t, d: mixed_out.at[d, t], routes[5:])
    for k in BOTH:
        held[me, k] = qkv_ref[0, :, pl.ds((k + 1) * COLUMNS, COLUMNS)]
    net.barrier()
    prompt.start()
    count = back_ref.shape[1]

    def send_rows(t):
        place = lax.broadcasted_iota(jnp.int32, (Q_TILE, count), 0) + t * Q_TILE == back_ref[...]
        rows = jnp.dot(place.astype(BF16), qkv_ref[1:].reshape(count, 3 * COLUMNS), preferred_element_type=F32).astype(BF16)
        stage[t] = rows.reshape(PEERS, Q_TILE // PEERS, 3 * COLUMNS)
        router.send(t)
        qkv_in[t, me] = stage[t, me]
        if t:
            router.relay(t - 1)

    send_rows(0)
    prompt.relay()
    send_rows(1)
    prompt.share()
    for t in range(PAIR, RING):
        send_rows(t)
    prompt.collect()
    for t in range(RING):
        router.collect(t)
        rows = jnp.dot(undeal(Q_TILE), qkv_in[t].reshape(Q_TILE, 3 * COLUMNS), preferred_element_type=F32).astype(BF16)
        k_s[pl.ds(t * Q_TILE, Q_TILE)] = rows[:, COLUMNS:PAIR * COLUMNS]
        v_s[pl.ds(t * Q_TILE, Q_TILE)] = rows[:, PAIR * COLUMNS:]
        mixed = attend_response(t, rows[:, :COLUMNS], held, k_s, v_s)
        deal_mixed(mixed_router, t, mixed, mixed_stage, mixed_out)
        if t == 0:
            router.relay(RING - 1)
    collect_mixed(mixed_router)
    for each in (router, mixed_router):
        each.finish()
    prompt.finish()


def second_attention(qkv, back, collective_id):
    rows = RING * Q_TILE
    wide = (32, 3 * COLUMNS)
    return pl.pallas_call(
        second_attention_kernel,
        out_shape=jax.ShapeDtypeStruct((PEERS, RING, 32, COLUMNS), BF16),
        in_specs=[VMEM, VMEM],
        out_specs=VMEM,
        scratch_shapes=[
            pltpu.VMEM((RING, PEERS) + wide, BF16), pltpu.VMEM((RING, PEERS) + wide, BF16),
            pltpu.VMEM((rows, COLUMNS), BF16), pltpu.VMEM((rows, COLUMNS), BF16),
            HELD, pltpu.VMEM((RING, PEERS, 32, COLUMNS), BF16), *GATHER_SEMS,
            *router_scratch(RING, wide), *router_scratch(RING, (32, COLUMNS)),
        ],
        compiler_params=pltpu.CompilerParams(collective_id=collective_id, has_side_effects=True, vmem_limit_bytes=VMEM_BYTES),
        name=f"second_attention{collective_id}",
    )(qkv, back)


class Answer:
    def __init__(self, every, out_ref, stat_send, stat_recv, row_send, row_recv):
        self.every, self.out = every, out_ref
        self.stat_sems, self.row_sems = (stat_send, stat_recv), (row_send, row_recv)
        self.me, self.home = lax.axis_index("model"), lax.axis_index("resp")
        self.models = [(self.me + k) % SHARDS for k in range(1, SHARDS)]
        self.homes = [(self.home + k) % PEERS for k in range(1, PEERS)]

    def barrier(self):
        sem = pltpu.get_barrier_semaphore()
        for axis, devices in (("model", self.models), ("resp", self.homes)):
            for device in devices:
                pl.semaphore_signal(sem, device_id={axis: device}, device_id_type=MESH)
        pl.semaphore_wait(sem, len(self.models) + len(self.homes))

    def stat_copy(self, owner, device, place):
        ref = self.every.at[owner]
        return pltpu.make_async_remote_copy(
            src_ref=ref, dst_ref=ref, send_sem=self.stat_sems[0].at[device], recv_sem=self.stat_sems[1].at[place],
            device_id={"model": device}, device_id_type=MESH)

    def row_copy(self, owner, device, place):
        ref = self.out.at[owner]
        return pltpu.make_async_remote_copy(
            src_ref=ref, dst_ref=ref, send_sem=self.row_sems[0].at[device], recv_sem=self.row_sems[1].at[place],
            device_id={"resp": device}, device_id_type=MESH)

def combine_kernel(stats_ref, out_ref, every, *sems):
    net = Answer(every, out_ref, *sems)
    chunks = stats_ref.shape[0]
    every[net.me] = stats_ref[...]
    net.barrier()
    for device in net.models:
        net.stat_copy(net.me, device, net.me).start()
    for device in net.models:
        net.stat_copy(device, device, device).wait_recv()
    found = []
    for c in range(chunks):
        tiles = [every[k, c] for k in range(SHARDS)]
        top = functools.reduce(jnp.maximum, [tile[:1] for tile in tiles])
        total = functools.reduce(jnp.add, [tile[1:PAIR] * jnp.exp(tile[:1] - top) for tile in tiles])
        found.append(functools.reduce(jnp.add, [tile[PAIR:3] for tile in tiles]) - top - jnp.log(total))
    if chunks < PEERS:
        found.append(jnp.zeros((PEERS - chunks, LANES), F32))
    out_ref[net.home] = jnp.concatenate(found, axis=0)
    for device in net.homes:
        net.row_copy(net.home, device, net.home).start()
    for device in net.homes:
        net.row_copy(device, device, device).wait_recv()
    for device in net.models:
        net.stat_copy(net.me, device, device).wait_send()
    for device in net.homes:
        net.row_copy(net.home, device, device).wait_send()


def combine(stats, collective_id):
    return pl.pallas_call(
        combine_kernel,
        out_shape=jax.ShapeDtypeStruct((PEERS, PEERS, LANES), F32),
        in_specs=[VMEM],
        out_specs=VMEM,
        scratch_shapes=[pltpu.VMEM((SHARDS,) + stats.shape, F32), *[DMA((SHARDS,)) for _ in BOTH], *[DMA((PEERS,)) for _ in BOTH]],
        compiler_params=pltpu.CompilerParams(collective_id=collective_id, has_side_effects=True),
        name=f"combine{collective_id}",
    )(stats)


ROPE_BASE = 10000.0
VARIANTS = (640, 768, 1024)


def rope_tables(positions):
    half = LANES // PAIR
    frequency = ROPE_BASE ** (-jnp.arange(half, dtype=F32) / half)
    angles = positions.astype(F32)[:, None] * frequency
    cos, sin = jnp.cos(angles), jnp.sin(angles)
    return jnp.concatenate([cos, cos], axis=1), jnp.concatenate([-sin, sin], axis=1)


def solution(mesh):
    groups = mesh.shape['resp']
    row_axes = ('prompts', 'resp')
    head_spec = P(None, None, 'model', None)
    in_specs = (P(row_axes, None), P(row_axes, None, None), P(row_axes, None), P(row_axes), P(None, None), head_spec, head_spec, head_spec, P(None, 'model', None, None), P(None, None), P(None, None, 'model'), P(None, None, 'model'), P(None, 'model', None), P(None), P(None, 'model'))

    def device_step(x_prompt, x_resp, targets, resp_lens, attn_gain, w_query, w_key, w_value, w_out, mlp_gain, w_gate, w_up, w_down, final_gain, w_vocab):
        prompt_rows = x_prompt.shape[0]
        resp_len, width = x_resp.shape[1:]
        prompt_len = prompt_rows * groups
        me = lax.axis_index('model')
        home = lax.axis_index('resp')
        per = resp_len // groups
        gate_t, up_t = jnp.swapaxes(w_gate, 1, 2), jnp.swapaxes(w_up, 1, 2)
        out_flat = w_out.reshape(w_out.shape[0], COLUMNS, width)
        flat = lambda w, layer: w[layer].reshape(width, COLUMNS)
        project_next = jnp.concatenate([flat(w, 1) for w in (w_query, w_key, w_value)], axis=1)
        prompt_pos = home * prompt_rows + jnp.arange(prompt_rows)

        cos, sin = rope_tables(jnp.concatenate([prompt_pos, prompt_len + jnp.arange(resp_len)]))
        info = jnp.concatenate([
            targets[0].reshape(per, groups).T[:, None, :],
            jnp.broadcast_to(resp_lens[0], (groups, groups - 1, per)).astype(jnp.int32)], axis=1)
        mixed, res, infos, prompt = first_attention(
            x_prompt, x_resp[0], flat(w_query, 0), flat(w_key, 0), flat(w_value, 0), attn_gain[0], cos, sin, info, 0)
        lens = infos[:, 1, 0]
        need = (lens + groups - 1) // groups
        ends = jnp.sum(jnp.where(jnp.arange(groups)[:, None] >= jnp.arange(groups), need, 0), axis=1)
        starts = ends - need
        dealt = groups * per

        def finish_with(size, ident):
            def run(operands):
                mixed, res, prompt = operands
                slot = jnp.arange(size)
                which = jnp.sum((slot[:, None] >= ends).astype(jnp.int32), axis=1)
                row = slot - jnp.sum(jnp.where(which[:, None] == jnp.arange(groups), starts, 0), axis=1)
                real = slot < ends[-1]
                source = jnp.where(real, which * per + row, -1)
                chosen = source[:, None] == jnp.arange(dealt)
                wanted = jnp.sum(jnp.where(chosen, infos[:, 0, :].reshape(dealt), 0), axis=1) - me * w_vocab.shape[1]
                ids = jnp.where(jnp.arange(LANES) == 0, source[:, None], wanted[:, None]).reshape(-1, LANES, LANES)
                tables = rope_tables(jnp.concatenate([prompt_pos, prompt_len + groups * row + home]))
                weights = (out_flat, gate_t, up_t, w_down)
                qkv, new_res = mega(
                    mlp_gain[0], attn_gain[1], ids, mixed.reshape(dealt, COLUMNS), res.reshape(dealt, COLUMNS),
                    [t.reshape(-1, LANES, LANES) for t in tables] + [prompt], *weights, project_next, 0, ident)
                part = per // RING
                back = jnp.where(real, (row // part) * (groups * part) + which * part + row % part, -1)
                mixed = second_attention(qkv, back[None], ident + 1)
                stats = mega(mlp_gain[1], final_gain, ids, mixed.reshape(dealt, COLUMNS), new_res, [], *weights, w_vocab, 1, ident + PAIR)
                found = combine(stats, ident + 3)
                start = jnp.sum(jnp.where(jnp.arange(groups) == home, starts, 0))
                mine = lax.dynamic_slice(jnp.pad(found.reshape(groups, dealt), ((0, 0), (0, per))), (0, start), (groups, per))
                return mine.T.reshape(resp_len)
            return run

        index = sum((ends[-1] > size).astype(jnp.int32) for size in VARIANTS[:-1])
        log_probs = lax.switch(index, [finish_with(size, 1 + RING * i) for i, size in enumerate(VARIANTS)], (mixed, res, prompt))
        log_probs = jnp.where(jnp.arange(resp_len) < resp_lens[0], log_probs, 0.0)
        return log_probs[None, :]

    return jax.shard_map(device_step, mesh=mesh, in_specs=in_specs, out_specs=P(row_axes, None), check_vma=False)
```

```python
import functools

import jax
import jax.numpy as jnp
from jax import lax
from jax.experimental import pallas as pl
from jax.experimental.pallas import tpu as pltpu
from jax.sharding import PartitionSpec as P

MESH = pl.DeviceIdType.MESH
F32 = jnp.float32
BF16 = jnp.bfloat16
EPS = 1e-6
LANES = 128
PAIR = 2
RING = 4
COLUMNS = PAIR * LANES
SHARDS = RING * RING
PEERS = 8
BOTH = range(PAIR)
VMEM_BYTES = 67_000_000
LATE_ROWS = 640
LOGITS = 512
VMEM = pl.BlockSpec(memory_space=pltpu.VMEM)
ANY = pl.BlockSpec(memory_space=pl.ANY)
DMA = pltpu.SemaphoreType.DMA
KINDS = range(RING * 3)
SUM_FAR, SUM_NEAR, SUM_RELAY, SUM2_FAR, SUM2_NEAR, SUM2_RELAY, TAKE_OWN, TAKE_REST, TAKE_RELAY, TAKE2_OWN, TAKE2_REST, TAKE2_RELAY = KINDS


def block_of(color, first, second):
    return RING * first + second if color else RING * second + first


def pair(index):
    return pl.ds(PAIR * index, PAIR)


class Torus:
    def __init__(self, refs, send_sem, recv_sem):
        self.refs = refs
        self.far, self.near, self.relayed, self.sums, self.relayed2, self.sums2, self.rows = refs
        self.send_sem, self.recv_sem = send_sem, recv_sem
        me = lax.axis_index("model")
        z, y = me // RING, me % RING
        self.place = ((y, z), (z, y))
        along_y = [z * RING + self.step(y, way) for way in (1, -1)]
        along_z = [self.step(z, way) * RING + y for way in (1, -1)]
        self.neighbors = ((along_y, along_z), (along_z, along_y))

    def step(self, place, by):
        return (place + by + RING) % RING

    def barrier(self):
        sem = pltpu.get_barrier_semaphore()
        for ring in self.neighbors[0]:
            for device in ring:
                pl.semaphore_signal(sem, device_id={"model": device}, device_id_type=MESH)
        pl.semaphore_wait(sem, RING)

    def ends(self, kind, c, q, d):
        (p, s), way, other = self.place[q], 1 - PAIR * d, 1 - d
        far, near, relayed, sums, relayed2, sums2, rows = (ref.at[c, q] for ref in self.refs)
        own = sums.at[0]
        back_s, back_p = self.step(s, -way), self.step(p, -way)
        return {
            SUM_FAR: lambda: (far.at[pair(d)], relayed.at[d], relayed.at[d]),
            SUM_NEAR: lambda: (near.at[d], sums.at[d, pair(other)], sums.at[d, pair(other)]),
            SUM_RELAY: lambda: (relayed.at[d], sums.at[d, pair(d)], sums.at[d, pair(d)]),
            SUM2_FAR: lambda: (own.at[self.step(s, PAIR), d], relayed2.at[d], relayed2.at[d]),
            SUM2_NEAR: lambda: (own.at[self.step(s, way), other], sums2.at[d, other], sums2.at[d, other]),
            SUM2_RELAY: lambda: (relayed2.at[d], sums2.at[d, d], sums2.at[d, d]),
            TAKE_OWN: lambda: (rows.at[p, s, d], rows.at[p, s, d], rows.at[p, back_s, d]),
            TAKE_REST: lambda: (rows.at[p, s, other], rows.at[p, s, other], rows.at[p, back_s, other]),
            TAKE_RELAY: lambda: (rows.at[p, back_s, d], rows.at[p, back_s, d], rows.at[p, self.step(s, PAIR), d]),
            TAKE2_OWN: lambda: (rows.at[p, pair(d)], rows.at[p, pair(d)], rows.at[back_p, pair(d)]),
            TAKE2_REST: lambda: (rows.at[p, pair(other)], rows.at[p, pair(other)], rows.at[back_p, pair(other)]),
            TAKE2_RELAY: lambda: (rows.at[back_p, pair(d)], rows.at[back_p, pair(d)], rows.at[self.step(p, PAIR), pair(d)]),
        }[kind]()

    def copy(self, kind, c, q, d, src, dst):
        second_ring = kind in (SUM2_FAR, SUM2_NEAR, SUM2_RELAY, TAKE_OWN, TAKE_REST, TAKE_RELAY)
        return pltpu.make_async_remote_copy(
            src_ref=src, dst_ref=dst, send_sem=self.send_sem.at[c, q, d, kind], recv_sem=self.recv_sem.at[c, q, d, kind],
            device_id={"model": self.neighbors[q][second_ring][d]}, device_id_type=MESH)

    def send(self, c, q, d, kind):
        src, dst, _ = self.ends(kind, c, q, d)
        self.copy(kind, c, q, d, src, dst).start()

    def sent(self, c, q, *kinds):
        for kind in kinds:
            for d in BOTH:
                src, dst, _ = self.ends(kind, c, q, d)
                self.copy(kind, c, q, d, src, dst).wait_send()

    def arrived(self, c, q, d, *kinds):
        for kind in kinds:
            _, _, here = self.ends(kind, c, q, d)
            self.copy(kind, c, q, d, here, here).wait_recv()


def halves(value):
    return value[:, :LANES], value[:, LANES:]


def store_block(ref, value):
    for half, part in enumerate(halves(value)):
        ref[half] = part


def add_block(ref, value):
    for half, part in enumerate(halves(value)):
        ref[half] += part


class Stage:
    def __init__(self, net, lhs_of, w_ref, finish):
        self.net, self.lhs_of, self.w_ref, self.finish = net, lhs_of, w_ref, finish

    def product(self, lhs, color, first, second):
        start = pl.multiple_of(block_of(color, first, second) * COLUMNS, COLUMNS)
        return jnp.dot(lhs, self.w_ref[:, pl.ds(start, COLUMNS)], preferred_element_type=F32)

    def begin(self, c, q):
        net, p, lhs = self.net, self.net.place[q][0], self.lhs_of(c, q)
        for k in range(RING):
            store_block(net.far.at[c, q, k], self.product(lhs, q, net.step(p, PAIR), k))
        for d in BOTH:
            net.send(c, q, d, SUM_FAR)
        for d in BOTH:
            for k in BOTH:
                store_block(net.near.at[c, q, d, k], self.product(lhs, q, net.step(p, 1 - PAIR * d), PAIR * (1 - d) + k))
            net.send(c, q, d, SUM_NEAR)

    def relay_sum(self, c, q):
        net, p, lhs = self.net, self.net.place[q][0], self.lhs_of(c, q)
        for d in BOTH:
            net.arrived(c, q, d, SUM_FAR)
            for k in BOTH:
                add_block(net.relayed.at[c, q, d, k], self.product(lhs, q, net.step(p, 1 - PAIR * d), PAIR * d + k))
            net.send(c, q, d, SUM_RELAY)

    def begin_second(self, c, q):
        net, lhs = self.net, self.lhs_of(c, q)
        for d in BOTH:
            net.arrived(c, q, d, SUM_NEAR, SUM_RELAY)
        for k in range(RING):
            for half, part in enumerate(halves(self.product(lhs, q, net.place[q][0], k))):
                net.sums[c, q, 0, k, half] += net.sums[c, q, 1, k, half] + part
        for kind in (SUM2_FAR, SUM2_NEAR):
            for d in BOTH:
                net.send(c, q, d, kind)
        net.sent(c, q, SUM_FAR)

    def relay_second(self, c, q):
        net = self.net
        for d in BOTH:
            net.arrived(c, q, d, SUM2_FAR)
            net.relayed2[c, q, d] += net.sums[c, q, 0, net.step(net.place[q][1], 1 - PAIR * d), d]
            net.send(c, q, d, SUM2_RELAY)

    def finish_sum(self, c, q):
        net = self.net
        net.sent(c, q, SUM_NEAR, SUM_RELAY)
        for d in BOTH:
            net.arrived(c, q, d, SUM2_NEAR, SUM2_RELAY)
        for half in BOTH:
            self.finish(c, q, half, net.sums[c, q, 0, net.place[q][1], half] + net.sums2[c, q, 0, half] + net.sums2[c, q, 1, half])
        for kind in (TAKE_OWN, TAKE_REST):
            for d in BOTH:
                net.send(c, q, d, kind)

    def relay_rows(self, c, q):
        net = self.net
        net.sent(c, q, SUM2_FAR, SUM2_NEAR, SUM2_RELAY)
        for d in BOTH:
            net.arrived(c, q, d, TAKE_OWN)
            net.send(c, q, d, TAKE_RELAY)

    def take_second(self, c, q):
        net = self.net
        for d in BOTH:
            net.arrived(c, q, d, TAKE_REST, TAKE_RELAY)
        for kind in (TAKE2_OWN, TAKE2_REST):
            for d in BOTH:
                net.send(c, q, d, kind)

    def relay_last(self, c, q):
        net = self.net
        for d in BOTH:
            net.arrived(c, q, d, TAKE2_OWN)
            net.send(c, q, d, TAKE2_RELAY)

    def complete(self, c, q):
        net = self.net
        for d in BOTH:
            net.arrived(c, q, d, TAKE2_REST, TAKE2_RELAY)
        net.sent(c, q, TAKE_OWN, TAKE_REST, TAKE_RELAY, TAKE2_OWN, TAKE2_REST, TAKE2_RELAY)

    def middle(self):
        return [self.relay_sum, self.begin_second, self.relay_second, self.finish_sum, self.relay_rows, self.take_second, self.relay_last]


def normed(net, c, q, gain_ref, layer):
    rows = net.rows.shape[-PAIR]
    tile = PAIR * 8 if rows % (PAIR * 8) == 0 else 8
    spots = [(first, second, half) for first in range(RING) for second in range(RING) for half in BOTH]

    @pl.loop(0, rows // tile)
    def _(i):
        span = pl.ds(pl.multiple_of(i * tile, tile), tile)
        acts = [net.rows[(c, q) + spot + (span,)].astype(F32) for spot in spots]
        squares = functools.reduce(jnp.add, [v * v for v in acts])
        inv = lax.rsqrt(jnp.sum(squares, axis=-1, keepdims=True) / (LANES * len(acts)) + EPS)
        for spot, v in zip(spots, acts):
            column = block_of(q, *spot[:PAIR]) * COLUMNS + spot[PAIR] * LANES
            net.rows[(c, q) + spot + (span,)] = (v * inv * gain_ref[pl.ds(layer, 1), pl.ds(column, LANES)]).astype(BF16)


def rows_of(net, c, q):
    parts = []
    for upper in range(RING):
        for lower in range(RING):
            first, second = (upper, lower) if q else (lower, upper)
            parts += [net.rows[c, q, first, second, half] for half in BOTH]
    return jnp.concatenate(parts, axis=1)


def times_transposed(lhs, rhs):
    return lax.dot_general(lhs, rhs, (((1,), (1,)), ((), ())), preferred_element_type=F32)


def late_plan(width, count):
    plan, start = [], 0
    for buffer in BOTH:
        for slot in range(width // count):
            size = min(LATE_ROWS, width - start)
            if size:
                plan.append((buffer, slot * count, start, size))
            start += size
    return plan, width - start


def rope(value, cos, sin):
    return jnp.concatenate([v * cos + pltpu.roll(v, LANES // PAIR, 1) * sin for v in halves(value)], axis=1)


def put_projected(product, cos_ref, sin_ref, out_ref, c):
    for k in range(3):
        value = product(k * COLUMNS, COLUMNS)
        if k < PAIR:
            value = rope(value, cos_ref[c], sin_ref[c])
        out_ref[c, :, pl.ds(k * COLUMNS, COLUMNS)] = value.astype(BF16)


def statistics(product, count, target):
    top = total = picked = None
    for k in range(count // LOGITS):
        logits = product(k * LOGITS, LOGITS)
        here = jnp.max(logits, axis=-1, keepdims=True)
        ids = lax.broadcasted_iota(jnp.int32, logits.shape, 1) + k * LOGITS
        found = jnp.sum(jnp.where(ids == target, logits, 0.0), axis=-1, keepdims=True)
        if k:
            both = jnp.maximum(top, here)
            total = total * jnp.exp(top - both) + jnp.sum(jnp.exp(logits - both), axis=-1, keepdims=True)
            top, picked = both, picked + found
        else:
            top, total, picked = here, jnp.sum(jnp.exp(logits - here), axis=-1, keepdims=True), found
    lane = lax.broadcasted_iota(jnp.int32, (LANES, LANES), 1)
    return jnp.where(lane == 0, top, jnp.where(lane == 1, total, picked)).T[:PEERS]


def mega_kernel(chunks, layer, last, gain_ref, next_gain_ref, ids_ref, dealt_ref, old_ref, *args):
    if last:
        side_refs, args = (), args
    else:
        side_refs, args = args[:3], args[3:]
    w_out_hbm, w_gate_hbm, w_up_hbm, w_down_hbm, *args = args
    lates, (out_ref, *args) = (args[:1], args[1:]) if last else ([ref.at[layer + 1] for ref in args[:3]], args[3:])
    if not last:
        new_res_ref, *args = args
    (w_out, w_gate, w_up, w_down, late_rest, acts, res, inner, middle,
     far, near, relayed, sums, relayed2, sums2, rows, w_sem, late_sem, send_sem, recv_sem) = args
    loads = [pltpu.make_async_copy(src.at[layer], dst, w_sem.at[i]) for i, (src, dst) in enumerate(
        ((w_out_hbm, w_out), (w_gate_hbm, w_gate), (w_up_hbm, w_up), (w_down_hbm, w_down)))]
    for load in loads:
        load.start()
    width, each = lates[0].shape
    count = each * len(lates)
    plan, left = late_plan(width, count)
    late_loads = []
    for k, ref in enumerate(lates):
        late = [(start, size, (w_gate, w_up)[buffer].at[pl.ds(0, size), pl.ds(lane + k * each, each)]) for buffer, lane, start, size in plan]
        if left:
            late.append((width - left, left, late_rest))
        for start, size, dst in late:
            late_loads.append(pltpu.make_async_copy(ref.at[pl.ds(start, size)], dst, late_sem.at[len(late_loads)]))
    net = Torus((far, near, relayed, sums, relayed2, sums2, rows), send_sem, recv_sem)
    net.barrier()
    loads[0].wait()
    if last:
        new_res_ref = middle
        out_ref[...] = jnp.zeros_like(out_ref)

    def picked(ids, ref):
        chosen = (ids == lax.broadcasted_iota(jnp.int32, (LANES, PEERS * LANES), 1)).astype(BF16)
        return jnp.dot(chosen, ref[...], preferred_element_type=F32).astype(BF16)

    def put(c, mixed, columns):
        for q in BOTH:
            span = slice(q * acts.shape[PAIR], (q + 1) * acts.shape[PAIR])
            acts[c, q] = mixed[span]
            for half, part in enumerate(halves(columns) if columns is not None else ()):
                res[c, q, half] = part[span]

    def begin(c):
        if last:
            put(c, picked(ids_ref[c, :, :1], dealt_ref), None)
        else:
            @pl.when(c == 0)
            def _():
                put(c, side_refs[PAIR][:, :COLUMNS], side_refs[PAIR][:, COLUMNS:])

            @pl.when(c > 0)
            def _():
                ids = ids_ref[c - 1, :, :1]
                put(c, picked(ids, dealt_ref), picked(ids, old_ref))
        for q in BOTH:
            first.begin(c, q)

    def finish_with(old_ref, new_ref, skip=0):
        def finish(c, q, half, total):
            value = (old_ref[c + skip, q, half].astype(F32) + total).astype(BF16)
            new_ref[c, q, half] = value
            rows[(c, q) + net.place[q] + (half,)] = value
        return finish

    first = Stage(net, lambda c, q: acts[c, q], w_out, finish_with(old_ref if last else res, middle, last))
    second = Stage(net, lambda c, q: inner[c, q], w_down, finish_with(middle, new_res_ref))

    def hidden_of(c, stage, gain, row):
        for q in BOTH:
            stage.complete(c, q)
            normed(net, c, q, gain, row)
        return jnp.concatenate([rows_of(net, c, q) for q in BOTH], axis=0)

    def mlp(c):
        hidden = hidden_of(c, first, gain_ref, layer)
        value = (jax.nn.silu(times_transposed(hidden, w_gate[...])) * times_transposed(hidden, w_up[...])).astype(BF16)
        inner[c] = value.reshape(inner.shape[1:])
        for q in BOTH:
            second.begin(c, q)

    def after(c):
        hidden = hidden_of(c, second, next_gain_ref, 0 if last else layer + 1)

        def product(lane, size):
            parts = [jnp.dot(hidden[:, start:start + rows_here], (w_gate, w_up)[buffer][pl.ds(0, rows_here), pl.ds(at + lane, size)], preferred_element_type=F32)
                     for buffer, at, start, rows_here in plan]
            if left:
                parts.append(jnp.dot(hidden[:, width - left:], late_rest[:, pl.ds(lane, size)], preferred_element_type=F32))
            return functools.reduce(jnp.add, parts)

        if last:
            out_ref[c] = statistics(product, count, ids_ref[c, :, 1:PAIR])
        else:
            put_projected(product, *side_refs[:PAIR], out_ref, c)

    def on_both(step):
        def run(c):
            for q in BOTH:
                step(c, q)
        return run

    steps = [begin, *map(on_both, first.middle()), mlp, *map(on_both, second.middle())]
    at_mlp = steps.index(mlp)
    steps += [None] * max(0, at_mlp + chunks - len(steps)) + [after]

    @pl.loop(0, len(steps) + chunks - 1)
    def _(slot):
        @pl.when(slot == at_mlp)
        def _():
            for load in loads[1:]:
                load.wait()

        @pl.when(slot == len(steps) - 1)
        def _():
            for load in late_loads:
                load.wait()

        for k, step in reversed(list(enumerate(steps))):
            if step is None:
                continue

            @pl.when(slot >= k)
            def _():
                @pl.when(slot < k + chunks)
                def _():
                    step(slot - k)

        @pl.when(slot == at_mlp + chunks - 1)
        def _():
            for load in late_loads:
                load.start()


def mega(gain, next_gain, ids, dealt, old, sides, w_out, w_gate_t, w_up_t, w_down, lates, layer, collective_id):
    last = not sides
    chunks = ids.shape[0] + (not last)
    _, depth, width = w_out.shape
    hidden = w_gate_t.shape[1]
    rows = LANES // PAIR
    per = (chunks, PAIR)
    tile = (rows, LANES)
    count = sum(late.shape[-1] for late in lates)
    _, left = late_plan(width, count)

    sem = DMA(per + (PAIR, len(KINDS)))
    out = jax.ShapeDtypeStruct((PEERS, PEERS, LANES), F32) if last else (
        jax.ShapeDtypeStruct((chunks, LANES, count), BF16), jax.ShapeDtypeStruct(per + (PAIR,) + tile, BF16))
    return pl.pallas_call(
        functools.partial(mega_kernel, chunks, layer, last),
        out_shape=out,
        in_specs=[VMEM] * (5 + len(sides)) + [ANY] * (RING + len(lates)),
        out_specs=VMEM if last else (VMEM, VMEM),
        scratch_shapes=[
            pltpu.VMEM((depth, width), BF16),
            *[pltpu.VMEM((hidden, width), BF16) for _ in range(3)],
            pltpu.VMEM((left or 8, count), BF16),
            pltpu.VMEM(per + (rows, depth), BF16),
            pltpu.VMEM(per + (PAIR,) + (tile if not last else (8, LANES)), BF16),
            pltpu.VMEM(per + (rows, hidden), BF16),
            pltpu.VMEM(per + (PAIR,) + tile, BF16),
            pltpu.VMEM(per + (RING, PAIR) + tile, F32),
            pltpu.VMEM(per + (PAIR, PAIR, PAIR) + tile, F32),
            pltpu.VMEM(per + (PAIR, PAIR, PAIR) + tile, F32),
            pltpu.VMEM(per + (PAIR, RING, PAIR) + tile, F32),
            pltpu.VMEM(per + (PAIR,) + tile, F32),
            pltpu.VMEM(per + (PAIR, PAIR) + tile, F32),
            pltpu.VMEM(per + (RING, RING, PAIR) + tile, BF16),
            DMA((RING,)), DMA((PAIR * SHARDS,)), sem, sem,
        ],
        compiler_params=pltpu.CompilerParams(collective_id=collective_id, has_side_effects=True, vmem_limit_bytes=VMEM_BYTES),
        name=f"mega{collective_id}",
    )(gain, next_gain, ids, dealt, old, *sides, w_out, w_gate_t, w_up_t, w_down, *lates)


TILE = 128
Q_TILE = 256
LOG2E = 1.4426950408889634
HELD = pltpu.VMEM((PEERS, PAIR, TILE, COLUMNS), BF16)
GATHER_SEMS = [DMA((PAIR, 3)), DMA((PAIR, 3)), DMA((RING,)), DMA((RING,))]


class Exchange:
    def __init__(self):
        self.me = lax.axis_index("resp")
        self.others = [(self.me + k) % PEERS for k in range(1, PEERS)]

    def barrier(self):
        sem = pltpu.get_barrier_semaphore()
        for device in self.others:
            pl.semaphore_signal(sem, inc=1, device_id={"resp": device}, device_id_type=MESH)
        pl.semaphore_wait(sem, PEERS - 1)

    def copy(self, src, dst, send_sem, recv_sem, device):
        return pltpu.make_async_remote_copy(src_ref=src, dst_ref=dst, send_sem=send_sem, recv_sem=recv_sem,
                                            device_id={"resp": device}, device_id_type=MESH)

    def scatter(self, src_of, dst, send_sem, recv_sem):
        for device in self.others:
            self.copy(src_of(device), dst, send_sem.at[device], recv_sem.at[self.me], device).start()

    def collected(self, dst_of, recv_sem):
        for device in self.others:
            self.copy(dst_of(device), dst_of(device), recv_sem.at[device], recv_sem.at[device], device).wait_recv()

    def sent(self, src_of, send_sem, recv_sem):
        for device in self.others:
            self.copy(src_of(device), src_of(device), send_sem.at[device], recv_sem.at[device], device).wait_send()


class Router:
    def __init__(self, net, tiles, src_of, dst_of, sems):
        self.net, self.tiles, self.src_of, self.dst_of = net, tiles, src_of, dst_of
        self.send_sem, self.recv_sem = sems

    def send(self, t):
        self.net.scatter(lambda d: self.src_of(t, d), self.dst_of(t, self.net.me), self.send_sem.at[t], self.recv_sem.at[t])

    def collect(self, t):
        self.net.collected(lambda d: self.dst_of(t, d), self.recv_sem.at[t])

    def finish(self):
        for t in range(self.tiles):
            self.net.sent(lambda d: self.src_of(t, d), self.send_sem.at[t], self.recv_sem.at[t])


class PromptGather:
    def __init__(self, net, held, ring_send, ring_recv, near_send, near_recv):
        self.net, self.held = net, held
        self.ring_sems, self.near_sems = (ring_send, ring_recv), (near_send, near_recv)
        x, core = net.me // PAIR, net.me % PAIR
        self.at = lambda by, here: (x + by + RING) % RING * PAIR + (core if here else 1 - core)

    def ring_copy(self, d, kind, ref):
        return self.net.copy(ref, ref, self.ring_sems[0].at[d, kind], self.ring_sems[1].at[d, kind], self.at(1 - PAIR * d, True))

    def near_copy(self, kind, ref):
        return self.net.copy(ref, ref, self.near_sems[0].at[kind], self.near_sems[1].at[kind], self.at(0, False))

    def sources(self, here):
        return [self.at(by, here) for by in (0, -1, 1, PAIR)]

    def start(self):
        own = self.held.at[self.net.me]
        for kind in BOTH:
            for d in BOTH:
                self.ring_copy(d, kind, own.at[1 - d if kind else d]).start()
        self.near_copy(0, own).start()

    def relay(self):
        for d in BOTH:
            ref = self.held.at[self.at(PAIR * d - 1, True), d]
            self.ring_copy(d, 0, ref).wait_recv()
            self.ring_copy(d, PAIR, ref).start()

    def share(self):
        for d in BOTH:
            device = self.at(PAIR * d - 1, True)
            self.ring_copy(d, 1, self.held.at[device, 1 - d]).wait_recv()
            self.near_copy(1 + d, self.held.at[device]).start()
        far = self.held.at[self.at(PAIR, True)]
        for d in BOTH:
            self.ring_copy(d, PAIR, far.at[d]).wait_recv()
        self.near_copy(3, far).start()

    def collect(self):
        for kind, device in enumerate(self.sources(False)):
            self.near_copy(kind, self.held.at[device]).wait_recv()

    def finish(self):
        for kind in range(3):
            for d in BOTH:
                self.ring_copy(d, kind, self.held.at[self.net.me, d]).wait_send()
        for kind in range(RING):
            self.near_copy(kind, self.held.at[self.net.me]).wait_send()


def deal(rows):
    out = lax.broadcasted_iota(jnp.int32, (rows, rows), 0)
    src = lax.broadcasted_iota(jnp.int32, (rows, rows), 1)
    per = rows // PEERS
    return jnp.where(src == (out % per) * PEERS + out // per, 1.0, 0.0).astype(BF16)


def undeal(rows):
    out = lax.broadcasted_iota(jnp.int32, (rows, rows), 0)
    src = lax.broadcasted_iota(jnp.int32, (rows, rows), 1)
    per = rows // PEERS
    return jnp.where(src == (out % PEERS) * per + out // PEERS, 1.0, 0.0).astype(BF16)


def norm_tile(x_ref, out_ref, gain_ref):
    for i in range(x_ref.shape[0] // 16):
        v = x_ref[pl.ds(16 * i, 16), :].astype(F32)
        inv = lax.rsqrt(jnp.mean(v * v, axis=-1, keepdims=True) + EPS)
        out_ref[pl.ds(16 * i, 16), :] = (v * inv * gain_ref[pl.ds(0, 1), :]).astype(BF16)


def softmax_mix(q, pieces):
    factor = LOG2E * 128 ** -0.5
    outs = []
    for h in range(2):
        lanes = slice(128 * h, 128 * h + 128)
        scores = []
        for keys, _, mask in pieces:
            s = lax.dot_general(q[:, lanes], keys[:, lanes], (((1,), (1,)), ((), ())), preferred_element_type=F32)
            scores.append(s if mask is None else jnp.where(mask, s, -jnp.inf))
        top = functools.reduce(jnp.maximum, [jnp.max(s, axis=-1, keepdims=True) for s in scores])
        probs = [jnp.exp2((s - top) * factor) for s in scores]
        total = functools.reduce(jnp.add, [jnp.sum(p, axis=-1, keepdims=True) for p in probs])
        mixed = functools.reduce(jnp.add, [jnp.dot(p.astype(BF16), values[:, lanes], preferred_element_type=F32) for p, (_, values, _) in zip(probs, pieces)])
        outs.append(mixed / total)
    return jnp.concatenate(outs, axis=1).astype(BF16)


def prompt_rows_of(held, which):
    return held[:, which].reshape(PEERS * TILE, COLUMNS)


def attend_response(t, q, held, k_own, v_own):
    row = lax.broadcasted_iota(jnp.int32, (Q_TILE, Q_TILE), 0)
    col = lax.broadcasted_iota(jnp.int32, (Q_TILE, Q_TILE), 1)
    pieces = [(prompt_rows_of(held, 0), prompt_rows_of(held, 1), None)]
    if t:
        pieces.append((k_own[:t * Q_TILE], v_own[:t * Q_TILE], None))
    span = slice(t * Q_TILE, (t + 1) * Q_TILE)
    pieces.append((k_own[span], v_own[span], col <= row))
    return softmax_mix(q, pieces)


def deal_mixed(router, t, mixed, stage, out):
    dealt = jnp.dot(deal(Q_TILE), mixed, preferred_element_type=F32).astype(BF16)
    stage[t] = dealt.reshape(PEERS, Q_TILE // PEERS, COLUMNS)
    router.send(t)
    out[router.net.me, t] = stage[t, router.net.me]


def first_attention_kernel(xp_hbm, xr_hbm, wq_hbm, wk_hbm, wv_hbm, gain_ref, cos_ref, sin_ref, info_ref,
                           mixed_out, res_out, info_out, prompt_out,
                           xs, w, even, odd, q_s, k_s, v_s, held, mixed_stage, res_stage,
                           x_sem, w_sem, ring_send, ring_recv, near_send, near_recv, info_send, info_recv, *routes):
    net = Exchange()
    mixed_router = Router(net, RING, lambda t, d: mixed_stage.at[t, d], lambda t, d: mixed_out.at[d, t], routes[:PAIR])
    res_router = Router(net, 1, lambda t, d: res_stage.at[d], lambda t, d: res_out.at[d], routes[PAIR:])
    prompt = PromptGather(net, held, ring_send, ring_recv, near_send, near_recv)
    me = net.me
    column = pl.multiple_of(lax.axis_index("model") * COLUMNS, COLUMNS)

    def load(t):
        src = xp_hbm if isinstance(t, int) and t == 0 else xr_hbm.at[pl.ds(pl.multiple_of((t - 1) * TILE, TILE), TILE)]
        return pltpu.make_async_copy(src, xs.at[t], x_sem.at[t])

    load(0).start()
    weights = [pltpu.make_async_copy(src.at[0], w.at[:, pl.ds(COLUMNS * i, COLUMNS)], w_sem.at[i]) for i, src in enumerate((wq_hbm, wk_hbm, wv_hbm))]
    for copy in weights:
        copy.start()
    for t in range(1, 9):
        load(t).start()
    net.barrier()
    net.scatter(lambda d: info_ref.at[d], info_out.at[me], info_send, info_recv)
    info_out[me] = info_ref[me]

    def project(t, hidden):
        span = pl.ds(pl.multiple_of(t * TILE, TILE), TILE)
        qkv = jnp.dot(hidden[...], w[...], preferred_element_type=F32)
        cos, sin = cos_ref[span], sin_ref[span]
        return span, rope(qkv[:, :COLUMNS], cos, sin).astype(BF16), rope(qkv[:, COLUMNS:512], cos, sin).astype(BF16), qkv[:, 512:].astype(BF16)

    load(0).wait()
    norm_tile(xs.at[0], even, gain_ref)
    for copy in weights:
        copy.wait()
    load(1).wait()
    span, q, k, v = project(0, even)
    norm_tile(xs.at[1], odd, gain_ref)
    q_s[span] = q
    held[me, 0] = k
    held[me, 1] = v
    prompt.start()
    for t in range(PAIR, 9):
        load(t).wait()
    spread = deal(TILE)

    @pl.loop(1, 9)
    def _(t):
        dealt = jnp.dot(spread, xs[t, :, pl.ds(column, COLUMNS)], preferred_element_type=F32).astype(BF16)
        res_stage[:, t - 1] = dealt.reshape(PEERS, TILE // PEERS, COLUMNS)

    res_router.send(0)
    res_out[me] = res_stage[me]

    def response_tile(t, here, there):
        span, q, k, v = project(t, here)
        norm_tile(xs.at[jnp.minimum(t + 1, 8)], there, gain_ref)
        q_s[span] = q
        own = pl.ds(pl.multiple_of((t - 1) * TILE, TILE), TILE)
        k_s[own] = k
        v_s[own] = v

    @pl.loop(0, RING)
    def _(i):
        response_tile(PAIR * i + 1, odd, even)
        response_tile(PAIR * i + PAIR, even, odd)
        pl.when(i == 0)(prompt.relay)
        pl.when(i == PAIR)(prompt.share)

    prompt.collect()
    for t in range(RING):
        mixed = attend_response(t, q_s[pl.ds(TILE + t * Q_TILE, Q_TILE)], held, k_s, v_s)
        deal_mixed(mixed_router, t, mixed, mixed_stage, mixed_out)
    row = lax.broadcasted_iota(jnp.int32, (TILE, PEERS * TILE), 0) + me * TILE
    col = lax.broadcasted_iota(jnp.int32, (TILE, PEERS * TILE), 1)
    prompt_out[:, :COLUMNS] = softmax_mix(q_s[pl.ds(0, TILE)], [(prompt_rows_of(held, 0), prompt_rows_of(held, 1), col <= row)])
    prompt_out[:, COLUMNS:] = xs[0, :, pl.ds(column, COLUMNS)]
    for router in (mixed_router, res_router):
        for t in range(router.tiles):
            router.collect(t)
        router.finish()
    net.collected(lambda d: info_out.at[d], info_recv)
    net.sent(lambda d: info_ref.at[d], info_send, info_recv)
    prompt.finish()


def first_attention(x_prompt, x_resp, w_query, w_key, w_value, gain, cos, sin, info, collective_id):
    rows = TILE + x_resp.shape[0]
    width = x_resp.shape[1]
    return pl.pallas_call(
        first_attention_kernel,
        out_shape=(jax.ShapeDtypeStruct((PEERS, RING, 32, COLUMNS), BF16), jax.ShapeDtypeStruct((PEERS, 8, 16, COLUMNS), BF16),
                   jax.ShapeDtypeStruct((PEERS, 8, 128), jnp.int32), jax.ShapeDtypeStruct((TILE, PAIR * COLUMNS), BF16)),
        in_specs=[ANY] * 5 + [VMEM] * 4,
        out_specs=(VMEM,) * 4,
        scratch_shapes=[
            pltpu.VMEM((9, TILE, width), BF16), pltpu.VMEM((width, 3 * COLUMNS), BF16), pltpu.VMEM((TILE, width), BF16), pltpu.VMEM((TILE, width), BF16),
            pltpu.VMEM((rows, COLUMNS), BF16), pltpu.VMEM((rows - TILE, COLUMNS), BF16), pltpu.VMEM((rows - TILE, COLUMNS), BF16),
            HELD, pltpu.VMEM((RING, PEERS, 32, COLUMNS), BF16), pltpu.VMEM((PEERS, 8, 16, COLUMNS), BF16),
            DMA((9,)), DMA((3,)), *GATHER_SEMS, DMA((PEERS,)), DMA((PEERS,)),
            *[DMA((RING, PEERS)) for _ in BOTH], *[DMA((1, PEERS)) for _ in BOTH],
        ],
        compiler_params=pltpu.CompilerParams(collective_id=collective_id, has_side_effects=True, vmem_limit_bytes=VMEM_BYTES),
        name="first_attention",
    )(x_prompt, x_resp, w_query, w_key, w_value, gain, cos, sin, info)


def second_attention_kernel(qkv_ref, back_ref, mixed_out, stage, qkv_in, k_s, v_s, held, mixed_stage,
                            ring_send, ring_recv, near_send, near_recv, *routes):
    net = Exchange()
    me = net.me
    prompt = PromptGather(net, held, ring_send, ring_recv, near_send, near_recv)
    router = Router(net, RING, lambda t, d: stage.at[t, d], lambda t, d: qkv_in.at[t, d], routes[:PAIR])
    mixed_router = Router(net, RING, lambda t, d: mixed_stage.at[t, d], lambda t, d: mixed_out.at[d, t], routes[PAIR:])
    for k in BOTH:
        held[me, k] = qkv_ref[0, :, pl.ds((k + 1) * COLUMNS, COLUMNS)]
    net.barrier()
    prompt.start()
    count = back_ref.shape[1]

    def send_rows(t):
        place = lax.broadcasted_iota(jnp.int32, (Q_TILE, count), 0) + t * Q_TILE == back_ref[...]
        rows = jnp.dot(place.astype(BF16), qkv_ref[1:].reshape(count, 3 * COLUMNS), preferred_element_type=F32).astype(BF16)
        stage[t] = rows.reshape(PEERS, Q_TILE // PEERS, 3 * COLUMNS)
        router.send(t)
        qkv_in[t, me] = stage[t, me]

    send_rows(0)
    prompt.relay()
    for t in range(1, RING):
        send_rows(t)
    prompt.share()
    prompt.collect()
    for t in range(RING):
        router.collect(t)
        rows = jnp.dot(undeal(Q_TILE), qkv_in[t].reshape(Q_TILE, 3 * COLUMNS), preferred_element_type=F32).astype(BF16)
        k_s[pl.ds(t * Q_TILE, Q_TILE)] = rows[:, COLUMNS:PAIR * COLUMNS]
        v_s[pl.ds(t * Q_TILE, Q_TILE)] = rows[:, PAIR * COLUMNS:]
        mixed = attend_response(t, rows[:, :COLUMNS], held, k_s, v_s)
        deal_mixed(mixed_router, t, mixed, mixed_stage, mixed_out)
    for t in range(RING):
        mixed_router.collect(t)
    for each in (router, mixed_router):
        each.finish()
    prompt.finish()


def second_attention(qkv, back, collective_id):
    rows = RING * Q_TILE
    wide = (32, 3 * COLUMNS)
    return pl.pallas_call(
        second_attention_kernel,
        out_shape=jax.ShapeDtypeStruct((PEERS, RING, 32, COLUMNS), BF16),
        in_specs=[VMEM, VMEM],
        out_specs=VMEM,
        scratch_shapes=[
            pltpu.VMEM((RING, PEERS) + wide, BF16), pltpu.VMEM((RING, PEERS) + wide, BF16),
            pltpu.VMEM((rows, COLUMNS), BF16), pltpu.VMEM((rows, COLUMNS), BF16),
            HELD, pltpu.VMEM((RING, PEERS, 32, COLUMNS), BF16), *GATHER_SEMS,
            *[DMA((RING, PEERS)) for _ in range(RING)],
        ],
        compiler_params=pltpu.CompilerParams(collective_id=collective_id, has_side_effects=True, vmem_limit_bytes=VMEM_BYTES),
        name=f"second_attention{collective_id}",
    )(qkv, back)


class Answer:
    def __init__(self, every, out_ref, stat_send, stat_recv, row_send, row_recv):
        self.every, self.out = every, out_ref
        self.stat_sems, self.row_sems = (stat_send, stat_recv), (row_send, row_recv)
        self.me, self.home = lax.axis_index("model"), lax.axis_index("resp")
        self.models = [(self.me + k) % SHARDS for k in range(1, SHARDS)]
        self.homes = [(self.home + k) % PEERS for k in range(1, PEERS)]

    def barrier(self):
        sem = pltpu.get_barrier_semaphore()
        for axis, devices in (("model", self.models), ("resp", self.homes)):
            for device in devices:
                pl.semaphore_signal(sem, device_id={axis: device}, device_id_type=MESH)
        pl.semaphore_wait(sem, len(self.models) + len(self.homes))

    def stat_copy(self, owner, device, place):
        ref = self.every.at[owner]
        return pltpu.make_async_remote_copy(
            src_ref=ref, dst_ref=ref, send_sem=self.stat_sems[0].at[device], recv_sem=self.stat_sems[1].at[place],
            device_id={"model": device}, device_id_type=MESH)

    def row_copy(self, owner, device, place):
        ref = self.out.at[owner]
        return pltpu.make_async_remote_copy(
            src_ref=ref, dst_ref=ref, send_sem=self.row_sems[0].at[device], recv_sem=self.row_sems[1].at[place],
            device_id={"resp": device}, device_id_type=MESH)

def combine_kernel(stats_ref, out_ref, every, *sems):
    net = Answer(every, out_ref, *sems)
    every[net.me] = stats_ref[...]
    net.barrier()
    for device in net.models:
        net.stat_copy(net.me, device, net.me).start()
    for device in net.models:
        net.stat_copy(device, device, device).wait_recv()
    found = []
    for c in range(stats_ref.shape[0]):
        tiles = [every[k, c] for k in range(SHARDS)]
        top = functools.reduce(jnp.maximum, [tile[:1] for tile in tiles])
        total = functools.reduce(jnp.add, [tile[1:PAIR] * jnp.exp(tile[:1] - top) for tile in tiles])
        found.append(functools.reduce(jnp.add, [tile[PAIR:3] for tile in tiles]) - top - jnp.log(total))
    out_ref[net.home] = jnp.concatenate(found, axis=0)
    for device in net.homes:
        net.row_copy(net.home, device, net.home).start()
    for device in net.homes:
        net.row_copy(device, device, device).wait_recv()
    for device in net.models:
        net.stat_copy(net.me, device, device).wait_send()
    for device in net.homes:
        net.row_copy(net.home, device, device).wait_send()


def combine(stats, collective_id):
    return pl.pallas_call(
        combine_kernel,
        out_shape=jax.ShapeDtypeStruct((PEERS, PEERS, LANES), F32),
        in_specs=[VMEM],
        out_specs=VMEM,
        scratch_shapes=[pltpu.VMEM((SHARDS,) + stats.shape, F32), *[DMA((SHARDS,)) for _ in BOTH], *[DMA((PEERS,)) for _ in BOTH]],
        compiler_params=pltpu.CompilerParams(collective_id=collective_id, has_side_effects=True),
        name="combine",
    )(stats)


ROPE_BASE = 10000.0
VARIANTS = (512, 640, 768, 1024)


def rope_tables(positions):
    half = LANES // PAIR
    lane = jnp.arange(LANES)
    frequency = ROPE_BASE ** (-(lane % half).astype(F32) / half)
    angles = positions.astype(F32)[:, None] * frequency
    return jnp.cos(angles), jnp.sin(angles) * jnp.where(lane < half, -1.0, 1.0)


def solution(mesh):
    groups = mesh.shape['resp']
    row_axes = ('prompts', 'resp')
    head_spec = P(None, None, 'model', None)
    in_specs = (P(row_axes, None), P(row_axes, None, None), P(row_axes, None), P(row_axes), P(None, None), head_spec, head_spec, head_spec, P(None, 'model', None, None), P(None, None), P(None, None, 'model'), P(None, None, 'model'), P(None, 'model', None), P(None), P(None, 'model'))

    def device_step(x_prompt, x_resp, targets, resp_lens, attn_gain, w_query, w_key, w_value, w_out, mlp_gain, w_gate, w_up, w_down, final_gain, w_vocab):
        prompt_rows = x_prompt.shape[0]
        resp_len, width = x_resp.shape[1:]
        prompt_len = prompt_rows * groups
        me = lax.axis_index('model')
        home = lax.axis_index('resp')
        per = resp_len // groups
        gate_t, up_t = jnp.swapaxes(w_gate, 1, 2), jnp.swapaxes(w_up, 1, 2)
        out_flat = w_out.reshape(w_out.shape[0], COLUMNS, width)
        projections = [w.reshape(w.shape[0], width, COLUMNS) for w in (w_query, w_key, w_value)]
        prompt_pos = home * prompt_rows + jnp.arange(prompt_rows)

        cos, sin = rope_tables(jnp.concatenate([prompt_pos, prompt_len + jnp.arange(resp_len)]))
        info = jnp.concatenate([
            targets[0].reshape(per, groups).T[:, None, :],
            jnp.broadcast_to(resp_lens[0], (groups, groups - 1, per)).astype(jnp.int32)], axis=1)
        mixed, res, infos, prompt = first_attention(
            x_prompt, x_resp[0], *projections, attn_gain, cos, sin, info, 0)
        lens = infos[:, 1, 0]
        need = (lens + groups - 1) // groups
        ends = jnp.sum(jnp.where(jnp.arange(groups)[:, None] >= jnp.arange(groups), need, 0), axis=1)
        starts = ends - need
        dealt = groups * per

        def finish_with(size, ident):
            def run(operands):
                mixed, res, prompt = operands
                slot = jnp.arange(size)
                which = jnp.sum((slot[:, None] >= ends).astype(jnp.int32), axis=1)
                row = slot - jnp.sum(jnp.where(which[:, None] == jnp.arange(groups), starts, 0), axis=1)
                real = slot < ends[-1]
                source = jnp.where(real, which * per + row, -1)
                chosen = source[:, None] == jnp.arange(dealt)
                wanted = jnp.sum(jnp.where(chosen, infos[:, 0, :].reshape(dealt), 0), axis=1) - me * w_vocab.shape[1]
                ids = jnp.where(jnp.arange(LANES) == 0, source[:, None], wanted[:, None]).reshape(-1, LANES, LANES)
                tables = rope_tables(jnp.concatenate([prompt_pos, prompt_len + groups * row + home]))
                weights = (out_flat, gate_t, up_t, w_down)
                qkv, new_res = mega(
                    mlp_gain, attn_gain, ids, mixed.reshape(dealt, COLUMNS), res.reshape(dealt, COLUMNS),
                    [t.reshape(-1, LANES, LANES) for t in tables] + [prompt], *weights, projections, 0, ident)
                part = per // RING
                back = jnp.where(real, (row // part) * (groups * part) + which * part + row % part, -1)
                mixed = second_attention(qkv, back[None], ident + 1)
                return mega(mlp_gain, final_gain[None], ids, mixed.reshape(dealt, COLUMNS), new_res, [], *weights, [w_vocab], 1, ident + PAIR)
            return run

        index = sum((ends[-1] > size).astype(jnp.int32) for size in VARIANTS[:-1])
        stats = lax.switch(index, [finish_with(size, PAIR + 3 * i) for i, size in enumerate(VARIANTS)], (mixed, res, prompt))
        found = combine(stats, 1).reshape(groups, dealt)
        start = jnp.sum(jnp.where(jnp.arange(groups) == home, starts, 0))
        mine = lax.dynamic_slice(jnp.pad(found, ((0, 0), (0, per))), (0, start), (groups, per))
        log_probs = mine.T.reshape(resp_len)
        log_probs = jnp.where(jnp.arange(resp_len) < resp_lens[0], log_probs, 0.0)
        return log_probs[None, :]

    return jax.shard_map(device_step, mesh=mesh, in_specs=in_specs, out_specs=P(row_axes, None), check_vma=False)
```

```python
import functools

import jax
import jax.numpy as jnp
from jax import lax
from jax.experimental import pallas as pl
from jax.experimental.pallas import tpu as pltpu
from jax.sharding import PartitionSpec as P

MESH = pl.DeviceIdType.MESH
F32 = jnp.float32
BF16 = jnp.bfloat16
EPS = 1e-6
LANES = 128
PAIR = 2
RING = 4
COLUMNS = PAIR * LANES
SHARDS = RING * RING
PEERS = 8
BOTH = range(PAIR)
VMEM_BYTES = 67_000_000
LATE_ROWS = 640
LOGITS = 512
VMEM = pl.BlockSpec(memory_space=pltpu.VMEM)
ANY = pl.BlockSpec(memory_space=pl.ANY)
DMA = pltpu.SemaphoreType.DMA
KINDS = range(RING * 3)
SUM_FAR, SUM_NEAR, SUM_RELAY, SUM2_FAR, SUM2_NEAR, SUM2_RELAY, TAKE_OWN, TAKE_REST, TAKE_RELAY, TAKE2_OWN, TAKE2_REST, TAKE2_RELAY = KINDS


def block_of(color, first, second):
    return RING * first + second if color else RING * second + first


def pair(index):
    return pl.ds(PAIR * index, PAIR)


class Torus:
    def __init__(self, refs, send_sem, recv_sem):
        self.refs = refs
        self.far, self.near, self.relayed, self.sums, self.relayed2, self.sums2, self.rows = refs
        self.send_sem, self.recv_sem = send_sem, recv_sem
        me = lax.axis_index("model")
        z, y = me // RING, me % RING
        self.place = ((y, z), (z, y))
        along_y = [z * RING + self.step(y, way) for way in (1, -1)]
        along_z = [self.step(z, way) * RING + y for way in (1, -1)]
        self.neighbors = ((along_y, along_z), (along_z, along_y))

    def step(self, place, by):
        return (place + by + RING) % RING

    def barrier(self):
        sem = pltpu.get_barrier_semaphore()
        for ring in self.neighbors[0]:
            for device in ring:
                pl.semaphore_signal(sem, device_id={"model": device}, device_id_type=MESH)
        pl.semaphore_wait(sem, RING)

    def ends(self, kind, c, q, d):
        (p, s), way, other = self.place[q], 1 - PAIR * d, 1 - d
        far, near, relayed, sums, relayed2, sums2, rows = (ref.at[c, q] for ref in self.refs)
        own = sums.at[0]
        back_s, back_p = self.step(s, -way), self.step(p, -way)
        return {
            SUM_FAR: lambda: (far.at[pair(d)], relayed.at[d], relayed.at[d]),
            SUM_NEAR: lambda: (near.at[d], sums.at[d, pair(other)], sums.at[d, pair(other)]),
            SUM_RELAY: lambda: (relayed.at[d], sums.at[d, pair(d)], sums.at[d, pair(d)]),
            SUM2_FAR: lambda: (own.at[self.step(s, PAIR), d], relayed2.at[d], relayed2.at[d]),
            SUM2_NEAR: lambda: (own.at[self.step(s, way), other], sums2.at[d, other], sums2.at[d, other]),
            SUM2_RELAY: lambda: (relayed2.at[d], sums2.at[d, d], sums2.at[d, d]),
            TAKE_OWN: lambda: (rows.at[p, s, d], rows.at[p, s, d], rows.at[p, back_s, d]),
            TAKE_REST: lambda: (rows.at[p, s, other], rows.at[p, s, other], rows.at[p, back_s, other]),
            TAKE_RELAY: lambda: (rows.at[p, back_s, d], rows.at[p, back_s, d], rows.at[p, self.step(s, PAIR), d]),
            TAKE2_OWN: lambda: (rows.at[p, pair(d)], rows.at[p, pair(d)], rows.at[back_p, pair(d)]),
            TAKE2_REST: lambda: (rows.at[p, pair(other)], rows.at[p, pair(other)], rows.at[back_p, pair(other)]),
            TAKE2_RELAY: lambda: (rows.at[back_p, pair(d)], rows.at[back_p, pair(d)], rows.at[self.step(p, PAIR), pair(d)]),
        }[kind]()

    def copy(self, kind, c, q, d, src, dst):
        second_ring = kind in (SUM2_FAR, SUM2_NEAR, SUM2_RELAY, TAKE_OWN, TAKE_REST, TAKE_RELAY)
        return pltpu.make_async_remote_copy(
            src_ref=src, dst_ref=dst, send_sem=self.send_sem.at[c, q, d, kind], recv_sem=self.recv_sem.at[c, q, d, kind],
            device_id={"model": self.neighbors[q][second_ring][d]}, device_id_type=MESH)

    def send(self, c, q, d, kind):
        src, dst, _ = self.ends(kind, c, q, d)
        self.copy(kind, c, q, d, src, dst).start()

    def sent(self, c, q, *kinds):
        for kind in kinds:
            for d in BOTH:
                src, dst, _ = self.ends(kind, c, q, d)
                self.copy(kind, c, q, d, src, dst).wait_send()

    def arrived(self, c, q, d, *kinds):
        for kind in kinds:
            _, _, here = self.ends(kind, c, q, d)
            self.copy(kind, c, q, d, here, here).wait_recv()


def halves(value):
    return value[:, :LANES], value[:, LANES:]


def store_block(ref, value):
    for half, part in enumerate(halves(value)):
        ref[half] = part


def add_block(ref, value):
    for half, part in enumerate(halves(value)):
        ref[half] += part


class Stage:
    def __init__(self, net, lhs_of, w_ref, finish):
        self.net, self.lhs_of, self.w_ref, self.finish = net, lhs_of, w_ref, finish

    def product(self, lhs, color, first, second):
        start = pl.multiple_of(block_of(color, first, second) * COLUMNS, COLUMNS)
        return jnp.dot(lhs, self.w_ref[:, pl.ds(start, COLUMNS)], preferred_element_type=F32)

    def begin(self, c, q):
        net, p, lhs = self.net, self.net.place[q][0], self.lhs_of(c, q)
        for k in range(RING):
            store_block(net.far.at[c, q, k], self.product(lhs, q, net.step(p, PAIR), k))
        for d in BOTH:
            net.send(c, q, d, SUM_FAR)
        for d in BOTH:
            for k in BOTH:
                store_block(net.near.at[c, q, d, k], self.product(lhs, q, net.step(p, 1 - PAIR * d), PAIR * (1 - d) + k))
            net.send(c, q, d, SUM_NEAR)

    def relay_sum(self, c, q):
        net, p, lhs = self.net, self.net.place[q][0], self.lhs_of(c, q)
        for d in BOTH:
            net.arrived(c, q, d, SUM_FAR)
            for k in BOTH:
                add_block(net.relayed.at[c, q, d, k], self.product(lhs, q, net.step(p, 1 - PAIR * d), PAIR * d + k))
            net.send(c, q, d, SUM_RELAY)

    def begin_second(self, c, q):
        net, lhs = self.net, self.lhs_of(c, q)
        for d in BOTH:
            net.arrived(c, q, d, SUM_NEAR, SUM_RELAY)
        for k in range(RING):
            for half, part in enumerate(halves(self.product(lhs, q, net.place[q][0], k))):
                net.sums[c, q, 0, k, half] += net.sums[c, q, 1, k, half] + part
        for kind in (SUM2_FAR, SUM2_NEAR):
            for d in BOTH:
                net.send(c, q, d, kind)
        net.sent(c, q, SUM_FAR)

    def relay_second(self, c, q):
        net = self.net
        for d in BOTH:
            net.arrived(c, q, d, SUM2_FAR)
            net.relayed2[c, q, d] += net.sums[c, q, 0, net.step(net.place[q][1], 1 - PAIR * d), d]
            net.send(c, q, d, SUM2_RELAY)

    def finish_sum(self, c, q):
        net = self.net
        net.sent(c, q, SUM_NEAR, SUM_RELAY)
        for d in BOTH:
            net.arrived(c, q, d, SUM2_NEAR, SUM2_RELAY)
        for half in BOTH:
            self.finish(c, q, half, net.sums[c, q, 0, net.place[q][1], half] + net.sums2[c, q, 0, half] + net.sums2[c, q, 1, half])
        for kind in (TAKE_OWN, TAKE_REST):
            for d in BOTH:
                net.send(c, q, d, kind)

    def relay_rows(self, c, q):
        net = self.net
        net.sent(c, q, SUM2_FAR, SUM2_NEAR, SUM2_RELAY)
        for d in BOTH:
            net.arrived(c, q, d, TAKE_OWN)
            net.send(c, q, d, TAKE_RELAY)

    def take_second(self, c, q):
        net = self.net
        for d in BOTH:
            net.arrived(c, q, d, TAKE_REST, TAKE_RELAY)
        for kind in (TAKE2_OWN, TAKE2_REST):
            for d in BOTH:
                net.send(c, q, d, kind)

    def relay_last(self, c, q):
        net = self.net
        for d in BOTH:
            net.arrived(c, q, d, TAKE2_OWN)
            net.send(c, q, d, TAKE2_RELAY)

    def complete(self, c, q):
        net = self.net
        for d in BOTH:
            net.arrived(c, q, d, TAKE2_REST, TAKE2_RELAY)
        net.sent(c, q, TAKE_OWN, TAKE_REST, TAKE_RELAY, TAKE2_OWN, TAKE2_REST, TAKE2_RELAY)

    def middle(self):
        return [self.relay_sum, self.begin_second, self.relay_second, self.finish_sum, self.relay_rows, self.take_second, self.relay_last]


def normed(net, c, q, gain_ref, layer):
    rows = net.rows.shape[-PAIR]
    tile = PAIR * 8 if rows % (PAIR * 8) == 0 else 8
    spots = [(first, second, half) for first in range(RING) for second in range(RING) for half in BOTH]

    @pl.loop(0, rows // tile)
    def _(i):
        span = pl.ds(pl.multiple_of(i * tile, tile), tile)
        acts = [net.rows[(c, q) + spot + (span,)].astype(F32) for spot in spots]
        squares = functools.reduce(jnp.add, [v * v for v in acts])
        inv = lax.rsqrt(jnp.sum(squares, axis=-1, keepdims=True) / (LANES * len(acts)) + EPS)
        for spot, v in zip(spots, acts):
            column = block_of(q, *spot[:PAIR]) * COLUMNS + spot[PAIR] * LANES
            net.rows[(c, q) + spot + (span,)] = (v * inv * gain_ref[pl.ds(layer, 1), pl.ds(column, LANES)]).astype(BF16)


def rows_of(net, c, q):
    parts = []
    for upper in range(RING):
        for lower in range(RING):
            first, second = (upper, lower) if q else (lower, upper)
            parts += [net.rows[c, q, first, second, half] for half in BOTH]
    return jnp.concatenate(parts, axis=1)


def times_transposed(lhs, rhs):
    return lax.dot_general(lhs, rhs, (((1,), (1,)), ((), ())), preferred_element_type=F32)


def late_plan(width, count):
    plan, start = [], 0
    for buffer in BOTH:
        for slot in range(width // count):
            size = min(LATE_ROWS, width - start)
            if size:
                plan.append((buffer, slot * count, start, size))
            start += size
    return plan, width - start


def rope(value, cos, sin):
    return jnp.concatenate([v * cos + pltpu.roll(v, LANES // PAIR, 1) * sin for v in halves(value)], axis=1)


def put_projected(product, cos_ref, sin_ref, out_ref, c):
    for k in range(3):
        value = product(k * COLUMNS, COLUMNS)
        if k < PAIR:
            value = rope(value, cos_ref[c], sin_ref[c])
        out_ref[c, :, pl.ds(k * COLUMNS, COLUMNS)] = value.astype(BF16)


def statistics(product, count, target):
    top = total = picked = None
    for k in range(count // LOGITS):
        logits = product(k * LOGITS, LOGITS)
        here = jnp.max(logits, axis=-1, keepdims=True)
        ids = lax.broadcasted_iota(jnp.int32, logits.shape, 1) + k * LOGITS
        found = jnp.sum(jnp.where(ids == target, logits, 0.0), axis=-1, keepdims=True)
        if k:
            both = jnp.maximum(top, here)
            total = total * jnp.exp(top - both) + jnp.sum(jnp.exp(logits - both), axis=-1, keepdims=True)
            top, picked = both, picked + found
        else:
            top, total, picked = here, jnp.sum(jnp.exp(logits - here), axis=-1, keepdims=True), found
    lane = lax.broadcasted_iota(jnp.int32, (LANES, LANES), 1)
    return jnp.where(lane == 0, top, jnp.where(lane == 1, total, picked)).T[:PEERS]


def mega_kernel(chunks, layer, last, gain_ref, next_gain_ref, ids_ref, dealt_ref, old_ref, *args):
    if last:
        side_refs, args = (), args
    else:
        side_refs, args = args[:3], args[3:]
    w_out_hbm, w_gate_hbm, w_up_hbm, w_down_hbm, *args = args
    late_hbm, out_ref, *args = args
    if not last:
        new_res_ref, *args = args
    (w_out, w_gate, w_up, w_down, late_rest, acts, res, inner, middle,
     far, near, relayed, sums, relayed2, sums2, rows, w_sem, late_sem, send_sem, recv_sem) = args
    loads = [pltpu.make_async_copy(src.at[layer], dst, w_sem.at[i]) for i, (src, dst) in enumerate(
        ((w_out_hbm, w_out), (w_gate_hbm, w_gate), (w_up_hbm, w_up), (w_down_hbm, w_down)))]
    for load in loads:
        load.start()
    width, count = late_hbm.shape
    plan, left = late_plan(width, count)
    late = [(late_hbm.at[pl.ds(start, size)], (w_gate, w_up)[buffer].at[pl.ds(0, size), pl.ds(lane, count)]) for buffer, lane, start, size in plan]
    if left:
        late.append((late_hbm.at[pl.ds(width - left, left)], late_rest))
    late_loads = [pltpu.make_async_copy(src, dst, late_sem.at[i]) for i, (src, dst) in enumerate(late)]
    net = Torus((far, near, relayed, sums, relayed2, sums2, rows), send_sem, recv_sem)
    net.barrier()
    loads[0].wait()
    if last:
        new_res_ref = middle
        out_ref[...] = jnp.zeros_like(out_ref)

    def picked(ids, ref):
        chosen = (ids == lax.broadcasted_iota(jnp.int32, (LANES, PEERS * LANES), 1)).astype(BF16)
        return jnp.dot(chosen, ref[...], preferred_element_type=F32).astype(BF16)

    def put(c, mixed, columns):
        for q in BOTH:
            span = slice(q * acts.shape[PAIR], (q + 1) * acts.shape[PAIR])
            acts[c, q] = mixed[span]
            for half, part in enumerate(halves(columns) if columns is not None else ()):
                res[c, q, half] = part[span]

    def begin(c):
        if last:
            put(c, picked(ids_ref[c, :, :1], dealt_ref), None)
        else:
            @pl.when(c == 0)
            def _():
                put(c, side_refs[PAIR][:, :COLUMNS], side_refs[PAIR][:, COLUMNS:])

            @pl.when(c > 0)
            def _():
                ids = ids_ref[c - 1, :, :1]
                put(c, picked(ids, dealt_ref), picked(ids, old_ref))
        for q in BOTH:
            first.begin(c, q)

    def finish_with(old_ref, new_ref, skip=0):
        def finish(c, q, half, total):
            value = (old_ref[c + skip, q, half].astype(F32) + total).astype(BF16)
            new_ref[c, q, half] = value
            rows[(c, q) + net.place[q] + (half,)] = value
        return finish

    first = Stage(net, lambda c, q: acts[c, q], w_out, finish_with(old_ref if last else res, middle, last))
    second = Stage(net, lambda c, q: inner[c, q], w_down, finish_with(middle, new_res_ref))

    def hidden_of(c, stage, gain, row):
        for q in BOTH:
            stage.complete(c, q)
            normed(net, c, q, gain, row)
        return jnp.concatenate([rows_of(net, c, q) for q in BOTH], axis=0)

    def mlp(c):
        hidden = hidden_of(c, first, gain_ref, layer)
        value = (jax.nn.silu(times_transposed(hidden, w_gate[...])) * times_transposed(hidden, w_up[...])).astype(BF16)
        inner[c] = value.reshape(inner.shape[1:])
        for q in BOTH:
            second.begin(c, q)

    def after(c):
        hidden = hidden_of(c, second, next_gain_ref, 0 if last else layer + 1)

        def product(lane, size):
            parts = [jnp.dot(hidden[:, start:start + rows_here], (w_gate, w_up)[buffer][pl.ds(0, rows_here), pl.ds(at + lane, size)], preferred_element_type=F32)
                     for buffer, at, start, rows_here in plan]
            if left:
                parts.append(jnp.dot(hidden[:, width - left:], late_rest[:, pl.ds(lane, size)], preferred_element_type=F32))
            return functools.reduce(jnp.add, parts)

        if last:
            out_ref[c] = statistics(product, count, ids_ref[c, :, 1:PAIR])
        else:
            put_projected(product, *side_refs[:PAIR], out_ref, c)

    def on_both(step):
        def run(c):
            for q in BOTH:
                step(c, q)
        return run

    steps = [begin, *map(on_both, first.middle()), mlp, *map(on_both, second.middle())]
    at_mlp = steps.index(mlp)
    steps += [None] * max(0, at_mlp + chunks - len(steps)) + [after]

    @pl.loop(0, len(steps) + chunks - 1)
    def _(slot):
        @pl.when(slot == at_mlp)
        def _():
            for load in loads[1:]:
                load.wait()

        @pl.when(slot == len(steps) - 1)
        def _():
            for load in late_loads:
                load.wait()

        for k, step in reversed(list(enumerate(steps))):
            if step is None:
                continue

            @pl.when(slot >= k)
            def _():
                @pl.when(slot < k + chunks)
                def _():
                    step(slot - k)

        @pl.when(slot == at_mlp + chunks - 1)
        def _():
            for load in late_loads:
                load.start()


def mega(gain, next_gain, ids, dealt, old, sides, w_out, w_gate_t, w_up_t, w_down, late, layer, collective_id):
    last = not sides
    chunks = ids.shape[0] + (not last)
    _, depth, width = w_out.shape
    hidden = w_gate_t.shape[1]
    rows = LANES // PAIR
    per = (chunks, PAIR)
    tile = (rows, LANES)
    count = late.shape[1]
    _, left = late_plan(width, count)

    sem = DMA(per + (PAIR, len(KINDS)))
    out = jax.ShapeDtypeStruct((PEERS, PEERS, LANES), F32) if last else (
        jax.ShapeDtypeStruct((chunks, LANES, count), BF16), jax.ShapeDtypeStruct(per + (PAIR,) + tile, BF16))
    return pl.pallas_call(
        functools.partial(mega_kernel, chunks, layer, last),
        out_shape=out,
        in_specs=[VMEM] * (5 + len(sides)) + [ANY] * 5,
        out_specs=VMEM if last else (VMEM, VMEM),
        scratch_shapes=[
            pltpu.VMEM((depth, width), BF16),
            *[pltpu.VMEM((hidden, width), BF16) for _ in range(3)],
            pltpu.VMEM((left or 8, count), BF16),
            pltpu.VMEM(per + (rows, depth), BF16),
            pltpu.VMEM(per + (PAIR,) + (tile if not last else (8, LANES)), BF16),
            pltpu.VMEM(per + (rows, hidden), BF16),
            pltpu.VMEM(per + (PAIR,) + tile, BF16),
            pltpu.VMEM(per + (RING, PAIR) + tile, F32),
            pltpu.VMEM(per + (PAIR, PAIR, PAIR) + tile, F32),
            pltpu.VMEM(per + (PAIR, PAIR, PAIR) + tile, F32),
            pltpu.VMEM(per + (PAIR, RING, PAIR) + tile, F32),
            pltpu.VMEM(per + (PAIR,) + tile, F32),
            pltpu.VMEM(per + (PAIR, PAIR) + tile, F32),
            pltpu.VMEM(per + (RING, RING, PAIR) + tile, BF16),
            DMA((RING,)), DMA((SHARDS,)), sem, sem,
        ],
        compiler_params=pltpu.CompilerParams(collective_id=collective_id, has_side_effects=True, vmem_limit_bytes=VMEM_BYTES),
        name=f"mega{collective_id}",
    )(gain, next_gain, ids, dealt, old, *sides, w_out, w_gate_t, w_up_t, w_down, late)


TILE = 128
Q_TILE = 256
LOG2E = 1.4426950408889634
HELD = pltpu.VMEM((PEERS, PAIR, TILE, COLUMNS), BF16)
GATHER_SEMS = [DMA((PAIR, 3)), DMA((PAIR, 3)), DMA((RING,)), DMA((RING,))]


class Exchange:
    def __init__(self):
        self.me = lax.axis_index("resp")
        self.others = [(self.me + k) % PEERS for k in range(1, PEERS)]

    def barrier(self):
        sem = pltpu.get_barrier_semaphore()
        for device in self.others:
            pl.semaphore_signal(sem, inc=1, device_id={"resp": device}, device_id_type=MESH)
        pl.semaphore_wait(sem, PEERS - 1)

    def copy(self, src, dst, send_sem, recv_sem, device):
        return pltpu.make_async_remote_copy(src_ref=src, dst_ref=dst, send_sem=send_sem, recv_sem=recv_sem,
                                            device_id={"resp": device}, device_id_type=MESH)

    def scatter(self, src_of, dst, send_sem, recv_sem):
        for device in self.others:
            self.copy(src_of(device), dst, send_sem.at[device], recv_sem.at[self.me], device).start()

    def collected(self, dst_of, recv_sem):
        for device in self.others:
            self.copy(dst_of(device), dst_of(device), recv_sem.at[device], recv_sem.at[device], device).wait_recv()

    def sent(self, src_of, send_sem, recv_sem):
        for device in self.others:
            self.copy(src_of(device), src_of(device), send_sem.at[device], recv_sem.at[device], device).wait_send()


class Router:
    def __init__(self, net, tiles, src_of, dst_of, sems):
        self.net, self.tiles, self.src_of, self.dst_of = net, tiles, src_of, dst_of
        self.send_sem, self.recv_sem = sems

    def send(self, t):
        self.net.scatter(lambda d: self.src_of(t, d), self.dst_of(t, self.net.me), self.send_sem.at[t], self.recv_sem.at[t])

    def collect(self, t):
        self.net.collected(lambda d: self.dst_of(t, d), self.recv_sem.at[t])

    def finish(self):
        for t in range(self.tiles):
            self.net.sent(lambda d: self.src_of(t, d), self.send_sem.at[t], self.recv_sem.at[t])


class PromptGather:
    def __init__(self, net, held, ring_send, ring_recv, near_send, near_recv):
        self.net, self.held = net, held
        self.ring_sems, self.near_sems = (ring_send, ring_recv), (near_send, near_recv)
        x, core = net.me // PAIR, net.me % PAIR
        self.at = lambda by, here: (x + by + RING) % RING * PAIR + (core if here else 1 - core)

    def ring_copy(self, d, kind, ref):
        return self.net.copy(ref, ref, self.ring_sems[0].at[d, kind], self.ring_sems[1].at[d, kind], self.at(1 - PAIR * d, True))

    def near_copy(self, kind, ref):
        return self.net.copy(ref, ref, self.near_sems[0].at[kind], self.near_sems[1].at[kind], self.at(0, False))

    def sources(self, here):
        return [self.at(by, here) for by in (0, -1, 1, PAIR)]

    def start(self):
        own = self.held.at[self.net.me]
        for kind in BOTH:
            for d in BOTH:
                self.ring_copy(d, kind, own.at[1 - d if kind else d]).start()
        self.near_copy(0, own).start()

    def relay(self):
        for d in BOTH:
            ref = self.held.at[self.at(PAIR * d - 1, True), d]
            self.ring_copy(d, 0, ref).wait_recv()
            self.ring_copy(d, PAIR, ref).start()

    def share(self):
        for d in BOTH:
            device = self.at(PAIR * d - 1, True)
            self.ring_copy(d, 1, self.held.at[device, 1 - d]).wait_recv()
            self.near_copy(1 + d, self.held.at[device]).start()
        far = self.held.at[self.at(PAIR, True)]
        for d in BOTH:
            self.ring_copy(d, PAIR, far.at[d]).wait_recv()
        self.near_copy(3, far).start()

    def collect(self):
        for kind, device in enumerate(self.sources(False)):
            self.near_copy(kind, self.held.at[device]).wait_recv()

    def finish(self):
        for kind in range(3):
            for d in BOTH:
                self.ring_copy(d, kind, self.held.at[self.net.me, d]).wait_send()
        for kind in range(RING):
            self.near_copy(kind, self.held.at[self.net.me]).wait_send()


def deal(rows):
    out = lax.broadcasted_iota(jnp.int32, (rows, rows), 0)
    src = lax.broadcasted_iota(jnp.int32, (rows, rows), 1)
    per = rows // PEERS
    return jnp.where(src == (out % per) * PEERS + out // per, 1.0, 0.0).astype(BF16)


def undeal(rows):
    out = lax.broadcasted_iota(jnp.int32, (rows, rows), 0)
    src = lax.broadcasted_iota(jnp.int32, (rows, rows), 1)
    per = rows // PEERS
    return jnp.where(src == (out % PEERS) * per + out // PEERS, 1.0, 0.0).astype(BF16)


def split_heads(raw_ref, w_ref):
    tile = PAIR * LANES
    out = lax.broadcasted_iota(jnp.int32, (tile, tile), 0)
    src = lax.broadcasted_iota(jnp.int32, (tile, tile), 1)
    pick = jnp.where(src == (out % LANES) * PAIR + out // LANES, 1.0, 0.0).astype(BF16)

    @pl.loop(0, raw_ref.shape[1] // tile)
    def _(b):
        rows = pl.ds(pl.multiple_of(b * tile, tile), tile)
        here = pl.ds(pl.multiple_of(b * LANES, LANES), LANES)
        heads = jnp.dot(pick, jnp.concatenate([raw_ref[i, rows] for i in range(3)], axis=1), preferred_element_type=F32).astype(BF16)
        for i in range(3):
            for h in BOTH:
                w_ref[here, pl.ds(i * COLUMNS + h * LANES, LANES)] = heads[h * LANES:(h + 1) * LANES, i * LANES:(i + 1) * LANES]


def norm_tile(x_ref, out_ref, gain_ref):
    for i in range(x_ref.shape[0] // 16):
        v = x_ref[pl.ds(16 * i, 16), :].astype(F32)
        inv = lax.rsqrt(jnp.mean(v * v, axis=-1, keepdims=True) + EPS)
        out_ref[pl.ds(16 * i, 16), :] = (v * inv * gain_ref[pl.ds(0, 1), :]).astype(BF16)


def softmax_mix(q, pieces):
    factor = LOG2E * 128 ** -0.5
    outs = []
    for h in range(2):
        lanes = slice(128 * h, 128 * h + 128)
        scores = []
        for keys, _, mask in pieces:
            s = lax.dot_general(q[:, lanes], keys[:, lanes], (((1,), (1,)), ((), ())), preferred_element_type=F32)
            scores.append(s if mask is None else jnp.where(mask, s, -jnp.inf))
        top = functools.reduce(jnp.maximum, [jnp.max(s, axis=-1, keepdims=True) for s in scores])
        probs = [jnp.exp2((s - top) * factor) for s in scores]
        total = functools.reduce(jnp.add, [jnp.sum(p, axis=-1, keepdims=True) for p in probs])
        mixed = functools.reduce(jnp.add, [jnp.dot(p.astype(BF16), values[:, lanes], preferred_element_type=F32) for p, (_, values, _) in zip(probs, pieces)])
        outs.append(mixed / total)
    return jnp.concatenate(outs, axis=1).astype(BF16)


def prompt_rows_of(held, which):
    return held[:, which].reshape(PEERS * TILE, COLUMNS)


def attend_response(t, q, held, k_own, v_own):
    row = lax.broadcasted_iota(jnp.int32, (Q_TILE, Q_TILE), 0)
    col = lax.broadcasted_iota(jnp.int32, (Q_TILE, Q_TILE), 1)
    pieces = [(prompt_rows_of(held, 0), prompt_rows_of(held, 1), None)]
    if t:
        pieces.append((k_own[:t * Q_TILE], v_own[:t * Q_TILE], None))
    span = slice(t * Q_TILE, (t + 1) * Q_TILE)
    pieces.append((k_own[span], v_own[span], col <= row))
    return softmax_mix(q, pieces)


def deal_mixed(router, t, mixed, stage, out):
    dealt = jnp.dot(deal(Q_TILE), mixed, preferred_element_type=F32).astype(BF16)
    stage[t] = dealt.reshape(PEERS, Q_TILE // PEERS, COLUMNS)
    router.send(t)
    out[router.net.me, t] = stage[t, router.net.me]


def first_attention_kernel(xp_hbm, xr_hbm, wq_hbm, wk_hbm, wv_hbm, gain_ref, cos_ref, sin_ref, info_ref,
                           mixed_out, res_out, info_out, prompt_out, next_hbm,
                           xs, raw, w, even, odd, q_s, k_s, v_s, held, mixed_stage, res_stage,
                           x_sem, w_sem, ring_send, ring_recv, near_send, near_recv, info_send, info_recv, *routes):
    net = Exchange()
    mixed_router = Router(net, RING, lambda t, d: mixed_stage.at[t, d], lambda t, d: mixed_out.at[d, t], routes[:PAIR])
    res_router = Router(net, 1, lambda t, d: res_stage.at[d], lambda t, d: res_out.at[d], routes[PAIR:])
    prompt = PromptGather(net, held, ring_send, ring_recv, near_send, near_recv)
    me = net.me
    column = pl.multiple_of(lax.axis_index("model") * COLUMNS, COLUMNS)

    def load(t):
        src = xp_hbm if isinstance(t, int) and t == 0 else xr_hbm.at[pl.ds(pl.multiple_of((t - 1) * TILE, TILE), TILE)]
        return pltpu.make_async_copy(src, xs.at[t], x_sem.at[t])

    load(0).start()
    weights, next_weights = ([pltpu.make_async_copy(src.at[layer], raw.at[i], w_sem.at[i]) for i, src in enumerate((wq_hbm, wk_hbm, wv_hbm))] for layer in BOTH)
    for copy in weights:
        copy.start()
    for t in range(1, 9):
        load(t).start()
    net.barrier()
    net.scatter(lambda d: info_ref.at[d], info_out.at[me], info_send, info_recv)
    info_out[me] = info_ref[me]

    def project(t, hidden):
        span = pl.ds(pl.multiple_of(t * TILE, TILE), TILE)
        qkv = jnp.dot(hidden[...], w[...], preferred_element_type=F32)
        cos, sin = cos_ref[span], sin_ref[span]
        return span, rope(qkv[:, :COLUMNS], cos, sin).astype(BF16), rope(qkv[:, COLUMNS:512], cos, sin).astype(BF16), qkv[:, 512:].astype(BF16)

    load(0).wait()
    norm_tile(xs.at[0], even, gain_ref)
    for copy in weights:
        copy.wait()
    split_heads(raw, w)
    for copy in next_weights:
        copy.start()
    load(1).wait()
    span, q, k, v = project(0, even)
    norm_tile(xs.at[1], odd, gain_ref)
    q_s[span] = q
    held[me, 0] = k
    held[me, 1] = v
    prompt.start()
    for t in range(PAIR, 9):
        load(t).wait()
    spread = deal(TILE)

    @pl.loop(1, 9)
    def _(t):
        dealt = jnp.dot(spread, xs[t, :, pl.ds(column, COLUMNS)], preferred_element_type=F32).astype(BF16)
        res_stage[:, t - 1] = dealt.reshape(PEERS, TILE // PEERS, COLUMNS)

    res_router.send(0)
    res_out[me] = res_stage[me]

    def response_tile(t, here, there):
        span, q, k, v = project(t, here)
        norm_tile(xs.at[jnp.minimum(t + 1, 8)], there, gain_ref)
        q_s[span] = q
        own = pl.ds(pl.multiple_of((t - 1) * TILE, TILE), TILE)
        k_s[own] = k
        v_s[own] = v

    @pl.loop(0, RING)
    def _(i):
        response_tile(PAIR * i + 1, odd, even)
        response_tile(PAIR * i + PAIR, even, odd)
        pl.when(i == 0)(prompt.relay)
        pl.when(i == PAIR)(prompt.share)

    prompt.collect()
    for t in range(RING):
        mixed = attend_response(t, q_s[pl.ds(TILE + t * Q_TILE, Q_TILE)], held, k_s, v_s)
        deal_mixed(mixed_router, t, mixed, mixed_stage, mixed_out)
    row = lax.broadcasted_iota(jnp.int32, (TILE, PEERS * TILE), 0) + me * TILE
    col = lax.broadcasted_iota(jnp.int32, (TILE, PEERS * TILE), 1)
    prompt_out[:, :COLUMNS] = softmax_mix(q_s[pl.ds(0, TILE)], [(prompt_rows_of(held, 0), prompt_rows_of(held, 1), col <= row)])
    prompt_out[:, COLUMNS:] = xs[0, :, pl.ds(column, COLUMNS)]
    for copy in next_weights:
        copy.wait()
    split_heads(raw, w)
    leave = pltpu.make_async_copy(w, next_hbm, w_sem.at[3])
    leave.start()
    for router in (mixed_router, res_router):
        for t in range(router.tiles):
            router.collect(t)
        router.finish()
    net.collected(lambda d: info_out.at[d], info_recv)
    net.sent(lambda d: info_ref.at[d], info_send, info_recv)
    prompt.finish()
    leave.wait()


def first_attention(x_prompt, x_resp, w_query, w_key, w_value, gain, cos, sin, info, collective_id):
    rows = TILE + x_resp.shape[0]
    width = x_resp.shape[1]
    return pl.pallas_call(
        first_attention_kernel,
        out_shape=(jax.ShapeDtypeStruct((PEERS, RING, 32, COLUMNS), BF16), jax.ShapeDtypeStruct((PEERS, 8, 16, COLUMNS), BF16),
                   jax.ShapeDtypeStruct((PEERS, 8, 128), jnp.int32), jax.ShapeDtypeStruct((TILE, PAIR * COLUMNS), BF16), jax.ShapeDtypeStruct((width, 3 * COLUMNS), BF16)),
        in_specs=[ANY] * 5 + [VMEM] * 4,
        out_specs=(VMEM,) * 4 + (ANY,),
        scratch_shapes=[
            pltpu.VMEM((9, TILE, width), BF16), pltpu.VMEM((3, PAIR * width, LANES), BF16), pltpu.VMEM((width, 3 * COLUMNS), BF16), pltpu.VMEM((TILE, width), BF16), pltpu.VMEM((TILE, width), BF16),
            pltpu.VMEM((rows, COLUMNS), BF16), pltpu.VMEM((rows - TILE, COLUMNS), BF16), pltpu.VMEM((rows - TILE, COLUMNS), BF16),
            HELD, pltpu.VMEM((RING, PEERS, 32, COLUMNS), BF16), pltpu.VMEM((PEERS, 8, 16, COLUMNS), BF16),
            DMA((9,)), DMA((RING,)), *GATHER_SEMS, DMA((PEERS,)), DMA((PEERS,)),
            *[DMA((RING, PEERS)) for _ in BOTH], *[DMA((1, PEERS)) for _ in BOTH],
        ],
        compiler_params=pltpu.CompilerParams(collective_id=collective_id, has_side_effects=True, vmem_limit_bytes=VMEM_BYTES),
        name="first_attention",
    )(x_prompt, x_resp, w_query, w_key, w_value, gain, cos, sin, info)


def second_attention_kernel(qkv_ref, back_ref, mixed_out, stage, qkv_in, k_s, v_s, held, mixed_stage,
                            ring_send, ring_recv, near_send, near_recv, *routes):
    net = Exchange()
    me = net.me
    prompt = PromptGather(net, held, ring_send, ring_recv, near_send, near_recv)
    router = Router(net, RING, lambda t, d: stage.at[t, d], lambda t, d: qkv_in.at[t, d], routes[:PAIR])
    mixed_router = Router(net, RING, lambda t, d: mixed_stage.at[t, d], lambda t, d: mixed_out.at[d, t], routes[PAIR:])
    for k in BOTH:
        held[me, k] = qkv_ref[0, :, pl.ds((k + 1) * COLUMNS, COLUMNS)]
    net.barrier()
    prompt.start()
    count = back_ref.shape[1]

    def send_rows(t):
        place = lax.broadcasted_iota(jnp.int32, (Q_TILE, count), 0) + t * Q_TILE == back_ref[...]
        rows = jnp.dot(place.astype(BF16), qkv_ref[1:].reshape(count, 3 * COLUMNS), preferred_element_type=F32).astype(BF16)
        stage[t] = rows.reshape(PEERS, Q_TILE // PEERS, 3 * COLUMNS)
        router.send(t)
        qkv_in[t, me] = stage[t, me]

    send_rows(0)
    prompt.relay()
    for t in range(1, RING):
        send_rows(t)
    prompt.share()
    prompt.collect()
    for t in range(RING):
        router.collect(t)
        rows = jnp.dot(undeal(Q_TILE), qkv_in[t].reshape(Q_TILE, 3 * COLUMNS), preferred_element_type=F32).astype(BF16)
        k_s[pl.ds(t * Q_TILE, Q_TILE)] = rows[:, COLUMNS:PAIR * COLUMNS]
        v_s[pl.ds(t * Q_TILE, Q_TILE)] = rows[:, PAIR * COLUMNS:]
        mixed = attend_response(t, rows[:, :COLUMNS], held, k_s, v_s)
        deal_mixed(mixed_router, t, mixed, mixed_stage, mixed_out)
    for t in range(RING):
        mixed_router.collect(t)
    for each in (router, mixed_router):
        each.finish()
    prompt.finish()


def second_attention(qkv, back, collective_id):
    rows = RING * Q_TILE
    wide = (32, 3 * COLUMNS)
    return pl.pallas_call(
        second_attention_kernel,
        out_shape=jax.ShapeDtypeStruct((PEERS, RING, 32, COLUMNS), BF16),
        in_specs=[VMEM, VMEM],
        out_specs=VMEM,
        scratch_shapes=[
            pltpu.VMEM((RING, PEERS) + wide, BF16), pltpu.VMEM((RING, PEERS) + wide, BF16),
            pltpu.VMEM((rows, COLUMNS), BF16), pltpu.VMEM((rows, COLUMNS), BF16),
            HELD, pltpu.VMEM((RING, PEERS, 32, COLUMNS), BF16), *GATHER_SEMS,
            *[DMA((RING, PEERS)) for _ in range(RING)],
        ],
        compiler_params=pltpu.CompilerParams(collective_id=collective_id, has_side_effects=True, vmem_limit_bytes=VMEM_BYTES),
        name=f"second_attention{collective_id}",
    )(qkv, back)


class Answer:
    def __init__(self, every, out_ref, stat_send, stat_recv, row_send, row_recv):
        self.every, self.out = every, out_ref
        self.stat_sems, self.row_sems = (stat_send, stat_recv), (row_send, row_recv)
        self.me, self.home = lax.axis_index("model"), lax.axis_index("resp")
        self.models = [(self.me + k) % SHARDS for k in range(1, SHARDS)]
        self.homes = [(self.home + k) % PEERS for k in range(1, PEERS)]

    def barrier(self):
        sem = pltpu.get_barrier_semaphore()
        for axis, devices in (("model", self.models), ("resp", self.homes)):
            for device in devices:
                pl.semaphore_signal(sem, device_id={axis: device}, device_id_type=MESH)
        pl.semaphore_wait(sem, len(self.models) + len(self.homes))

    def stat_copy(self, owner, device, place):
        ref = self.every.at[owner]
        return pltpu.make_async_remote_copy(
            src_ref=ref, dst_ref=ref, send_sem=self.stat_sems[0].at[device], recv_sem=self.stat_sems[1].at[place],
            device_id={"model": device}, device_id_type=MESH)

    def row_copy(self, owner, device, place):
        ref = self.out.at[owner]
        return pltpu.make_async_remote_copy(
            src_ref=ref, dst_ref=ref, send_sem=self.row_sems[0].at[device], recv_sem=self.row_sems[1].at[place],
            device_id={"resp": device}, device_id_type=MESH)

def combine_kernel(stats_ref, out_ref, every, *sems):
    net = Answer(every, out_ref, *sems)
    every[net.me] = stats_ref[...]
    net.barrier()
    for device in net.models:
        net.stat_copy(net.me, device, net.me).start()
    for device in net.models:
        net.stat_copy(device, device, device).wait_recv()
    found = []
    for c in range(stats_ref.shape[0]):
        tiles = [every[k, c] for k in range(SHARDS)]
        top = functools.reduce(jnp.maximum, [tile[:1] for tile in tiles])
        total = functools.reduce(jnp.add, [tile[1:PAIR] * jnp.exp(tile[:1] - top) for tile in tiles])
        found.append(functools.reduce(jnp.add, [tile[PAIR:3] for tile in tiles]) - top - jnp.log(total))
    out_ref[net.home] = jnp.concatenate(found, axis=0)
    for device in net.homes:
        net.row_copy(net.home, device, net.home).start()
    for device in net.homes:
        net.row_copy(device, device, device).wait_recv()
    for device in net.models:
        net.stat_copy(net.me, device, device).wait_send()
    for device in net.homes:
        net.row_copy(net.home, device, device).wait_send()


def combine(stats, collective_id):
    return pl.pallas_call(
        combine_kernel,
        out_shape=jax.ShapeDtypeStruct((PEERS, PEERS, LANES), F32),
        in_specs=[VMEM],
        out_specs=VMEM,
        scratch_shapes=[pltpu.VMEM((SHARDS,) + stats.shape, F32), *[DMA((SHARDS,)) for _ in BOTH], *[DMA((PEERS,)) for _ in BOTH]],
        compiler_params=pltpu.CompilerParams(collective_id=collective_id, has_side_effects=True),
        name="combine",
    )(stats)


ROPE_BASE = 10000.0
VARIANTS = (512, 640, 768, 1024)


def rope_tables(positions):
    half = LANES // PAIR
    lane = jnp.arange(LANES)
    frequency = ROPE_BASE ** (-(lane % half).astype(F32) / half)
    angles = positions.astype(F32)[:, None] * frequency
    return jnp.cos(angles), jnp.sin(angles) * jnp.where(lane < half, -1.0, 1.0)


def solution(mesh):
    groups = mesh.shape['resp']
    row_axes = ('prompts', 'resp')
    head_spec = P(None, None, 'model', None)
    in_specs = (P(row_axes, None), P(row_axes, None, None), P(row_axes, None), P(row_axes), P(None, None), head_spec, head_spec, head_spec, P(None, 'model', None, None), P(None, None), P(None, None, 'model'), P(None, None, 'model'), P(None, 'model', None), P(None), P(None, 'model'))

    def device_step(x_prompt, x_resp, targets, resp_lens, attn_gain, w_query, w_key, w_value, w_out, mlp_gain, w_gate, w_up, w_down, final_gain, w_vocab):
        prompt_rows = x_prompt.shape[0]
        resp_len, width = x_resp.shape[1:]
        prompt_len = prompt_rows * groups
        me = lax.axis_index('model')
        home = lax.axis_index('resp')
        per = resp_len // groups
        gate_t, up_t = jnp.swapaxes(w_gate, 1, 2), jnp.swapaxes(w_up, 1, 2)
        out_flat = w_out.reshape(w_out.shape[0], COLUMNS, width)
        projections = [w.reshape(w.shape[0], PAIR * width, LANES) for w in (w_query, w_key, w_value)]
        prompt_pos = home * prompt_rows + jnp.arange(prompt_rows)

        cos, sin = rope_tables(jnp.concatenate([prompt_pos, prompt_len + jnp.arange(resp_len)]))
        info = jnp.concatenate([
            targets[0].reshape(per, groups).T[:, None, :],
            jnp.broadcast_to(resp_lens[0], (groups, groups - 1, per)).astype(jnp.int32)], axis=1)
        mixed, res, infos, prompt, project_next = first_attention(
            x_prompt, x_resp[0], *projections, attn_gain, cos, sin, info, 0)
        lens = infos[:, 1, 0]
        need = (lens + groups - 1) // groups
        ends = jnp.sum(jnp.where(jnp.arange(groups)[:, None] >= jnp.arange(groups), need, 0), axis=1)
        starts = ends - need
        dealt = groups * per

        def finish_with(size, ident):
            def run(operands):
                mixed, res, prompt = operands
                slot = jnp.arange(size)
                which = jnp.sum((slot[:, None] >= ends).astype(jnp.int32), axis=1)
                row = slot - jnp.sum(jnp.where(which[:, None] == jnp.arange(groups), starts, 0), axis=1)
                real = slot < ends[-1]
                source = jnp.where(real, which * per + row, -1)
                chosen = source[:, None] == jnp.arange(dealt)
                wanted = jnp.sum(jnp.where(chosen, infos[:, 0, :].reshape(dealt), 0), axis=1) - me * w_vocab.shape[1]
                ids = jnp.where(jnp.arange(LANES) == 0, source[:, None], wanted[:, None]).reshape(-1, LANES, LANES)
                tables = rope_tables(jnp.concatenate([prompt_pos, prompt_len + groups * row + home]))
                weights = (out_flat, gate_t, up_t, w_down)
                qkv, new_res = mega(
                    mlp_gain, attn_gain, ids, mixed.reshape(dealt, COLUMNS), res.reshape(dealt, COLUMNS),
                    [t.reshape(-1, LANES, LANES) for t in tables] + [prompt], *weights, project_next, 0, ident)
                part = per // RING
                back = jnp.where(real, (row // part) * (groups * part) + which * part + row % part, -1)
                mixed = second_attention(qkv, back[None], ident + 1)
                return mega(mlp_gain, final_gain[None], ids, mixed.reshape(dealt, COLUMNS), new_res, [], *weights, w_vocab, 1, ident + PAIR)
            return run

        index = sum((ends[-1] > size).astype(jnp.int32) for size in VARIANTS[:-1])
        stats = lax.switch(index, [finish_with(size, PAIR + 3 * i) for i, size in enumerate(VARIANTS)], (mixed, res, prompt))
        found = combine(stats, 1).reshape(groups, dealt)
        start = jnp.sum(jnp.where(jnp.arange(groups) == home, starts, 0))
        mine = lax.dynamic_slice(jnp.pad(found, ((0, 0), (0, per))), (0, start), (groups, per))
        log_probs = mine.T.reshape(resp_len)
        log_probs = jnp.where(jnp.arange(resp_len) < resp_lens[0], log_probs, 0.0)
        return log_probs[None, :]

    return jax.shard_map(device_step, mesh=mesh, in_specs=in_specs, out_specs=P(row_axes, None), check_vma=False)
```

```python
import functools

import jax
import jax.numpy as jnp
from jax import lax
from jax.experimental import pallas as pl
from jax.experimental.pallas import tpu as pltpu
from jax.sharding import PartitionSpec as P

MESH = pl.DeviceIdType.MESH
F32 = jnp.float32
BF16 = jnp.bfloat16
EPS = 1e-6
LANES = 128
PAIR = 2
RING = 4
COLUMNS = PAIR * LANES
SHARDS = RING * RING
PEERS = 8
BOTH = range(PAIR)
VMEM_BYTES = 67_000_000
LATE_ROWS = 640
LOGITS = 512
VMEM = pl.BlockSpec(memory_space=pltpu.VMEM)
ANY = pl.BlockSpec(memory_space=pl.ANY)
DMA = pltpu.SemaphoreType.DMA
KINDS = range(RING * 3)
SUM_FAR, SUM_NEAR, SUM_RELAY, SUM2_FAR, SUM2_NEAR, SUM2_RELAY, TAKE_OWN, TAKE_REST, TAKE_RELAY, TAKE2_OWN, TAKE2_REST, TAKE2_RELAY = KINDS


def block_of(color, first, second):
    return RING * first + second if color else RING * second + first


def pair(index):
    return pl.ds(PAIR * index, PAIR)


class Torus:
    def __init__(self, refs, send_sem, recv_sem):
        self.refs = refs
        self.far, self.near, self.relayed, self.sums, self.relayed2, self.sums2, self.rows = refs
        self.send_sem, self.recv_sem = send_sem, recv_sem
        me = lax.axis_index("model")
        z, y = me // RING, me % RING
        self.place = ((y, z), (z, y))
        along_y = [z * RING + self.step(y, way) for way in (1, -1)]
        along_z = [self.step(z, way) * RING + y for way in (1, -1)]
        self.neighbors = ((along_y, along_z), (along_z, along_y))

    def step(self, place, by):
        return (place + by + RING) % RING

    def barrier(self):
        sem = pltpu.get_barrier_semaphore()
        for ring in self.neighbors[0]:
            for device in ring:
                pl.semaphore_signal(sem, device_id={"model": device}, device_id_type=MESH)
        pl.semaphore_wait(sem, RING)

    def ends(self, kind, c, q, d):
        (p, s), way, other = self.place[q], 1 - PAIR * d, 1 - d
        far, near, relayed, sums, relayed2, sums2, rows = (ref.at[c, q] for ref in self.refs)
        own = sums.at[0]
        back_s, back_p = self.step(s, -way), self.step(p, -way)
        return {
            SUM_FAR: lambda: (far.at[pair(d)], relayed.at[d], relayed.at[d]),
            SUM_NEAR: lambda: (near.at[d], sums.at[d, pair(other)], sums.at[d, pair(other)]),
            SUM_RELAY: lambda: (relayed.at[d], sums.at[d, pair(d)], sums.at[d, pair(d)]),
            SUM2_FAR: lambda: (own.at[self.step(s, PAIR), d], relayed2.at[d], relayed2.at[d]),
            SUM2_NEAR: lambda: (own.at[self.step(s, way), other], sums2.at[d, other], sums2.at[d, other]),
            SUM2_RELAY: lambda: (relayed2.at[d], sums2.at[d, d], sums2.at[d, d]),
            TAKE_OWN: lambda: (rows.at[p, s, d], rows.at[p, s, d], rows.at[p, back_s, d]),
            TAKE_REST: lambda: (rows.at[p, s, other], rows.at[p, s, other], rows.at[p, back_s, other]),
            TAKE_RELAY: lambda: (rows.at[p, back_s, d], rows.at[p, back_s, d], rows.at[p, self.step(s, PAIR), d]),
            TAKE2_OWN: lambda: (rows.at[p, pair(d)], rows.at[p, pair(d)], rows.at[back_p, pair(d)]),
            TAKE2_REST: lambda: (rows.at[p, pair(other)], rows.at[p, pair(other)], rows.at[back_p, pair(other)]),
            TAKE2_RELAY: lambda: (rows.at[back_p, pair(d)], rows.at[back_p, pair(d)], rows.at[self.step(p, PAIR), pair(d)]),
        }[kind]()

    def copy(self, kind, c, q, d, src, dst):
        second_ring = kind in (SUM2_FAR, SUM2_NEAR, SUM2_RELAY, TAKE_OWN, TAKE_REST, TAKE_RELAY)
        return pltpu.make_async_remote_copy(
            src_ref=src, dst_ref=dst, send_sem=self.send_sem.at[c, q, d, kind], recv_sem=self.recv_sem.at[c, q, d, kind],
            device_id={"model": self.neighbors[q][second_ring][d]}, device_id_type=MESH)

    def send(self, c, q, d, kind):
        src, dst, _ = self.ends(kind, c, q, d)
        self.copy(kind, c, q, d, src, dst).start()

    def sent(self, c, q, *kinds):
        for kind in kinds:
            for d in BOTH:
                src, dst, _ = self.ends(kind, c, q, d)
                self.copy(kind, c, q, d, src, dst).wait_send()

    def arrived(self, c, q, d, *kinds):
        for kind in kinds:
            _, _, here = self.ends(kind, c, q, d)
            self.copy(kind, c, q, d, here, here).wait_recv()


def halves(value):
    return value[:, :LANES], value[:, LANES:]


def store_block(ref, value):
    for half, part in enumerate(halves(value)):
        ref[half] = part


def add_block(ref, value):
    for half, part in enumerate(halves(value)):
        ref[half] += part


class Gather:
    def __init__(self, net):
        self.net = net

    def begin_rows(self, c, q):
        for kind in (TAKE_OWN, TAKE_REST):
            for d in BOTH:
                self.net.send(c, q, d, kind)

    def relay_rows(self, c, q):
        for d in BOTH:
            self.net.arrived(c, q, d, TAKE_OWN)
            self.net.send(c, q, d, TAKE_RELAY)

    def take_second(self, c, q):
        for d in BOTH:
            self.net.arrived(c, q, d, TAKE_REST, TAKE_RELAY)
        for kind in (TAKE2_OWN, TAKE2_REST):
            for d in BOTH:
                self.net.send(c, q, d, kind)

    def relay_last(self, c, q):
        for d in BOTH:
            self.net.arrived(c, q, d, TAKE2_OWN)
            self.net.send(c, q, d, TAKE2_RELAY)

    def complete(self, c, q):
        for d in BOTH:
            self.net.arrived(c, q, d, TAKE2_REST, TAKE2_RELAY)
        self.net.sent(c, q, TAKE_OWN, TAKE_REST, TAKE_RELAY, TAKE2_OWN, TAKE2_REST, TAKE2_RELAY)

    def middle(self):
        return [self.relay_rows, self.take_second, self.relay_last]


class Sum(Gather):
    def __init__(self, net, lhs_of, w_ref, finish):
        self.net, self.lhs_of, self.w_ref, self.finish = net, lhs_of, w_ref, finish

    def product(self, lhs, color, first, second):
        start = pl.multiple_of(block_of(color, first, second) * COLUMNS, COLUMNS)
        return jnp.dot(lhs, self.w_ref[:, pl.ds(start, COLUMNS)], preferred_element_type=F32)

    def begin(self, c, q):
        net, p, lhs = self.net, self.net.place[q][0], self.lhs_of(c, q)
        for k in range(RING):
            store_block(net.far.at[c, q, k], self.product(lhs, q, net.step(p, PAIR), k))
        for d in BOTH:
            net.send(c, q, d, SUM_FAR)
        for d in BOTH:
            for k in BOTH:
                store_block(net.near.at[c, q, d, k], self.product(lhs, q, net.step(p, 1 - PAIR * d), PAIR * (1 - d) + k))
            net.send(c, q, d, SUM_NEAR)

    def relay_sum(self, c, q):
        net, p, lhs = self.net, self.net.place[q][0], self.lhs_of(c, q)
        for d in BOTH:
            net.arrived(c, q, d, SUM_FAR)
            for k in BOTH:
                add_block(net.relayed.at[c, q, d, k], self.product(lhs, q, net.step(p, 1 - PAIR * d), PAIR * d + k))
            net.send(c, q, d, SUM_RELAY)

    def begin_second(self, c, q):
        net, lhs = self.net, self.lhs_of(c, q)
        for d in BOTH:
            net.arrived(c, q, d, SUM_NEAR, SUM_RELAY)
        for k in range(RING):
            for half, part in enumerate(halves(self.product(lhs, q, net.place[q][0], k))):
                net.sums[c, q, 0, k, half] += net.sums[c, q, 1, k, half] + part
        for kind in (SUM2_FAR, SUM2_NEAR):
            for d in BOTH:
                net.send(c, q, d, kind)
        net.sent(c, q, SUM_FAR)

    def relay_second(self, c, q):
        net = self.net
        for d in BOTH:
            net.arrived(c, q, d, SUM2_FAR)
            net.relayed2[c, q, d] += net.sums[c, q, 0, net.step(net.place[q][1], 1 - PAIR * d), d]
            net.send(c, q, d, SUM2_RELAY)

    def finish_sum(self, c, q):
        net = self.net
        net.sent(c, q, SUM_NEAR, SUM_RELAY)
        for d in BOTH:
            net.arrived(c, q, d, SUM2_NEAR, SUM2_RELAY)
        for half in BOTH:
            self.finish(c, q, half, net.sums[c, q, 0, net.place[q][1], half] + net.sums2[c, q, 0, half] + net.sums2[c, q, 1, half])
        self.begin_rows(c, q)

    def relay_rows(self, c, q):
        self.net.sent(c, q, SUM2_FAR, SUM2_NEAR, SUM2_RELAY)
        super().relay_rows(c, q)

    def middle(self):
        return [self.relay_sum, self.begin_second, self.relay_second, self.finish_sum, *super().middle()]


def normed(net, c, q, gain_ref, layer):
    rows = net.rows.shape[-PAIR]
    tile = PAIR * 8 if rows % (PAIR * 8) == 0 else 8
    spots = [(first, second, half) for first in range(RING) for second in range(RING) for half in BOTH]

    @pl.loop(0, rows // tile)
    def _(i):
        span = pl.ds(pl.multiple_of(i * tile, tile), tile)
        acts = [net.rows[(c, q) + spot + (span,)].astype(F32) for spot in spots]
        squares = functools.reduce(jnp.add, [v * v for v in acts])
        inv = lax.rsqrt(jnp.sum(squares, axis=-1, keepdims=True) / (LANES * len(acts)) + EPS)
        for spot, v in zip(spots, acts):
            column = block_of(q, *spot[:PAIR]) * COLUMNS + spot[PAIR] * LANES
            net.rows[(c, q) + spot + (span,)] = (v * inv * gain_ref[pl.ds(layer, 1), pl.ds(column, LANES)]).astype(BF16)


def rows_of(net, c, q):
    parts = []
    for upper in range(RING):
        for lower in range(RING):
            first, second = (upper, lower) if q else (lower, upper)
            parts += [net.rows[c, q, first, second, half] for half in BOTH]
    return jnp.concatenate(parts, axis=1)


def times_transposed(lhs, rhs):
    return lax.dot_general(lhs, rhs, (((1,), (1,)), ((), ())), preferred_element_type=F32)


def late_plan(width, count):
    plan, start = [], 0
    for buffer in BOTH:
        for slot in range(width // count):
            size = min(LATE_ROWS, width - start)
            if size:
                plan.append((buffer, slot * count, start, size))
            start += size
    return plan, width - start


def rope(value, cos, sin):
    return jnp.concatenate([v * cos + pltpu.roll(v, LANES // PAIR, 1) * sin for v in halves(value)], axis=1)


def put_projected(product, cos_ref, sin_ref, out_ref, c):
    for k in range(3):
        value = product(k * COLUMNS, COLUMNS)
        if k < PAIR:
            value = rope(value, cos_ref[c], sin_ref[c])
        out_ref[c, :, pl.ds(k * COLUMNS, COLUMNS)] = value.astype(BF16)


def statistics(product, count, target):
    top = total = picked = None
    for k in range(count // LOGITS):
        logits = product(k * LOGITS, LOGITS)
        here = jnp.max(logits, axis=-1, keepdims=True)
        ids = lax.broadcasted_iota(jnp.int32, logits.shape, 1) + k * LOGITS
        found = jnp.sum(jnp.where(ids == target, logits, 0.0), axis=-1, keepdims=True)
        if k:
            both = jnp.maximum(top, here)
            total = total * jnp.exp(top - both) + jnp.sum(jnp.exp(logits - both), axis=-1, keepdims=True)
            top, picked = both, picked + found
        else:
            top, total, picked = here, jnp.sum(jnp.exp(logits - here), axis=-1, keepdims=True), found
    lane = lax.broadcasted_iota(jnp.int32, (LANES, LANES), 1)
    return jnp.where(lane == 0, top, jnp.where(lane == 1, total, picked)).T[:PEERS]


def mega_kernel(chunks, layer, last, gain_ref, next_gain_ref, ids_ref, dealt_ref, old_ref, *args):
    if last:
        side_refs, args = (), args
    else:
        side_refs, args = args[:3], args[3:]
    w_out_hbm, w_gate_hbm, w_up_hbm, w_down_hbm, *args = args
    late_hbm, out_ref, *args = args
    if not last:
        new_res_ref, *args = args
    (w_out, w_gate, w_up, w_down, late_rest, res, inner, middle,
     far, near, relayed, sums, relayed2, sums2, rows, w_sem, late_sem, send_sem, recv_sem, ready_sem) = args
    loads = [pltpu.make_async_copy(src.at[layer], dst, w_sem.at[i]) for i, (src, dst) in enumerate(
        ((w_out_hbm, w_out), (w_gate_hbm, w_gate), (w_up_hbm, w_up), (w_down_hbm, w_down)))]
    for load in loads:
        load.start()
    width, count = late_hbm.shape
    plan, left = late_plan(width, count)
    late = [(late_hbm.at[pl.ds(start, size)], (w_gate, w_up)[buffer].at[pl.ds(0, size), pl.ds(lane, count)]) for buffer, lane, start, size in plan]
    if left:
        late.append((late_hbm.at[pl.ds(width - left, left)], late_rest))
    late_loads = [pltpu.make_async_copy(src, dst, late_sem.at[i]) for i, (src, dst) in enumerate(late)]
    net = Torus((far, near, relayed, sums, relayed2, sums2, rows), send_sem, recv_sem)
    net.barrier()
    if last:
        new_res_ref = middle
        out_ref[...] = jnp.zeros_like(out_ref)

    def picked(ids, ref):
        chosen = (ids == lax.broadcasted_iota(jnp.int32, (LANES, PEERS * LANES), 1)).astype(BF16)
        return jnp.dot(chosen, ref[...], preferred_element_type=F32).astype(BF16)

    def put(ref, value, place_of):
        part = value.shape[0] // PAIR
        for q in BOTH:
            for half, columns in enumerate(halves(value)):
                ref[place_of(q) + (half,)] = columns[q * part:(q + 1) * part]

    def own_rows(c):
        return lambda q: (c, q) + net.place[q]

    def begin(c):
        if last:
            put(rows, picked(ids_ref[c, :, :1], dealt_ref), own_rows(c))
        else:
            @pl.when(c == 0)
            def _():
                put(rows, side_refs[PAIR][:, :COLUMNS], own_rows(c))
                put(res, side_refs[PAIR][:, COLUMNS:], lambda q: (c, q))

            @pl.when(c > 0)
            def _():
                ids = ids_ref[c - 1, :, :1]
                put(rows, picked(ids, dealt_ref), own_rows(c))
                put(res, picked(ids, old_ref), lambda q: (c, q))
        for q in BOTH:
            first.begin_rows(c, q)

    def finish(c, q, half, total):
        value = (middle[c, q, half].astype(F32) + total).astype(BF16)
        new_res_ref[c, q, half] = value
        rows[(c, q) + net.place[q] + (half,)] = value

    first = Gather(net)
    second = Sum(net, lambda c, q: inner[c, q], w_down, finish)

    def project_out(c):
        for q in BOTH:
            first.complete(c, q)
        total = jnp.dot(jnp.concatenate([rows_of(net, c, q) for q in BOTH], axis=0), w_out[...], preferred_element_type=F32)
        part = total.shape[0] // PAIR
        for q in BOTH:
            for half, columns in enumerate(halves(total)):
                old = old_ref[c + 1, q, half] if last else res[c, q, half]
                value = (old.astype(F32) + columns[q * part:(q + 1) * part]).astype(BF16)
                middle[c, q, half] = value
                rows[(c, q) + net.place[q] + (half,)] = value
        for ring in net.neighbors[0]:
            for device in ring:
                pl.semaphore_signal(ready_sem.at[c], device_id={"model": device}, device_id_type=MESH)

    def begin_again(c):
        pl.semaphore_wait(ready_sem.at[c], RING)
        for q in BOTH:
            first.begin_rows(c, q)

    def hidden_of(c, stage, gain, row):
        for q in BOTH:
            stage.complete(c, q)
            normed(net, c, q, gain, row)
        return jnp.concatenate([rows_of(net, c, q) for q in BOTH], axis=0)

    def mlp(c):
        hidden = hidden_of(c, first, gain_ref, layer)
        value = (jax.nn.silu(times_transposed(hidden, w_gate[...])) * times_transposed(hidden, w_up[...])).astype(BF16)
        inner[c] = value.reshape(inner.shape[1:])
        for q in BOTH:
            second.begin(c, q)

    def after(c):
        hidden = hidden_of(c, second, next_gain_ref, 0 if last else layer + 1)

        def product(lane, size):
            parts = [jnp.dot(hidden[:, start:start + rows_here], (w_gate, w_up)[buffer][pl.ds(0, rows_here), pl.ds(at + lane, size)], preferred_element_type=F32)
                     for buffer, at, start, rows_here in plan]
            if left:
                parts.append(jnp.dot(hidden[:, width - left:], late_rest[:, pl.ds(lane, size)], preferred_element_type=F32))
            return functools.reduce(jnp.add, parts)

        if last:
            out_ref[c] = statistics(product, count, ids_ref[c, :, 1:PAIR])
        else:
            put_projected(product, *side_refs[:PAIR], out_ref, c)

    def on_both(step):
        def run(c):
            for q in BOTH:
                step(c, q)
        return run

    gather = [on_both(step) for step in first.middle()]
    steps = [begin, *gather, project_out, begin_again, *gather, mlp, *map(on_both, second.middle())]
    at_mlp = steps.index(mlp)
    steps += [None] * max(0, at_mlp + chunks - len(steps)) + [after]

    @pl.loop(0, len(steps) + chunks - 1)
    def _(slot):
        @pl.when(slot == steps.index(project_out))
        def _():
            for load in loads:
                load.wait()

        @pl.when(slot == len(steps) - 1)
        def _():
            for load in late_loads:
                load.wait()

        for k, step in reversed(list(enumerate(steps))):
            if step is None:
                continue

            @pl.when(slot >= k)
            def _():
                @pl.when(slot < k + chunks)
                def _():
                    step(slot - k)

        @pl.when(slot == at_mlp + chunks - 1)
        def _():
            for load in late_loads:
                load.start()


def mega(gain, next_gain, ids, dealt, old, sides, w_out, w_gate_t, w_up_t, w_down, late, layer, collective_id):
    last = not sides
    chunks = ids.shape[0] + (not last)
    _, hidden, width = w_gate_t.shape
    rows = LANES // PAIR
    per = (chunks, PAIR)
    tile = (rows, LANES)
    count = late.shape[1]
    _, left = late_plan(width, count)

    sem = DMA(per + (PAIR, len(KINDS)))
    out = jax.ShapeDtypeStruct((PEERS, PEERS, LANES), F32) if last else (
        jax.ShapeDtypeStruct((chunks, LANES, count), BF16), jax.ShapeDtypeStruct(per + (PAIR,) + tile, BF16))
    return pl.pallas_call(
        functools.partial(mega_kernel, chunks, layer, last),
        out_shape=out,
        in_specs=[VMEM] * (5 + len(sides)) + [ANY] * 5,
        out_specs=VMEM if last else (VMEM, VMEM),
        scratch_shapes=[
            pltpu.VMEM((width, COLUMNS), BF16),
            *[pltpu.VMEM((hidden, width), BF16) for _ in range(3)],
            pltpu.VMEM((left or 8, count), BF16),
            pltpu.VMEM(per + (PAIR,) + (tile if not last else (8, LANES)), BF16),
            pltpu.VMEM(per + (rows, hidden), BF16),
            pltpu.VMEM(per + (PAIR,) + tile, BF16),
            pltpu.VMEM(per + (RING, PAIR) + tile, F32),
            pltpu.VMEM(per + (PAIR, PAIR, PAIR) + tile, F32),
            pltpu.VMEM(per + (PAIR, PAIR, PAIR) + tile, F32),
            pltpu.VMEM(per + (PAIR, RING, PAIR) + tile, F32),
            pltpu.VMEM(per + (PAIR,) + tile, F32),
            pltpu.VMEM(per + (PAIR, PAIR) + tile, F32),
            pltpu.VMEM(per + (RING, RING, PAIR) + tile, BF16),
            DMA((RING,)), DMA((SHARDS,)), sem, sem, pltpu.SemaphoreType.REGULAR((chunks,)),
        ],
        compiler_params=pltpu.CompilerParams(collective_id=collective_id, has_side_effects=True, vmem_limit_bytes=VMEM_BYTES),
        name=f"mega{collective_id}",
    )(gain, next_gain, ids, dealt, old, *sides, w_out, w_gate_t, w_up_t, w_down, late)


TILE = 128
Q_TILE = 256
LOG2E = 1.4426950408889634
HELD = pltpu.VMEM((PEERS, PAIR, TILE, COLUMNS), BF16)
GATHER_SEMS = [DMA((PAIR, 3)), DMA((PAIR, 3)), DMA((RING,)), DMA((RING,))]


class Exchange:
    def __init__(self):
        self.me = lax.axis_index("resp")
        self.others = [(self.me + k) % PEERS for k in range(1, PEERS)]

    def barrier(self):
        sem = pltpu.get_barrier_semaphore()
        for device in self.others:
            pl.semaphore_signal(sem, inc=1, device_id={"resp": device}, device_id_type=MESH)
        pl.semaphore_wait(sem, PEERS - 1)

    def copy(self, src, dst, send_sem, recv_sem, device):
        return pltpu.make_async_remote_copy(src_ref=src, dst_ref=dst, send_sem=send_sem, recv_sem=recv_sem,
                                            device_id={"resp": device}, device_id_type=MESH)

    def scatter(self, src_of, dst, send_sem, recv_sem):
        for device in self.others:
            self.copy(src_of(device), dst, send_sem.at[device], recv_sem.at[self.me], device).start()

    def collected(self, dst_of, recv_sem):
        for device in self.others:
            self.copy(dst_of(device), dst_of(device), recv_sem.at[device], recv_sem.at[device], device).wait_recv()

    def sent(self, src_of, send_sem, recv_sem):
        for device in self.others:
            self.copy(src_of(device), src_of(device), send_sem.at[device], recv_sem.at[device], device).wait_send()


class Router:
    def __init__(self, net, tiles, src_of, dst_of, sems):
        self.net, self.tiles, self.src_of, self.dst_of = net, tiles, src_of, dst_of
        self.send_sem, self.recv_sem = sems

    def send(self, t):
        self.net.scatter(lambda d: self.src_of(t, d), self.dst_of(t, self.net.me), self.send_sem.at[t], self.recv_sem.at[t])

    def collect(self, t):
        self.net.collected(lambda d: self.dst_of(t, d), self.recv_sem.at[t])

    def finish(self):
        for t in range(self.tiles):
            self.net.sent(lambda d: self.src_of(t, d), self.send_sem.at[t], self.recv_sem.at[t])


class RespGather:
    def __init__(self, net, held, ring_send, ring_recv, near_send, near_recv):
        self.net, self.held = net, held
        self.ring_sems, self.near_sems = (ring_send, ring_recv), (near_send, near_recv)
        x, core = net.me // PAIR, net.me % PAIR
        self.at = lambda by, here: (x + by + RING) % RING * PAIR + (core if here else 1 - core)

    def ring_copy(self, d, kind, ref):
        return self.net.copy(ref, ref, self.ring_sems[0].at[d, kind], self.ring_sems[1].at[d, kind], self.at(1 - PAIR * d, True))

    def near_copy(self, kind, ref):
        return self.net.copy(ref, ref, self.near_sems[0].at[kind], self.near_sems[1].at[kind], self.at(0, False))

    def sources(self, here):
        return [self.at(by, here) for by in (0, -1, 1, PAIR)]

    def start(self):
        for d in BOTH:
            self.ring_copy(d, 0, self.held.at[self.net.me, d]).start()
        self.near_copy(0, self.held.at[self.net.me]).start()

    def start_rest(self):
        for d in BOTH:
            self.ring_copy(d, 1, self.held.at[self.net.me, 1 - d]).start()

    def relay(self):
        for d in BOTH:
            ref = self.held.at[self.at(PAIR * d - 1, True), d]
            self.ring_copy(d, 0, ref).wait_recv()
            self.ring_copy(d, PAIR, ref).start()

    def share(self):
        for d in BOTH:
            device = self.at(PAIR * d - 1, True)
            self.ring_copy(d, 1, self.held.at[device, 1 - d]).wait_recv()
            self.near_copy(1 + d, self.held.at[device]).start()
        far = self.held.at[self.at(PAIR, True)]
        for d in BOTH:
            self.ring_copy(d, PAIR, far.at[d]).wait_recv()
        self.near_copy(3, far).start()

    def collect(self):
        for kind, device in enumerate(self.sources(False)):
            self.near_copy(kind, self.held.at[device]).wait_recv()

    def finish(self):
        for kind in range(3):
            for d in BOTH:
                self.ring_copy(d, kind, self.held.at[self.net.me, d]).wait_send()
        for kind in range(RING):
            self.near_copy(kind, self.held.at[self.net.me]).wait_send()


def deal(rows):
    out = lax.broadcasted_iota(jnp.int32, (rows, rows), 0)
    src = lax.broadcasted_iota(jnp.int32, (rows, rows), 1)
    per = rows // PEERS
    return jnp.where(src == (out % per) * PEERS + out // per, 1.0, 0.0).astype(BF16)


def undeal(rows):
    out = lax.broadcasted_iota(jnp.int32, (rows, rows), 0)
    src = lax.broadcasted_iota(jnp.int32, (rows, rows), 1)
    per = rows // PEERS
    return jnp.where(src == (out % PEERS) * per + out // PEERS, 1.0, 0.0).astype(BF16)


def split_heads(raw_ref, w_ref):
    tile = PAIR * LANES
    out = lax.broadcasted_iota(jnp.int32, (tile, tile), 0)
    src = lax.broadcasted_iota(jnp.int32, (tile, tile), 1)
    pick = jnp.where(src == (out % LANES) * PAIR + out // LANES, 1.0, 0.0).astype(BF16)

    @pl.loop(0, raw_ref.shape[1] // (RING * tile))
    def _(b):
        raws = [raw_ref[i, pl.ds(pl.multiple_of((b * RING + k) * tile, tile), tile)] for k in range(RING) for i in range(3)]
        heads = jnp.dot(pick, jnp.concatenate(raws, axis=1), preferred_element_type=F32).astype(BF16)
        for k in range(RING):
            here = pl.ds(pl.multiple_of((b * RING + k) * LANES, LANES), LANES)
            for i in range(3):
                for h in BOTH:
                    at = (k * 3 + i) * LANES
                    w_ref[here, pl.ds(i * COLUMNS + h * LANES, LANES)] = heads[h * LANES:(h + 1) * LANES, at:at + LANES]


def norm_tile(x_ref, out_ref, gain_ref):
    for i in range(x_ref.shape[0] // 16):
        v = x_ref[pl.ds(16 * i, 16), :].astype(F32)
        inv = lax.rsqrt(jnp.mean(v * v, axis=-1, keepdims=True) + EPS)
        out_ref[pl.ds(16 * i, 16), :] = (v * inv * gain_ref[pl.ds(0, 1), :]).astype(BF16)


def softmax_mix(q, pieces):
    factor = LOG2E * 128 ** -0.5
    outs = []
    for h in range(2):
        lanes = slice(128 * h, 128 * h + 128)
        scores = []
        for keys, _, mask in pieces:
            s = lax.dot_general(q[:, lanes], keys[:, lanes], (((1,), (1,)), ((), ())), preferred_element_type=F32)
            scores.append(s if mask is None else jnp.where(mask, s, -jnp.inf))
        top = functools.reduce(jnp.maximum, [jnp.max(s, axis=-1, keepdims=True) for s in scores])
        probs = [jnp.exp2((s - top) * factor) for s in scores]
        total = functools.reduce(jnp.add, [jnp.sum(p, axis=-1, keepdims=True) for p in probs])
        mixed = functools.reduce(jnp.add, [jnp.dot(p.astype(BF16), values[:, lanes], preferred_element_type=F32) for p, (_, values, _) in zip(probs, pieces)])
        outs.append(mixed / total)
    return jnp.concatenate(outs, axis=1).astype(BF16)


def prompt_rows_of(held, which):
    return held[:, which].reshape(PEERS * TILE, COLUMNS)


def attend_response(t, q, held, k_own, v_own):
    row = lax.broadcasted_iota(jnp.int32, (Q_TILE, Q_TILE), 0)
    col = lax.broadcasted_iota(jnp.int32, (Q_TILE, Q_TILE), 1)
    pieces = [(prompt_rows_of(held, 0), prompt_rows_of(held, 1), None)]
    if t:
        pieces.append((k_own[:t * Q_TILE], v_own[:t * Q_TILE], None))
    span = slice(t * Q_TILE, (t + 1) * Q_TILE)
    pieces.append((k_own[span], v_own[span], col <= row))
    return softmax_mix(q, pieces)


def deal_mixed(router, t, mixed, stage, out):
    dealt = jnp.dot(deal(Q_TILE), mixed, preferred_element_type=F32).astype(BF16)
    stage[t] = dealt.reshape(PEERS, Q_TILE // PEERS, COLUMNS)
    router.send(t)
    out[router.net.me, t] = stage[t, router.net.me]


def first_attention_kernel(xp_hbm, xr_hbm, wq_hbm, wk_hbm, wv_hbm, gain_ref, cos_ref, sin_ref, info_ref, slice_ref,
                           mixed_out, res_out, info_out, prompt_out, next_hbm, columns_hbm,
                           xs, raw, w, even, odd, q_s, k_s, v_s, held, mixed_stage, res_stage,
                           x_sem, w_sem, ring_send, ring_recv, near_send, near_recv, info_send, info_recv, spread_held, spread_sem, *routes):
    net = Exchange()
    spread_sems, routes = routes[:RING], routes[RING:]
    columns = RespGather(net, spread_held, *spread_sems)
    mixed_router = Router(net, RING, lambda t, d: mixed_stage.at[t, d], lambda t, d: mixed_out.at[d, t], routes[:PAIR])
    res_router = Router(net, 1, lambda t, d: res_stage.at[d], lambda t, d: res_out.at[d], routes[PAIR:])
    prompt = RespGather(net, held, ring_send, ring_recv, near_send, near_recv)
    me = net.me
    column = pl.multiple_of(lax.axis_index("model") * COLUMNS, COLUMNS)

    def load(t):
        src = xp_hbm if isinstance(t, int) and t == 0 else xr_hbm.at[pl.ds(pl.multiple_of((t - 1) * TILE, TILE), TILE)]
        return pltpu.make_async_copy(src, xs.at[t], x_sem.at[t])

    load(0).start()
    weights, next_weights = ([pltpu.make_async_copy(src.at[layer], raw.at[i], w_sem.at[i]) for i, src in enumerate((wq_hbm, wk_hbm, wv_hbm))] for layer in BOTH)
    for copy in weights:
        copy.start()
    for t in range(1, 9):
        load(t).start()
    spread_held[me] = slice_ref[...]
    net.barrier()
    columns.start()
    net.scatter(lambda d: info_ref.at[d], info_out.at[me], info_send, info_recv)
    info_out[me] = info_ref[me]

    def project(t, hidden):
        span = pl.ds(pl.multiple_of(t * TILE, TILE), TILE)
        qkv = jnp.dot(hidden[...], w[...], preferred_element_type=F32)
        cos, sin = cos_ref[span], sin_ref[span]
        return span, rope(qkv[:, :COLUMNS], cos, sin).astype(BF16), rope(qkv[:, COLUMNS:512], cos, sin).astype(BF16), qkv[:, 512:].astype(BF16)

    load(0).wait()
    norm_tile(xs.at[0], even, gain_ref)
    for copy in weights:
        copy.wait()
    split_heads(raw, w)
    for copy in next_weights:
        copy.start()
    load(1).wait()
    span, q, k, v = project(0, even)
    norm_tile(xs.at[1], odd, gain_ref)
    q_s[span] = q
    held[me, 0] = k
    held[me, 1] = v
    prompt.start()
    prompt.start_rest()
    for t in range(PAIR, 9):
        load(t).wait()
    spread = deal(TILE)

    @pl.loop(1, 9)
    def _(t):
        dealt = jnp.dot(spread, xs[t, :, pl.ds(column, COLUMNS)], preferred_element_type=F32).astype(BF16)
        res_stage[:, t - 1] = dealt.reshape(PEERS, TILE // PEERS, COLUMNS)

    res_out[me] = res_stage[me]

    def response_tile(t, here, there):
        span, q, k, v = project(t, here)
        norm_tile(xs.at[jnp.minimum(t + 1, 8)], there, gain_ref)
        q_s[span] = q
        own = pl.ds(pl.multiple_of((t - 1) * TILE, TILE), TILE)
        k_s[own] = k
        v_s[own] = v

    @pl.loop(0, RING)
    def _(i):
        response_tile(PAIR * i + 1, odd, even)
        response_tile(PAIR * i + PAIR, even, odd)

        @pl.when(i == 0)
        def _():
            prompt.relay()
            res_router.send(0)

        @pl.when(i == 1)
        def _():
            columns.relay()
            columns.start_rest()

        pl.when(i == PAIR)(prompt.share)

    prompt.collect()
    for t in range(RING):
        mixed = attend_response(t, q_s[pl.ds(TILE + t * Q_TILE, Q_TILE)], held, k_s, v_s)
        deal_mixed(mixed_router, t, mixed, mixed_stage, mixed_out)
    row = lax.broadcasted_iota(jnp.int32, (TILE, PEERS * TILE), 0) + me * TILE
    col = lax.broadcasted_iota(jnp.int32, (TILE, PEERS * TILE), 1)
    prompt_out[:, :COLUMNS] = softmax_mix(q_s[pl.ds(0, TILE)], [(prompt_rows_of(held, 0), prompt_rows_of(held, 1), col <= row)])
    prompt_out[:, COLUMNS:] = xs[0, :, pl.ds(column, COLUMNS)]
    for copy in next_weights:
        copy.wait()
    split_heads(raw, w)
    leave = pltpu.make_async_copy(w, next_hbm, w_sem.at[3])
    leave.start()
    columns.share()
    columns.collect()
    out_copies = [pltpu.make_async_copy(spread_held.at[device, layer], columns_hbm.at[layer, :, device], spread_sem.at[layer, device])
                  for device in range(PEERS) for layer in BOTH]
    for copy in out_copies:
        copy.start()
    for router in (mixed_router, res_router):
        for t in range(router.tiles):
            router.collect(t)
        router.finish()
    net.collected(lambda d: info_out.at[d], info_recv)
    net.sent(lambda d: info_ref.at[d], info_send, info_recv)
    prompt.finish()
    columns.finish()
    for copy in out_copies:
        copy.wait()
    leave.wait()


def first_attention(x_prompt, x_resp, w_query, w_key, w_value, gain, cos, sin, info, out_slice, collective_id):
    rows = TILE + x_resp.shape[0]
    width = x_resp.shape[1]
    return pl.pallas_call(
        first_attention_kernel,
        out_shape=(jax.ShapeDtypeStruct((PEERS, RING, 32, COLUMNS), BF16), jax.ShapeDtypeStruct((PEERS, 8, 16, COLUMNS), BF16),
                   jax.ShapeDtypeStruct((PEERS, 8, 128), jnp.int32), jax.ShapeDtypeStruct((TILE, PAIR * COLUMNS), BF16), jax.ShapeDtypeStruct((width, 3 * COLUMNS), BF16),
                   jax.ShapeDtypeStruct((PAIR, SHARDS, PEERS, 32, COLUMNS), BF16)),
        in_specs=[ANY] * 5 + [VMEM] * 5,
        out_specs=(VMEM,) * 4 + (ANY, ANY),
        scratch_shapes=[
            pltpu.VMEM((9, TILE, width), BF16), pltpu.VMEM((3, PAIR * width, LANES), BF16), pltpu.VMEM((width, 3 * COLUMNS), BF16), pltpu.VMEM((TILE, width), BF16), pltpu.VMEM((TILE, width), BF16),
            pltpu.VMEM((rows, COLUMNS), BF16), pltpu.VMEM((rows - TILE, COLUMNS), BF16), pltpu.VMEM((rows - TILE, COLUMNS), BF16),
            HELD, pltpu.VMEM((RING, PEERS, 32, COLUMNS), BF16), pltpu.VMEM((PEERS, 8, 16, COLUMNS), BF16),
            DMA((9,)), DMA((RING,)), *GATHER_SEMS, DMA((PEERS,)), DMA((PEERS,)),
            pltpu.VMEM((PEERS, PAIR, SHARDS, 32, COLUMNS), BF16), DMA((PAIR, PEERS)), *GATHER_SEMS,
            *[DMA((RING, PEERS)) for _ in BOTH], *[DMA((1, PEERS)) for _ in BOTH],
        ],
        compiler_params=pltpu.CompilerParams(collective_id=collective_id, has_side_effects=True, vmem_limit_bytes=VMEM_BYTES),
        name="first_attention",
    )(x_prompt, x_resp, w_query, w_key, w_value, gain, cos, sin, info, out_slice)


def second_attention_kernel(qkv_ref, back_ref, mixed_out, stage, qkv_in, k_s, v_s, held, mixed_stage,
                            ring_send, ring_recv, near_send, near_recv, *routes):
    net = Exchange()
    me = net.me
    prompt = RespGather(net, held, ring_send, ring_recv, near_send, near_recv)
    router = Router(net, RING, lambda t, d: stage.at[t, d], lambda t, d: qkv_in.at[t, d], routes[:PAIR])
    mixed_router = Router(net, RING, lambda t, d: mixed_stage.at[t, d], lambda t, d: mixed_out.at[d, t], routes[PAIR:])
    for k in BOTH:
        held[me, k] = qkv_ref[0, :, pl.ds((k + 1) * COLUMNS, COLUMNS)]
    net.barrier()
    prompt.start()
    prompt.start_rest()
    count = back_ref.shape[1]

    def send_rows(t):
        place = lax.broadcasted_iota(jnp.int32, (Q_TILE, count), 0) + t * Q_TILE == back_ref[...]
        rows = jnp.dot(place.astype(BF16), qkv_ref[1:].reshape(count, 3 * COLUMNS), preferred_element_type=F32).astype(BF16)
        stage[t] = rows.reshape(PEERS, Q_TILE // PEERS, 3 * COLUMNS)
        router.send(t)
        qkv_in[t, me] = stage[t, me]

    send_rows(0)
    prompt.relay()
    for t in range(1, RING):
        send_rows(t)
    prompt.share()
    prompt.collect()
    for t in range(RING):
        router.collect(t)
        rows = jnp.dot(undeal(Q_TILE), qkv_in[t].reshape(Q_TILE, 3 * COLUMNS), preferred_element_type=F32).astype(BF16)
        k_s[pl.ds(t * Q_TILE, Q_TILE)] = rows[:, COLUMNS:PAIR * COLUMNS]
        v_s[pl.ds(t * Q_TILE, Q_TILE)] = rows[:, PAIR * COLUMNS:]
        mixed = attend_response(t, rows[:, :COLUMNS], held, k_s, v_s)
        deal_mixed(mixed_router, t, mixed, mixed_stage, mixed_out)
    for t in range(RING):
        mixed_router.collect(t)
    for each in (router, mixed_router):
        each.finish()
    prompt.finish()


def second_attention(qkv, back, collective_id):
    rows = RING * Q_TILE
    wide = (32, 3 * COLUMNS)
    return pl.pallas_call(
        second_attention_kernel,
        out_shape=jax.ShapeDtypeStruct((PEERS, RING, 32, COLUMNS), BF16),
        in_specs=[VMEM, VMEM],
        out_specs=VMEM,
        scratch_shapes=[
            pltpu.VMEM((RING, PEERS) + wide, BF16), pltpu.VMEM((RING, PEERS) + wide, BF16),
            pltpu.VMEM((rows, COLUMNS), BF16), pltpu.VMEM((rows, COLUMNS), BF16),
            HELD, pltpu.VMEM((RING, PEERS, 32, COLUMNS), BF16), *GATHER_SEMS,
            *[DMA((RING, PEERS)) for _ in range(RING)],
        ],
        compiler_params=pltpu.CompilerParams(collective_id=collective_id, has_side_effects=True, vmem_limit_bytes=VMEM_BYTES),
        name=f"second_attention{collective_id}",
    )(qkv, back)


def slice_kernel(w_hbm, out_ref, send_sem, recv_sem):
    me, home = lax.axis_index("model"), lax.axis_index("resp")
    others = [(me + k) % SHARDS for k in range(1, SHARDS)]
    rows = pl.ds(pl.multiple_of(home * 32, 32), 32)

    def part(device):
        return w_hbm.at[:, rows, pl.ds(pl.multiple_of(device * COLUMNS, COLUMNS), COLUMNS)]

    def copy(device, place):
        return pltpu.make_async_remote_copy(
            src_ref=part(device), dst_ref=out_ref.at[:, place], send_sem=send_sem.at[device], recv_sem=recv_sem.at[place],
            device_id={"model": device}, device_id_type=MESH)

    own = pltpu.make_async_copy(part(me), out_ref.at[:, me], send_sem.at[me])
    own.start()
    barrier = pltpu.get_barrier_semaphore()
    for device in others:
        pl.semaphore_signal(barrier, device_id={"model": device}, device_id_type=MESH)
    pl.semaphore_wait(barrier, len(others))
    for device in others:
        copy(device, me).start()
    for device in others:
        copy(device, device).wait_recv()
    for device in others:
        copy(device, me).wait_send()
    own.wait()


def slice_columns(w_out, collective_id):
    return pl.pallas_call(
        slice_kernel,
        out_shape=jax.ShapeDtypeStruct((PAIR, SHARDS, 32, COLUMNS), BF16),
        in_specs=[ANY],
        out_specs=VMEM,
        scratch_shapes=[DMA((SHARDS,)), DMA((SHARDS,))],
        compiler_params=pltpu.CompilerParams(collective_id=collective_id, has_side_effects=True),
        name="slice_columns",
    )(w_out)


class Answer:
    def __init__(self, every, out_ref, stat_send, stat_recv, row_send, row_recv):
        self.every, self.out = every, out_ref
        self.stat_sems, self.row_sems = (stat_send, stat_recv), (row_send, row_recv)
        self.me, self.home = lax.axis_index("model"), lax.axis_index("resp")
        self.models = [(self.me + k) % SHARDS for k in range(1, SHARDS)]
        self.homes = [(self.home + k) % PEERS for k in range(1, PEERS)]

    def barrier(self):
        sem = pltpu.get_barrier_semaphore()
        for axis, devices in (("model", self.models), ("resp", self.homes)):
            for device in devices:
                pl.semaphore_signal(sem, device_id={axis: device}, device_id_type=MESH)
        pl.semaphore_wait(sem, len(self.models) + len(self.homes))

    def stat_copy(self, owner, device, place):
        ref = self.every.at[owner]
        return pltpu.make_async_remote_copy(
            src_ref=ref, dst_ref=ref, send_sem=self.stat_sems[0].at[device], recv_sem=self.stat_sems[1].at[place],
            device_id={"model": device}, device_id_type=MESH)

    def row_copy(self, owner, device, place):
        ref = self.out.at[owner]
        return pltpu.make_async_remote_copy(
            src_ref=ref, dst_ref=ref, send_sem=self.row_sems[0].at[device], recv_sem=self.row_sems[1].at[place],
            device_id={"resp": device}, device_id_type=MESH)

def combine_kernel(stats_ref, out_ref, every, *sems):
    net = Answer(every, out_ref, *sems)
    every[net.me] = stats_ref[...]
    net.barrier()
    for device in net.models:
        net.stat_copy(net.me, device, net.me).start()
    for device in net.models:
        net.stat_copy(device, device, device).wait_recv()
    found = []
    for c in range(stats_ref.shape[0]):
        tiles = [every[k, c] for k in range(SHARDS)]
        top = functools.reduce(jnp.maximum, [tile[:1] for tile in tiles])
        total = functools.reduce(jnp.add, [tile[1:PAIR] * jnp.exp(tile[:1] - top) for tile in tiles])
        found.append(functools.reduce(jnp.add, [tile[PAIR:3] for tile in tiles]) - top - jnp.log(total))
    out_ref[net.home] = jnp.concatenate(found, axis=0)
    for device in net.homes:
        net.row_copy(net.home, device, net.home).start()
    for device in net.homes:
        net.row_copy(device, device, device).wait_recv()
    for device in net.models:
        net.stat_copy(net.me, device, device).wait_send()
    for device in net.homes:
        net.row_copy(net.home, device, device).wait_send()


def combine(stats, collective_id):
    return pl.pallas_call(
        combine_kernel,
        out_shape=jax.ShapeDtypeStruct((PEERS, PEERS, LANES), F32),
        in_specs=[VMEM],
        out_specs=VMEM,
        scratch_shapes=[pltpu.VMEM((SHARDS,) + stats.shape, F32), *[DMA((SHARDS,)) for _ in BOTH], *[DMA((PEERS,)) for _ in BOTH]],
        compiler_params=pltpu.CompilerParams(collective_id=collective_id, has_side_effects=True),
        name="combine",
    )(stats)


ROPE_BASE = 10000.0
VARIANTS = (640, 768, 512, 1024)


def rope_tables(positions):
    half = LANES // PAIR
    lane = jnp.arange(LANES)
    frequency = ROPE_BASE ** (-(lane % half).astype(F32) / half)
    angles = positions.astype(F32)[:, None] * frequency
    return jnp.cos(angles), jnp.sin(angles) * jnp.where(lane < half, -1.0, 1.0)


def solution(mesh):
    groups = mesh.shape['resp']
    row_axes = ('prompts', 'resp')
    head_spec = P(None, None, 'model', None)
    in_specs = (P(row_axes, None), P(row_axes, None, None), P(row_axes, None), P(row_axes), P(None, None), head_spec, head_spec, head_spec, P(None, 'model', None, None), P(None, None), P(None, None, 'model'), P(None, None, 'model'), P(None, 'model', None), P(None), P(None, 'model'))

    def device_step(x_prompt, x_resp, targets, resp_lens, attn_gain, w_query, w_key, w_value, w_out, mlp_gain, w_gate, w_up, w_down, final_gain, w_vocab):
        prompt_rows = x_prompt.shape[0]
        resp_len, width = x_resp.shape[1:]
        prompt_len = prompt_rows * groups
        me = lax.axis_index('model')
        home = lax.axis_index('resp')
        per = resp_len // groups
        gate_t, up_t = jnp.swapaxes(w_gate, 1, 2), jnp.swapaxes(w_up, 1, 2)
        out_flat = w_out.reshape(w_out.shape[0], COLUMNS, width)
        projections = [w.reshape(w.shape[0], PAIR * width, LANES) for w in (w_query, w_key, w_value)]
        prompt_pos = home * prompt_rows + jnp.arange(prompt_rows)

        cos, sin = rope_tables(jnp.concatenate([prompt_pos, prompt_len + jnp.arange(resp_len)]))
        info = jnp.concatenate([
            targets[0].reshape(per, groups).T[:, None, :],
            jnp.broadcast_to(resp_lens[0], (groups, groups - 1, per)).astype(jnp.int32)], axis=1)
        mixed, res, infos, prompt, project_next, out_columns = first_attention(
            x_prompt, x_resp[0], *projections, attn_gain, cos, sin, info, slice_columns(out_flat, PAIR), 0)
        lens = infos[:, 1, 0]
        need = (lens + groups - 1) // groups
        ends = jnp.sum(jnp.where(jnp.arange(groups)[:, None] >= jnp.arange(groups), need, 0), axis=1)
        starts = ends - need
        dealt = groups * per

        def finish_with(size, ident):
            def run(operands):
                mixed, res, prompt = operands
                slot = jnp.arange(size)
                which = jnp.sum((slot[:, None] >= ends).astype(jnp.int32), axis=1)
                row = slot - jnp.sum(jnp.where(which[:, None] == jnp.arange(groups), starts, 0), axis=1)
                real = slot < ends[-1]
                source = jnp.where(real, which * per + row, -1)
                chosen = source[:, None] == jnp.arange(dealt)
                wanted = jnp.sum(jnp.where(chosen, infos[:, 0, :].reshape(dealt), 0), axis=1) - me * w_vocab.shape[1]
                ids = jnp.where(jnp.arange(LANES) == 0, source[:, None], wanted[:, None]).reshape(-1, LANES, LANES)
                tables = rope_tables(jnp.concatenate([prompt_pos, prompt_len + groups * row + home]))
                weights = (out_columns.reshape(PAIR, width, COLUMNS), gate_t, up_t, w_down)
                qkv, new_res = mega(
                    mlp_gain, attn_gain, ids, mixed.reshape(dealt, COLUMNS), res.reshape(dealt, COLUMNS),
                    [t.reshape(-1, LANES, LANES) for t in tables] + [prompt], *weights, project_next, 0, ident)
                part = per // RING
                back = jnp.where(real, (row // part) * (groups * part) + which * part + row % part, -1)
                mixed = second_attention(qkv, back[None], ident + 1)
                return mega(mlp_gain, final_gain[None], ids, mixed.reshape(dealt, COLUMNS), new_res, [], *weights, w_vocab, 1, ident + PAIR)
            return run

        smallest = sorted(VARIANTS)
        fit = sum((ends[-1] > size).astype(jnp.int32) for size in smallest[:-1])
        index = sum(jnp.where(fit == smallest.index(size), i, 0) for i, size in enumerate(VARIANTS))
        stats = lax.switch(index, [finish_with(size, 3 + 3 * i) for i, size in enumerate(VARIANTS)], (mixed, res, prompt))
        found = combine(stats, 1).reshape(groups, dealt)
        start = jnp.sum(jnp.where(jnp.arange(groups) == home, starts, 0))
        mine = lax.dynamic_slice(jnp.pad(found, ((0, 0), (0, per))), (0, start), (groups, per))
        log_probs = mine.T.reshape(resp_len)
        log_probs = jnp.where(jnp.arange(resp_len) < resp_lens[0], log_probs, 0.0)
        return log_probs[None, :]

    return jax.shard_map(device_step, mesh=mesh, in_specs=in_specs, out_specs=P(row_axes, None), check_vma=False)
```

```python
import functools

import jax
import jax.numpy as jnp
from jax import lax
from jax.experimental import pallas as pl
from jax.experimental.pallas import tpu as pltpu
from jax.sharding import PartitionSpec as P

MESH = pl.DeviceIdType.MESH
F32 = jnp.float32
BF16 = jnp.bfloat16
EPS = 1e-6
LANES = 128
PAIR = 2
RING = 4
COLUMNS = PAIR * LANES
SHARDS = RING * RING
PEERS = 8
BOTH = range(PAIR)
VMEM_BYTES = 67_000_000
LATE_ROWS = 640
LOGITS = 512
CHUNKS = 4
VMEM = pl.BlockSpec(memory_space=pltpu.VMEM)
ANY = pl.BlockSpec(memory_space=pl.ANY)
DMA = pltpu.SemaphoreType.DMA
KINDS = range(RING * 3)
SUM_FAR, SUM_NEAR, SUM_RELAY, SUM2_FAR, SUM2_NEAR, SUM2_RELAY, TAKE_OWN, TAKE_REST, TAKE_RELAY, TAKE2_OWN, TAKE2_REST, TAKE2_RELAY = KINDS


def block_of(color, first, second):
    return RING * first + second if color else RING * second + first


def pair(index):
    return pl.ds(PAIR * index, PAIR)


class Torus:
    def __init__(self, refs, send_sem, recv_sem):
        self.refs = refs
        self.far, self.near, self.relayed, self.sums, self.relayed2, self.sums2, self.rows = refs
        self.send_sem, self.recv_sem = send_sem, recv_sem
        me = lax.axis_index("model")
        z, y = me // RING, me % RING
        self.place = ((y, z), (z, y))
        along_y = [z * RING + self.step(y, way) for way in (1, -1)]
        along_z = [self.step(z, way) * RING + y for way in (1, -1)]
        self.neighbors = ((along_y, along_z), (along_z, along_y))

    def step(self, place, by):
        return (place + by + RING) % RING

    def barrier(self):
        sem = pltpu.get_barrier_semaphore()
        for ring in self.neighbors[0]:
            for device in ring:
                pl.semaphore_signal(sem, device_id={"model": device}, device_id_type=MESH)
        pl.semaphore_wait(sem, RING)

    def ends(self, kind, c, q, d):
        (p, s), way, other = self.place[q], 1 - PAIR * d, 1 - d
        far, near, relayed, sums, relayed2, sums2, rows = (ref.at[c, q] for ref in self.refs)
        own = sums.at[0]
        back_s, back_p = self.step(s, -way), self.step(p, -way)
        return {
            SUM_FAR: lambda: (far.at[pair(d)], relayed.at[d], relayed.at[d]),
            SUM_NEAR: lambda: (near.at[d], sums.at[d, pair(other)], sums.at[d, pair(other)]),
            SUM_RELAY: lambda: (relayed.at[d], sums.at[d, pair(d)], sums.at[d, pair(d)]),
            SUM2_FAR: lambda: (own.at[self.step(s, PAIR), d], relayed2.at[d], relayed2.at[d]),
            SUM2_NEAR: lambda: (own.at[self.step(s, way), other], sums2.at[d, other], sums2.at[d, other]),
            SUM2_RELAY: lambda: (relayed2.at[d], sums2.at[d, d], sums2.at[d, d]),
            TAKE_OWN: lambda: (rows.at[p, s, d], rows.at[p, s, d], rows.at[p, back_s, d]),
            TAKE_REST: lambda: (rows.at[p, s, other], rows.at[p, s, other], rows.at[p, back_s, other]),
            TAKE_RELAY: lambda: (rows.at[p, back_s, d], rows.at[p, back_s, d], rows.at[p, self.step(s, PAIR), d]),
            TAKE2_OWN: lambda: (rows.at[p, pair(d)], rows.at[p, pair(d)], rows.at[back_p, pair(d)]),
            TAKE2_REST: lambda: (rows.at[p, pair(other)], rows.at[p, pair(other)], rows.at[back_p, pair(other)]),
            TAKE2_RELAY: lambda: (rows.at[back_p, pair(d)], rows.at[back_p, pair(d)], rows.at[self.step(p, PAIR), pair(d)]),
        }[kind]()

    def copy(self, kind, c, q, d, src, dst):
        second_ring = kind in (SUM2_FAR, SUM2_NEAR, SUM2_RELAY, TAKE_OWN, TAKE_REST, TAKE_RELAY)
        return pltpu.make_async_remote_copy(
            src_ref=src, dst_ref=dst, send_sem=self.send_sem.at[c, q, d, kind], recv_sem=self.recv_sem.at[c, q, d, kind],
            device_id={"model": self.neighbors[q][second_ring][d]}, device_id_type=MESH)

    def send(self, c, q, d, kind):
        src, dst, _ = self.ends(kind, c, q, d)
        self.copy(kind, c, q, d, src, dst).start()

    def sent(self, c, q, *kinds):
        for kind in kinds:
            for d in BOTH:
                src, dst, _ = self.ends(kind, c, q, d)
                self.copy(kind, c, q, d, src, dst).wait_send()

    def arrived(self, c, q, d, *kinds):
        for kind in kinds:
            _, _, here = self.ends(kind, c, q, d)
            self.copy(kind, c, q, d, here, here).wait_recv()


def halves_of(ref):
    return ref[:, :COLUMNS], ref[:, COLUMNS:]


def halves(value):
    return value[:, :LANES], value[:, LANES:]


def store_block(ref, value):
    for half, part in enumerate(halves(value)):
        ref[half] = part


def add_block(ref, value):
    for half, part in enumerate(halves(value)):
        ref[half] += part


class Gather:
    def __init__(self, net):
        self.net = net

    def begin_rows(self, c, q):
        for kind in (TAKE_OWN, TAKE_REST):
            for d in BOTH:
                self.net.send(c, q, d, kind)

    def relay_rows(self, c, q):
        for d in BOTH:
            self.net.arrived(c, q, d, TAKE_OWN)
            self.net.send(c, q, d, TAKE_RELAY)

    def take_second(self, c, q):
        for d in BOTH:
            self.net.arrived(c, q, d, TAKE_REST, TAKE_RELAY)
        for kind in (TAKE2_OWN, TAKE2_REST):
            for d in BOTH:
                self.net.send(c, q, d, kind)

    def relay_last(self, c, q):
        for d in BOTH:
            self.net.arrived(c, q, d, TAKE2_OWN)
            self.net.send(c, q, d, TAKE2_RELAY)

    def complete(self, c, q):
        for d in BOTH:
            self.net.arrived(c, q, d, TAKE2_REST, TAKE2_RELAY)
        self.net.sent(c, q, TAKE_OWN, TAKE_REST, TAKE_RELAY, TAKE2_OWN, TAKE2_REST, TAKE2_RELAY)

    def middle(self):
        return [self.relay_rows, self.take_second, self.relay_last]


class Sum(Gather):
    def __init__(self, net, lhs_of, w_ref, finish):
        self.net, self.lhs_of, self.w_ref, self.finish = net, lhs_of, w_ref, finish

    def product(self, lhs, color, first, second):
        start = pl.multiple_of(block_of(color, first, second) * COLUMNS, COLUMNS)
        return jnp.dot(lhs, self.w_ref[:, pl.ds(start, COLUMNS)], preferred_element_type=F32)

    def begin(self, c, q):
        net, p, lhs = self.net, self.net.place[q][0], self.lhs_of(c, q)
        for k in range(RING):
            store_block(net.far.at[c, q, k], self.product(lhs, q, net.step(p, PAIR), k))
        for d in BOTH:
            net.send(c, q, d, SUM_FAR)
        for d in BOTH:
            for k in BOTH:
                store_block(net.near.at[c, q, d, k], self.product(lhs, q, net.step(p, 1 - PAIR * d), PAIR * (1 - d) + k))
            net.send(c, q, d, SUM_NEAR)

    def relay_sum(self, c, q):
        net, p, lhs = self.net, self.net.place[q][0], self.lhs_of(c, q)
        for d in BOTH:
            net.arrived(c, q, d, SUM_FAR)
            for k in BOTH:
                add_block(net.relayed.at[c, q, d, k], self.product(lhs, q, net.step(p, 1 - PAIR * d), PAIR * d + k))
            net.send(c, q, d, SUM_RELAY)

    def begin_second(self, c, q):
        net, lhs = self.net, self.lhs_of(c, q)
        for d in BOTH:
            net.arrived(c, q, d, SUM_NEAR, SUM_RELAY)
        for k in range(RING):
            for half, part in enumerate(halves(self.product(lhs, q, net.place[q][0], k))):
                net.sums[c, q, 0, k, half] += net.sums[c, q, 1, k, half] + part
        for kind in (SUM2_FAR, SUM2_NEAR):
            for d in BOTH:
                net.send(c, q, d, kind)
        net.sent(c, q, SUM_FAR)

    def relay_second(self, c, q):
        net = self.net
        for d in BOTH:
            net.arrived(c, q, d, SUM2_FAR)
            net.relayed2[c, q, d] += net.sums[c, q, 0, net.step(net.place[q][1], 1 - PAIR * d), d]
            net.send(c, q, d, SUM2_RELAY)

    def finish_sum(self, c, q):
        net = self.net
        net.sent(c, q, SUM_NEAR, SUM_RELAY)
        for d in BOTH:
            net.arrived(c, q, d, SUM2_NEAR, SUM2_RELAY)
        for half in BOTH:
            self.finish(c, q, half, net.sums[c, q, 0, net.place[q][1], half] + net.sums2[c, q, 0, half] + net.sums2[c, q, 1, half])
        self.begin_rows(c, q)

    def relay_rows(self, c, q):
        self.net.sent(c, q, SUM2_FAR, SUM2_NEAR, SUM2_RELAY)
        super().relay_rows(c, q)

    def middle(self):
        return [self.relay_sum, self.begin_second, self.relay_second, self.finish_sum, *super().middle()]


def normed(net, c, q, gain_ref, layer):
    rows = net.rows.shape[-PAIR]
    tile = PAIR * 8 if rows % (PAIR * 8) == 0 else 8
    spots = [(first, second, half) for first in range(RING) for second in range(RING) for half in BOTH]

    @pl.loop(0, rows // tile)
    def _(i):
        span = pl.ds(pl.multiple_of(i * tile, tile), tile)
        acts = [net.rows[(c, q) + spot + (span,)].astype(F32) for spot in spots]
        squares = functools.reduce(jnp.add, [v * v for v in acts])
        inv = lax.rsqrt(jnp.sum(squares, axis=-1, keepdims=True) / (LANES * len(acts)) + EPS)
        for spot, v in zip(spots, acts):
            column = block_of(q, *spot[:PAIR]) * COLUMNS + spot[PAIR] * LANES
            net.rows[(c, q) + spot + (span,)] = (v * inv * gain_ref[pl.ds(layer, 1), pl.ds(column, LANES)]).astype(BF16)


def rows_of(net, c, q):
    parts = []
    for upper in range(RING):
        for lower in range(RING):
            first, second = (upper, lower) if q else (lower, upper)
            parts += [net.rows[c, q, first, second, half] for half in BOTH]
    return jnp.concatenate(parts, axis=1)


def times_transposed(lhs, rhs):
    return lax.dot_general(lhs, rhs, (((1,), (1,)), ((), ())), preferred_element_type=F32)


def late_plan(width, count):
    plan, start = [], 0
    for buffer in BOTH:
        for slot in range(width // count):
            size = min(LATE_ROWS, width - start)
            if size:
                plan.append((buffer, slot * count, start, size))
            start += size
    return plan, width - start


def rope(value, cos, sin):
    return jnp.concatenate([v * cos + pltpu.roll(v, LANES // PAIR, 1) * sin for v in halves(value)], axis=1)


def put_projected(product, cos_ref, sin_ref, out_ref, span):
    for k in range(3):
        value = product(k * COLUMNS, COLUMNS)
        if k < PAIR:
            value = rope(value, cos_ref[span], sin_ref[span])
        out_ref[span, pl.ds(k * COLUMNS, COLUMNS)] = value.astype(BF16)


def statistics(product, count, target):
    top = total = picked = None
    for k in range(count // LOGITS):
        logits = product(k * LOGITS, LOGITS)
        here = jnp.max(logits, axis=-1, keepdims=True)
        ids = lax.broadcasted_iota(jnp.int32, logits.shape, 1) + k * LOGITS
        found = jnp.sum(jnp.where(ids == target, logits, 0.0), axis=-1, keepdims=True)
        if k:
            both = jnp.maximum(top, here)
            total = total * jnp.exp(top - both) + jnp.sum(jnp.exp(logits - both), axis=-1, keepdims=True)
            top, picked = both, picked + found
        else:
            top, total, picked = here, jnp.sum(jnp.exp(logits - here), axis=-1, keepdims=True), found
    lane = lax.broadcasted_iota(jnp.int32, (target.shape[0], LANES), 1)
    return jnp.where(lane == 0, top, jnp.where(lane == 1, total, picked))


def mega_kernel(chunks, layer, last, gain_ref, next_gain_ref, ids_ref, dealt_ref, old_ref, *args):
    if last:
        side_refs, args = (), args
    else:
        side_refs, args = args[:3], args[3:]
    w_out_hbm, w_gate_hbm, w_up_hbm, w_down_hbm, *args = args
    late_hbm, out_ref, *args = args
    if not last:
        new_res_ref, *args = args
    (w_out, w_gate, w_up, w_down, late_rest, res, inner, middle, stats,
     far, near, relayed, sums, relayed2, sums2, rows, w_sem, late_sem, send_sem, recv_sem, ready_sem) = args
    loads = [pltpu.make_async_copy(src.at[layer], dst, w_sem.at[i]) for i, (src, dst) in enumerate(
        ((w_out_hbm, w_out), (w_gate_hbm, w_gate), (w_up_hbm, w_up), (w_down_hbm, w_down)))]
    for load in loads:
        load.start()
    width, count = late_hbm.shape
    plan, left = late_plan(width, count)
    late = [(late_hbm.at[pl.ds(start, size)], (w_gate, w_up)[buffer].at[pl.ds(0, size), pl.ds(lane, count)]) for buffer, lane, start, size in plan]
    if left:
        late.append((late_hbm.at[pl.ds(width - left, left)], late_rest))
    late_loads = [pltpu.make_async_copy(src, dst, late_sem.at[i]) for i, (src, dst) in enumerate(late)]
    net = Torus((far, near, relayed, sums, relayed2, sums2, rows), send_sem, recv_sem)
    net.barrier()

    part = rows.shape[-PAIR]

    def span_of(c, q=0, parts=1):
        return pl.ds(pl.multiple_of((PAIR * c + q) * part, 16), parts * part)

    def after_prompt(c, q=0, parts=1):
        return pl.ds(pl.multiple_of((PAIR * c + q) * part + LANES * last, 16), parts * part)

    def picked(c, ref, prompt):
        ids = ids_ref[after_prompt(c, parts=PAIR), :1]
        chosen = (ids == lax.broadcasted_iota(jnp.int32, (PAIR * part, PEERS * LANES), 1)).astype(BF16)
        value = jnp.dot(chosen, ref[...], preferred_element_type=F32)
        if prompt is not None:
            row = lax.broadcasted_iota(jnp.int32, (PAIR * part, LANES), 0) + PAIR * part * c
            chosen = (row == lax.broadcasted_iota(jnp.int32, (PAIR * part, LANES), 1)).astype(BF16)
            value += jnp.dot(chosen, prompt, preferred_element_type=F32)
        return value.astype(BF16)

    def put(ref, value, place_of):
        for q in BOTH:
            for half, columns in enumerate(halves(value)):
                ref[place_of(q) + (half,)] = columns[q * part:(q + 1) * part]

    def begin(c):
        prompts = (None, None) if last else halves_of(side_refs[PAIR])
        put(rows, picked(c, dealt_ref, prompts[0]), lambda q: (c, q) + net.place[q])
        if not last:
            put(res, picked(c, old_ref, prompts[1]), lambda q: (c, q))
        for q in BOTH:
            first.begin_rows(c, q)

    def finish(c, q, half, total):
        value = (middle[c, q, half].astype(F32) + total).astype(BF16)
        if not last:
            new_res_ref[span_of(c, q), pl.ds(half * LANES, LANES)] = value
        rows[(c, q) + net.place[q] + (half,)] = value

    first = Gather(net)
    second = Sum(net, lambda c, q: inner[c, q], w_down, finish)

    def project_out(c):
        for q in BOTH:
            first.complete(c, q)
        total = jnp.dot(jnp.concatenate([rows_of(net, c, q) for q in BOTH], axis=0), w_out[...], preferred_element_type=F32)
        for q in BOTH:
            for half, columns in enumerate(halves(total)):
                old = old_ref[after_prompt(c, q), pl.ds(half * LANES, LANES)] if last else res[c, q, half]
                value = (old.astype(F32) + columns[q * part:(q + 1) * part]).astype(BF16)
                middle[c, q, half] = value
                rows[(c, q) + net.place[q] + (half,)] = value
        for ring in net.neighbors[0]:
            for device in ring:
                pl.semaphore_signal(ready_sem.at[c], device_id={"model": device}, device_id_type=MESH)

    def begin_again(c):
        pl.semaphore_wait(ready_sem.at[c], RING)
        for q in BOTH:
            first.begin_rows(c, q)

    def hidden_of(c, stage, gain, row):
        for q in BOTH:
            stage.complete(c, q)
            normed(net, c, q, gain, row)
        return jnp.concatenate([rows_of(net, c, q) for q in BOTH], axis=0)

    def mlp(c):
        hidden = hidden_of(c, first, gain_ref, layer)
        value = (jax.nn.silu(times_transposed(hidden, w_gate[...])) * times_transposed(hidden, w_up[...])).astype(BF16)
        inner[c] = value.reshape(inner.shape[1:])
        for q in BOTH:
            second.begin(c, q)

    def after(c):
        hidden = hidden_of(c, second, next_gain_ref, 0 if last else layer + 1)

        def product(lane, size):
            parts = [jnp.dot(hidden[:, start:start + rows_here], (w_gate, w_up)[buffer][pl.ds(0, rows_here), pl.ds(at + lane, size)], preferred_element_type=F32)
                     for buffer, at, start, rows_here in plan]
            if left:
                parts.append(jnp.dot(hidden[:, width - left:], late_rest[:, pl.ds(lane, size)], preferred_element_type=F32))
            return functools.reduce(jnp.add, parts)

        if last:
            stats[span_of(c, parts=PAIR)] = statistics(product, count, ids_ref[after_prompt(c, parts=PAIR), 1:PAIR])
        else:
            put_projected(product, *side_refs[:PAIR], out_ref, span_of(c, parts=PAIR))

    def on_both(step):
        def run(c):
            for q in BOTH:
                step(c, q)
        return run

    gather = [on_both(step) for step in first.middle()]
    steps = [begin, *gather, project_out, begin_again, *gather, mlp, *map(on_both, second.middle())]
    at_mlp = steps.index(mlp)
    steps += [None] * max(0, at_mlp + chunks - len(steps)) + [after]

    @pl.loop(0, len(steps) + chunks - 1)
    def _(slot):
        @pl.when(slot == steps.index(project_out))
        def _():
            for load in loads:
                load.wait()

        @pl.when(slot == len(steps) - 1)
        def _():
            for load in late_loads:
                load.wait()

        for k, step in reversed(list(enumerate(steps))):
            if step is None:
                continue

            @pl.when(slot >= k)
            def _():
                @pl.when(slot < k + chunks)
                def _():
                    step(slot - k)

        @pl.when(slot == at_mlp + chunks - 1)
        def _():
            for load in late_loads:
                load.start()

    if last:
        for k in range(PEERS):
            here = stats[pl.ds(k * LANES, LANES)] if k * LANES < stats.shape[0] else jnp.zeros((LANES, LANES), F32)
            out_ref[k] = here.T[:PEERS]


def mega(gain, next_gain, ids, dealt, old, sides, w_out, w_gate_t, w_up_t, w_down, late, layer, collective_id):
    last = not sides
    chunks = CHUNKS
    total = ids.shape[0] - LANES * last
    _, hidden, width = w_gate_t.shape
    rows = total // (PAIR * chunks)
    per = (chunks, PAIR)
    tile = (rows, LANES)
    count = late.shape[1]
    _, left = late_plan(width, count)

    sem = DMA(per + (PAIR, len(KINDS)))
    out = jax.ShapeDtypeStruct((PEERS, PEERS, LANES), F32) if last else (
        jax.ShapeDtypeStruct((total, count), BF16), jax.ShapeDtypeStruct((total, COLUMNS), BF16))
    return pl.pallas_call(
        functools.partial(mega_kernel, chunks, layer, last),
        out_shape=out,
        in_specs=[VMEM] * (5 + len(sides)) + [ANY] * 5,
        out_specs=VMEM if last else (VMEM, VMEM),
        scratch_shapes=[
            pltpu.VMEM((width, COLUMNS), BF16),
            *[pltpu.VMEM((hidden, width), BF16) for _ in range(3)],
            pltpu.VMEM((left or 8, count), BF16),
            pltpu.VMEM(per + (PAIR,) + (tile if not last else (8, LANES)), BF16),
            pltpu.VMEM(per + (rows, hidden), BF16),
            pltpu.VMEM(per + (PAIR,) + tile, BF16),
            pltpu.VMEM((total if last else 8, LANES), F32),
            pltpu.VMEM(per + (RING, PAIR) + tile, F32),
            pltpu.VMEM(per + (PAIR, PAIR, PAIR) + tile, F32),
            pltpu.VMEM(per + (PAIR, PAIR, PAIR) + tile, F32),
            pltpu.VMEM(per + (PAIR, RING, PAIR) + tile, F32),
            pltpu.VMEM(per + (PAIR,) + tile, F32),
            pltpu.VMEM(per + (PAIR, PAIR) + tile, F32),
            pltpu.VMEM(per + (RING, RING, PAIR) + tile, BF16),
            DMA((RING,)), DMA((SHARDS,)), sem, sem, pltpu.SemaphoreType.REGULAR((chunks,)),
        ],
        compiler_params=pltpu.CompilerParams(collective_id=collective_id, has_side_effects=True, vmem_limit_bytes=VMEM_BYTES),
        name=f"mega{collective_id}",
    )(gain, next_gain, ids, dealt, old, *sides, w_out, w_gate_t, w_up_t, w_down, late)


TILE = 128
Q_TILE = 256
LOG2E = 1.4426950408889634
HELD = pltpu.VMEM((PEERS, PAIR, TILE, COLUMNS), BF16)
GATHER_SEMS = [DMA((PAIR, 3)), DMA((PAIR, 3)), DMA((RING,)), DMA((RING,))]


class Exchange:
    def __init__(self):
        self.me = lax.axis_index("resp")
        self.others = [(self.me + k) % PEERS for k in range(1, PEERS)]

    def barrier(self):
        sem = pltpu.get_barrier_semaphore()
        for device in self.others:
            pl.semaphore_signal(sem, inc=1, device_id={"resp": device}, device_id_type=MESH)
        pl.semaphore_wait(sem, PEERS - 1)

    def copy(self, src, dst, send_sem, recv_sem, device):
        return pltpu.make_async_remote_copy(src_ref=src, dst_ref=dst, send_sem=send_sem, recv_sem=recv_sem,
                                            device_id={"resp": device}, device_id_type=MESH)

    def scatter(self, src_of, dst, send_sem, recv_sem):
        for device in self.others:
            self.copy(src_of(device), dst, send_sem.at[device], recv_sem.at[self.me], device).start()

    def collected(self, dst_of, recv_sem):
        for device in self.others:
            self.copy(dst_of(device), dst_of(device), recv_sem.at[device], recv_sem.at[device], device).wait_recv()

    def sent(self, src_of, send_sem, recv_sem):
        for device in self.others:
            self.copy(src_of(device), src_of(device), send_sem.at[device], recv_sem.at[device], device).wait_send()


class Router:
    def __init__(self, net, tiles, src_of, dst_of, sems):
        self.net, self.tiles, self.src_of, self.dst_of = net, tiles, src_of, dst_of
        self.send_sem, self.recv_sem = sems

    def send(self, t):
        self.net.scatter(lambda d: self.src_of(t, d), self.dst_of(t, self.net.me), self.send_sem.at[t], self.recv_sem.at[t])

    def collect(self, t):
        self.net.collected(lambda d: self.dst_of(t, d), self.recv_sem.at[t])

    def finish(self):
        for t in range(self.tiles):
            self.net.sent(lambda d: self.src_of(t, d), self.send_sem.at[t], self.recv_sem.at[t])


class RespGather:
    def __init__(self, net, held, ring_send, ring_recv, near_send, near_recv):
        self.net, self.held = net, held
        self.ring_sems, self.near_sems = (ring_send, ring_recv), (near_send, near_recv)
        x, core = net.me // PAIR, net.me % PAIR
        self.at = lambda by, here: (x + by + RING) % RING * PAIR + (core if here else 1 - core)

    def ring_copy(self, d, kind, ref):
        return self.net.copy(ref, ref, self.ring_sems[0].at[d, kind], self.ring_sems[1].at[d, kind], self.at(1 - PAIR * d, True))

    def near_copy(self, kind, ref):
        return self.net.copy(ref, ref, self.near_sems[0].at[kind], self.near_sems[1].at[kind], self.at(0, False))

    def sources(self, here):
        return [self.at(by, here) for by in (0, -1, 1, PAIR)]

    def start(self):
        for d in BOTH:
            self.ring_copy(d, 0, self.held.at[self.net.me, d]).start()
        self.near_copy(0, self.held.at[self.net.me]).start()

    def start_rest(self):
        for d in BOTH:
            self.ring_copy(d, 1, self.held.at[self.net.me, 1 - d]).start()

    def relay(self):
        for d in BOTH:
            ref = self.held.at[self.at(PAIR * d - 1, True), d]
            self.ring_copy(d, 0, ref).wait_recv()
            self.ring_copy(d, PAIR, ref).start()

    def share(self):
        for d in BOTH:
            device = self.at(PAIR * d - 1, True)
            self.ring_copy(d, 1, self.held.at[device, 1 - d]).wait_recv()
            self.near_copy(1 + d, self.held.at[device]).start()
        far = self.held.at[self.at(PAIR, True)]
        for d in BOTH:
            self.ring_copy(d, PAIR, far.at[d]).wait_recv()
        self.near_copy(3, far).start()

    def collect(self):
        for kind, device in enumerate(self.sources(False)):
            self.near_copy(kind, self.held.at[device]).wait_recv()

    def finish(self):
        for kind in range(3):
            for d in BOTH:
                self.ring_copy(d, kind, self.held.at[self.net.me, d]).wait_send()
        for kind in range(RING):
            self.near_copy(kind, self.held.at[self.net.me]).wait_send()


def deal(rows):
    out = lax.broadcasted_iota(jnp.int32, (rows, rows), 0)
    src = lax.broadcasted_iota(jnp.int32, (rows, rows), 1)
    per = rows // PEERS
    return jnp.where(src == (out % per) * PEERS + out // per, 1.0, 0.0).astype(BF16)


def undeal(rows):
    out = lax.broadcasted_iota(jnp.int32, (rows, rows), 0)
    src = lax.broadcasted_iota(jnp.int32, (rows, rows), 1)
    per = rows // PEERS
    return jnp.where(src == (out % PEERS) * per + out // PEERS, 1.0, 0.0).astype(BF16)


def split_heads(raw_ref, w_ref):
    tile = PAIR * LANES
    out = lax.broadcasted_iota(jnp.int32, (tile, tile), 0)
    src = lax.broadcasted_iota(jnp.int32, (tile, tile), 1)
    pick = jnp.where(src == (out % LANES) * PAIR + out // LANES, 1.0, 0.0).astype(BF16)

    @pl.loop(0, raw_ref.shape[1] // (RING * tile))
    def _(b):
        raws = [raw_ref[i, pl.ds(pl.multiple_of((b * RING + k) * tile, tile), tile)] for k in range(RING) for i in range(3)]
        heads = jnp.dot(pick, jnp.concatenate(raws, axis=1), preferred_element_type=F32).astype(BF16)
        for k in range(RING):
            here = pl.ds(pl.multiple_of((b * RING + k) * LANES, LANES), LANES)
            for i in range(3):
                for h in BOTH:
                    at = (k * 3 + i) * LANES
                    w_ref[here, pl.ds(i * COLUMNS + h * LANES, LANES)] = heads[h * LANES:(h + 1) * LANES, at:at + LANES]


def norm_tile(x_ref, out_ref, gain_ref):
    for i in range(x_ref.shape[0] // 16):
        v = x_ref[pl.ds(16 * i, 16), :].astype(F32)
        inv = lax.rsqrt(jnp.mean(v * v, axis=-1, keepdims=True) + EPS)
        out_ref[pl.ds(16 * i, 16), :] = (v * inv * gain_ref[pl.ds(0, 1), :]).astype(BF16)


def softmax_mix(q, pieces):
    factor = LOG2E * 128 ** -0.5
    outs = []
    for h in range(2):
        lanes = slice(128 * h, 128 * h + 128)
        scores = []
        for keys, _, mask in pieces:
            s = lax.dot_general(q[:, lanes], keys[:, lanes], (((1,), (1,)), ((), ())), preferred_element_type=F32)
            scores.append(s if mask is None else jnp.where(mask, s, -jnp.inf))
        top = functools.reduce(jnp.maximum, [jnp.max(s, axis=-1, keepdims=True) for s in scores])
        probs = [jnp.exp2((s - top) * factor) for s in scores]
        total = functools.reduce(jnp.add, [jnp.sum(p, axis=-1, keepdims=True) for p in probs])
        mixed = functools.reduce(jnp.add, [jnp.dot(p.astype(BF16), values[:, lanes], preferred_element_type=F32) for p, (_, values, _) in zip(probs, pieces)])
        outs.append(mixed / total)
    return jnp.concatenate(outs, axis=1).astype(BF16)


def prompt_rows_of(held, which):
    return held[:, which].reshape(PEERS * TILE, COLUMNS)


def attend_response(t, q, held, k_own, v_own):
    row = lax.broadcasted_iota(jnp.int32, (Q_TILE, Q_TILE), 0)
    col = lax.broadcasted_iota(jnp.int32, (Q_TILE, Q_TILE), 1)
    pieces = [(prompt_rows_of(held, 0), prompt_rows_of(held, 1), None)]
    if t:
        pieces.append((k_own[:t * Q_TILE], v_own[:t * Q_TILE], None))
    span = slice(t * Q_TILE, (t + 1) * Q_TILE)
    pieces.append((k_own[span], v_own[span], col <= row))
    return softmax_mix(q, pieces)


def deal_mixed(router, t, mixed, stage, out):
    dealt = jnp.dot(deal(Q_TILE), mixed, preferred_element_type=F32).astype(BF16)
    stage[t] = dealt.reshape(PEERS, Q_TILE // PEERS, COLUMNS)
    router.send(t)
    out[router.net.me, t] = stage[t, router.net.me]


def first_attention_kernel(xp_hbm, xr_hbm, w_hbm, gain_ref, cos_ref, sin_ref, info_ref, slice_ref,
                           mixed_out, res_out, info_out, prompt_out, columns_hbm,
                           xs, w, even, odd, q_s, k_s, v_s, held, mixed_stage, res_stage,
                           x_sem, w_sem, ring_send, ring_recv, near_send, near_recv, info_send, info_recv, spread_held, spread_sem, *routes):
    net = Exchange()
    spread_sems, routes = routes[:RING], routes[RING:]
    columns = RespGather(net, spread_held, *spread_sems)
    mixed_router = Router(net, RING, lambda t, d: mixed_stage.at[t, d], lambda t, d: mixed_out.at[d, t], routes[:PAIR])
    res_router = Router(net, 1, lambda t, d: res_stage.at[d], lambda t, d: res_out.at[d], routes[PAIR:])
    prompt = RespGather(net, held, ring_send, ring_recv, near_send, near_recv)
    me = net.me
    column = pl.multiple_of(lax.axis_index("model") * COLUMNS, COLUMNS)

    def load(t):
        src = xp_hbm if isinstance(t, int) and t == 0 else xr_hbm.at[pl.ds(pl.multiple_of((t - 1) * TILE, TILE), TILE)]
        return pltpu.make_async_copy(src, xs.at[t], x_sem.at[t])

    load(0).start()
    weights = pltpu.make_async_copy(w_hbm, w, w_sem)
    weights.start()
    for t in range(1, 9):
        load(t).start()
    spread_held[me] = slice_ref[...]
    net.barrier()
    columns.start()
    net.scatter(lambda d: info_ref.at[d], info_out.at[me], info_send, info_recv)
    info_out[me] = info_ref[me]

    def project(t, hidden):
        span = pl.ds(pl.multiple_of(t * TILE, TILE), TILE)
        qkv = jnp.dot(hidden[...], w[...], preferred_element_type=F32)
        cos, sin = cos_ref[span], sin_ref[span]
        return span, rope(qkv[:, :COLUMNS], cos, sin).astype(BF16), rope(qkv[:, COLUMNS:512], cos, sin).astype(BF16), qkv[:, 512:].astype(BF16)

    load(0).wait()
    norm_tile(xs.at[0], even, gain_ref)
    weights.wait()
    load(1).wait()
    span, q, k, v = project(0, even)
    norm_tile(xs.at[1], odd, gain_ref)
    q_s[span] = q
    held[me, 0] = k
    held[me, 1] = v
    prompt.start()
    prompt.start_rest()
    for t in range(PAIR, 9):
        load(t).wait()
    spread = deal(TILE)

    @pl.loop(1, 9)
    def _(t):
        dealt = jnp.dot(spread, xs[t, :, pl.ds(column, COLUMNS)], preferred_element_type=F32).astype(BF16)
        res_stage[:, t - 1] = dealt.reshape(PEERS, TILE // PEERS, COLUMNS)

    res_out[me] = res_stage[me]

    def response_tile(t, here, there):
        span, q, k, v = project(t, here)
        norm_tile(xs.at[jnp.minimum(t + 1, 8)], there, gain_ref)
        q_s[span] = q
        own = pl.ds(pl.multiple_of((t - 1) * TILE, TILE), TILE)
        k_s[own] = k
        v_s[own] = v

    @pl.loop(0, RING)
    def _(i):
        response_tile(PAIR * i + 1, odd, even)
        response_tile(PAIR * i + PAIR, even, odd)

        @pl.when(i == 0)
        def _():
            prompt.relay()
            res_router.send(0)

        @pl.when(i == 1)
        def _():
            columns.relay()
            columns.start_rest()

        pl.when(i == PAIR)(prompt.share)

    prompt.collect()
    for t in range(RING):
        mixed = attend_response(t, q_s[pl.ds(TILE + t * Q_TILE, Q_TILE)], held, k_s, v_s)
        deal_mixed(mixed_router, t, mixed, mixed_stage, mixed_out)
    row = lax.broadcasted_iota(jnp.int32, (TILE, PEERS * TILE), 0) + me * TILE
    col = lax.broadcasted_iota(jnp.int32, (TILE, PEERS * TILE), 1)
    prompt_out[:, :COLUMNS] = softmax_mix(q_s[pl.ds(0, TILE)], [(prompt_rows_of(held, 0), prompt_rows_of(held, 1), col <= row)])
    prompt_out[:, COLUMNS:] = xs[0, :, pl.ds(column, COLUMNS)]
    columns.share()
    columns.collect()
    out_copies = [pltpu.make_async_copy(spread_held.at[device, layer], columns_hbm.at[layer, :, device], spread_sem.at[layer, device])
                  for device in range(PEERS) for layer in BOTH]
    for copy in out_copies:
        copy.start()
    for router in (mixed_router, res_router):
        for t in range(router.tiles):
            router.collect(t)
        router.finish()
    net.collected(lambda d: info_out.at[d], info_recv)
    net.sent(lambda d: info_ref.at[d], info_send, info_recv)
    prompt.finish()
    columns.finish()
    for copy in out_copies:
        copy.wait()


def first_attention(x_prompt, x_resp, w, gain, cos, sin, info, out_slice, collective_id):
    rows = TILE + x_resp.shape[0]
    width = x_resp.shape[1]
    return pl.pallas_call(
        first_attention_kernel,
        out_shape=(jax.ShapeDtypeStruct((PEERS, RING, 32, COLUMNS), BF16), jax.ShapeDtypeStruct((PEERS, 8, 16, COLUMNS), BF16),
                   jax.ShapeDtypeStruct((PEERS, 8, 128), jnp.int32), jax.ShapeDtypeStruct((TILE, PAIR * COLUMNS), BF16),
                   jax.ShapeDtypeStruct((PAIR, SHARDS, PEERS, 32, COLUMNS), BF16)),
        in_specs=[ANY] * 3 + [VMEM] * 5,
        out_specs=(VMEM,) * 4 + (ANY,),
        scratch_shapes=[
            pltpu.VMEM((9, TILE, width), BF16), pltpu.VMEM((width, 3 * COLUMNS), BF16), pltpu.VMEM((TILE, width), BF16), pltpu.VMEM((TILE, width), BF16),
            pltpu.VMEM((rows, COLUMNS), BF16), pltpu.VMEM((rows - TILE, COLUMNS), BF16), pltpu.VMEM((rows - TILE, COLUMNS), BF16),
            HELD, pltpu.VMEM((RING, PEERS, 32, COLUMNS), BF16), pltpu.VMEM((PEERS, 8, 16, COLUMNS), BF16),
            DMA((9,)), DMA, *GATHER_SEMS, DMA((PEERS,)), DMA((PEERS,)),
            pltpu.VMEM((PEERS, PAIR, SHARDS, 32, COLUMNS), BF16), DMA((PAIR, PEERS)), *GATHER_SEMS,
            *[DMA((RING, PEERS)) for _ in BOTH], *[DMA((1, PEERS)) for _ in BOTH],
        ],
        compiler_params=pltpu.CompilerParams(collective_id=collective_id, has_side_effects=True, vmem_limit_bytes=VMEM_BYTES),
        name="first_attention",
    )(x_prompt, x_resp, w, gain, cos, sin, info, out_slice)


def second_attention_kernel(qkv_ref, back_ref, mixed_out, stage, qkv_in, k_s, v_s, held, mixed_stage,
                            ring_send, ring_recv, near_send, near_recv, *routes):
    net = Exchange()
    me = net.me
    prompt = RespGather(net, held, ring_send, ring_recv, near_send, near_recv)
    router = Router(net, RING, lambda t, d: stage.at[t, d], lambda t, d: qkv_in.at[t, d], routes[:PAIR])
    mixed_router = Router(net, RING, lambda t, d: mixed_stage.at[t, d], lambda t, d: mixed_out.at[d, t], routes[PAIR:])
    for k in BOTH:
        held[me, k] = qkv_ref[pl.ds(0, TILE), pl.ds((k + 1) * COLUMNS, COLUMNS)]
    net.barrier()
    prompt.start()
    prompt.start_rest()
    count = back_ref.shape[1]

    def send_rows(t):
        place = lax.broadcasted_iota(jnp.int32, (Q_TILE, count), 0) + t * Q_TILE == back_ref[...]
        rows = jnp.dot(place.astype(BF16), qkv_ref[pl.ds(TILE, count)], preferred_element_type=F32).astype(BF16)
        stage[t] = rows.reshape(PEERS, Q_TILE // PEERS, 3 * COLUMNS)
        router.send(t)
        qkv_in[t, me] = stage[t, me]

    send_rows(0)
    prompt.relay()
    for t in range(1, RING):
        send_rows(t)
    prompt.share()
    prompt.collect()
    for t in range(RING):
        router.collect(t)
        rows = jnp.dot(undeal(Q_TILE), qkv_in[t].reshape(Q_TILE, 3 * COLUMNS), preferred_element_type=F32).astype(BF16)
        k_s[pl.ds(t * Q_TILE, Q_TILE)] = rows[:, COLUMNS:PAIR * COLUMNS]
        v_s[pl.ds(t * Q_TILE, Q_TILE)] = rows[:, PAIR * COLUMNS:]
        mixed = attend_response(t, rows[:, :COLUMNS], held, k_s, v_s)
        deal_mixed(mixed_router, t, mixed, mixed_stage, mixed_out)
    for t in range(RING):
        mixed_router.collect(t)
    for each in (router, mixed_router):
        each.finish()
    prompt.finish()


def second_attention(qkv, back, collective_id):
    rows = RING * Q_TILE
    wide = (32, 3 * COLUMNS)
    return pl.pallas_call(
        second_attention_kernel,
        out_shape=jax.ShapeDtypeStruct((PEERS, RING, 32, COLUMNS), BF16),
        in_specs=[VMEM, VMEM],
        out_specs=VMEM,
        scratch_shapes=[
            pltpu.VMEM((RING, PEERS) + wide, BF16), pltpu.VMEM((RING, PEERS) + wide, BF16),
            pltpu.VMEM((rows, COLUMNS), BF16), pltpu.VMEM((rows, COLUMNS), BF16),
            HELD, pltpu.VMEM((RING, PEERS, 32, COLUMNS), BF16), *GATHER_SEMS,
            *[DMA((RING, PEERS)) for _ in range(RING)],
        ],
        compiler_params=pltpu.CompilerParams(collective_id=collective_id, has_side_effects=True, vmem_limit_bytes=VMEM_BYTES),
        name=f"second_attention{collective_id}",
    )(qkv, back)


def prepare_kernel(w_hbm, wq_hbm, wk_hbm, wv_hbm, out_ref, first_hbm, second_hbm, raw, whole, send_sem, recv_sem, raw_sem, whole_sem):
    me, home = lax.axis_index("model"), lax.axis_index("resp")
    others = [(me + k) % SHARDS for k in range(1, SHARDS)]
    rows = pl.ds(pl.multiple_of(home * 32, 32), 32)

    def part(device):
        return w_hbm.at[:, rows, pl.ds(pl.multiple_of(device * COLUMNS, COLUMNS), COLUMNS)]

    def copy(device, place):
        return pltpu.make_async_remote_copy(
            src_ref=part(device), dst_ref=out_ref.at[:, place], send_sem=send_sem.at[device], recv_sem=recv_sem.at[place],
            device_id={"model": device}, device_id_type=MESH)

    loads = [[pltpu.make_async_copy(src.at[layer], raw.at[layer, i], raw_sem.at[layer, i]) for i, src in enumerate((wq_hbm, wk_hbm, wv_hbm))] for layer in BOTH]
    for load in loads[0] + loads[1]:
        load.start()
    own = pltpu.make_async_copy(part(me), out_ref.at[:, me], send_sem.at[me])
    own.start()
    barrier = pltpu.get_barrier_semaphore()
    for device in others:
        pl.semaphore_signal(barrier, device_id={"model": device}, device_id_type=MESH)
    pl.semaphore_wait(barrier, len(others))
    for device in others:
        copy(device, me).start()
    leave = [pltpu.make_async_copy(whole.at[layer], dst, whole_sem.at[layer]) for layer, dst in enumerate((first_hbm, second_hbm))]
    for layer in BOTH:
        for load in loads[layer]:
            load.wait()
        split_heads(raw.at[layer], whole.at[layer])
        leave[layer].start()
    for device in others:
        copy(device, device).wait_recv()
    for device in others:
        copy(device, me).wait_send()
    own.wait()
    for each in leave:
        each.wait()


def prepare(w_out, w_query, w_key, w_value, collective_id):
    width = w_query.shape[1] // PAIR
    whole = (width, 3 * COLUMNS)
    return pl.pallas_call(
        prepare_kernel,
        out_shape=(jax.ShapeDtypeStruct((PAIR, SHARDS, 32, COLUMNS), BF16), *[jax.ShapeDtypeStruct(whole, BF16) for _ in BOTH]),
        in_specs=[ANY] * RING,
        out_specs=(VMEM, ANY, ANY),
        scratch_shapes=[pltpu.VMEM((PAIR, 3, PAIR * width, LANES), BF16), pltpu.VMEM((PAIR,) + whole, BF16),
                        DMA((SHARDS,)), DMA((SHARDS,)), DMA((PAIR, 3)), DMA((PAIR,))],
        compiler_params=pltpu.CompilerParams(collective_id=collective_id, has_side_effects=True, vmem_limit_bytes=VMEM_BYTES),
        name="prepare",
    )(w_out, w_query, w_key, w_value)


class Answer:
    def __init__(self, every, out_ref, stat_send, stat_recv, row_send, row_recv):
        self.every, self.out = every, out_ref
        self.stat_sems, self.row_sems = (stat_send, stat_recv), (row_send, row_recv)
        self.me, self.home = lax.axis_index("model"), lax.axis_index("resp")
        self.models = [(self.me + k) % SHARDS for k in range(1, SHARDS)]
        self.homes = [(self.home + k) % PEERS for k in range(1, PEERS)]

    def barrier(self):
        sem = pltpu.get_barrier_semaphore()
        for axis, devices in (("model", self.models), ("resp", self.homes)):
            for device in devices:
                pl.semaphore_signal(sem, device_id={axis: device}, device_id_type=MESH)
        pl.semaphore_wait(sem, len(self.models) + len(self.homes))

    def stat_copy(self, owner, device, place):
        ref = self.every.at[owner]
        return pltpu.make_async_remote_copy(
            src_ref=ref, dst_ref=ref, send_sem=self.stat_sems[0].at[device], recv_sem=self.stat_sems[1].at[place],
            device_id={"model": device}, device_id_type=MESH)

    def row_copy(self, owner, device, place):
        ref = self.out.at[owner]
        return pltpu.make_async_remote_copy(
            src_ref=ref, dst_ref=ref, send_sem=self.row_sems[0].at[device], recv_sem=self.row_sems[1].at[place],
            device_id={"resp": device}, device_id_type=MESH)

def combine_kernel(stats_ref, out_ref, every, *sems):
    net = Answer(every, out_ref, *sems)
    every[net.me] = stats_ref[...]
    net.barrier()
    for device in net.models:
        net.stat_copy(net.me, device, net.me).start()
    for device in net.models:
        net.stat_copy(device, device, device).wait_recv()
    found = []
    for c in range(stats_ref.shape[0]):
        tiles = [every[k, c] for k in range(SHARDS)]
        top = functools.reduce(jnp.maximum, [tile[:1] for tile in tiles])
        total = functools.reduce(jnp.add, [tile[1:PAIR] * jnp.exp(tile[:1] - top) for tile in tiles])
        found.append(functools.reduce(jnp.add, [tile[PAIR:3] for tile in tiles]) - top - jnp.log(total))
    out_ref[net.home] = jnp.concatenate(found, axis=0)
    for device in net.homes:
        net.row_copy(net.home, device, net.home).start()
    for device in net.homes:
        net.row_copy(device, device, device).wait_recv()
    for device in net.models:
        net.stat_copy(net.me, device, device).wait_send()
    for device in net.homes:
        net.row_copy(net.home, device, device).wait_send()


def combine(stats, collective_id):
    return pl.pallas_call(
        combine_kernel,
        out_shape=jax.ShapeDtypeStruct((PEERS, PEERS, LANES), F32),
        in_specs=[VMEM],
        out_specs=VMEM,
        scratch_shapes=[pltpu.VMEM((SHARDS,) + stats.shape, F32), *[DMA((SHARDS,)) for _ in BOTH], *[DMA((PEERS,)) for _ in BOTH]],
        compiler_params=pltpu.CompilerParams(collective_id=collective_id, has_side_effects=True),
        name="combine",
    )(stats)


ROPE_BASE = 10000.0
VARIANTS = (640, 768, 1024)


def rope_tables(positions):
    half = LANES // PAIR
    lane = jnp.arange(LANES)
    frequency = ROPE_BASE ** (-(lane % half).astype(F32) / half)
    angles = positions.astype(F32)[:, None] * frequency
    return jnp.cos(angles), jnp.sin(angles) * jnp.where(lane < half, -1.0, 1.0)


def solution(mesh):
    groups = mesh.shape['resp']
    row_axes = ('prompts', 'resp')
    head_spec = P(None, None, 'model', None)
    in_specs = (P(row_axes, None), P(row_axes, None, None), P(row_axes, None), P(row_axes), P(None, None), head_spec, head_spec, head_spec, P(None, 'model', None, None), P(None, None), P(None, None, 'model'), P(None, None, 'model'), P(None, 'model', None), P(None), P(None, 'model'))

    def device_step(x_prompt, x_resp, targets, resp_lens, attn_gain, w_query, w_key, w_value, w_out, mlp_gain, w_gate, w_up, w_down, final_gain, w_vocab):
        prompt_rows = x_prompt.shape[0]
        resp_len, width = x_resp.shape[1:]
        prompt_len = prompt_rows * groups
        me = lax.axis_index('model')
        home = lax.axis_index('resp')
        per = resp_len // groups
        gate_t, up_t = jnp.swapaxes(w_gate, 1, 2), jnp.swapaxes(w_up, 1, 2)
        out_flat = w_out.reshape(w_out.shape[0], COLUMNS, width)
        projections = [w.reshape(w.shape[0], PAIR * width, LANES) for w in (w_query, w_key, w_value)]
        prompt_pos = home * prompt_rows + jnp.arange(prompt_rows)

        cos, sin = rope_tables(jnp.concatenate([prompt_pos, prompt_len + jnp.arange(resp_len)]))
        info = jnp.concatenate([
            targets[0].reshape(per, groups).T[:, None, :],
            jnp.broadcast_to(resp_lens[0], (groups, groups - 1, per)).astype(jnp.int32)], axis=1)
        out_slice, w_first, w_second = prepare(out_flat, *projections, PAIR)
        mixed, res, infos, prompt, out_columns = first_attention(x_prompt, x_resp[0], w_first, attn_gain, cos, sin, info, out_slice, 0)
        lens = infos[:, 1, 0]
        need = (lens + groups - 1) // groups
        ends = jnp.sum(jnp.where(jnp.arange(groups)[:, None] >= jnp.arange(groups), need, 0), axis=1)
        starts = ends - need
        dealt = groups * per

        def finish_with(size, ident):
            def run(operands):
                mixed, res, prompt = operands
                slot = jnp.arange(size)
                which = jnp.sum((slot[:, None] >= ends).astype(jnp.int32), axis=1)
                row = slot - jnp.sum(jnp.where(which[:, None] == jnp.arange(groups), starts, 0), axis=1)
                real = slot < ends[-1]
                source = jnp.where(real, which * per + row, -1)
                chosen = source[:, None] == jnp.arange(dealt)
                wanted = jnp.sum(jnp.where(chosen, infos[:, 0, :].reshape(dealt), 0), axis=1) - me * w_vocab.shape[1]
                ids = jnp.where(jnp.arange(LANES) == 0, source[:, None], wanted[:, None])
                ids = jnp.pad(ids, ((prompt_rows, 0), (0, 0)), constant_values=-1)
                tables = rope_tables(jnp.concatenate([prompt_pos, prompt_len + groups * row + home]))
                weights = (out_columns.reshape(PAIR, width, COLUMNS), gate_t, up_t, w_down)
                qkv, new_res = mega(
                    mlp_gain, attn_gain, ids, mixed.reshape(dealt, COLUMNS), res.reshape(dealt, COLUMNS),
                    [*tables, prompt], *weights, w_second, 0, ident)
                part = per // RING
                back = jnp.where(real, (row // part) * (groups * part) + which * part + row % part, -1)
                mixed = second_attention(qkv, back[None], ident + 1)
                return mega(mlp_gain, final_gain[None], ids, mixed.reshape(dealt, COLUMNS), new_res, [], *weights, w_vocab, 1, ident + PAIR)
            return run

        smallest = sorted(VARIANTS)
        fit = sum((ends[-1] > size).astype(jnp.int32) for size in smallest[:-1])
        index = sum(jnp.where(fit == smallest.index(size), i, 0) for i, size in enumerate(VARIANTS))
        stats = lax.switch(index, [finish_with(size, 3 + 3 * i) for i, size in enumerate(VARIANTS)], (mixed, res, prompt))
        found = combine(stats, 1).reshape(groups, dealt)
        start = jnp.sum(jnp.where(jnp.arange(groups) == home, starts, 0))
        mine = lax.dynamic_slice(jnp.pad(found, ((0, 0), (0, per))), (0, start), (groups, per))
        log_probs = mine.T.reshape(resp_len)
        log_probs = jnp.where(jnp.arange(resp_len) < resp_lens[0], log_probs, 0.0)
        return log_probs[None, :]

    return jax.shard_map(device_step, mesh=mesh, in_specs=in_specs, out_specs=P(row_axes, None), check_vma=False)
```

```python
import functools

import jax
import jax.numpy as jnp
from jax import lax
from jax.experimental import pallas as pl
from jax.experimental.pallas import tpu as pltpu
from jax.sharding import PartitionSpec as P

MESH = pl.DeviceIdType.MESH
F32 = jnp.float32
BF16 = jnp.bfloat16
EPS = 1e-6
LANES = 128
PAIR = 2
RING = 4
COLUMNS = PAIR * LANES
SHARDS = RING * RING
PEERS = 8
BOTH = range(PAIR)
VMEM_BYTES = 67_000_000
LATE_ROWS = 640
LOGITS = 512
CHUNKS = 4
VMEM = pl.BlockSpec(memory_space=pltpu.VMEM)
ANY = pl.BlockSpec(memory_space=pl.ANY)
DMA = pltpu.SemaphoreType.DMA
KINDS = range(RING * 3)
SUM_FAR, SUM_NEAR, SUM_RELAY, SUM2_FAR, SUM2_NEAR, SUM2_RELAY, TAKE_OWN, TAKE_REST, TAKE_RELAY, TAKE2_OWN, TAKE2_REST, TAKE2_RELAY = KINDS


def block_of(color, first, second):
    return RING * first + second if color else RING * second + first


def pair(index):
    return pl.ds(PAIR * index, PAIR)


class Torus:
    def __init__(self, refs, send_sem, recv_sem):
        self.refs = refs
        self.far, self.near, self.relayed, self.sums, self.relayed2, self.sums2, self.rows = refs
        self.send_sem, self.recv_sem = send_sem, recv_sem
        me = lax.axis_index("model")
        z, y = me // RING, me % RING
        self.place = ((y, z), (z, y))
        along_y = [z * RING + self.step(y, way) for way in (1, -1)]
        along_z = [self.step(z, way) * RING + y for way in (1, -1)]
        self.neighbors = ((along_y, along_z), (along_z, along_y))

    def step(self, place, by):
        return (place + by + RING) % RING

    def barrier(self):
        sem = pltpu.get_barrier_semaphore()
        for ring in self.neighbors[0]:
            for device in ring:
                pl.semaphore_signal(sem, device_id={"model": device}, device_id_type=MESH)
        pl.semaphore_wait(sem, RING)

    def ends(self, kind, c, q, d):
        (p, s), way, other = self.place[q], 1 - PAIR * d, 1 - d
        far, near, relayed, sums, relayed2, sums2, rows = (ref.at[c, q] for ref in self.refs)
        own = sums.at[0]
        back_s, back_p = self.step(s, -way), self.step(p, -way)
        return {
            SUM_FAR: lambda: (far.at[pair(d)], relayed.at[d], relayed.at[d]),
            SUM_NEAR: lambda: (near.at[d], sums.at[d, pair(other)], sums.at[d, pair(other)]),
            SUM_RELAY: lambda: (relayed.at[d], sums.at[d, pair(d)], sums.at[d, pair(d)]),
            SUM2_FAR: lambda: (own.at[self.step(s, PAIR), d], relayed2.at[d], relayed2.at[d]),
            SUM2_NEAR: lambda: (own.at[self.step(s, way), other], sums2.at[d, other], sums2.at[d, other]),
            SUM2_RELAY: lambda: (relayed2.at[d], sums2.at[d, d], sums2.at[d, d]),
            TAKE_OWN: lambda: (rows.at[p, s, d], rows.at[p, s, d], rows.at[p, back_s, d]),
            TAKE_REST: lambda: (rows.at[p, s, other], rows.at[p, s, other], rows.at[p, back_s, other]),
            TAKE_RELAY: lambda: (rows.at[p, back_s, d], rows.at[p, back_s, d], rows.at[p, self.step(s, PAIR), d]),
            TAKE2_OWN: lambda: (rows.at[p, pair(d)], rows.at[p, pair(d)], rows.at[back_p, pair(d)]),
            TAKE2_REST: lambda: (rows.at[p, pair(other)], rows.at[p, pair(other)], rows.at[back_p, pair(other)]),
            TAKE2_RELAY: lambda: (rows.at[back_p, pair(d)], rows.at[back_p, pair(d)], rows.at[self.step(p, PAIR), pair(d)]),
        }[kind]()

    def copy(self, kind, c, q, d, src, dst):
        second_ring = kind in (SUM2_FAR, SUM2_NEAR, SUM2_RELAY, TAKE_OWN, TAKE_REST, TAKE_RELAY)
        return pltpu.make_async_remote_copy(
            src_ref=src, dst_ref=dst, send_sem=self.send_sem.at[c, q, d, kind], recv_sem=self.recv_sem.at[c, q, d, kind],
            device_id={"model": self.neighbors[q][second_ring][d]}, device_id_type=MESH)

    def send(self, c, q, d, kind):
        src, dst, _ = self.ends(kind, c, q, d)
        self.copy(kind, c, q, d, src, dst).start()

    def sent(self, c, q, *kinds):
        for kind in kinds:
            for d in BOTH:
                src, dst, _ = self.ends(kind, c, q, d)
                self.copy(kind, c, q, d, src, dst).wait_send()

    def arrived(self, c, q, d, *kinds):
        for kind in kinds:
            _, _, here = self.ends(kind, c, q, d)
            self.copy(kind, c, q, d, here, here).wait_recv()


def halves_of(ref):
    return ref[:, :COLUMNS], ref[:, COLUMNS:]


def halves(value):
    return value[:, :LANES], value[:, LANES:]


def store_block(ref, value):
    for half, part in enumerate(halves(value)):
        ref[half] = part


def add_block(ref, value):
    for half, part in enumerate(halves(value)):
        ref[half] += part


class Gather:
    def __init__(self, net):
        self.net = net

    def begin_rows(self, c, q):
        for kind in (TAKE_OWN, TAKE_REST):
            for d in BOTH:
                self.net.send(c, q, d, kind)

    def relay_rows(self, c, q):
        for d in BOTH:
            self.net.arrived(c, q, d, TAKE_OWN)
            self.net.send(c, q, d, TAKE_RELAY)

    def take_second(self, c, q):
        for d in BOTH:
            self.net.arrived(c, q, d, TAKE_REST, TAKE_RELAY)
        for kind in (TAKE2_OWN, TAKE2_REST):
            for d in BOTH:
                self.net.send(c, q, d, kind)

    def relay_last(self, c, q):
        for d in BOTH:
            self.net.arrived(c, q, d, TAKE2_OWN)
            self.net.send(c, q, d, TAKE2_RELAY)

    def complete(self, c, q):
        for d in BOTH:
            self.net.arrived(c, q, d, TAKE2_REST, TAKE2_RELAY)
        self.net.sent(c, q, TAKE_OWN, TAKE_REST, TAKE_RELAY, TAKE2_OWN, TAKE2_REST, TAKE2_RELAY)

    def middle(self):
        return [self.relay_rows, self.take_second, self.relay_last]


class Sum(Gather):
    def __init__(self, net, lhs_of, w_ref, finish):
        self.net, self.lhs_of, self.w_ref, self.finish = net, lhs_of, w_ref, finish

    def product(self, lhs, color, first, second):
        start = pl.multiple_of(block_of(color, first, second) * COLUMNS, COLUMNS)
        return jnp.dot(lhs, self.w_ref[:, pl.ds(start, COLUMNS)], preferred_element_type=F32)

    def begin(self, c, q):
        net, p, lhs = self.net, self.net.place[q][0], self.lhs_of(c, q)
        for k in range(RING):
            store_block(net.far.at[c, q, k], self.product(lhs, q, net.step(p, PAIR), k))
        for d in BOTH:
            net.send(c, q, d, SUM_FAR)
        for d in BOTH:
            for k in BOTH:
                store_block(net.near.at[c, q, d, k], self.product(lhs, q, net.step(p, 1 - PAIR * d), PAIR * (1 - d) + k))
            net.send(c, q, d, SUM_NEAR)

    def relay_sum(self, c, q):
        net, p, lhs = self.net, self.net.place[q][0], self.lhs_of(c, q)
        for d in BOTH:
            net.arrived(c, q, d, SUM_FAR)
            for k in BOTH:
                add_block(net.relayed.at[c, q, d, k], self.product(lhs, q, net.step(p, 1 - PAIR * d), PAIR * d + k))
            net.send(c, q, d, SUM_RELAY)

    def begin_second(self, c, q):
        net, lhs = self.net, self.lhs_of(c, q)
        for d in BOTH:
            net.arrived(c, q, d, SUM_NEAR, SUM_RELAY)
        for k in range(RING):
            for half, part in enumerate(halves(self.product(lhs, q, net.place[q][0], k))):
                net.sums[c, q, 0, k, half] += net.sums[c, q, 1, k, half] + part
        for kind in (SUM2_FAR, SUM2_NEAR):
            for d in BOTH:
                net.send(c, q, d, kind)
        net.sent(c, q, SUM_FAR)

    def relay_second(self, c, q):
        net = self.net
        for d in BOTH:
            net.arrived(c, q, d, SUM2_FAR)
            net.relayed2[c, q, d] += net.sums[c, q, 0, net.step(net.place[q][1], 1 - PAIR * d), d]
            net.send(c, q, d, SUM2_RELAY)

    def finish_sum(self, c, q):
        net = self.net
        net.sent(c, q, SUM_NEAR, SUM_RELAY)
        for d in BOTH:
            net.arrived(c, q, d, SUM2_NEAR, SUM2_RELAY)
        for half in BOTH:
            self.finish(c, q, half, net.sums[c, q, 0, net.place[q][1], half] + net.sums2[c, q, 0, half] + net.sums2[c, q, 1, half])
        self.begin_rows(c, q)

    def relay_rows(self, c, q):
        self.net.sent(c, q, SUM2_FAR, SUM2_NEAR, SUM2_RELAY)
        super().relay_rows(c, q)

    def middle(self):
        return [self.relay_sum, self.begin_second, self.relay_second, self.finish_sum, *super().middle()]


def normed(net, c, q, gain_ref, layer):
    rows = net.rows.shape[-PAIR]
    tile = PAIR * 8 if rows % (PAIR * 8) == 0 else 8
    spots = [(first, second, half) for first in range(RING) for second in range(RING) for half in BOTH]

    @pl.loop(0, rows // tile)
    def _(i):
        span = pl.ds(pl.multiple_of(i * tile, tile), tile)
        acts = [net.rows[(c, q) + spot + (span,)].astype(F32) for spot in spots]
        squares = functools.reduce(jnp.add, [v * v for v in acts])
        inv = lax.rsqrt(jnp.sum(squares, axis=-1, keepdims=True) / (LANES * len(acts)) + EPS)
        for spot, v in zip(spots, acts):
            column = block_of(q, *spot[:PAIR]) * COLUMNS + spot[PAIR] * LANES
            net.rows[(c, q) + spot + (span,)] = (v * inv * gain_ref[pl.ds(layer, 1), pl.ds(column, LANES)]).astype(BF16)


def rows_of(net, c, q):
    parts = []
    for upper in range(RING):
        for lower in range(RING):
            first, second = (upper, lower) if q else (lower, upper)
            parts += [net.rows[c, q, first, second, half] for half in BOTH]
    return jnp.concatenate(parts, axis=1)


def times_transposed(lhs, rhs):
    return lax.dot_general(lhs, rhs, (((1,), (1,)), ((), ())), preferred_element_type=F32)


def late_plan(width, count):
    plan, start = [], 0
    for buffer in BOTH:
        for slot in range(width // count):
            size = min(LATE_ROWS, width - start)
            if size:
                plan.append((buffer, slot * count, start, size))
            start += size
    return plan, width - start


def rope(value, cos, sin):
    return jnp.concatenate([v * cos + pltpu.roll(v, LANES // PAIR, 1) * sin for v in halves(value)], axis=1)


def put_projected(product, cos_ref, sin_ref, out_ref, span):
    for k in range(3):
        value = product(k * COLUMNS, COLUMNS)
        if k < PAIR:
            value = rope(value, cos_ref[span], sin_ref[span])
        out_ref[span, pl.ds(k * COLUMNS, COLUMNS)] = value.astype(BF16)


def statistics(product, count, target):
    top = total = picked = None
    for k in range(count // LOGITS):
        logits = product(k * LOGITS, LOGITS)
        here = jnp.max(logits, axis=-1, keepdims=True)
        ids = lax.broadcasted_iota(jnp.int32, logits.shape, 1) + k * LOGITS
        found = jnp.sum(jnp.where(ids == target, logits, 0.0), axis=-1, keepdims=True)
        if k:
            both = jnp.maximum(top, here)
            total = total * jnp.exp(top - both) + jnp.sum(jnp.exp(logits - both), axis=-1, keepdims=True)
            top, picked = both, picked + found
        else:
            top, total, picked = here, jnp.sum(jnp.exp(logits - here), axis=-1, keepdims=True), found
    lane = lax.broadcasted_iota(jnp.int32, (target.shape[0], LANES), 1)
    return jnp.where(lane == 0, top, jnp.where(lane == 1, total, picked))


def mega_kernel(chunks, layer, last, gain_ref, next_gain_ref, ids_ref, dealt_ref, old_ref, *args):
    if last:
        side_refs, args = (), args
    else:
        side_refs, args = args[:3], args[3:]
    w_out_hbm, w_gate_hbm, w_up_hbm, w_down_hbm, *args = args
    late_hbm, out_ref, *args = args
    if not last:
        new_res_ref, *args = args
    (w_out, w_gate, w_up, w_down, late_rest, res, inner, middle, stats,
     far, near, relayed, sums, relayed2, sums2, rows, w_sem, late_sem, send_sem, recv_sem, ready_sem) = args
    loads = [pltpu.make_async_copy(src.at[layer], dst, w_sem.at[i]) for i, (src, dst) in enumerate(
        ((w_out_hbm, w_out), (w_gate_hbm, w_gate), (w_up_hbm, w_up), (w_down_hbm, w_down)))]
    for load in loads:
        load.start()
    width, count = late_hbm.shape
    plan, left = late_plan(width, count)
    late = [(late_hbm.at[pl.ds(start, size)], (w_gate, w_up)[buffer].at[pl.ds(0, size), pl.ds(lane, count)]) for buffer, lane, start, size in plan]
    if left:
        late.append((late_hbm.at[pl.ds(width - left, left)], late_rest))
    late_loads = [pltpu.make_async_copy(src, dst, late_sem.at[i]) for i, (src, dst) in enumerate(late)]
    net = Torus((far, near, relayed, sums, relayed2, sums2, rows), send_sem, recv_sem)
    net.barrier()

    part = rows.shape[-PAIR]

    def span_of(c, q=0, parts=1):
        return pl.ds(pl.multiple_of((PAIR * c + q) * part, 16), parts * part)

    def after_prompt(c, q=0, parts=1):
        return pl.ds(pl.multiple_of((PAIR * c + q) * part + LANES * last, 16), parts * part)

    def picked(c, ref, prompt):
        ids = ids_ref[after_prompt(c, parts=PAIR), :1]
        chosen = (ids == lax.broadcasted_iota(jnp.int32, (PAIR * part, PEERS * LANES), 1)).astype(BF16)
        value = jnp.dot(chosen, ref[...], preferred_element_type=F32)
        if prompt is not None:
            row = lax.broadcasted_iota(jnp.int32, (PAIR * part, LANES), 0) + PAIR * part * c
            chosen = (row == lax.broadcasted_iota(jnp.int32, (PAIR * part, LANES), 1)).astype(BF16)
            value += jnp.dot(chosen, prompt, preferred_element_type=F32)
        return value.astype(BF16)

    def put(ref, value, place_of):
        for q in BOTH:
            for half, columns in enumerate(halves(value)):
                ref[place_of(q) + (half,)] = columns[q * part:(q + 1) * part]

    def begin(c):
        prompts = (None, None) if last else halves_of(side_refs[PAIR])
        put(rows, picked(c, dealt_ref, prompts[0]), lambda q: (c, q) + net.place[q])
        if not last:
            put(res, picked(c, old_ref, prompts[1]), lambda q: (c, q))
        for q in BOTH:
            first.begin_rows(c, q)

    def finish(c, q, half, total):
        value = (middle[c, q, half].astype(F32) + total).astype(BF16)
        if not last:
            new_res_ref[span_of(c, q), pl.ds(half * LANES, LANES)] = value
        rows[(c, q) + net.place[q] + (half,)] = value

    first = Gather(net)
    second = Sum(net, lambda c, q: inner[c, q], w_down, finish)

    def project_out(c):
        for q in BOTH:
            first.complete(c, q)
        total = jnp.dot(jnp.concatenate([rows_of(net, c, q) for q in BOTH], axis=0), w_out[...], preferred_element_type=F32)
        for q in BOTH:
            for half, columns in enumerate(halves(total)):
                old = old_ref[after_prompt(c, q), pl.ds(half * LANES, LANES)] if last else res[c, q, half]
                value = (old.astype(F32) + columns[q * part:(q + 1) * part]).astype(BF16)
                middle[c, q, half] = value
                rows[(c, q) + net.place[q] + (half,)] = value
        for ring in net.neighbors[0]:
            for device in ring:
                pl.semaphore_signal(ready_sem.at[c], device_id={"model": device}, device_id_type=MESH)

    def begin_again(c):
        pl.semaphore_wait(ready_sem.at[c], RING)
        for q in BOTH:
            first.begin_rows(c, q)

    def hidden_of(c, stage, gain, row):
        for q in BOTH:
            stage.complete(c, q)
            normed(net, c, q, gain, row)
        return jnp.concatenate([rows_of(net, c, q) for q in BOTH], axis=0)

    def mlp(c):
        hidden = hidden_of(c, first, gain_ref, layer)
        value = (jax.nn.silu(times_transposed(hidden, w_gate[...])) * times_transposed(hidden, w_up[...])).astype(BF16)
        inner[c] = value.reshape(inner.shape[1:])
        for q in BOTH:
            second.begin(c, q)

    def after(c):
        hidden = hidden_of(c, second, next_gain_ref, 0 if last else layer + 1)

        def product(lane, size):
            parts = [jnp.dot(hidden[:, start:start + rows_here], (w_gate, w_up)[buffer][pl.ds(0, rows_here), pl.ds(at + lane, size)], preferred_element_type=F32)
                     for buffer, at, start, rows_here in plan]
            if left:
                parts.append(jnp.dot(hidden[:, width - left:], late_rest[:, pl.ds(lane, size)], preferred_element_type=F32))
            return functools.reduce(jnp.add, parts)

        if last:
            stats[span_of(c, parts=PAIR)] = statistics(product, count, ids_ref[after_prompt(c, parts=PAIR), 1:PAIR])
        else:
            put_projected(product, *side_refs[:PAIR], out_ref, span_of(c, parts=PAIR))

    def on_both(step):
        def run(c):
            for q in BOTH:
                step(c, q)
        return run

    gather = [on_both(step) for step in first.middle()]
    steps = [begin, *gather, project_out, begin_again, *gather, mlp, *map(on_both, second.middle())]
    at_mlp = steps.index(mlp)
    steps += [None] * max(0, at_mlp + chunks - len(steps)) + [after]

    @pl.loop(0, len(steps) + chunks - 1)
    def _(slot):
        @pl.when(slot == steps.index(project_out))
        def _():
            for load in loads:
                load.wait()

        @pl.when(slot == len(steps) - 1)
        def _():
            for load in late_loads:
                load.wait()

        for k, step in reversed(list(enumerate(steps))):
            if step is None:
                continue

            @pl.when(slot >= k)
            def _():
                @pl.when(slot < k + chunks)
                def _():
                    step(slot - k)

        @pl.when(slot == at_mlp + chunks - 1)
        def _():
            for load in late_loads:
                load.start()

    if last:
        out_ref[...] = jnp.zeros_like(out_ref)
        for k in range(stats.shape[0] // LANES):
            turned = stats[pl.ds(k * LANES, LANES)].T
            for i in range(3):
                out_ref[i, pl.ds(k, 1)] = turned[i:i + 1]


def mega(gain, next_gain, ids, dealt, old, sides, w_out, w_gate_t, w_up_t, w_down, late, layer, collective_id):
    last = not sides
    chunks = CHUNKS
    total = ids.shape[0] - LANES * last
    _, hidden, width = w_gate_t.shape
    rows = total // (PAIR * chunks)
    per = (chunks, PAIR)
    tile = (rows, LANES)
    count = late.shape[1]
    _, left = late_plan(width, count)

    sem = DMA(per + (PAIR, len(KINDS)))
    out = jax.ShapeDtypeStruct((3, PEERS, LANES), F32) if last else (
        jax.ShapeDtypeStruct((total, count), BF16), jax.ShapeDtypeStruct((total, COLUMNS), BF16))
    return pl.pallas_call(
        functools.partial(mega_kernel, chunks, layer, last),
        out_shape=out,
        in_specs=[VMEM] * (5 + len(sides)) + [ANY] * 5,
        out_specs=VMEM if last else (VMEM, VMEM),
        scratch_shapes=[
            pltpu.VMEM((width, COLUMNS), BF16),
            *[pltpu.VMEM((hidden, width), BF16) for _ in range(3)],
            pltpu.VMEM((left or 8, count), BF16),
            pltpu.VMEM(per + (PAIR,) + (tile if not last else (8, LANES)), BF16),
            pltpu.VMEM(per + (rows, hidden), BF16),
            pltpu.VMEM(per + (PAIR,) + tile, BF16),
            pltpu.VMEM((total if last else 8, LANES), F32),
            pltpu.VMEM(per + (RING, PAIR) + tile, F32),
            pltpu.VMEM(per + (PAIR, PAIR, PAIR) + tile, F32),
            pltpu.VMEM(per + (PAIR, PAIR, PAIR) + tile, F32),
            pltpu.VMEM(per + (PAIR, RING, PAIR) + tile, F32),
            pltpu.VMEM(per + (PAIR,) + tile, F32),
            pltpu.VMEM(per + (PAIR, PAIR) + tile, F32),
            pltpu.VMEM(per + (RING, RING, PAIR) + tile, BF16),
            DMA((RING,)), DMA((SHARDS,)), sem, sem, pltpu.SemaphoreType.REGULAR((chunks,)),
        ],
        compiler_params=pltpu.CompilerParams(collective_id=collective_id, has_side_effects=True, vmem_limit_bytes=VMEM_BYTES),
        name=f"mega{collective_id}",
    )(gain, next_gain, ids, dealt, old, *sides, w_out, w_gate_t, w_up_t, w_down, late)


TILE = 128
Q_TILE = 256
LOG2E = 1.4426950408889634
HELD = pltpu.VMEM((PEERS, PAIR, TILE, COLUMNS), BF16)
GATHER_SEMS = [DMA((PAIR, 3)), DMA((PAIR, 3)), DMA((RING,)), DMA((RING,))]


class Exchange:
    def __init__(self):
        self.me = lax.axis_index("resp")
        self.others = [(self.me + k) % PEERS for k in range(1, PEERS)]

    def barrier(self, models=()):
        sem = pltpu.get_barrier_semaphore()
        for axis, devices in (("resp", self.others), ("model", models)):
            for device in devices:
                pl.semaphore_signal(sem, device_id={axis: device}, device_id_type=MESH)
        pl.semaphore_wait(sem, len(self.others) + len(models))

    def copy(self, src, dst, send_sem, recv_sem, device):
        return pltpu.make_async_remote_copy(src_ref=src, dst_ref=dst, send_sem=send_sem, recv_sem=recv_sem,
                                            device_id={"resp": device}, device_id_type=MESH)

    def scatter(self, src_of, dst, send_sem, recv_sem):
        for device in self.others:
            self.copy(src_of(device), dst, send_sem.at[device], recv_sem.at[self.me], device).start()

    def collected(self, dst_of, recv_sem):
        for device in self.others:
            self.copy(dst_of(device), dst_of(device), recv_sem.at[device], recv_sem.at[device], device).wait_recv()

    def sent(self, src_of, send_sem, recv_sem):
        for device in self.others:
            self.copy(src_of(device), src_of(device), send_sem.at[device], recv_sem.at[device], device).wait_send()


class Router:
    def __init__(self, net, tiles, src_of, dst_of, sems):
        self.net, self.tiles, self.src_of, self.dst_of = net, tiles, src_of, dst_of
        self.send_sem, self.recv_sem = sems

    def send(self, t):
        self.net.scatter(lambda d: self.src_of(t, d), self.dst_of(t, self.net.me), self.send_sem.at[t], self.recv_sem.at[t])

    def collect(self, t):
        self.net.collected(lambda d: self.dst_of(t, d), self.recv_sem.at[t])

    def finish(self):
        for t in range(self.tiles):
            self.net.sent(lambda d: self.src_of(t, d), self.send_sem.at[t], self.recv_sem.at[t])


class Slices:
    def __init__(self, w_hbm, held, send_sem, recv_sem):
        self.w, self.held, self.send_sem, self.recv_sem = w_hbm, held, send_sem, recv_sem
        self.me, self.home = lax.axis_index("model"), lax.axis_index("resp")
        self.others = [(self.me + k) % SHARDS for k in range(1, SHARDS)]
        self.own = pltpu.make_async_copy(self.part(self.me), held.at[self.home, :, self.me], send_sem.at[self.me])

    def part(self, device):
        rows = pl.ds(pl.multiple_of(self.home * 32, 32), 32)
        return self.w.at[:, rows, pl.ds(pl.multiple_of(device * COLUMNS, COLUMNS), COLUMNS)]

    def copy(self, device, place):
        return pltpu.make_async_remote_copy(
            src_ref=self.part(device), dst_ref=self.held.at[self.home, :, place], send_sem=self.send_sem.at[device],
            recv_sem=self.recv_sem.at[place], device_id={"model": device}, device_id_type=MESH)

    def start(self):
        self.own.start()
        for device in self.others:
            self.copy(device, self.me).start()

    def collect(self):
        for device in self.others:
            self.copy(device, device).wait_recv()
        self.own.wait()

    def finish(self):
        for device in self.others:
            self.copy(device, self.me).wait_send()


class RespGather:
    def __init__(self, net, held, ring_send, ring_recv, near_send, near_recv):
        self.net, self.held = net, held
        self.ring_sems, self.near_sems = (ring_send, ring_recv), (near_send, near_recv)
        x, core = net.me // PAIR, net.me % PAIR
        self.at = lambda by, here: (x + by + RING) % RING * PAIR + (core if here else 1 - core)

    def ring_copy(self, d, kind, ref):
        return self.net.copy(ref, ref, self.ring_sems[0].at[d, kind], self.ring_sems[1].at[d, kind], self.at(1 - PAIR * d, True))

    def near_copy(self, kind, ref):
        return self.net.copy(ref, ref, self.near_sems[0].at[kind], self.near_sems[1].at[kind], self.at(0, False))

    def sources(self, here):
        return [self.at(by, here) for by in (0, -1, 1, PAIR)]

    def start(self):
        for d in BOTH:
            self.ring_copy(d, 0, self.held.at[self.net.me, d]).start()
        self.near_copy(0, self.held.at[self.net.me]).start()

    def start_rest(self):
        for d in BOTH:
            self.ring_copy(d, 1, self.held.at[self.net.me, 1 - d]).start()

    def relay(self):
        for d in BOTH:
            ref = self.held.at[self.at(PAIR * d - 1, True), d]
            self.ring_copy(d, 0, ref).wait_recv()
            self.ring_copy(d, PAIR, ref).start()

    def share(self):
        for d in BOTH:
            device = self.at(PAIR * d - 1, True)
            self.ring_copy(d, 1, self.held.at[device, 1 - d]).wait_recv()
            self.near_copy(1 + d, self.held.at[device]).start()
        far = self.held.at[self.at(PAIR, True)]
        for d in BOTH:
            self.ring_copy(d, PAIR, far.at[d]).wait_recv()
        self.near_copy(3, far).start()

    def collect(self):
        for kind, device in enumerate(self.sources(False)):
            self.near_copy(kind, self.held.at[device]).wait_recv()

    def finish(self):
        for kind in range(3):
            for d in BOTH:
                self.ring_copy(d, kind, self.held.at[self.net.me, d]).wait_send()
        for kind in range(RING):
            self.near_copy(kind, self.held.at[self.net.me]).wait_send()


def deal(rows):
    out = lax.broadcasted_iota(jnp.int32, (rows, rows), 0)
    src = lax.broadcasted_iota(jnp.int32, (rows, rows), 1)
    per = rows // PEERS
    return jnp.where(src == (out % per) * PEERS + out // per, 1.0, 0.0).astype(BF16)


def undeal(rows):
    out = lax.broadcasted_iota(jnp.int32, (rows, rows), 0)
    src = lax.broadcasted_iota(jnp.int32, (rows, rows), 1)
    per = rows // PEERS
    return jnp.where(src == (out % PEERS) * per + out // PEERS, 1.0, 0.0).astype(BF16)


def split_heads(raw_ref, w_ref):
    tile = PAIR * LANES
    out = lax.broadcasted_iota(jnp.int32, (tile, tile), 0)
    src = lax.broadcasted_iota(jnp.int32, (tile, tile), 1)
    pick = jnp.where(src == (out % LANES) * PAIR + out // LANES, 1.0, 0.0).astype(BF16)

    @pl.loop(0, raw_ref.shape[1] // (RING * tile))
    def _(b):
        raws = [raw_ref[i, pl.ds(pl.multiple_of((b * RING + k) * tile, tile), tile)] for k in range(RING) for i in range(3)]
        heads = jnp.dot(pick, jnp.concatenate(raws, axis=1), preferred_element_type=F32).astype(BF16)
        for k in range(RING):
            here = pl.ds(pl.multiple_of((b * RING + k) * LANES, LANES), LANES)
            for i in range(3):
                for h in BOTH:
                    at = (k * 3 + i) * LANES
                    w_ref[here, pl.ds(i * COLUMNS + h * LANES, LANES)] = heads[h * LANES:(h + 1) * LANES, at:at + LANES]


def norm_tile(x_ref, out_ref, gain_ref):
    for i in range(x_ref.shape[0] // 16):
        v = x_ref[pl.ds(16 * i, 16), :].astype(F32)
        inv = lax.rsqrt(jnp.mean(v * v, axis=-1, keepdims=True) + EPS)
        out_ref[pl.ds(16 * i, 16), :] = (v * inv * gain_ref[pl.ds(0, 1), :]).astype(BF16)


def softmax_mix(q, pieces):
    factor = LOG2E * 128 ** -0.5
    outs = []
    for h in range(2):
        lanes = slice(128 * h, 128 * h + 128)
        scores = []
        for keys, _, mask in pieces:
            s = lax.dot_general(q[:, lanes], keys[:, lanes], (((1,), (1,)), ((), ())), preferred_element_type=F32)
            scores.append(s if mask is None else jnp.where(mask, s, -jnp.inf))
        top = functools.reduce(jnp.maximum, [jnp.max(s, axis=-1, keepdims=True) for s in scores])
        probs = [jnp.exp2((s - top) * factor) for s in scores]
        total = functools.reduce(jnp.add, [jnp.sum(p, axis=-1, keepdims=True) for p in probs])
        mixed = functools.reduce(jnp.add, [jnp.dot(p.astype(BF16), values[:, lanes], preferred_element_type=F32) for p, (_, values, _) in zip(probs, pieces)])
        outs.append(mixed / total)
    return jnp.concatenate(outs, axis=1).astype(BF16)


def prompt_rows_of(held, which):
    return held[:, which].reshape(PEERS * TILE, COLUMNS)


def attend_response(t, q, held, k_own, v_own):
    row = lax.broadcasted_iota(jnp.int32, (Q_TILE, Q_TILE), 0)
    col = lax.broadcasted_iota(jnp.int32, (Q_TILE, Q_TILE), 1)
    pieces = [(prompt_rows_of(held, 0), prompt_rows_of(held, 1), None)]
    if t:
        pieces.append((k_own[:t * Q_TILE], v_own[:t * Q_TILE], None))
    span = slice(t * Q_TILE, (t + 1) * Q_TILE)
    pieces.append((k_own[span], v_own[span], col <= row))
    return softmax_mix(q, pieces)


def deal_mixed(router, t, mixed, stage, out):
    dealt = jnp.dot(deal(Q_TILE), mixed, preferred_element_type=F32).astype(BF16)
    stage[t] = dealt.reshape(PEERS, Q_TILE // PEERS, COLUMNS)
    router.send(t)
    out[router.net.me, t] = stage[t, router.net.me]


def first_attention_kernel(xp_hbm, xr_hbm, out_hbm, wq_hbm, wk_hbm, wv_hbm, gain_ref, cos_ref, sin_ref, info_ref,
                           mixed_out, res_out, info_out, prompt_out, next_hbm, columns_hbm,
                           xs, raw, w, even, odd, q_s, k_s, v_s, held, mixed_stage, res_stage,
                           x_sem, w_sem, ring_send, ring_recv, near_send, near_recv, info_send, info_recv, spread_held, spread_sem, *routes):
    net = Exchange()
    spread_sems, slice_sems, routes = routes[:RING], routes[RING:RING + PAIR], routes[RING + PAIR:]
    slices = Slices(out_hbm, spread_held, *slice_sems)
    columns = RespGather(net, spread_held, *spread_sems)
    mixed_router = Router(net, RING, lambda t, d: mixed_stage.at[t, d], lambda t, d: mixed_out.at[d, t], routes[:PAIR])
    res_router = Router(net, 1, lambda t, d: res_stage.at[d], lambda t, d: res_out.at[d], routes[PAIR:])
    prompt = RespGather(net, held, ring_send, ring_recv, near_send, near_recv)
    me = net.me
    column = pl.multiple_of(lax.axis_index("model") * COLUMNS, COLUMNS)

    def load(t):
        src = xp_hbm if isinstance(t, int) and t == 0 else xr_hbm.at[pl.ds(pl.multiple_of((t - 1) * TILE, TILE), TILE)]
        return pltpu.make_async_copy(src, xs.at[t], x_sem.at[t])

    load(0).start()
    weights, next_weights = ([pltpu.make_async_copy(src.at[layer], raw.at[i], w_sem.at[i]) for i, src in enumerate((wq_hbm, wk_hbm, wv_hbm))] for layer in BOTH)
    for copy in weights:
        copy.start()
    for t in range(1, 9):
        load(t).start()
    net.barrier(slices.others)
    slices.start()
    net.scatter(lambda d: info_ref.at[d], info_out.at[me], info_send, info_recv)
    info_out[me] = info_ref[me]

    def project(t, hidden):
        span = pl.ds(pl.multiple_of(t * TILE, TILE), TILE)
        qkv = jnp.dot(hidden[...], w[...], preferred_element_type=F32)
        cos, sin = cos_ref[span], sin_ref[span]
        return span, rope(qkv[:, :COLUMNS], cos, sin).astype(BF16), rope(qkv[:, COLUMNS:512], cos, sin).astype(BF16), qkv[:, 512:].astype(BF16)

    load(0).wait()
    norm_tile(xs.at[0], even, gain_ref)
    for copy in weights:
        copy.wait()
    split_heads(raw, w)
    for copy in next_weights:
        copy.start()
    load(1).wait()
    span, q, k, v = project(0, even)
    norm_tile(xs.at[1], odd, gain_ref)
    q_s[span] = q
    held[me, 0] = k
    held[me, 1] = v
    prompt.start()
    prompt.start_rest()
    for t in range(PAIR, 9):
        load(t).wait()
    spread = deal(TILE)

    @pl.loop(1, 9)
    def _(t):
        dealt = jnp.dot(spread, xs[t, :, pl.ds(column, COLUMNS)], preferred_element_type=F32).astype(BF16)
        res_stage[:, t - 1] = dealt.reshape(PEERS, TILE // PEERS, COLUMNS)

    res_out[me] = res_stage[me]

    def response_tile(t, here, there):
        span, q, k, v = project(t, here)
        norm_tile(xs.at[jnp.minimum(t + 1, 8)], there, gain_ref)
        q_s[span] = q
        own = pl.ds(pl.multiple_of((t - 1) * TILE, TILE), TILE)
        k_s[own] = k
        v_s[own] = v

    @pl.loop(0, RING)
    def _(i):
        response_tile(PAIR * i + 1, odd, even)
        response_tile(PAIR * i + PAIR, even, odd)

        @pl.when(i == 0)
        def _():
            prompt.relay()
            res_router.send(0)

        @pl.when(i == 1)
        def _():
            slices.collect()
            columns.start()
            columns.start_rest()

        pl.when(i == PAIR)(prompt.share)
        pl.when(i == 3)(columns.relay)

    prompt.collect()
    for t in range(RING):
        mixed = attend_response(t, q_s[pl.ds(TILE + t * Q_TILE, Q_TILE)], held, k_s, v_s)
        deal_mixed(mixed_router, t, mixed, mixed_stage, mixed_out)
    row = lax.broadcasted_iota(jnp.int32, (TILE, PEERS * TILE), 0) + me * TILE
    col = lax.broadcasted_iota(jnp.int32, (TILE, PEERS * TILE), 1)
    prompt_out[:, :COLUMNS] = softmax_mix(q_s[pl.ds(0, TILE)], [(prompt_rows_of(held, 0), prompt_rows_of(held, 1), col <= row)])
    prompt_out[:, COLUMNS:] = xs[0, :, pl.ds(column, COLUMNS)]
    for copy in next_weights:
        copy.wait()
    split_heads(raw, w)
    leave = pltpu.make_async_copy(w, next_hbm, w_sem.at[3])
    leave.start()
    columns.share()
    columns.collect()
    out_copies = [pltpu.make_async_copy(spread_held.at[device, layer], columns_hbm.at[layer, :, device], spread_sem.at[layer, device])
                  for device in range(PEERS) for layer in BOTH]
    for copy in out_copies:
        copy.start()
    for router in (mixed_router, res_router):
        for t in range(router.tiles):
            router.collect(t)
        router.finish()
    net.collected(lambda d: info_out.at[d], info_recv)
    net.sent(lambda d: info_ref.at[d], info_send, info_recv)
    prompt.finish()
    columns.finish()
    slices.finish()
    leave.wait()
    for copy in out_copies:
        copy.wait()


def first_attention(x_prompt, x_resp, w_out, w_query, w_key, w_value, gain, cos, sin, info, collective_id):
    rows = TILE + x_resp.shape[0]
    width = x_resp.shape[1]
    return pl.pallas_call(
        first_attention_kernel,
        out_shape=(jax.ShapeDtypeStruct((PEERS, RING, 32, COLUMNS), BF16), jax.ShapeDtypeStruct((PEERS, 8, 16, COLUMNS), BF16),
                   jax.ShapeDtypeStruct((PEERS, 8, 128), jnp.int32), jax.ShapeDtypeStruct((TILE, PAIR * COLUMNS), BF16), jax.ShapeDtypeStruct((width, 3 * COLUMNS), BF16),
                   jax.ShapeDtypeStruct((PAIR, SHARDS, PEERS, 32, COLUMNS), BF16)),
        in_specs=[ANY] * 6 + [VMEM] * 4,
        out_specs=(VMEM,) * 4 + (ANY, ANY),
        scratch_shapes=[
            pltpu.VMEM((9, TILE, width), BF16), pltpu.VMEM((3, PAIR * width, LANES), BF16), pltpu.VMEM((width, 3 * COLUMNS), BF16), pltpu.VMEM((TILE, width), BF16), pltpu.VMEM((TILE, width), BF16),
            pltpu.VMEM((rows, COLUMNS), BF16), pltpu.VMEM((rows - TILE, COLUMNS), BF16), pltpu.VMEM((rows - TILE, COLUMNS), BF16),
            HELD, pltpu.VMEM((RING, PEERS, 32, COLUMNS), BF16), pltpu.VMEM((PEERS, 8, 16, COLUMNS), BF16),
            DMA((9,)), DMA((RING,)), *GATHER_SEMS, DMA((PEERS,)), DMA((PEERS,)),
            pltpu.VMEM((PEERS, PAIR, SHARDS, 32, COLUMNS), BF16), DMA((PAIR, PEERS)), *GATHER_SEMS, DMA((SHARDS,)), DMA((SHARDS,)),
            *[DMA((RING, PEERS)) for _ in BOTH], *[DMA((1, PEERS)) for _ in BOTH],
        ],
        compiler_params=pltpu.CompilerParams(collective_id=collective_id, has_side_effects=True, vmem_limit_bytes=VMEM_BYTES),
        name="first_attention",
    )(x_prompt, x_resp, w_out, w_query, w_key, w_value, gain, cos, sin, info)


def second_attention_kernel(qkv_ref, back_ref, mixed_out, stage, qkv_in, k_s, v_s, held, mixed_stage,
                            ring_send, ring_recv, near_send, near_recv, *routes):
    net = Exchange()
    me = net.me
    prompt = RespGather(net, held, ring_send, ring_recv, near_send, near_recv)
    router = Router(net, RING, lambda t, d: stage.at[t, d], lambda t, d: qkv_in.at[t, d], routes[:PAIR])
    mixed_router = Router(net, RING, lambda t, d: mixed_stage.at[t, d], lambda t, d: mixed_out.at[d, t], routes[PAIR:])
    for k in BOTH:
        held[me, k] = qkv_ref[pl.ds(0, TILE), pl.ds((k + 1) * COLUMNS, COLUMNS)]
    net.barrier()
    prompt.start()
    prompt.start_rest()
    count = back_ref.shape[1]

    def send_rows(t):
        place = lax.broadcasted_iota(jnp.int32, (Q_TILE, count), 0) + t * Q_TILE == back_ref[...]
        rows = jnp.dot(place.astype(BF16), qkv_ref[pl.ds(TILE, count)], preferred_element_type=F32).astype(BF16)
        stage[t] = rows.reshape(PEERS, Q_TILE // PEERS, 3 * COLUMNS)
        router.send(t)
        qkv_in[t, me] = stage[t, me]

    send_rows(0)
    prompt.relay()
    for t in range(1, RING):
        send_rows(t)
    prompt.share()
    prompt.collect()
    for t in range(RING):
        router.collect(t)
        rows = jnp.dot(undeal(Q_TILE), qkv_in[t].reshape(Q_TILE, 3 * COLUMNS), preferred_element_type=F32).astype(BF16)
        k_s[pl.ds(t * Q_TILE, Q_TILE)] = rows[:, COLUMNS:PAIR * COLUMNS]
        v_s[pl.ds(t * Q_TILE, Q_TILE)] = rows[:, PAIR * COLUMNS:]
        mixed = attend_response(t, rows[:, :COLUMNS], held, k_s, v_s)
        deal_mixed(mixed_router, t, mixed, mixed_stage, mixed_out)
    for t in range(RING):
        mixed_router.collect(t)
    for each in (router, mixed_router):
        each.finish()
    prompt.finish()


def second_attention(qkv, back, collective_id):
    rows = RING * Q_TILE
    wide = (32, 3 * COLUMNS)
    return pl.pallas_call(
        second_attention_kernel,
        out_shape=jax.ShapeDtypeStruct((PEERS, RING, 32, COLUMNS), BF16),
        in_specs=[VMEM, VMEM],
        out_specs=VMEM,
        scratch_shapes=[
            pltpu.VMEM((RING, PEERS) + wide, BF16), pltpu.VMEM((RING, PEERS) + wide, BF16),
            pltpu.VMEM((rows, COLUMNS), BF16), pltpu.VMEM((rows, COLUMNS), BF16),
            HELD, pltpu.VMEM((RING, PEERS, 32, COLUMNS), BF16), *GATHER_SEMS,
            *[DMA((RING, PEERS)) for _ in range(RING)],
        ],
        compiler_params=pltpu.CompilerParams(collective_id=collective_id, has_side_effects=True, vmem_limit_bytes=VMEM_BYTES),
        name=f"second_attention{collective_id}",
    )(qkv, back)


class Answer:
    def __init__(self, every, out_ref, stat_send, stat_recv, row_send, row_recv):
        self.every, self.out = every, out_ref
        self.stat_sems, self.row_sems = (stat_send, stat_recv), (row_send, row_recv)
        self.me, self.home = lax.axis_index("model"), lax.axis_index("resp")
        self.models = [(self.me + k) % SHARDS for k in range(1, SHARDS)]
        self.homes = [(self.home + k) % PEERS for k in range(1, PEERS)]

    def barrier(self):
        sem = pltpu.get_barrier_semaphore()
        for axis, devices in (("model", self.models), ("resp", self.homes)):
            for device in devices:
                pl.semaphore_signal(sem, device_id={axis: device}, device_id_type=MESH)
        pl.semaphore_wait(sem, len(self.models) + len(self.homes))

    def stat_copy(self, owner, device, place):
        ref = self.every.at[owner]
        return pltpu.make_async_remote_copy(
            src_ref=ref, dst_ref=ref, send_sem=self.stat_sems[0].at[device], recv_sem=self.stat_sems[1].at[place],
            device_id={"model": device}, device_id_type=MESH)

    def row_copy(self, owner, device, place):
        ref = self.out.at[owner]
        return pltpu.make_async_remote_copy(
            src_ref=ref, dst_ref=ref, send_sem=self.row_sems[0].at[device], recv_sem=self.row_sems[1].at[place],
            device_id={"resp": device}, device_id_type=MESH)

def combine_kernel(stats_ref, out_ref, every, *sems):
    net = Answer(every, out_ref, *sems)
    every[net.me] = stats_ref[...]
    net.barrier()
    for device in net.models:
        net.stat_copy(net.me, device, net.me).start()
    for device in net.models:
        net.stat_copy(device, device, device).wait_recv()
    shards = range(SHARDS)
    top = functools.reduce(jnp.maximum, [every[k, 0] for k in shards])
    total = functools.reduce(jnp.add, [every[k, 1] * jnp.exp(every[k, 0] - top) for k in shards])
    out_ref[net.home] = functools.reduce(jnp.add, [every[k, PAIR] for k in shards]) - top - jnp.log(total)
    for device in net.homes:
        net.row_copy(net.home, device, net.home).start()
    for device in net.homes:
        net.row_copy(device, device, device).wait_recv()
    for device in net.models:
        net.stat_copy(net.me, device, device).wait_send()
    for device in net.homes:
        net.row_copy(net.home, device, device).wait_send()


def combine(stats, collective_id):
    return pl.pallas_call(
        combine_kernel,
        out_shape=jax.ShapeDtypeStruct((PEERS, PEERS, LANES), F32),
        in_specs=[VMEM],
        out_specs=VMEM,
        scratch_shapes=[pltpu.VMEM((SHARDS,) + stats.shape, F32), *[DMA((SHARDS,)) for _ in BOTH], *[DMA((PEERS,)) for _ in BOTH]],
        compiler_params=pltpu.CompilerParams(collective_id=collective_id, has_side_effects=True),
        name="combine",
    )(stats)


ROPE_BASE = 10000.0
VARIANTS = (640, 768, 1024)


def rope_tables(positions):
    half = LANES // PAIR
    lane = jnp.arange(LANES)
    frequency = ROPE_BASE ** (-(lane % half).astype(F32) / half)
    angles = positions.astype(F32)[:, None] * frequency
    return jnp.cos(angles), jnp.sin(angles) * jnp.where(lane < half, -1.0, 1.0)


def solution(mesh):
    groups = mesh.shape['resp']
    row_axes = ('prompts', 'resp')
    head_spec = P(None, None, 'model', None)
    in_specs = (P(row_axes, None), P(row_axes, None, None), P(row_axes, None), P(row_axes), P(None, None), head_spec, head_spec, head_spec, P(None, 'model', None, None), P(None, None), P(None, None, 'model'), P(None, None, 'model'), P(None, 'model', None), P(None), P(None, 'model'))

    def device_step(x_prompt, x_resp, targets, resp_lens, attn_gain, w_query, w_key, w_value, w_out, mlp_gain, w_gate, w_up, w_down, final_gain, w_vocab):
        prompt_rows = x_prompt.shape[0]
        resp_len, width = x_resp.shape[1:]
        prompt_len = prompt_rows * groups
        me = lax.axis_index('model')
        home = lax.axis_index('resp')
        per = resp_len // groups
        gate_t, up_t = jnp.swapaxes(w_gate, 1, 2), jnp.swapaxes(w_up, 1, 2)
        out_flat = w_out.reshape(w_out.shape[0], COLUMNS, width)
        projections = [w.reshape(w.shape[0], PAIR * width, LANES) for w in (w_query, w_key, w_value)]
        prompt_pos = home * prompt_rows + jnp.arange(prompt_rows)

        cos, sin = rope_tables(jnp.concatenate([prompt_pos, prompt_len + jnp.arange(resp_len)]))
        info = jnp.concatenate([
            targets.reshape(per, groups).T[:, None, :],
            jnp.broadcast_to(resp_lens, (groups, groups - 1, per))], axis=1)
        mixed, res, infos, prompt, w_second, out_columns = first_attention(x_prompt, x_resp[0], out_flat, *projections, attn_gain, cos, sin, info, 0)
        lens = infos[:, 1, 0]
        need = (lens + groups - 1) // groups
        ends = jnp.sum(jnp.where(jnp.arange(groups)[:, None] >= jnp.arange(groups), need, 0), axis=1)
        starts = ends - need
        dealt = groups * per

        def finish_with(size, ident):
            def run(operands):
                mixed, res, prompt = operands
                slot = jnp.arange(size)
                which = jnp.sum((slot[:, None] >= ends).astype(jnp.int32), axis=1)
                row = slot - jnp.sum(jnp.where(which[:, None] == jnp.arange(groups), starts, 0), axis=1)
                real = slot < ends[-1]
                source = jnp.where(real, which * per + row, -1)
                chosen = source[:, None] == jnp.arange(dealt)
                wanted = jnp.sum(jnp.where(chosen, infos[:, 0, :].reshape(dealt), 0), axis=1) - me * w_vocab.shape[1]
                ids = jnp.where(jnp.arange(LANES) == 0, source[:, None], wanted[:, None])
                ids = jnp.pad(ids, ((prompt_rows, 0), (0, 0)), constant_values=-1)
                tables = rope_tables(jnp.concatenate([prompt_pos, prompt_len + groups * row + home]))
                weights = (out_columns.reshape(PAIR, width, COLUMNS), gate_t, up_t, w_down)
                qkv, new_res = mega(
                    mlp_gain, attn_gain, ids, mixed.reshape(dealt, COLUMNS), res.reshape(dealt, COLUMNS),
                    [*tables, prompt], *weights, w_second, 0, ident)
                part = per // RING
                back = jnp.where(real, (row // part) * (groups * part) + which * part + row % part, -1)
                mixed = second_attention(qkv, back[None], ident + 1)
                return mega(mlp_gain, final_gain[None], ids, mixed.reshape(dealt, COLUMNS), new_res, [], *weights, w_vocab, 1, ident + PAIR)
            return run

        smallest = sorted(VARIANTS)
        fit = sum((ends[-1] > size).astype(jnp.int32) for size in smallest[:-1])
        index = sum(jnp.where(fit == smallest.index(size), i, 0) for i, size in enumerate(VARIANTS))
        stats = lax.switch(index, [finish_with(size, 3 + 3 * i) for i, size in enumerate(VARIANTS)], (mixed, res, prompt))
        found = combine(stats, 1).reshape(groups, dealt)
        start = jnp.sum(jnp.where(jnp.arange(groups) == home, starts, 0))
        mine = lax.dynamic_slice(jnp.pad(found, ((0, 0), (0, per))), (0, start), (groups, per))
        log_probs = mine.T.reshape(resp_len)
        log_probs = jnp.where(jnp.arange(resp_len) < resp_lens[0], log_probs, 0.0)
        return log_probs[None, :]

    return jax.shard_map(device_step, mesh=mesh, in_specs=in_specs, out_specs=P(row_axes, None), check_vma=False)
```

```python
import functools

import jax
import jax.numpy as jnp
from jax import lax
from jax.experimental import pallas as pl
from jax.experimental.pallas import tpu as pltpu
from jax.sharding import PartitionSpec as P

MESH = pl.DeviceIdType.MESH
F32 = jnp.float32
BF16 = jnp.bfloat16
EPS = 1e-6
LANES = 128
PAIR = 2
RING = 4
COLUMNS = PAIR * LANES
SHARDS = RING * RING
PEERS = 8
BOTH = range(PAIR)
VMEM_BYTES = 67_000_000
LATE_ROWS = 640
LOGITS = 512
CHUNKS = 4
VMEM = pl.BlockSpec(memory_space=pltpu.VMEM)
ANY = pl.BlockSpec(memory_space=pl.ANY)
DMA = pltpu.SemaphoreType.DMA
KINDS = range(RING * 3)
SUM_FAR, SUM_NEAR, SUM_RELAY, SUM2_FAR, SUM2_NEAR, SUM2_RELAY, TAKE_OWN, TAKE_REST, TAKE_RELAY, TAKE2_OWN, TAKE2_REST, TAKE2_RELAY = KINDS


def block_of(color, first, second):
    return RING * first + second if color else RING * second + first


def pair(index):
    return pl.ds(PAIR * index, PAIR)


class Torus:
    def __init__(self, refs, send_sem, recv_sem):
        self.refs = refs
        self.far, self.near, self.relayed, self.sums, self.relayed2, self.sums2, self.rows = refs
        self.send_sem, self.recv_sem = send_sem, recv_sem
        me = lax.axis_index("model")
        z, y = me // RING, me % RING
        self.place = ((y, z), (z, y))
        along_y = [z * RING + self.step(y, way) for way in (1, -1)]
        along_z = [self.step(z, way) * RING + y for way in (1, -1)]
        self.neighbors = ((along_y, along_z), (along_z, along_y))

    def step(self, place, by):
        return (place + by + RING) % RING

    def barrier(self):
        sem = pltpu.get_barrier_semaphore()
        for ring in self.neighbors[0]:
            for device in ring:
                pl.semaphore_signal(sem, device_id={"model": device}, device_id_type=MESH)
        pl.semaphore_wait(sem, RING)

    def ends(self, kind, c, q, d):
        (p, s), way, other = self.place[q], 1 - PAIR * d, 1 - d
        far, near, relayed, sums, relayed2, sums2, rows = (ref.at[c, q] for ref in self.refs)
        own = sums.at[0]
        back_s, back_p = self.step(s, -way), self.step(p, -way)
        return {
            SUM_FAR: lambda: (far.at[pair(d)], relayed.at[d], relayed.at[d]),
            SUM_NEAR: lambda: (near.at[d], sums.at[d, pair(other)], sums.at[d, pair(other)]),
            SUM_RELAY: lambda: (relayed.at[d], sums.at[d, pair(d)], sums.at[d, pair(d)]),
            SUM2_FAR: lambda: (own.at[self.step(s, PAIR), d], relayed2.at[d], relayed2.at[d]),
            SUM2_NEAR: lambda: (own.at[self.step(s, way), other], sums2.at[d, other], sums2.at[d, other]),
            SUM2_RELAY: lambda: (relayed2.at[d], sums2.at[d, d], sums2.at[d, d]),
            TAKE_OWN: lambda: (rows.at[p, s, d], rows.at[p, s, d], rows.at[p, back_s, d]),
            TAKE_REST: lambda: (rows.at[p, s, other], rows.at[p, s, other], rows.at[p, back_s, other]),
            TAKE_RELAY: lambda: (rows.at[p, back_s, d], rows.at[p, back_s, d], rows.at[p, self.step(s, PAIR), d]),
            TAKE2_OWN: lambda: (rows.at[p, pair(d)], rows.at[p, pair(d)], rows.at[back_p, pair(d)]),
            TAKE2_REST: lambda: (rows.at[p, pair(other)], rows.at[p, pair(other)], rows.at[back_p, pair(other)]),
            TAKE2_RELAY: lambda: (rows.at[back_p, pair(d)], rows.at[back_p, pair(d)], rows.at[self.step(p, PAIR), pair(d)]),
        }[kind]()

    def copy(self, kind, c, q, d, src, dst):
        second_ring = kind in (SUM2_FAR, SUM2_NEAR, SUM2_RELAY, TAKE_OWN, TAKE_REST, TAKE_RELAY)
        return pltpu.make_async_remote_copy(
            src_ref=src, dst_ref=dst, send_sem=self.send_sem.at[c, q, d, kind], recv_sem=self.recv_sem.at[c, q, d, kind],
            device_id={"model": self.neighbors[q][second_ring][d]}, device_id_type=MESH)

    def send(self, c, q, d, kind):
        src, dst, _ = self.ends(kind, c, q, d)
        self.copy(kind, c, q, d, src, dst).start()

    def sent(self, c, q, *kinds):
        for kind in kinds:
            for d in BOTH:
                src, dst, _ = self.ends(kind, c, q, d)
                self.copy(kind, c, q, d, src, dst).wait_send()

    def arrived(self, c, q, d, *kinds):
        for kind in kinds:
            _, _, here = self.ends(kind, c, q, d)
            self.copy(kind, c, q, d, here, here).wait_recv()


def halves_of(ref):
    return ref[:, :COLUMNS], ref[:, COLUMNS:]


def halves(value):
    return value[:, :LANES], value[:, LANES:]


def store_block(ref, value):
    for half, part in enumerate(halves(value)):
        ref[half] = part


def add_block(ref, value):
    for half, part in enumerate(halves(value)):
        ref[half] += part


class Gather:
    def __init__(self, net):
        self.net = net

    def begin_rows(self, c, q):
        for kind in (TAKE_OWN, TAKE_REST):
            for d in BOTH:
                self.net.send(c, q, d, kind)

    def relay_rows(self, c, q):
        for d in BOTH:
            self.net.arrived(c, q, d, TAKE_OWN)
            self.net.send(c, q, d, TAKE_RELAY)

    def take_second(self, c, q):
        for d in BOTH:
            self.net.arrived(c, q, d, TAKE_REST, TAKE_RELAY)
        for kind in (TAKE2_OWN, TAKE2_REST):
            for d in BOTH:
                self.net.send(c, q, d, kind)

    def relay_last(self, c, q):
        for d in BOTH:
            self.net.arrived(c, q, d, TAKE2_OWN)
            self.net.send(c, q, d, TAKE2_RELAY)

    def complete(self, c, q):
        for d in BOTH:
            self.net.arrived(c, q, d, TAKE2_REST, TAKE2_RELAY)
        self.net.sent(c, q, TAKE_OWN, TAKE_REST, TAKE_RELAY, TAKE2_OWN, TAKE2_REST, TAKE2_RELAY)

    def middle(self):
        return [self.relay_rows, self.take_second, self.relay_last]


class Sum(Gather):
    def __init__(self, net, lhs_of, w_ref, finish):
        self.net, self.lhs_of, self.w_ref, self.finish = net, lhs_of, w_ref, finish

    def product(self, lhs, color, first, second):
        start = pl.multiple_of(block_of(color, first, second) * COLUMNS, COLUMNS)
        return jnp.dot(lhs, self.w_ref[:, pl.ds(start, COLUMNS)], preferred_element_type=F32)

    def begin(self, c, q):
        net, p, lhs = self.net, self.net.place[q][0], self.lhs_of(c, q)
        for k in range(RING):
            store_block(net.far.at[c, q, k], self.product(lhs, q, net.step(p, PAIR), k))
        for d in BOTH:
            net.send(c, q, d, SUM_FAR)
        for d in BOTH:
            for k in BOTH:
                store_block(net.near.at[c, q, d, k], self.product(lhs, q, net.step(p, 1 - PAIR * d), PAIR * (1 - d) + k))
            net.send(c, q, d, SUM_NEAR)

    def relay_sum(self, c, q):
        net, p, lhs = self.net, self.net.place[q][0], self.lhs_of(c, q)
        for d in BOTH:
            net.arrived(c, q, d, SUM_FAR)
            for k in BOTH:
                add_block(net.relayed.at[c, q, d, k], self.product(lhs, q, net.step(p, 1 - PAIR * d), PAIR * d + k))
            net.send(c, q, d, SUM_RELAY)

    def begin_second(self, c, q):
        net, lhs = self.net, self.lhs_of(c, q)
        for d in BOTH:
            net.arrived(c, q, d, SUM_NEAR, SUM_RELAY)
        for k in range(RING):
            for half, part in enumerate(halves(self.product(lhs, q, net.place[q][0], k))):
                net.sums[c, q, 0, k, half] += net.sums[c, q, 1, k, half] + part
        for kind in (SUM2_FAR, SUM2_NEAR):
            for d in BOTH:
                net.send(c, q, d, kind)
        net.sent(c, q, SUM_FAR)

    def relay_second(self, c, q):
        net = self.net
        for d in BOTH:
            net.arrived(c, q, d, SUM2_FAR)
            net.relayed2[c, q, d] += net.sums[c, q, 0, net.step(net.place[q][1], 1 - PAIR * d), d]
            net.send(c, q, d, SUM2_RELAY)

    def finish_sum(self, c, q):
        net = self.net
        net.sent(c, q, SUM_NEAR, SUM_RELAY)
        for d in BOTH:
            net.arrived(c, q, d, SUM2_NEAR, SUM2_RELAY)
        for half in BOTH:
            self.finish(c, q, half, net.sums[c, q, 0, net.place[q][1], half] + net.sums2[c, q, 0, half] + net.sums2[c, q, 1, half])
        self.begin_rows(c, q)

    def relay_rows(self, c, q):
        self.net.sent(c, q, SUM2_FAR, SUM2_NEAR, SUM2_RELAY)
        super().relay_rows(c, q)

    def middle(self):
        return [self.relay_sum, self.begin_second, self.relay_second, self.finish_sum, *super().middle()]


def normed(net, c, q, gain_ref, layer):
    rows = net.rows.shape[-PAIR]
    tile = PAIR * 8 if rows % (PAIR * 8) == 0 else 8
    spots = [(first, second, half) for first in range(RING) for second in range(RING) for half in BOTH]

    @pl.loop(0, rows // tile)
    def _(i):
        span = pl.ds(pl.multiple_of(i * tile, tile), tile)
        acts = [net.rows[(c, q) + spot + (span,)].astype(F32) for spot in spots]
        squares = functools.reduce(jnp.add, [v * v for v in acts])
        inv = lax.rsqrt(jnp.sum(squares, axis=-1, keepdims=True) / (LANES * len(acts)) + EPS)
        for spot, v in zip(spots, acts):
            column = block_of(q, *spot[:PAIR]) * COLUMNS + spot[PAIR] * LANES
            net.rows[(c, q) + spot + (span,)] = (v * inv * gain_ref[pl.ds(layer, 1), pl.ds(column, LANES)]).astype(BF16)


def rows_of(net, c, q):
    parts = []
    for upper in range(RING):
        for lower in range(RING):
            first, second = (upper, lower) if q else (lower, upper)
            parts += [net.rows[c, q, first, second, half] for half in BOTH]
    return jnp.concatenate(parts, axis=1)


def times_transposed(lhs, rhs):
    return lax.dot_general(lhs, rhs, (((1,), (1,)), ((), ())), preferred_element_type=F32)


def late_plan(width, count):
    plan, start = [], 0
    for buffer in BOTH:
        for slot in range(width // count):
            size = min(LATE_ROWS, width - start)
            if size:
                plan.append((buffer, slot * count, start, size))
            start += size
    return plan, width - start


def rope(value, cos, sin):
    return jnp.concatenate([v * cos + pltpu.roll(v, LANES // PAIR, 1) * sin for v in halves(value)], axis=1)


def put_projected(product, cos_ref, sin_ref, out_ref, span):
    for k in range(3):
        value = product(k * COLUMNS, COLUMNS)
        if k < PAIR:
            value = rope(value, cos_ref[span], sin_ref[span])
        out_ref[span, pl.ds(k * COLUMNS, COLUMNS)] = value.astype(BF16)


def statistics(product, count, target):
    top = total = picked = None
    for k in range(count // LOGITS):
        logits = product(k * LOGITS, LOGITS)
        here = jnp.max(logits, axis=-1, keepdims=True)
        ids = lax.broadcasted_iota(jnp.int32, logits.shape, 1) + k * LOGITS
        found = jnp.sum(jnp.where(ids == target, logits, 0.0), axis=-1, keepdims=True)
        if k:
            both = jnp.maximum(top, here)
            total = total * jnp.exp(top - both) + jnp.sum(jnp.exp(logits - both), axis=-1, keepdims=True)
            top, picked = both, picked + found
        else:
            top, total, picked = here, jnp.sum(jnp.exp(logits - here), axis=-1, keepdims=True), found
    lane = lax.broadcasted_iota(jnp.int32, (target.shape[0], LANES), 1)
    return jnp.where(lane == 0, top, jnp.where(lane == 1, total, picked))


def mega_kernel(chunks, layer, last, gain_ref, next_gain_ref, ids_ref, dealt_ref, old_ref, *args):
    if last:
        side_refs, args = (), args
    else:
        side_refs, args = args[:3], args[3:]
    w_out_hbm, w_gate_hbm, w_up_hbm, w_down_hbm, *args = args
    late_hbm, out_ref, *args = args
    if not last:
        new_res_ref, *args = args
    (w_out, w_gate, w_up, w_down, late_rest, res, inner, middle, stats,
     far, near, relayed, sums, relayed2, sums2, rows, w_sem, late_sem, send_sem, recv_sem, ready_sem) = args
    loads = [pltpu.make_async_copy(src.at[layer], dst, w_sem.at[i]) for i, (src, dst) in enumerate(
        ((w_out_hbm, w_out), (w_gate_hbm, w_gate), (w_up_hbm, w_up), (w_down_hbm, w_down)))]
    for load in loads:
        load.start()
    width, count = late_hbm.shape
    plan, left = late_plan(width, count)
    late = [(late_hbm.at[pl.ds(start, size)], (w_gate, w_up)[buffer].at[pl.ds(0, size), pl.ds(lane, count)]) for buffer, lane, start, size in plan]
    if left:
        late.append((late_hbm.at[pl.ds(width - left, left)], late_rest))
    late_loads = [pltpu.make_async_copy(src, dst, late_sem.at[i]) for i, (src, dst) in enumerate(late)]
    net = Torus((far, near, relayed, sums, relayed2, sums2, rows), send_sem, recv_sem)
    net.barrier()

    part = rows.shape[-PAIR]

    def span_of(c, q=0, parts=1):
        return pl.ds(pl.multiple_of((PAIR * c + q) * part, 16), parts * part)

    def after_prompt(c, q=0, parts=1):
        return pl.ds(pl.multiple_of((PAIR * c + q) * part + LANES * last, 16), parts * part)

    def picked(c, ref, prompt):
        ids = ids_ref[after_prompt(c, parts=PAIR), :1]
        chosen = (ids == lax.broadcasted_iota(jnp.int32, (PAIR * part, PEERS * LANES), 1)).astype(BF16)
        value = jnp.dot(chosen, ref[...], preferred_element_type=F32)
        if prompt is not None:
            row = lax.broadcasted_iota(jnp.int32, (PAIR * part, LANES), 0) + PAIR * part * c
            chosen = (row == lax.broadcasted_iota(jnp.int32, (PAIR * part, LANES), 1)).astype(BF16)
            value += jnp.dot(chosen, prompt, preferred_element_type=F32)
        return value.astype(BF16)

    def put(ref, value, place_of):
        for q in BOTH:
            for half, columns in enumerate(halves(value)):
                ref[place_of(q) + (half,)] = columns[q * part:(q + 1) * part]

    def begin(c):
        prompts = (None, None) if last else halves_of(side_refs[PAIR])
        put(rows, picked(c, dealt_ref, prompts[0]), lambda q: (c, q) + net.place[q])
        if not last:
            put(res, picked(c, old_ref, prompts[1]), lambda q: (c, q))
        for q in BOTH:
            first.begin_rows(c, q)

    def finish(c, q, half, total):
        value = (middle[c, q, half].astype(F32) + total).astype(BF16)
        if not last:
            new_res_ref[span_of(c, q), pl.ds(half * LANES, LANES)] = value
        rows[(c, q) + net.place[q] + (half,)] = value

    first = Gather(net)
    second = Sum(net, lambda c, q: inner[c, q], w_down, finish)

    def project_out(c):
        for q in BOTH:
            first.complete(c, q)
        total = jnp.dot(jnp.concatenate([rows_of(net, c, q) for q in BOTH], axis=0), w_out[...], preferred_element_type=F32)
        for q in BOTH:
            for half, columns in enumerate(halves(total)):
                old = old_ref[after_prompt(c, q), pl.ds(half * LANES, LANES)] if last else res[c, q, half]
                value = (old.astype(F32) + columns[q * part:(q + 1) * part]).astype(BF16)
                middle[c, q, half] = value
                rows[(c, q) + net.place[q] + (half,)] = value
        for ring in net.neighbors[0]:
            for device in ring:
                pl.semaphore_signal(ready_sem.at[c], device_id={"model": device}, device_id_type=MESH)

    def begin_again(c):
        pl.semaphore_wait(ready_sem.at[c], RING)
        for q in BOTH:
            first.begin_rows(c, q)

    def hidden_of(c, stage, gain, row):
        for q in BOTH:
            stage.complete(c, q)
            normed(net, c, q, gain, row)
        return jnp.concatenate([rows_of(net, c, q) for q in BOTH], axis=0)

    def mlp(c):
        hidden = hidden_of(c, first, gain_ref, layer)
        value = (jax.nn.silu(times_transposed(hidden, w_gate[...])) * times_transposed(hidden, w_up[...])).astype(BF16)
        inner[c] = value.reshape(inner.shape[1:])
        for q in BOTH:
            second.begin(c, q)

    def after(c):
        hidden = hidden_of(c, second, next_gain_ref, 0 if last else layer + 1)

        def product(lane, size):
            parts = [jnp.dot(hidden[:, start:start + rows_here], (w_gate, w_up)[buffer][pl.ds(0, rows_here), pl.ds(at + lane, size)], preferred_element_type=F32)
                     for buffer, at, start, rows_here in plan]
            if left:
                parts.append(jnp.dot(hidden[:, width - left:], late_rest[:, pl.ds(lane, size)], preferred_element_type=F32))
            return functools.reduce(jnp.add, parts)

        if last:
            stats[span_of(c, parts=PAIR)] = statistics(product, count, ids_ref[after_prompt(c, parts=PAIR), 1:PAIR])
        else:
            put_projected(product, *side_refs[:PAIR], out_ref, span_of(c, parts=PAIR))

    def on_both(step):
        def run(c):
            for q in BOTH:
                step(c, q)
        return run

    gather = [on_both(step) for step in first.middle()]
    steps = [begin, *gather, project_out, begin_again, *gather, mlp, *map(on_both, second.middle())]
    at_mlp = steps.index(mlp)
    steps += [None] * max(0, at_mlp + chunks - len(steps)) + [after]

    @pl.loop(0, len(steps) + chunks - 1)
    def _(slot):
        @pl.when(slot == steps.index(project_out))
        def _():
            for load in loads:
                load.wait()

        @pl.when(slot == len(steps) - 1)
        def _():
            for load in late_loads:
                load.wait()

        for k, step in reversed(list(enumerate(steps))):
            if step is None:
                continue

            @pl.when(slot >= k)
            def _():
                @pl.when(slot < k + chunks)
                def _():
                    step(slot - k)

        @pl.when(slot == at_mlp + chunks - 1)
        def _():
            for load in late_loads:
                load.start()

    if last:
        out_ref[...] = jnp.zeros_like(out_ref)
        for k in range(stats.shape[0] // LANES):
            turned = stats[pl.ds(k * LANES, LANES)].T
            for i in range(3):
                out_ref[i, pl.ds(k, 1)] = turned[i:i + 1]


def mega(gain, next_gain, ids, dealt, old, sides, w_out, w_gate_t, w_up_t, w_down, late, layer, collective_id):
    last = not sides
    chunks = CHUNKS
    total = ids.shape[0] - LANES * last
    _, hidden, width = w_gate_t.shape
    rows = total // (PAIR * chunks)
    per = (chunks, PAIR)
    tile = (rows, LANES)
    count = late.shape[1]
    _, left = late_plan(width, count)

    sem = DMA(per + (PAIR, len(KINDS)))
    out = jax.ShapeDtypeStruct((3, PEERS, LANES), F32) if last else (
        jax.ShapeDtypeStruct((total, count), BF16), jax.ShapeDtypeStruct((total, COLUMNS), BF16))
    return pl.pallas_call(
        functools.partial(mega_kernel, chunks, layer, last),
        out_shape=out,
        in_specs=[VMEM] * (5 + len(sides)) + [ANY] * 5,
        out_specs=VMEM if last else (VMEM, VMEM),
        scratch_shapes=[
            pltpu.VMEM((width, COLUMNS), BF16),
            *[pltpu.VMEM((hidden, width), BF16) for _ in range(3)],
            pltpu.VMEM((left or 8, count), BF16),
            pltpu.VMEM(per + (PAIR,) + (tile if not last else (8, LANES)), BF16),
            pltpu.VMEM(per + (rows, hidden), BF16),
            pltpu.VMEM(per + (PAIR,) + tile, BF16),
            pltpu.VMEM((total if last else 8, LANES), F32),
            pltpu.VMEM(per + (RING, PAIR) + tile, F32),
            pltpu.VMEM(per + (PAIR, PAIR, PAIR) + tile, F32),
            pltpu.VMEM(per + (PAIR, PAIR, PAIR) + tile, F32),
            pltpu.VMEM(per + (PAIR, RING, PAIR) + tile, F32),
            pltpu.VMEM(per + (PAIR,) + tile, F32),
            pltpu.VMEM(per + (PAIR, PAIR) + tile, F32),
            pltpu.VMEM(per + (RING, RING, PAIR) + tile, BF16),
            DMA((RING,)), DMA((SHARDS,)), sem, sem, pltpu.SemaphoreType.REGULAR((chunks,)),
        ],
        compiler_params=pltpu.CompilerParams(collective_id=collective_id, has_side_effects=True, vmem_limit_bytes=VMEM_BYTES),
        name=f"mega{collective_id}",
    )(gain, next_gain, ids, dealt, old, *sides, w_out, w_gate_t, w_up_t, w_down, late)


TILE = 128
Q_TILE = 256
LOG2E = 1.4426950408889634
HELD = pltpu.VMEM((PEERS, PAIR, TILE, COLUMNS), BF16)
GATHER_SEMS = [DMA((PAIR, 3)), DMA((PAIR, 3)), DMA((RING,)), DMA((RING,))]


class Exchange:
    def __init__(self):
        self.me = lax.axis_index("resp")
        self.others = [(self.me + k) % PEERS for k in range(1, PEERS)]

    def barrier(self, models=()):
        sem = pltpu.get_barrier_semaphore()
        for axis, devices in (("resp", self.others), ("model", models)):
            for device in devices:
                pl.semaphore_signal(sem, device_id={axis: device}, device_id_type=MESH)
        pl.semaphore_wait(sem, len(self.others) + len(models))

    def copy(self, src, dst, send_sem, recv_sem, device):
        return pltpu.make_async_remote_copy(src_ref=src, dst_ref=dst, send_sem=send_sem, recv_sem=recv_sem,
                                            device_id={"resp": device}, device_id_type=MESH)

    def scatter(self, src_of, dst, send_sem, recv_sem):
        for device in self.others:
            self.copy(src_of(device), dst, send_sem.at[device], recv_sem.at[self.me], device).start()

    def collected(self, dst_of, recv_sem):
        for device in self.others:
            self.copy(dst_of(device), dst_of(device), recv_sem.at[device], recv_sem.at[device], device).wait_recv()

    def sent(self, src_of, send_sem, recv_sem):
        for device in self.others:
            self.copy(src_of(device), src_of(device), send_sem.at[device], recv_sem.at[device], device).wait_send()


class Router:
    def __init__(self, net, tiles, src_of, dst_of, sems):
        self.net, self.tiles, self.src_of, self.dst_of = net, tiles, src_of, dst_of
        self.send_sem, self.recv_sem = sems

    def send(self, t):
        self.net.scatter(lambda d: self.src_of(t, d), self.dst_of(t, self.net.me), self.send_sem.at[t], self.recv_sem.at[t])

    def collect(self, t):
        self.net.collected(lambda d: self.dst_of(t, d), self.recv_sem.at[t])

    def finish(self):
        for t in range(self.tiles):
            self.net.sent(lambda d: self.src_of(t, d), self.send_sem.at[t], self.recv_sem.at[t])


class Slices:
    def __init__(self, w_hbm, held, send_sem, recv_sem):
        self.w, self.held, self.send_sem, self.recv_sem = w_hbm, held, send_sem, recv_sem
        self.me, home = lax.axis_index("model"), lax.axis_index("resp")
        self.homes = (home, (home + RING) % PEERS)
        self.others = [(self.me + k) % SHARDS for k in range(1, SHARDS)]

    def part(self, which, device):
        rows = pl.ds(pl.multiple_of(self.homes[which] * 32, 32), 32)
        return self.w.at[:, rows, pl.ds(pl.multiple_of(device * COLUMNS, COLUMNS), COLUMNS)]

    def own(self, which):
        return pltpu.make_async_copy(self.part(which, self.me), self.held.at[self.homes[which], :, self.me], self.send_sem.at[which, self.me])

    def copy(self, which, device, place):
        return pltpu.make_async_remote_copy(
            src_ref=self.part(which, device), dst_ref=self.held.at[self.homes[which], :, place], send_sem=self.send_sem.at[which, device],
            recv_sem=self.recv_sem.at[which, place], device_id={"model": device}, device_id_type=MESH)

    def start(self):
        for which in BOTH:
            self.own(which).start()
            for device in self.others:
                self.copy(which, device, self.me).start()

    def collect(self):
        for which in BOTH:
            for device in self.others:
                self.copy(which, device, device).wait_recv()
            self.own(which).wait()

    def finish(self):
        for which in BOTH:
            for device in self.others:
                self.copy(which, device, self.me).wait_send()


class RespGather:
    def __init__(self, net, held, ring_send, ring_recv, near_send, near_recv):
        self.net, self.held = net, held
        self.ring_sems, self.near_sems = (ring_send, ring_recv), (near_send, near_recv)
        x, core = net.me // PAIR, net.me % PAIR
        self.at = lambda by, here: (x + by + RING) % RING * PAIR + (core if here else 1 - core)

    def ring_copy(self, d, kind, ref):
        return self.net.copy(ref, ref, self.ring_sems[0].at[d, kind], self.ring_sems[1].at[d, kind], self.at(1 - PAIR * d, True))

    def near_copy(self, kind, ref):
        return self.net.copy(ref, ref, self.near_sems[0].at[kind], self.near_sems[1].at[kind], self.at(0, False))

    def sources(self, here):
        return [self.at(by, here) for by in (0, -1, 1, PAIR)]

    def start(self):
        for d in BOTH:
            self.ring_copy(d, 0, self.held.at[self.net.me, d]).start()
        self.near_copy(0, self.held.at[self.net.me]).start()

    def start_rest(self):
        for d in BOTH:
            self.ring_copy(d, 1, self.held.at[self.net.me, 1 - d]).start()

    def relay(self):
        for d in BOTH:
            ref = self.held.at[self.at(PAIR * d - 1, True), d]
            self.ring_copy(d, 0, ref).wait_recv()
            self.ring_copy(d, PAIR, ref).start()

    def share(self):
        for d in BOTH:
            device = self.at(PAIR * d - 1, True)
            self.ring_copy(d, 1, self.held.at[device, 1 - d]).wait_recv()
            self.near_copy(1 + d, self.held.at[device]).start()
        far = self.held.at[self.at(PAIR, True)]
        for d in BOTH:
            self.ring_copy(d, PAIR, far.at[d]).wait_recv()
        self.near_copy(3, far).start()

    def collect(self):
        for kind, device in enumerate(self.sources(False)):
            self.near_copy(kind, self.held.at[device]).wait_recv()

    def finish(self):
        for kind in range(3):
            for d in BOTH:
                self.ring_copy(d, kind, self.held.at[self.net.me, d]).wait_send()
        for kind in range(RING):
            self.near_copy(kind, self.held.at[self.net.me]).wait_send()


class ColumnGather(RespGather):
    def start(self):
        for d in BOTH:
            self.ring_copy(d, 0, self.held.at[self.net.me]).start()
        for kind, device in ((0, self.net.me), (3, self.at(PAIR, True))):
            self.near_copy(kind, self.held.at[device]).start()

    def share(self):
        for d in BOTH:
            ref = self.held.at[self.at(PAIR * d - 1, True)]
            self.ring_copy(d, 0, ref).wait_recv()
            self.near_copy(1 + d, ref).start()

    def finish(self):
        for d in BOTH:
            self.ring_copy(d, 0, self.held.at[self.net.me]).wait_send()
        for kind in range(RING):
            self.near_copy(kind, self.held.at[self.net.me]).wait_send()


def deal(rows):
    out = lax.broadcasted_iota(jnp.int32, (rows, rows), 0)
    src = lax.broadcasted_iota(jnp.int32, (rows, rows), 1)
    per = rows // PEERS
    return jnp.where(src == (out % per) * PEERS + out // per, 1.0, 0.0).astype(BF16)


def undeal(rows):
    out = lax.broadcasted_iota(jnp.int32, (rows, rows), 0)
    src = lax.broadcasted_iota(jnp.int32, (rows, rows), 1)
    per = rows // PEERS
    return jnp.where(src == (out % PEERS) * per + out // PEERS, 1.0, 0.0).astype(BF16)


def split_heads(raw_ref, w_ref):
    tile = PAIR * LANES
    out = lax.broadcasted_iota(jnp.int32, (tile, tile), 0)
    src = lax.broadcasted_iota(jnp.int32, (tile, tile), 1)
    pick = jnp.where(src == (out % LANES) * PAIR + out // LANES, 1.0, 0.0).astype(BF16)

    @pl.loop(0, raw_ref.shape[1] // (RING * tile))
    def _(b):
        raws = [raw_ref[i, pl.ds(pl.multiple_of((b * RING + k) * tile, tile), tile)] for k in range(RING) for i in range(3)]
        heads = jnp.dot(pick, jnp.concatenate(raws, axis=1), preferred_element_type=F32).astype(BF16)
        for k in range(RING):
            here = pl.ds(pl.multiple_of((b * RING + k) * LANES, LANES), LANES)
            for i in range(3):
                for h in BOTH:
                    at = (k * 3 + i) * LANES
                    w_ref[here, pl.ds(i * COLUMNS + h * LANES, LANES)] = heads[h * LANES:(h + 1) * LANES, at:at + LANES]


def norm_tile(x_ref, out_ref, gain_ref):
    for i in range(x_ref.shape[0] // 16):
        v = x_ref[pl.ds(16 * i, 16), :].astype(F32)
        inv = lax.rsqrt(jnp.mean(v * v, axis=-1, keepdims=True) + EPS)
        out_ref[pl.ds(16 * i, 16), :] = (v * inv * gain_ref[pl.ds(0, 1), :]).astype(BF16)


def softmax_mix(q, pieces):
    factor = LOG2E * 128 ** -0.5
    outs = []
    for h in range(2):
        lanes = slice(128 * h, 128 * h + 128)
        scores = []
        for keys, _, mask in pieces:
            s = lax.dot_general(q[:, lanes], keys[:, lanes], (((1,), (1,)), ((), ())), preferred_element_type=F32)
            scores.append(s if mask is None else jnp.where(mask, s, -jnp.inf))
        top = functools.reduce(jnp.maximum, [jnp.max(s, axis=-1, keepdims=True) for s in scores])
        probs = [jnp.exp2((s - top) * factor) for s in scores]
        total = functools.reduce(jnp.add, [jnp.sum(p, axis=-1, keepdims=True) for p in probs])
        mixed = functools.reduce(jnp.add, [jnp.dot(p.astype(BF16), values[:, lanes], preferred_element_type=F32) for p, (_, values, _) in zip(probs, pieces)])
        outs.append(mixed / total)
    return jnp.concatenate(outs, axis=1).astype(BF16)


def prompt_rows_of(held, which):
    return held[:, which].reshape(PEERS * TILE, COLUMNS)


def attend_response(t, q, held, k_own, v_own):
    row = lax.broadcasted_iota(jnp.int32, (Q_TILE, Q_TILE), 0)
    col = lax.broadcasted_iota(jnp.int32, (Q_TILE, Q_TILE), 1)
    pieces = [(prompt_rows_of(held, 0), prompt_rows_of(held, 1), None)]
    if t:
        pieces.append((k_own[:t * Q_TILE], v_own[:t * Q_TILE], None))
    span = slice(t * Q_TILE, (t + 1) * Q_TILE)
    pieces.append((k_own[span], v_own[span], col <= row))
    return softmax_mix(q, pieces)


def deal_mixed(router, t, mixed, stage, out):
    dealt = jnp.dot(deal(Q_TILE), mixed, preferred_element_type=F32).astype(BF16)
    stage[t] = dealt.reshape(PEERS, Q_TILE // PEERS, COLUMNS)
    router.send(t)
    out[router.net.me, t] = stage[t, router.net.me]


def first_attention_kernel(xp_hbm, xr_hbm, out_hbm, wq_hbm, wk_hbm, wv_hbm, gain_ref, cos_ref, sin_ref, info_ref,
                           mixed_out, res_out, info_out, prompt_out, next_hbm, columns_hbm,
                           xs, raw, w, even, odd, q_s, k_s, v_s, held, mixed_stage, res_stage,
                           x_sem, w_sem, ring_send, ring_recv, near_send, near_recv, info_send, info_recv, spread_held, spread_sem, *routes):
    net = Exchange()
    spread_sems, slice_sems, routes = routes[:RING], routes[RING:RING + PAIR], routes[RING + PAIR:]
    slices = Slices(out_hbm, spread_held, *slice_sems)
    columns = ColumnGather(net, spread_held, *spread_sems)
    mixed_router = Router(net, RING, lambda t, d: mixed_stage.at[t, d], lambda t, d: mixed_out.at[d, t], routes[:PAIR])
    res_router = Router(net, 1, lambda t, d: res_stage.at[d], lambda t, d: res_out.at[d], routes[PAIR:])
    prompt = RespGather(net, held, ring_send, ring_recv, near_send, near_recv)
    me = net.me
    column = pl.multiple_of(lax.axis_index("model") * COLUMNS, COLUMNS)

    def load(t):
        src = xp_hbm if isinstance(t, int) and t == 0 else xr_hbm.at[pl.ds(pl.multiple_of((t - 1) * TILE, TILE), TILE)]
        return pltpu.make_async_copy(src, xs.at[t], x_sem.at[t])

    load(0).start()
    weights, next_weights = ([pltpu.make_async_copy(src.at[layer], raw.at[i], w_sem.at[i]) for i, src in enumerate((wq_hbm, wk_hbm, wv_hbm))] for layer in BOTH)
    for copy in weights:
        copy.start()
    for t in range(1, 9):
        load(t).start()
    net.barrier(slices.others)
    slices.start()
    net.scatter(lambda d: info_ref.at[d], info_out.at[me], info_send, info_recv)
    info_out[me] = info_ref[me]

    def project(t, hidden):
        span = pl.ds(pl.multiple_of(t * TILE, TILE), TILE)
        qkv = jnp.dot(hidden[...], w[...], preferred_element_type=F32)
        cos, sin = cos_ref[span], sin_ref[span]
        return span, rope(qkv[:, :COLUMNS], cos, sin).astype(BF16), rope(qkv[:, COLUMNS:512], cos, sin).astype(BF16), qkv[:, 512:].astype(BF16)

    load(0).wait()
    norm_tile(xs.at[0], even, gain_ref)
    for copy in weights:
        copy.wait()
    split_heads(raw, w)
    for copy in next_weights:
        copy.start()
    load(1).wait()
    span, q, k, v = project(0, even)
    norm_tile(xs.at[1], odd, gain_ref)
    q_s[span] = q
    held[me, 0] = k
    held[me, 1] = v
    prompt.start()
    prompt.start_rest()
    for t in range(PAIR, 9):
        load(t).wait()
    spread = deal(TILE)

    @pl.loop(1, 9)
    def _(t):
        dealt = jnp.dot(spread, xs[t, :, pl.ds(column, COLUMNS)], preferred_element_type=F32).astype(BF16)
        res_stage[:, t - 1] = dealt.reshape(PEERS, TILE // PEERS, COLUMNS)

    res_out[me] = res_stage[me]

    def response_tile(t, here, there):
        span, q, k, v = project(t, here)
        norm_tile(xs.at[jnp.minimum(t + 1, 8)], there, gain_ref)
        q_s[span] = q
        own = pl.ds(pl.multiple_of((t - 1) * TILE, TILE), TILE)
        k_s[own] = k
        v_s[own] = v

    @pl.loop(0, RING)
    def _(i):
        response_tile(PAIR * i + 1, odd, even)
        response_tile(PAIR * i + PAIR, even, odd)

        @pl.when(i == 0)
        def _():
            prompt.relay()
            res_router.send(0)

        @pl.when(i == 1)
        def _():
            slices.collect()
            columns.start()

        pl.when(i == PAIR)(prompt.share)

    prompt.collect()
    for t in range(RING):
        mixed = attend_response(t, q_s[pl.ds(TILE + t * Q_TILE, Q_TILE)], held, k_s, v_s)
        deal_mixed(mixed_router, t, mixed, mixed_stage, mixed_out)
    columns.share()
    row = lax.broadcasted_iota(jnp.int32, (TILE, PEERS * TILE), 0) + me * TILE
    col = lax.broadcasted_iota(jnp.int32, (TILE, PEERS * TILE), 1)
    prompt_out[:, :COLUMNS] = softmax_mix(q_s[pl.ds(0, TILE)], [(prompt_rows_of(held, 0), prompt_rows_of(held, 1), col <= row)])
    prompt_out[:, COLUMNS:] = xs[0, :, pl.ds(column, COLUMNS)]
    for copy in next_weights:
        copy.wait()
    split_heads(raw, w)
    leave = pltpu.make_async_copy(w, next_hbm, w_sem.at[3])
    leave.start()
    columns.collect()
    out_copies = [pltpu.make_async_copy(spread_held.at[device, layer], columns_hbm.at[layer, :, device], spread_sem.at[layer, device])
                  for device in range(PEERS) for layer in BOTH]
    for copy in out_copies:
        copy.start()
    for router in (mixed_router, res_router):
        for t in range(router.tiles):
            router.collect(t)
        router.finish()
    net.collected(lambda d: info_out.at[d], info_recv)
    net.sent(lambda d: info_ref.at[d], info_send, info_recv)
    prompt.finish()
    columns.finish()
    slices.finish()
    leave.wait()
    for copy in out_copies:
        copy.wait()


def first_attention(x_prompt, x_resp, w_out, w_query, w_key, w_value, gain, cos, sin, info, collective_id):
    rows = TILE + x_resp.shape[0]
    width = x_resp.shape[1]
    return pl.pallas_call(
        first_attention_kernel,
        out_shape=(jax.ShapeDtypeStruct((PEERS, RING, 32, COLUMNS), BF16), jax.ShapeDtypeStruct((PEERS, 8, 16, COLUMNS), BF16),
                   jax.ShapeDtypeStruct((PEERS, 8, 128), jnp.int32), jax.ShapeDtypeStruct((TILE, PAIR * COLUMNS), BF16), jax.ShapeDtypeStruct((width, 3 * COLUMNS), BF16),
                   jax.ShapeDtypeStruct((PAIR, SHARDS, PEERS, 32, COLUMNS), BF16)),
        in_specs=[ANY] * 6 + [VMEM] * 4,
        out_specs=(VMEM,) * 4 + (ANY, ANY),
        scratch_shapes=[
            pltpu.VMEM((9, TILE, width), BF16), pltpu.VMEM((3, PAIR * width, LANES), BF16), pltpu.VMEM((width, 3 * COLUMNS), BF16), pltpu.VMEM((TILE, width), BF16), pltpu.VMEM((TILE, width), BF16),
            pltpu.VMEM((rows, COLUMNS), BF16), pltpu.VMEM((rows - TILE, COLUMNS), BF16), pltpu.VMEM((rows - TILE, COLUMNS), BF16),
            HELD, pltpu.VMEM((RING, PEERS, 32, COLUMNS), BF16), pltpu.VMEM((PEERS, 8, 16, COLUMNS), BF16),
            DMA((9,)), DMA((RING,)), *GATHER_SEMS, DMA((PEERS,)), DMA((PEERS,)),
            pltpu.VMEM((PEERS, PAIR, SHARDS, 32, COLUMNS), BF16), DMA((PAIR, PEERS)), *GATHER_SEMS, DMA((PAIR, SHARDS)), DMA((PAIR, SHARDS)),
            *[DMA((RING, PEERS)) for _ in BOTH], *[DMA((1, PEERS)) for _ in BOTH],
        ],
        compiler_params=pltpu.CompilerParams(collective_id=collective_id, has_side_effects=True, vmem_limit_bytes=VMEM_BYTES),
        name="first_attention",
    )(x_prompt, x_resp, w_out, w_query, w_key, w_value, gain, cos, sin, info)


def second_attention_kernel(qkv_ref, back_ref, mixed_out, stage, qkv_in, k_s, v_s, held, mixed_stage,
                            ring_send, ring_recv, near_send, near_recv, *routes):
    net = Exchange()
    me = net.me
    prompt = RespGather(net, held, ring_send, ring_recv, near_send, near_recv)
    router = Router(net, RING, lambda t, d: stage.at[t, d], lambda t, d: qkv_in.at[t, d], routes[:PAIR])
    mixed_router = Router(net, RING, lambda t, d: mixed_stage.at[t, d], lambda t, d: mixed_out.at[d, t], routes[PAIR:])
    for k in BOTH:
        held[me, k] = qkv_ref[pl.ds(0, TILE), pl.ds((k + 1) * COLUMNS, COLUMNS)]
    net.barrier()
    prompt.start()
    prompt.start_rest()
    count = back_ref.shape[1]

    def send_rows(t):
        place = lax.broadcasted_iota(jnp.int32, (Q_TILE, count), 0) + t * Q_TILE == back_ref[...]
        rows = jnp.dot(place.astype(BF16), qkv_ref[pl.ds(TILE, count)], preferred_element_type=F32).astype(BF16)
        stage[t] = rows.reshape(PEERS, Q_TILE // PEERS, 3 * COLUMNS)
        router.send(t)
        qkv_in[t, me] = stage[t, me]

    send_rows(0)
    prompt.relay()
    for t in range(1, RING):
        send_rows(t)
    prompt.share()
    prompt.collect()
    for t in range(RING):
        router.collect(t)
        rows = jnp.dot(undeal(Q_TILE), qkv_in[t].reshape(Q_TILE, 3 * COLUMNS), preferred_element_type=F32).astype(BF16)
        k_s[pl.ds(t * Q_TILE, Q_TILE)] = rows[:, COLUMNS:PAIR * COLUMNS]
        v_s[pl.ds(t * Q_TILE, Q_TILE)] = rows[:, PAIR * COLUMNS:]
        mixed = attend_response(t, rows[:, :COLUMNS], held, k_s, v_s)
        deal_mixed(mixed_router, t, mixed, mixed_stage, mixed_out)
    for t in range(RING):
        mixed_router.collect(t)
    for each in (router, mixed_router):
        each.finish()
    prompt.finish()


def second_attention(qkv, back, collective_id):
    rows = RING * Q_TILE
    wide = (32, 3 * COLUMNS)
    return pl.pallas_call(
        second_attention_kernel,
        out_shape=jax.ShapeDtypeStruct((PEERS, RING, 32, COLUMNS), BF16),
        in_specs=[VMEM, VMEM],
        out_specs=VMEM,
        scratch_shapes=[
            pltpu.VMEM((RING, PEERS) + wide, BF16), pltpu.VMEM((RING, PEERS) + wide, BF16),
            pltpu.VMEM((rows, COLUMNS), BF16), pltpu.VMEM((rows, COLUMNS), BF16),
            HELD, pltpu.VMEM((RING, PEERS, 32, COLUMNS), BF16), *GATHER_SEMS,
            *[DMA((RING, PEERS)) for _ in range(RING)],
        ],
        compiler_params=pltpu.CompilerParams(collective_id=collective_id, has_side_effects=True, vmem_limit_bytes=VMEM_BYTES),
        name=f"second_attention{collective_id}",
    )(qkv, back)


class Answer:
    def __init__(self, every, out_ref, stat_send, stat_recv, row_send, row_recv):
        self.every, self.out = every, out_ref
        self.stat_sems, self.row_sems = (stat_send, stat_recv), (row_send, row_recv)
        self.me, self.home = lax.axis_index("model"), lax.axis_index("resp")
        self.models = [(self.me + k) % SHARDS for k in range(1, SHARDS)]
        self.homes = [(self.home + k) % PEERS for k in range(1, PEERS)]

    def barrier(self):
        sem = pltpu.get_barrier_semaphore()
        for axis, devices in (("model", self.models), ("resp", self.homes)):
            for device in devices:
                pl.semaphore_signal(sem, device_id={axis: device}, device_id_type=MESH)
        pl.semaphore_wait(sem, len(self.models) + len(self.homes))

    def stat_copy(self, owner, device, place):
        ref = self.every.at[owner]
        return pltpu.make_async_remote_copy(
            src_ref=ref, dst_ref=ref, send_sem=self.stat_sems[0].at[device], recv_sem=self.stat_sems[1].at[place],
            device_id={"model": device}, device_id_type=MESH)

    def row_copy(self, owner, device, place):
        ref = self.out.at[owner]
        return pltpu.make_async_remote_copy(
            src_ref=ref, dst_ref=ref, send_sem=self.row_sems[0].at[device], recv_sem=self.row_sems[1].at[place],
            device_id={"resp": device}, device_id_type=MESH)

def combine_kernel(stats_ref, out_ref, every, *sems):
    net = Answer(every, out_ref, *sems)
    every[net.me] = stats_ref[...]
    net.barrier()
    for device in net.models:
        net.stat_copy(net.me, device, net.me).start()
    for device in net.models:
        net.stat_copy(device, device, device).wait_recv()
    shards = range(SHARDS)
    top = functools.reduce(jnp.maximum, [every[k, 0] for k in shards])
    total = functools.reduce(jnp.add, [every[k, 1] * jnp.exp(every[k, 0] - top) for k in shards])
    out_ref[net.home] = functools.reduce(jnp.add, [every[k, PAIR] for k in shards]) - top - jnp.log(total)
    for device in net.homes:
        net.row_copy(net.home, device, net.home).start()
    for device in net.homes:
        net.row_copy(device, device, device).wait_recv()
    for device in net.models:
        net.stat_copy(net.me, device, device).wait_send()
    for device in net.homes:
        net.row_copy(net.home, device, device).wait_send()


def combine(stats, collective_id):
    return pl.pallas_call(
        combine_kernel,
        out_shape=jax.ShapeDtypeStruct((PEERS, PEERS, LANES), F32),
        in_specs=[VMEM],
        out_specs=VMEM,
        scratch_shapes=[pltpu.VMEM((SHARDS,) + stats.shape, F32), *[DMA((SHARDS,)) for _ in BOTH], *[DMA((PEERS,)) for _ in BOTH]],
        compiler_params=pltpu.CompilerParams(collective_id=collective_id, has_side_effects=True),
        name="combine",
    )(stats)


ROPE_BASE = 10000.0
VARIANTS = (640, 768, 1024)


def rope_tables(positions):
    half = LANES // PAIR
    lane = jnp.arange(LANES)
    frequency = ROPE_BASE ** (-(lane % half).astype(F32) / half)
    angles = positions.astype(F32)[:, None] * frequency
    return jnp.cos(angles), jnp.sin(angles) * jnp.where(lane < half, -1.0, 1.0)


def solution(mesh):
    groups = mesh.shape['resp']
    row_axes = ('prompts', 'resp')
    head_spec = P(None, None, 'model', None)
    in_specs = (P(row_axes, None), P(row_axes, None, None), P(row_axes, None), P(row_axes), P(None, None), head_spec, head_spec, head_spec, P(None, 'model', None, None), P(None, None), P(None, None, 'model'), P(None, None, 'model'), P(None, 'model', None), P(None), P(None, 'model'))

    def device_step(x_prompt, x_resp, targets, resp_lens, attn_gain, w_query, w_key, w_value, w_out, mlp_gain, w_gate, w_up, w_down, final_gain, w_vocab):
        prompt_rows = x_prompt.shape[0]
        resp_len, width = x_resp.shape[1:]
        prompt_len = prompt_rows * groups
        me = lax.axis_index('model')
        home = lax.axis_index('resp')
        per = resp_len // groups
        gate_t, up_t = jnp.swapaxes(w_gate, 1, 2), jnp.swapaxes(w_up, 1, 2)
        out_flat = w_out.reshape(w_out.shape[0], COLUMNS, width)
        projections = [w.reshape(w.shape[0], PAIR * width, LANES) for w in (w_query, w_key, w_value)]
        prompt_pos = home * prompt_rows + jnp.arange(prompt_rows)

        cos, sin = rope_tables(jnp.concatenate([prompt_pos, prompt_len + jnp.arange(resp_len)]))
        info = jnp.concatenate([
            targets.reshape(per, groups).T[:, None, :],
            jnp.broadcast_to(resp_lens, (groups, groups - 1, per))], axis=1)
        mixed, res, infos, prompt, w_second, out_columns = first_attention(x_prompt, x_resp[0], out_flat, *projections, attn_gain, cos, sin, info, 0)
        lens = infos[:, 1, 0]
        need = (lens + groups - 1) // groups
        ends = jnp.sum(jnp.where(jnp.arange(groups)[:, None] >= jnp.arange(groups), need, 0), axis=1)
        starts = ends - need
        dealt = groups * per

        def finish_with(size, ident):
            def run(operands):
                mixed, res, prompt = operands
                slot = jnp.arange(size)
                which = jnp.sum((slot[:, None] >= ends).astype(jnp.int32), axis=1)
                row = slot - jnp.sum(jnp.where(which[:, None] == jnp.arange(groups), starts, 0), axis=1)
                real = slot < ends[-1]
                source = jnp.where(real, which * per + row, -1)
                chosen = source[:, None] == jnp.arange(dealt)
                wanted = jnp.sum(jnp.where(chosen, infos[:, 0, :].reshape(dealt), 0), axis=1) - me * w_vocab.shape[1]
                ids = jnp.where(jnp.arange(LANES) == 0, source[:, None], wanted[:, None])
                ids = jnp.pad(ids, ((prompt_rows, 0), (0, 0)), constant_values=-1)
                tables = rope_tables(jnp.concatenate([prompt_pos, prompt_len + groups * row + home]))
                weights = (out_columns.reshape(PAIR, width, COLUMNS), gate_t, up_t, w_down)
                qkv, new_res = mega(
                    mlp_gain, attn_gain, ids, mixed.reshape(dealt, COLUMNS), res.reshape(dealt, COLUMNS),
                    [*tables, prompt], *weights, w_second, 0, ident)
                part = per // RING
                back = jnp.where(real, (row // part) * (groups * part) + which * part + row % part, -1)
                mixed = second_attention(qkv, back[None], ident + 1)
                return mega(mlp_gain, final_gain[None], ids, mixed.reshape(dealt, COLUMNS), new_res, [], *weights, w_vocab, 1, ident + PAIR)
            return run

        smallest = sorted(VARIANTS)
        fit = sum((ends[-1] > size).astype(jnp.int32) for size in smallest[:-1])
        index = sum(jnp.where(fit == smallest.index(size), i, 0) for i, size in enumerate(VARIANTS))
        stats = lax.switch(index, [finish_with(size, 3 + 3 * i) for i, size in enumerate(VARIANTS)], (mixed, res, prompt))
        found = combine(stats, 1).reshape(groups, dealt)
        start = jnp.sum(jnp.where(jnp.arange(groups) == home, starts, 0))
        mine = lax.dynamic_slice(jnp.pad(found, ((0, 0), (0, per))), (0, start), (groups, per))
        log_probs = mine.T.reshape(resp_len)
        log_probs = jnp.where(jnp.arange(resp_len) < resp_lens[0], log_probs, 0.0)
        return log_probs[None, :]

    return jax.shard_map(device_step, mesh=mesh, in_specs=in_specs, out_specs=P(row_axes, None), check_vma=False)
```

```python
import functools

import jax
import jax.numpy as jnp
from jax import lax
from jax.experimental import pallas as pl
from jax.experimental.pallas import tpu as pltpu
from jax.sharding import PartitionSpec as P

MESH = pl.DeviceIdType.MESH
F32 = jnp.float32
BF16 = jnp.bfloat16
EPS = 1e-6
LANES = 128
PAIR = 2
RING = 4
COLUMNS = PAIR * LANES
SHARDS = RING * RING
PEERS = 8
BOTH = range(PAIR)
VMEM_BYTES = 67_000_000
LATE_ROWS = 640
LOGITS = 512
CHUNKS = 4
VMEM = pl.BlockSpec(memory_space=pltpu.VMEM)
ANY = pl.BlockSpec(memory_space=pl.ANY)
DMA = pltpu.SemaphoreType.DMA
KINDS = range(RING * 3)
SUM_FAR, SUM_NEAR, SUM_RELAY, SUM2_FAR, SUM2_NEAR, SUM2_RELAY, TAKE_OWN, TAKE_REST, TAKE_RELAY, TAKE2_OWN, TAKE2_REST, TAKE2_RELAY = KINDS


def block_of(color, first, second):
    return RING * first + second if color else RING * second + first


def pair(index):
    return pl.ds(PAIR * index, PAIR)


class Torus:
    def __init__(self, refs, send_sem, recv_sem):
        self.refs = refs
        self.far, self.near, self.relayed, self.sums, self.relayed2, self.sums2, self.rows = refs
        self.send_sem, self.recv_sem = send_sem, recv_sem
        me = lax.axis_index("model")
        z, y = me // RING, me % RING
        self.place = ((y, z), (z, y))
        along_y = [z * RING + self.step(y, way) for way in (1, -1)]
        along_z = [self.step(z, way) * RING + y for way in (1, -1)]
        self.neighbors = ((along_y, along_z), (along_z, along_y))

    def step(self, place, by):
        return (place + by + RING) % RING

    def enter(self):
        sem = pltpu.get_barrier_semaphore()
        for ring in self.neighbors[0]:
            for device in ring:
                pl.semaphore_signal(sem, device_id={"model": device}, device_id_type=MESH)

    def all_here(self):
        pl.semaphore_wait(pltpu.get_barrier_semaphore(), RING)

    def ends(self, kind, c, q, d):
        (p, s), way, other = self.place[q], 1 - PAIR * d, 1 - d
        far, near, relayed, sums, relayed2, sums2, rows = (ref.at[c, q] for ref in self.refs)
        own = sums.at[0]
        back_s, back_p = self.step(s, -way), self.step(p, -way)
        return {
            SUM_FAR: lambda: (far.at[pair(d)], relayed.at[d], relayed.at[d]),
            SUM_NEAR: lambda: (near.at[d], sums.at[d, pair(other)], sums.at[d, pair(other)]),
            SUM_RELAY: lambda: (relayed.at[d], sums.at[d, pair(d)], sums.at[d, pair(d)]),
            SUM2_FAR: lambda: (own.at[self.step(s, PAIR), d], relayed2.at[d], relayed2.at[d]),
            SUM2_NEAR: lambda: (own.at[self.step(s, way), other], sums2.at[d, other], sums2.at[d, other]),
            SUM2_RELAY: lambda: (relayed2.at[d], sums2.at[d, d], sums2.at[d, d]),
            TAKE_OWN: lambda: (rows.at[p, s, d], rows.at[p, s, d], rows.at[p, back_s, d]),
            TAKE_REST: lambda: (rows.at[p, s, other], rows.at[p, s, other], rows.at[p, back_s, other]),
            TAKE_RELAY: lambda: (rows.at[p, back_s, d], rows.at[p, back_s, d], rows.at[p, self.step(s, PAIR), d]),
            TAKE2_OWN: lambda: (rows.at[p, pair(d)], rows.at[p, pair(d)], rows.at[back_p, pair(d)]),
            TAKE2_REST: lambda: (rows.at[p, pair(other)], rows.at[p, pair(other)], rows.at[back_p, pair(other)]),
            TAKE2_RELAY: lambda: (rows.at[back_p, pair(d)], rows.at[back_p, pair(d)], rows.at[self.step(p, PAIR), pair(d)]),
        }[kind]()

    def copy(self, kind, c, q, d, src, dst):
        second_ring = kind in (SUM2_FAR, SUM2_NEAR, SUM2_RELAY, TAKE_OWN, TAKE_REST, TAKE_RELAY)
        return pltpu.make_async_remote_copy(
            src_ref=src, dst_ref=dst, send_sem=self.send_sem.at[c, q, d, kind], recv_sem=self.recv_sem.at[c, q, d, kind],
            device_id={"model": self.neighbors[q][second_ring][d]}, device_id_type=MESH)

    def send(self, c, q, d, kind):
        src, dst, _ = self.ends(kind, c, q, d)
        self.copy(kind, c, q, d, src, dst).start()

    def sent(self, c, q, *kinds):
        for kind in kinds:
            for d in BOTH:
                src, dst, _ = self.ends(kind, c, q, d)
                self.copy(kind, c, q, d, src, dst).wait_send()

    def arrived(self, c, q, d, *kinds):
        for kind in kinds:
            _, _, here = self.ends(kind, c, q, d)
            self.copy(kind, c, q, d, here, here).wait_recv()


def halves_of(ref):
    return ref[:, :COLUMNS], ref[:, COLUMNS:]


def halves(value):
    return value[:, :LANES], value[:, LANES:]


def store_block(ref, value):
    for half, part in enumerate(halves(value)):
        ref[half] = part


def add_block(ref, value):
    for half, part in enumerate(halves(value)):
        ref[half] += part


class Gather:
    def __init__(self, net):
        self.net = net

    def begin_rows(self, c, q):
        for kind in (TAKE_OWN, TAKE_REST):
            for d in BOTH:
                self.net.send(c, q, d, kind)

    def relay_rows(self, c, q):
        for d in BOTH:
            self.net.arrived(c, q, d, TAKE_OWN)
            self.net.send(c, q, d, TAKE_RELAY)

    def take_second(self, c, q):
        for d in BOTH:
            self.net.arrived(c, q, d, TAKE_REST, TAKE_RELAY)
        for kind in (TAKE2_OWN, TAKE2_REST):
            for d in BOTH:
                self.net.send(c, q, d, kind)

    def relay_last(self, c, q):
        for d in BOTH:
            self.net.arrived(c, q, d, TAKE2_OWN)
            self.net.send(c, q, d, TAKE2_RELAY)

    def complete(self, c, q):
        for d in BOTH:
            self.net.arrived(c, q, d, TAKE2_REST, TAKE2_RELAY)
        self.net.sent(c, q, TAKE_OWN, TAKE_REST, TAKE_RELAY, TAKE2_OWN, TAKE2_REST, TAKE2_RELAY)

    def middle(self):
        return [self.relay_rows, self.take_second, self.relay_last]


class Sum(Gather):
    def __init__(self, net, lhs_of, w_ref, finish):
        self.net, self.lhs_of, self.w_ref, self.finish = net, lhs_of, w_ref, finish

    def product(self, lhs, color, first, second):
        start = pl.multiple_of(block_of(color, first, second) * COLUMNS, COLUMNS)
        return jnp.dot(lhs, self.w_ref[:, pl.ds(start, COLUMNS)], preferred_element_type=F32)

    def begin(self, c, q):
        net, p, lhs = self.net, self.net.place[q][0], self.lhs_of(c, q)
        for k in range(RING):
            store_block(net.far.at[c, q, k], self.product(lhs, q, net.step(p, PAIR), k))
        for d in BOTH:
            net.send(c, q, d, SUM_FAR)
        for d in BOTH:
            for k in BOTH:
                store_block(net.near.at[c, q, d, k], self.product(lhs, q, net.step(p, 1 - PAIR * d), PAIR * (1 - d) + k))
            net.send(c, q, d, SUM_NEAR)

    def relay_sum(self, c, q):
        net, p, lhs = self.net, self.net.place[q][0], self.lhs_of(c, q)
        for d in BOTH:
            net.arrived(c, q, d, SUM_FAR)
            for k in BOTH:
                add_block(net.relayed.at[c, q, d, k], self.product(lhs, q, net.step(p, 1 - PAIR * d), PAIR * d + k))
            net.send(c, q, d, SUM_RELAY)

    def begin_second(self, c, q):
        net, lhs = self.net, self.lhs_of(c, q)
        for d in BOTH:
            net.arrived(c, q, d, SUM_NEAR, SUM_RELAY)
        for k in range(RING):
            for half, part in enumerate(halves(self.product(lhs, q, net.place[q][0], k))):
                net.sums[c, q, 0, k, half] += net.sums[c, q, 1, k, half] + part
        for kind in (SUM2_FAR, SUM2_NEAR):
            for d in BOTH:
                net.send(c, q, d, kind)
        net.sent(c, q, SUM_FAR)

    def relay_second(self, c, q):
        net = self.net
        for d in BOTH:
            net.arrived(c, q, d, SUM2_FAR)
            net.relayed2[c, q, d] += net.sums[c, q, 0, net.step(net.place[q][1], 1 - PAIR * d), d]
            net.send(c, q, d, SUM2_RELAY)

    def finish_sum(self, c, q):
        net = self.net
        net.sent(c, q, SUM_NEAR, SUM_RELAY)
        for d in BOTH:
            net.arrived(c, q, d, SUM2_NEAR, SUM2_RELAY)
        for half in BOTH:
            self.finish(c, q, half, net.sums[c, q, 0, net.place[q][1], half] + net.sums2[c, q, 0, half] + net.sums2[c, q, 1, half])
        self.begin_rows(c, q)

    def relay_rows(self, c, q):
        self.net.sent(c, q, SUM2_FAR, SUM2_NEAR, SUM2_RELAY)
        super().relay_rows(c, q)

    def middle(self):
        return [self.relay_sum, self.begin_second, self.relay_second, self.finish_sum, *super().middle()]


def normed(net, c, q, gain_ref, layer):
    rows = net.rows.shape[-PAIR]
    tile = PAIR * 8 if rows % (PAIR * 8) == 0 else 8
    spots = [(first, second, half) for first in range(RING) for second in range(RING) for half in BOTH]

    @pl.loop(0, rows // tile)
    def _(i):
        span = pl.ds(pl.multiple_of(i * tile, tile), tile)
        acts = [net.rows[(c, q) + spot + (span,)].astype(F32) for spot in spots]
        squares = functools.reduce(jnp.add, [v * v for v in acts])
        inv = lax.rsqrt(jnp.sum(squares, axis=-1, keepdims=True) / (LANES * len(acts)) + EPS)
        for spot, v in zip(spots, acts):
            column = block_of(q, *spot[:PAIR]) * COLUMNS + spot[PAIR] * LANES
            net.rows[(c, q) + spot + (span,)] = (v * inv * gain_ref[pl.ds(layer, 1), pl.ds(column, LANES)]).astype(BF16)


def rows_of(net, c, q):
    parts = []
    for upper in range(RING):
        for lower in range(RING):
            first, second = (upper, lower) if q else (lower, upper)
            parts += [net.rows[c, q, first, second, half] for half in BOTH]
    return jnp.concatenate(parts, axis=1)


def times_transposed(lhs, rhs):
    return lax.dot_general(lhs, rhs, (((1,), (1,)), ((), ())), preferred_element_type=F32)


def late_plan(width, count):
    plan, start = [], 0
    for buffer in BOTH:
        for slot in range(width // count):
            size = min(LATE_ROWS, width - start)
            if size:
                plan.append((buffer, slot * count, start, size))
            start += size
    return plan, width - start


def rope(value, cos, sin):
    return jnp.concatenate([v * cos + pltpu.roll(v, LANES // PAIR, 1) * sin for v in halves(value)], axis=1)


def put_projected(product, cos_ref, sin_ref, out_ref, span):
    for k in range(3):
        value = product(k * COLUMNS, COLUMNS)
        if k < PAIR:
            value = rope(value, cos_ref[span], sin_ref[span])
        out_ref[span, pl.ds(k * COLUMNS, COLUMNS)] = value.astype(BF16)


def statistics(product, count, target):
    top = total = picked = None
    for k in range(count // LOGITS):
        logits = product(k * LOGITS, LOGITS)
        here = jnp.max(logits, axis=-1, keepdims=True)
        ids = lax.broadcasted_iota(jnp.int32, logits.shape, 1) + k * LOGITS
        found = jnp.sum(jnp.where(ids == target, logits, 0.0), axis=-1, keepdims=True)
        if k:
            both = jnp.maximum(top, here)
            total = total * jnp.exp(top - both) + jnp.sum(jnp.exp(logits - both), axis=-1, keepdims=True)
            top, picked = both, picked + found
        else:
            top, total, picked = here, jnp.sum(jnp.exp(logits - here), axis=-1, keepdims=True), found
    lane = lax.broadcasted_iota(jnp.int32, (target.shape[0], LANES), 1)
    return jnp.where(lane == 0, top, jnp.where(lane == 1, total, picked))


def mega_kernel(chunks, layer, last, gain_ref, next_gain_ref, ids_ref, dealt_ref, old_ref, *args):
    if last:
        side_refs, args = (), args
    else:
        side_refs, args = args[:3], args[3:]
    w_out_hbm, w_gate_hbm, w_up_hbm, w_down_hbm, *args = args
    late_hbm, out_ref, *args = args
    if not last:
        new_res_ref, *args = args
    (w_out, w_gate, w_up, w_down, late_rest, res, inner, middle, stats,
     far, near, relayed, sums, relayed2, sums2, rows, w_sem, late_sem, send_sem, recv_sem, ready_sem) = args
    loads = [pltpu.make_async_copy(src.at[layer], dst, w_sem.at[i]) for i, (src, dst) in enumerate(
        ((w_out_hbm, w_out), (w_gate_hbm, w_gate), (w_up_hbm, w_up), (w_down_hbm, w_down)))]
    for load in loads:
        load.start()
    width, count = late_hbm.shape
    plan, left = late_plan(width, count)
    late = [(late_hbm.at[pl.ds(start, size)], (w_gate, w_up)[buffer].at[pl.ds(0, size), pl.ds(lane, count)]) for buffer, lane, start, size in plan]
    if left:
        late.append((late_hbm.at[pl.ds(width - left, left)], late_rest))
    late_loads = [pltpu.make_async_copy(src, dst, late_sem.at[i]) for i, (src, dst) in enumerate(late)]
    net = Torus((far, near, relayed, sums, relayed2, sums2, rows), send_sem, recv_sem)
    net.enter()
    net.all_here()

    part = rows.shape[-PAIR]

    def span_of(c, q=0, parts=1):
        return pl.ds(pl.multiple_of((PAIR * c + q) * part, 16), parts * part)

    def after_prompt(c, q=0, parts=1):
        return pl.ds(pl.multiple_of((PAIR * c + q) * part + LANES * last, 16), parts * part)

    def picked(c, ref, prompt):
        ids = ids_ref[after_prompt(c, parts=PAIR), :1]
        chosen = (ids == lax.broadcasted_iota(jnp.int32, (PAIR * part, PEERS * LANES), 1)).astype(BF16)
        value = jnp.dot(chosen, ref[...], preferred_element_type=F32)
        if prompt is not None:
            row = lax.broadcasted_iota(jnp.int32, (PAIR * part, LANES), 0) + PAIR * part * c
            chosen = (row == lax.broadcasted_iota(jnp.int32, (PAIR * part, LANES), 1)).astype(BF16)
            value += jnp.dot(chosen, prompt, preferred_element_type=F32)
        return value.astype(BF16)

    def put(ref, value, place_of):
        for q in BOTH:
            for half, columns in enumerate(halves(value)):
                ref[place_of(q) + (half,)] = columns[q * part:(q + 1) * part]

    def begin(c):
        prompts = (None, None) if last else halves_of(side_refs[PAIR])
        put(rows, picked(c, dealt_ref, prompts[0]), lambda q: (c, q) + net.place[q])
        if not last:
            put(res, picked(c, old_ref, prompts[1]), lambda q: (c, q))
        for q in BOTH:
            first.begin_rows(c, q)

    def finish(c, q, half, total):
        value = (middle[c, q, half].astype(F32) + total).astype(BF16)
        if not last:
            new_res_ref[span_of(c, q), pl.ds(half * LANES, LANES)] = value
        rows[(c, q) + net.place[q] + (half,)] = value

    first = Gather(net)
    second = Sum(net, lambda c, q: inner[c, q], w_down, finish)

    def project_out(c):
        for q in BOTH:
            first.complete(c, q)
        total = jnp.dot(jnp.concatenate([rows_of(net, c, q) for q in BOTH], axis=0), w_out[...], preferred_element_type=F32)
        for q in BOTH:
            for half, columns in enumerate(halves(total)):
                old = old_ref[after_prompt(c, q), pl.ds(half * LANES, LANES)] if last else res[c, q, half]
                value = (old.astype(F32) + columns[q * part:(q + 1) * part]).astype(BF16)
                middle[c, q, half] = value
                rows[(c, q) + net.place[q] + (half,)] = value
        for ring in net.neighbors[0]:
            for device in ring:
                pl.semaphore_signal(ready_sem.at[c], device_id={"model": device}, device_id_type=MESH)

    def begin_again(c):
        pl.semaphore_wait(ready_sem.at[c], RING)
        for q in BOTH:
            first.begin_rows(c, q)

    def hidden_of(c, stage, gain, row):
        for q in BOTH:
            stage.complete(c, q)
            normed(net, c, q, gain, row)
        return jnp.concatenate([rows_of(net, c, q) for q in BOTH], axis=0)

    def mlp(c):
        hidden = hidden_of(c, first, gain_ref, layer)
        value = (jax.nn.silu(times_transposed(hidden, w_gate[...])) * times_transposed(hidden, w_up[...])).astype(BF16)
        inner[c] = value.reshape(inner.shape[1:])
        for q in BOTH:
            second.begin(c, q)

    def after(c):
        hidden = hidden_of(c, second, next_gain_ref, 0 if last else layer + 1)

        def product(lane, size):
            parts = [jnp.dot(hidden[:, start:start + rows_here], (w_gate, w_up)[buffer][pl.ds(0, rows_here), pl.ds(at + lane, size)], preferred_element_type=F32)
                     for buffer, at, start, rows_here in plan]
            if left:
                parts.append(jnp.dot(hidden[:, width - left:], late_rest[:, pl.ds(lane, size)], preferred_element_type=F32))
            return functools.reduce(jnp.add, parts)

        if last:
            stats[span_of(c, parts=PAIR)] = statistics(product, count, ids_ref[after_prompt(c, parts=PAIR), 1:PAIR])
        else:
            put_projected(product, *side_refs[:PAIR], out_ref, span_of(c, parts=PAIR))

    def on_both(step):
        def run(c):
            for q in BOTH:
                step(c, q)
        return run

    gather = [on_both(step) for step in first.middle()]
    steps = [begin, *gather, project_out, begin_again, *gather, mlp, *map(on_both, second.middle())]
    at_mlp = steps.index(mlp)
    steps += [None] * max(0, at_mlp + chunks - len(steps)) + [after]

    @pl.loop(0, len(steps) + chunks - 1)
    def _(slot):
        @pl.when(slot == steps.index(project_out))
        def _():
            for load in loads:
                load.wait()

        @pl.when(slot == len(steps) - 1)
        def _():
            for load in late_loads:
                load.wait()

        for k, step in reversed(list(enumerate(steps))):
            if step is None:
                continue

            @pl.when(slot >= k)
            def _():
                @pl.when(slot < k + chunks)
                def _():
                    step(slot - k)

        @pl.when(slot == at_mlp + chunks - 1)
        def _():
            for load in late_loads:
                load.start()

    if last:
        out_ref[...] = jnp.zeros_like(out_ref)
        for k in range(stats.shape[0] // LANES):
            turned = stats[pl.ds(k * LANES, LANES)].T
            for i in range(3):
                out_ref[i, pl.ds(k, 1)] = turned[i:i + 1]


def mega(gain, next_gain, ids, dealt, old, sides, w_out, w_gate_t, w_up_t, w_down, late, layer, collective_id):
    last = not sides
    chunks = CHUNKS
    total = ids.shape[0] - LANES * last
    _, hidden, width = w_gate_t.shape
    rows = total // (PAIR * chunks)
    per = (chunks, PAIR)
    tile = (rows, LANES)
    count = late.shape[1]
    _, left = late_plan(width, count)

    sem = DMA(per + (PAIR, len(KINDS)))
    out = jax.ShapeDtypeStruct((3, PEERS, LANES), F32) if last else (
        jax.ShapeDtypeStruct((total, count), BF16), jax.ShapeDtypeStruct((total, COLUMNS), BF16))
    return pl.pallas_call(
        functools.partial(mega_kernel, chunks, layer, last),
        out_shape=out,
        in_specs=[VMEM] * (5 + len(sides)) + [ANY] * 5,
        out_specs=VMEM if last else (VMEM, VMEM),
        scratch_shapes=[
            pltpu.VMEM((width, COLUMNS), BF16),
            *[pltpu.VMEM((hidden, width), BF16) for _ in range(3)],
            pltpu.VMEM((left or 8, count), BF16),
            pltpu.VMEM(per + (PAIR,) + (tile if not last else (8, LANES)), BF16),
            pltpu.VMEM(per + (rows, hidden), BF16),
            pltpu.VMEM(per + (PAIR,) + tile, BF16),
            pltpu.VMEM((total if last else 8, LANES), F32),
            pltpu.VMEM(per + (RING, PAIR) + tile, F32),
            pltpu.VMEM(per + (PAIR, PAIR, PAIR) + tile, F32),
            pltpu.VMEM(per + (PAIR, PAIR, PAIR) + tile, F32),
            pltpu.VMEM(per + (PAIR, RING, PAIR) + tile, F32),
            pltpu.VMEM(per + (PAIR,) + tile, F32),
            pltpu.VMEM(per + (PAIR, PAIR) + tile, F32),
            pltpu.VMEM(per + (RING, RING, PAIR) + tile, BF16),
            DMA((RING,)), DMA((SHARDS,)), sem, sem, pltpu.SemaphoreType.REGULAR((chunks,)),
        ],
        compiler_params=pltpu.CompilerParams(collective_id=collective_id, has_side_effects=True, vmem_limit_bytes=VMEM_BYTES),
        name=f"mega{collective_id}",
    )(gain, next_gain, ids, dealt, old, *sides, w_out, w_gate_t, w_up_t, w_down, late)


TILE = 128
Q_TILE = 256
LOG2E = 1.4426950408889634
HELD = pltpu.VMEM((PEERS, PAIR, TILE, COLUMNS), BF16)
GATHER_SEMS = [DMA((PAIR, 3)), DMA((PAIR, 3)), DMA((RING,)), DMA((RING,))]


class Exchange:
    def __init__(self):
        self.me = lax.axis_index("resp")
        self.others = [(self.me + k) % PEERS for k in range(1, PEERS)]

    def enter(self, models=()):
        sem = pltpu.get_barrier_semaphore()
        for axis, devices in (("resp", self.others), ("model", models)):
            for device in devices:
                pl.semaphore_signal(sem, device_id={axis: device}, device_id_type=MESH)

    def all_here(self, models=()):
        pl.semaphore_wait(pltpu.get_barrier_semaphore(), len(self.others) + len(models))

    def copy(self, src, dst, send_sem, recv_sem, device):
        return pltpu.make_async_remote_copy(src_ref=src, dst_ref=dst, send_sem=send_sem, recv_sem=recv_sem,
                                            device_id={"resp": device}, device_id_type=MESH)

    def scatter(self, src_of, dst, send_sem, recv_sem):
        for device in self.others:
            self.copy(src_of(device), dst, send_sem.at[device], recv_sem.at[self.me], device).start()

    def collected(self, dst_of, recv_sem):
        for device in self.others:
            self.copy(dst_of(device), dst_of(device), recv_sem.at[device], recv_sem.at[device], device).wait_recv()

    def sent(self, src_of, send_sem, recv_sem):
        for device in self.others:
            self.copy(src_of(device), src_of(device), send_sem.at[device], recv_sem.at[device], device).wait_send()


class Router:
    def __init__(self, net, tiles, src_of, dst_of, sems):
        self.net, self.tiles, self.src_of, self.dst_of = net, tiles, src_of, dst_of
        self.send_sem, self.recv_sem = sems

    def send(self, t):
        self.net.scatter(lambda d: self.src_of(t, d), self.dst_of(t, self.net.me), self.send_sem.at[t], self.recv_sem.at[t])

    def collect(self, t):
        self.net.collected(lambda d: self.dst_of(t, d), self.recv_sem.at[t])

    def finish(self):
        for t in range(self.tiles):
            self.net.sent(lambda d: self.src_of(t, d), self.send_sem.at[t], self.recv_sem.at[t])


class Slices:
    def __init__(self, w_hbm, held, send_sem, recv_sem):
        self.w, self.held, self.send_sem, self.recv_sem = w_hbm, held, send_sem, recv_sem
        self.me, home = lax.axis_index("model"), lax.axis_index("resp")
        self.homes = (home, (home + RING) % PEERS)
        self.others = [(self.me + k) % SHARDS for k in range(1, SHARDS)]

    def part(self, which, device):
        rows = pl.ds(pl.multiple_of(self.homes[which] * 32, 32), 32)
        return self.w.at[:, rows, pl.ds(pl.multiple_of(device * COLUMNS, COLUMNS), COLUMNS)]

    def own(self, which):
        return pltpu.make_async_copy(self.part(which, self.me), self.held.at[self.homes[which], :, self.me], self.send_sem.at[which, self.me])

    def copy(self, which, device, place):
        return pltpu.make_async_remote_copy(
            src_ref=self.part(which, device), dst_ref=self.held.at[self.homes[which], :, place], send_sem=self.send_sem.at[which, device],
            recv_sem=self.recv_sem.at[which, place], device_id={"model": device}, device_id_type=MESH)

    def start(self):
        for which in BOTH:
            self.own(which).start()
            for device in self.others:
                self.copy(which, device, self.me).start()

    def collect(self):
        for which in BOTH:
            for device in self.others:
                self.copy(which, device, device).wait_recv()
            self.own(which).wait()

    def finish(self):
        for which in BOTH:
            for device in self.others:
                self.copy(which, device, self.me).wait_send()


class RespGather:
    def __init__(self, net, held, ring_send, ring_recv, near_send, near_recv):
        self.net, self.held = net, held
        self.ring_sems, self.near_sems = (ring_send, ring_recv), (near_send, near_recv)
        x, core = net.me // PAIR, net.me % PAIR
        self.at = lambda by, here: (x + by + RING) % RING * PAIR + (core if here else 1 - core)

    def ring_copy(self, d, kind, ref):
        return self.net.copy(ref, ref, self.ring_sems[0].at[d, kind], self.ring_sems[1].at[d, kind], self.at(1 - PAIR * d, True))

    def near_copy(self, kind, ref):
        return self.net.copy(ref, ref, self.near_sems[0].at[kind], self.near_sems[1].at[kind], self.at(0, False))

    def sources(self, here):
        return [self.at(by, here) for by in (0, -1, 1, PAIR)]

    def start(self):
        for d in BOTH:
            self.ring_copy(d, 0, self.held.at[self.net.me, d]).start()
        self.near_copy(0, self.held.at[self.net.me]).start()

    def start_rest(self):
        for d in BOTH:
            self.ring_copy(d, 1, self.held.at[self.net.me, 1 - d]).start()

    def relay(self):
        for d in BOTH:
            ref = self.held.at[self.at(PAIR * d - 1, True), d]
            self.ring_copy(d, 0, ref).wait_recv()
            self.ring_copy(d, PAIR, ref).start()

    def share(self):
        for d in BOTH:
            device = self.at(PAIR * d - 1, True)
            self.ring_copy(d, 1, self.held.at[device, 1 - d]).wait_recv()
            self.near_copy(1 + d, self.held.at[device]).start()
        far = self.held.at[self.at(PAIR, True)]
        for d in BOTH:
            self.ring_copy(d, PAIR, far.at[d]).wait_recv()
        self.near_copy(3, far).start()

    def collect(self):
        for kind, device in enumerate(self.sources(False)):
            self.near_copy(kind, self.held.at[device]).wait_recv()

    def finish(self):
        for kind in range(3):
            for d in BOTH:
                self.ring_copy(d, kind, self.held.at[self.net.me, d]).wait_send()
        for kind in range(RING):
            self.near_copy(kind, self.held.at[self.net.me]).wait_send()


class ColumnGather(RespGather):
    def start(self):
        for d in BOTH:
            self.ring_copy(d, 0, self.held.at[self.net.me]).start()
        for kind, device in ((0, self.net.me), (3, self.at(PAIR, True))):
            self.near_copy(kind, self.held.at[device]).start()

    def share(self):
        for d in BOTH:
            ref = self.held.at[self.at(PAIR * d - 1, True)]
            self.ring_copy(d, 0, ref).wait_recv()
            self.near_copy(1 + d, ref).start()

    def finish(self):
        for d in BOTH:
            self.ring_copy(d, 0, self.held.at[self.net.me]).wait_send()
        for kind in range(RING):
            self.near_copy(kind, self.held.at[self.net.me]).wait_send()


def deal(rows):
    out = lax.broadcasted_iota(jnp.int32, (rows, rows), 0)
    src = lax.broadcasted_iota(jnp.int32, (rows, rows), 1)
    per = rows // PEERS
    return jnp.where(src == (out % per) * PEERS + out // per, 1.0, 0.0).astype(BF16)


def undeal(rows):
    out = lax.broadcasted_iota(jnp.int32, (rows, rows), 0)
    src = lax.broadcasted_iota(jnp.int32, (rows, rows), 1)
    per = rows // PEERS
    return jnp.where(src == (out % PEERS) * per + out // PEERS, 1.0, 0.0).astype(BF16)


def split_heads(raw_ref, w_ref):
    tile = PAIR * LANES
    out = lax.broadcasted_iota(jnp.int32, (tile, tile), 0)
    src = lax.broadcasted_iota(jnp.int32, (tile, tile), 1)
    pick = jnp.where(src == (out % LANES) * PAIR + out // LANES, 1.0, 0.0).astype(BF16)

    @pl.loop(0, raw_ref.shape[1] // (RING * tile))
    def _(b):
        raws = [raw_ref[i, pl.ds(pl.multiple_of((b * RING + k) * tile, tile), tile)] for k in range(RING) for i in range(3)]
        heads = jnp.dot(pick, jnp.concatenate(raws, axis=1), preferred_element_type=F32).astype(BF16)
        for k in range(RING):
            here = pl.ds(pl.multiple_of((b * RING + k) * LANES, LANES), LANES)
            for i in range(3):
                for h in BOTH:
                    at = (k * 3 + i) * LANES
                    w_ref[here, pl.ds(i * COLUMNS + h * LANES, LANES)] = heads[h * LANES:(h + 1) * LANES, at:at + LANES]


def norm_tile(x_ref, out_ref, gain_ref):
    for i in range(x_ref.shape[0] // 16):
        v = x_ref[pl.ds(16 * i, 16), :].astype(F32)
        inv = lax.rsqrt(jnp.mean(v * v, axis=-1, keepdims=True) + EPS)
        out_ref[pl.ds(16 * i, 16), :] = (v * inv * gain_ref[pl.ds(0, 1), :]).astype(BF16)


def softmax_mix(q, pieces):
    factor = LOG2E * 128 ** -0.5
    outs = []
    for h in range(2):
        lanes = slice(128 * h, 128 * h + 128)
        scores = []
        for keys, _, mask in pieces:
            s = lax.dot_general(q[:, lanes], keys[:, lanes], (((1,), (1,)), ((), ())), preferred_element_type=F32)
            scores.append(s if mask is None else jnp.where(mask, s, -jnp.inf))
        top = functools.reduce(jnp.maximum, [jnp.max(s, axis=-1, keepdims=True) for s in scores])
        probs = [jnp.exp2((s - top) * factor) for s in scores]
        total = functools.reduce(jnp.add, [jnp.sum(p, axis=-1, keepdims=True) for p in probs])
        mixed = functools.reduce(jnp.add, [jnp.dot(p.astype(BF16), values[:, lanes], preferred_element_type=F32) for p, (_, values, _) in zip(probs, pieces)])
        outs.append(mixed / total)
    return jnp.concatenate(outs, axis=1).astype(BF16)


def prompt_rows_of(held, which):
    return held[:, which].reshape(PEERS * TILE, COLUMNS)


def attend_response(t, q, held, k_own, v_own):
    row = lax.broadcasted_iota(jnp.int32, (Q_TILE, Q_TILE), 0)
    col = lax.broadcasted_iota(jnp.int32, (Q_TILE, Q_TILE), 1)
    pieces = [(prompt_rows_of(held, 0), prompt_rows_of(held, 1), None)]
    if t:
        pieces.append((k_own[:t * Q_TILE], v_own[:t * Q_TILE], None))
    span = slice(t * Q_TILE, (t + 1) * Q_TILE)
    pieces.append((k_own[span], v_own[span], col <= row))
    return softmax_mix(q, pieces)


def deal_mixed(router, t, mixed, stage, out):
    dealt = jnp.dot(deal(Q_TILE), mixed, preferred_element_type=F32).astype(BF16)
    stage[t] = dealt.reshape(PEERS, Q_TILE // PEERS, COLUMNS)
    router.send(t)
    out[router.net.me, t] = stage[t, router.net.me]


def first_attention_kernel(xp_hbm, xr_hbm, out_hbm, wq_hbm, wk_hbm, wv_hbm, gain_ref, cos_ref, sin_ref, info_ref,
                           mixed_out, res_out, info_out, prompt_out, next_hbm, columns_hbm,
                           xs, raw, w, even, odd, q_s, k_s, v_s, held, mixed_stage, res_stage,
                           x_sem, w_sem, ring_send, ring_recv, near_send, near_recv, info_send, info_recv, spread_held, spread_sem, *routes):
    net = Exchange()
    spread_sems, slice_sems, routes = routes[:RING], routes[RING:RING + PAIR], routes[RING + PAIR:]
    slices = Slices(out_hbm, spread_held, *slice_sems)
    columns = ColumnGather(net, spread_held, *spread_sems)
    mixed_router = Router(net, RING, lambda t, d: mixed_stage.at[t, d], lambda t, d: mixed_out.at[d, t], routes[:PAIR])
    res_router = Router(net, 1, lambda t, d: res_stage.at[d], lambda t, d: res_out.at[d], routes[PAIR:])
    prompt = RespGather(net, held, ring_send, ring_recv, near_send, near_recv)
    me = net.me
    column = pl.multiple_of(lax.axis_index("model") * COLUMNS, COLUMNS)

    def load(t):
        src = xp_hbm if isinstance(t, int) and t == 0 else xr_hbm.at[pl.ds(pl.multiple_of((t - 1) * TILE, TILE), TILE)]
        return pltpu.make_async_copy(src, xs.at[t], x_sem.at[t])

    load(0).start()
    weights, next_weights = ([pltpu.make_async_copy(src.at[layer], raw.at[i], w_sem.at[i]) for i, src in enumerate((wq_hbm, wk_hbm, wv_hbm))] for layer in BOTH)
    for copy in weights:
        copy.start()
    for t in range(1, 9):
        load(t).start()
    net.enter(slices.others)

    def project(t, hidden):
        span = pl.ds(pl.multiple_of(t * TILE, TILE), TILE)
        qkv = jnp.dot(hidden[...], w[...], preferred_element_type=F32)
        cos, sin = cos_ref[span], sin_ref[span]
        return span, rope(qkv[:, :COLUMNS], cos, sin).astype(BF16), rope(qkv[:, COLUMNS:512], cos, sin).astype(BF16), qkv[:, 512:].astype(BF16)

    load(0).wait()
    norm_tile(xs.at[0], even, gain_ref)
    for copy in weights:
        copy.wait()
    split_heads(raw, w)
    net.all_here(slices.others)
    slices.start()
    net.scatter(lambda d: info_ref.at[d], info_out.at[me], info_send, info_recv)
    info_out[me] = info_ref[me]
    for copy in next_weights:
        copy.start()
    load(1).wait()
    span, q, k, v = project(0, even)
    norm_tile(xs.at[1], odd, gain_ref)
    q_s[span] = q
    held[me, 0] = k
    held[me, 1] = v
    prompt.start()
    prompt.start_rest()
    for t in range(PAIR, 9):
        load(t).wait()
    spread = deal(TILE)

    @pl.loop(1, 9)
    def _(t):
        dealt = jnp.dot(spread, xs[t, :, pl.ds(column, COLUMNS)], preferred_element_type=F32).astype(BF16)
        res_stage[:, t - 1] = dealt.reshape(PEERS, TILE // PEERS, COLUMNS)

    res_out[me] = res_stage[me]

    def response_tile(t, here, there):
        span, q, k, v = project(t, here)
        norm_tile(xs.at[jnp.minimum(t + 1, 8)], there, gain_ref)
        q_s[span] = q
        own = pl.ds(pl.multiple_of((t - 1) * TILE, TILE), TILE)
        k_s[own] = k
        v_s[own] = v

    @pl.loop(0, RING)
    def _(i):
        response_tile(PAIR * i + 1, odd, even)
        response_tile(PAIR * i + PAIR, even, odd)

        @pl.when(i == 0)
        def _():
            prompt.relay()
            res_router.send(0)

        @pl.when(i == 1)
        def _():
            slices.collect()
            columns.start()

        pl.when(i == PAIR)(prompt.share)

    prompt.collect()
    for t in range(RING):
        mixed = attend_response(t, q_s[pl.ds(TILE + t * Q_TILE, Q_TILE)], held, k_s, v_s)
        deal_mixed(mixed_router, t, mixed, mixed_stage, mixed_out)
    columns.share()
    row = lax.broadcasted_iota(jnp.int32, (TILE, PEERS * TILE), 0) + me * TILE
    col = lax.broadcasted_iota(jnp.int32, (TILE, PEERS * TILE), 1)
    prompt_out[:, :COLUMNS] = softmax_mix(q_s[pl.ds(0, TILE)], [(prompt_rows_of(held, 0), prompt_rows_of(held, 1), col <= row)])
    prompt_out[:, COLUMNS:] = xs[0, :, pl.ds(column, COLUMNS)]
    for copy in next_weights:
        copy.wait()
    split_heads(raw, w)
    leave = pltpu.make_async_copy(w, next_hbm, w_sem.at[3])
    leave.start()
    columns.collect()
    out_copies = [pltpu.make_async_copy(spread_held.at[device, layer], columns_hbm.at[layer, :, device], spread_sem.at[layer, device])
                  for device in range(PEERS) for layer in BOTH]
    for copy in out_copies:
        copy.start()
    for router in (mixed_router, res_router):
        for t in range(router.tiles):
            router.collect(t)
        router.finish()
    net.collected(lambda d: info_out.at[d], info_recv)
    net.sent(lambda d: info_ref.at[d], info_send, info_recv)
    prompt.finish()
    columns.finish()
    slices.finish()
    leave.wait()
    for copy in out_copies:
        copy.wait()


def first_attention(x_prompt, x_resp, w_out, w_query, w_key, w_value, gain, cos, sin, info, collective_id):
    rows = TILE + x_resp.shape[0]
    width = x_resp.shape[1]
    return pl.pallas_call(
        first_attention_kernel,
        out_shape=(jax.ShapeDtypeStruct((PEERS, RING, 32, COLUMNS), BF16), jax.ShapeDtypeStruct((PEERS, 8, 16, COLUMNS), BF16),
                   jax.ShapeDtypeStruct((PEERS, 8, 128), jnp.int32), jax.ShapeDtypeStruct((TILE, PAIR * COLUMNS), BF16), jax.ShapeDtypeStruct((width, 3 * COLUMNS), BF16),
                   jax.ShapeDtypeStruct((PAIR, SHARDS, PEERS, 32, COLUMNS), BF16)),
        in_specs=[ANY] * 6 + [VMEM] * 4,
        out_specs=(VMEM,) * 4 + (ANY, ANY),
        scratch_shapes=[
            pltpu.VMEM((9, TILE, width), BF16), pltpu.VMEM((3, PAIR * width, LANES), BF16), pltpu.VMEM((width, 3 * COLUMNS), BF16), pltpu.VMEM((TILE, width), BF16), pltpu.VMEM((TILE, width), BF16),
            pltpu.VMEM((rows, COLUMNS), BF16), pltpu.VMEM((rows - TILE, COLUMNS), BF16), pltpu.VMEM((rows - TILE, COLUMNS), BF16),
            HELD, pltpu.VMEM((RING, PEERS, 32, COLUMNS), BF16), pltpu.VMEM((PEERS, 8, 16, COLUMNS), BF16),
            DMA((9,)), DMA((RING,)), *GATHER_SEMS, DMA((PEERS,)), DMA((PEERS,)),
            pltpu.VMEM((PEERS, PAIR, SHARDS, 32, COLUMNS), BF16), DMA((PAIR, PEERS)), *GATHER_SEMS, DMA((PAIR, SHARDS)), DMA((PAIR, SHARDS)),
            *[DMA((RING, PEERS)) for _ in BOTH], *[DMA((1, PEERS)) for _ in BOTH],
        ],
        compiler_params=pltpu.CompilerParams(collective_id=collective_id, has_side_effects=True, vmem_limit_bytes=VMEM_BYTES),
        name="first_attention",
    )(x_prompt, x_resp, w_out, w_query, w_key, w_value, gain, cos, sin, info)


def second_attention_kernel(qkv_ref, back_ref, mixed_out, stage, qkv_in, k_s, v_s, held, mixed_stage,
                            ring_send, ring_recv, near_send, near_recv, *routes):
    net = Exchange()
    me = net.me
    prompt = RespGather(net, held, ring_send, ring_recv, near_send, near_recv)
    router = Router(net, RING, lambda t, d: stage.at[t, d], lambda t, d: qkv_in.at[t, d], routes[:PAIR])
    mixed_router = Router(net, RING, lambda t, d: mixed_stage.at[t, d], lambda t, d: mixed_out.at[d, t], routes[PAIR:])
    for k in BOTH:
        held[me, k] = qkv_ref[pl.ds(0, TILE), pl.ds((k + 1) * COLUMNS, COLUMNS)]
    net.enter()
    count = back_ref.shape[1]

    def send_rows(t):
        place = lax.broadcasted_iota(jnp.int32, (Q_TILE, count), 0) + t * Q_TILE == back_ref[...]
        rows = jnp.dot(place.astype(BF16), qkv_ref[...], preferred_element_type=F32).astype(BF16)
        stage[t] = rows.reshape(PEERS, Q_TILE // PEERS, 3 * COLUMNS)
        if t == 0:
            net.all_here()
            prompt.start()
            prompt.start_rest()
        router.send(t)
        qkv_in[t, me] = stage[t, me]

    send_rows(0)
    prompt.relay()
    for t in range(1, RING):
        send_rows(t)
    prompt.share()
    prompt.collect()
    for t in range(RING):
        router.collect(t)
        rows = jnp.dot(undeal(Q_TILE), qkv_in[t].reshape(Q_TILE, 3 * COLUMNS), preferred_element_type=F32).astype(BF16)
        k_s[pl.ds(t * Q_TILE, Q_TILE)] = rows[:, COLUMNS:PAIR * COLUMNS]
        v_s[pl.ds(t * Q_TILE, Q_TILE)] = rows[:, PAIR * COLUMNS:]
        mixed = attend_response(t, rows[:, :COLUMNS], held, k_s, v_s)
        deal_mixed(mixed_router, t, mixed, mixed_stage, mixed_out)
    for t in range(RING):
        mixed_router.collect(t)
    for each in (router, mixed_router):
        each.finish()
    prompt.finish()


def second_attention(qkv, back, collective_id):
    rows = RING * Q_TILE
    wide = (32, 3 * COLUMNS)
    return pl.pallas_call(
        second_attention_kernel,
        out_shape=jax.ShapeDtypeStruct((PEERS, RING, 32, COLUMNS), BF16),
        in_specs=[VMEM, VMEM],
        out_specs=VMEM,
        scratch_shapes=[
            pltpu.VMEM((RING, PEERS) + wide, BF16), pltpu.VMEM((RING, PEERS) + wide, BF16),
            pltpu.VMEM((rows, COLUMNS), BF16), pltpu.VMEM((rows, COLUMNS), BF16),
            HELD, pltpu.VMEM((RING, PEERS, 32, COLUMNS), BF16), *GATHER_SEMS,
            *[DMA((RING, PEERS)) for _ in range(RING)],
        ],
        compiler_params=pltpu.CompilerParams(collective_id=collective_id, has_side_effects=True, vmem_limit_bytes=VMEM_BYTES),
        name=f"second_attention{collective_id}",
    )(qkv, back)


class Answer:
    def __init__(self, every, out_ref, stat_send, stat_recv, row_send, row_recv):
        self.every, self.out = every, out_ref
        self.stat_sems, self.row_sems = (stat_send, stat_recv), (row_send, row_recv)
        self.me, self.home = lax.axis_index("model"), lax.axis_index("resp")
        self.models = [(self.me + k) % SHARDS for k in range(1, SHARDS)]
        self.homes = [(self.home + k) % PEERS for k in range(1, PEERS)]

    def barrier(self):
        sem = pltpu.get_barrier_semaphore()
        for axis, devices in (("model", self.models), ("resp", self.homes)):
            for device in devices:
                pl.semaphore_signal(sem, device_id={axis: device}, device_id_type=MESH)
        pl.semaphore_wait(sem, len(self.models) + len(self.homes))

    def stat_copy(self, owner, device, place):
        ref = self.every.at[owner]
        return pltpu.make_async_remote_copy(
            src_ref=ref, dst_ref=ref, send_sem=self.stat_sems[0].at[device], recv_sem=self.stat_sems[1].at[place],
            device_id={"model": device}, device_id_type=MESH)

    def row_copy(self, owner, device, place):
        ref = self.out.at[owner]
        return pltpu.make_async_remote_copy(
            src_ref=ref, dst_ref=ref, send_sem=self.row_sems[0].at[device], recv_sem=self.row_sems[1].at[place],
            device_id={"resp": device}, device_id_type=MESH)

def combine_kernel(stats_ref, out_ref, every, *sems):
    net = Answer(every, out_ref, *sems)
    every[net.me] = stats_ref[...]
    net.barrier()
    for device in net.models:
        net.stat_copy(net.me, device, net.me).start()
    for device in net.models:
        net.stat_copy(device, device, device).wait_recv()
    shards = range(SHARDS)
    top = functools.reduce(jnp.maximum, [every[k, 0] for k in shards])
    total = functools.reduce(jnp.add, [every[k, 1] * jnp.exp(every[k, 0] - top) for k in shards])
    out_ref[net.home] = functools.reduce(jnp.add, [every[k, PAIR] for k in shards]) - top - jnp.log(total)
    for device in net.homes:
        net.row_copy(net.home, device, net.home).start()
    for device in net.homes:
        net.row_copy(device, device, device).wait_recv()
    for device in net.models:
        net.stat_copy(net.me, device, device).wait_send()
    for device in net.homes:
        net.row_copy(net.home, device, device).wait_send()


def combine(stats, collective_id):
    return pl.pallas_call(
        combine_kernel,
        out_shape=jax.ShapeDtypeStruct((PEERS, PEERS, LANES), F32),
        in_specs=[VMEM],
        out_specs=VMEM,
        scratch_shapes=[pltpu.VMEM((SHARDS,) + stats.shape, F32), *[DMA((SHARDS,)) for _ in BOTH], *[DMA((PEERS,)) for _ in BOTH]],
        compiler_params=pltpu.CompilerParams(collective_id=collective_id, has_side_effects=True),
        name="combine",
    )(stats)


ROPE_BASE = 10000.0
VARIANTS = (640, 768, 1024)


def rope_tables(positions):
    half = LANES // PAIR
    lane = jnp.arange(LANES)
    frequency = ROPE_BASE ** (-(lane % half).astype(F32) / half)
    angles = positions.astype(F32)[:, None] * frequency
    return jnp.cos(angles), jnp.sin(angles) * jnp.where(lane < half, -1.0, 1.0)


def solution(mesh):
    groups = mesh.shape['resp']
    row_axes = ('prompts', 'resp')
    head_spec = P(None, None, 'model', None)
    in_specs = (P(row_axes, None), P(row_axes, None, None), P(row_axes, None), P(row_axes), P(None, None), head_spec, head_spec, head_spec, P(None, 'model', None, None), P(None, None), P(None, None, 'model'), P(None, None, 'model'), P(None, 'model', None), P(None), P(None, 'model'))

    def device_step(x_prompt, x_resp, targets, resp_lens, attn_gain, w_query, w_key, w_value, w_out, mlp_gain, w_gate, w_up, w_down, final_gain, w_vocab):
        prompt_rows = x_prompt.shape[0]
        resp_len, width = x_resp.shape[1:]
        prompt_len = prompt_rows * groups
        me = lax.axis_index('model')
        home = lax.axis_index('resp')
        per = resp_len // groups
        gate_t, up_t = jnp.swapaxes(w_gate, 1, 2), jnp.swapaxes(w_up, 1, 2)
        out_flat = w_out.reshape(w_out.shape[0], COLUMNS, width)
        projections = [w.reshape(w.shape[0], PAIR * width, LANES) for w in (w_query, w_key, w_value)]
        prompt_pos = home * prompt_rows + jnp.arange(prompt_rows)

        cos, sin = rope_tables(jnp.concatenate([prompt_pos, prompt_len + jnp.arange(resp_len)]))
        info = jnp.concatenate([
            targets.reshape(per, groups).T[:, None, :],
            jnp.broadcast_to(resp_lens, (groups, groups - 1, per))], axis=1)
        mixed, res, infos, prompt, w_second, out_columns = first_attention(x_prompt, x_resp[0], out_flat, *projections, attn_gain, cos, sin, info, 0)
        lens = infos[:, 1, 0]
        need = (lens + groups - 1) // groups
        ends = jnp.sum(jnp.where(jnp.arange(groups)[:, None] >= jnp.arange(groups), need, 0), axis=1)
        starts = ends - need
        dealt = groups * per

        def finish_with(size, ident):
            def run(operands):
                mixed, res, prompt = operands
                slot = jnp.arange(prompt_rows + size) - prompt_rows
                which = jnp.sum((slot[:, None] >= ends).astype(jnp.int32), axis=1)
                row = slot - jnp.sum(jnp.where(which[:, None] == jnp.arange(groups), starts, 0), axis=1)
                real = (slot >= 0) & (slot < ends[-1])
                source = jnp.where(real, which * per + row, -1)
                chosen = source[:, None] == jnp.arange(dealt)
                wanted = jnp.sum(jnp.where(chosen, infos[:, 0, :].reshape(dealt), 0), axis=1) - me * w_vocab.shape[1]
                ids = jnp.where(jnp.arange(LANES) == 0, source[:, None], wanted[:, None])
                tables = rope_tables(jnp.where(slot < 0, home * prompt_rows + slot + prompt_rows, prompt_len + groups * row + home))
                weights = (out_columns.reshape(PAIR, width, COLUMNS), gate_t, up_t, w_down)
                qkv, new_res = mega(
                    mlp_gain, attn_gain, ids, mixed.reshape(dealt, COLUMNS), res.reshape(dealt, COLUMNS),
                    [*tables, prompt], *weights, w_second, 0, ident)
                part = per // RING
                back = jnp.where(real, (row // part) * (groups * part) + which * part + row % part, -1)
                mixed = second_attention(qkv, back[None], ident + 1)
                return mega(mlp_gain, final_gain[None], ids, mixed.reshape(dealt, COLUMNS), new_res, [], *weights, w_vocab, 1, ident + PAIR)
            return run

        smallest = sorted(VARIANTS)
        fit = sum((ends[-1] > size).astype(jnp.int32) for size in smallest[:-1])
        index = sum(jnp.where(fit == smallest.index(size), i, 0) for i, size in enumerate(VARIANTS))
        stats = lax.switch(index, [finish_with(size, 3 + 3 * i) for i, size in enumerate(VARIANTS)], (mixed, res, prompt))
        found = combine(stats, 1).reshape(groups, dealt)
        start = jnp.sum(jnp.where(jnp.arange(groups) == home, starts, 0))
        mine = lax.dynamic_slice(jnp.pad(found, ((0, 0), (0, per))), (0, start), (groups, per))
        log_probs = mine.T.reshape(resp_len)
        log_probs = jnp.where(jnp.arange(resp_len) < resp_lens[0], log_probs, 0.0)
        return log_probs[None, :]

    return jax.shard_map(device_step, mesh=mesh, in_specs=in_specs, out_specs=P(row_axes, None), check_vma=False)
```

```python
import functools

import jax
import jax.numpy as jnp
from jax import lax
from jax.experimental import pallas as pl
from jax.experimental.pallas import tpu as pltpu
from jax.sharding import PartitionSpec as P

MESH = pl.DeviceIdType.MESH
F32 = jnp.float32
BF16 = jnp.bfloat16
EPS = 1e-6
LANES = 128
PAIR = 2
RING = 4
COLUMNS = PAIR * LANES
SHARDS = RING * RING
PEERS = 8
BOTH = range(PAIR)
VMEM_BYTES = 67_000_000
LATE_ROWS = 640
LOGITS = 512
CHUNKS = 4
VMEM = pl.BlockSpec(memory_space=pltpu.VMEM)
ANY = pl.BlockSpec(memory_space=pl.ANY)
DMA = pltpu.SemaphoreType.DMA
KINDS = range(RING * 3)
SUM_FAR, SUM_NEAR, SUM_RELAY, SUM2_FAR, SUM2_NEAR, SUM2_RELAY, TAKE_OWN, TAKE_REST, TAKE_RELAY, TAKE2_OWN, TAKE2_REST, TAKE2_RELAY = KINDS


def block_of(color, first, second):
    return RING * first + second if color else RING * second + first


def pair(index):
    return pl.ds(PAIR * index, PAIR)


class Torus:
    def __init__(self, refs, send_sem, recv_sem):
        self.refs = refs
        self.far, self.near, self.relayed, self.sums, self.relayed2, self.sums2, self.rows = refs
        self.send_sem, self.recv_sem = send_sem, recv_sem
        me = lax.axis_index("model")
        z, y = me // RING, me % RING
        self.place = ((y, z), (z, y))
        along_y = [z * RING + self.step(y, way) for way in (1, -1)]
        along_z = [self.step(z, way) * RING + y for way in (1, -1)]
        self.neighbors = ((along_y, along_z), (along_z, along_y))

    def step(self, place, by):
        return (place + by + RING) % RING

    def enter(self):
        sem = pltpu.get_barrier_semaphore()
        for ring in self.neighbors[0]:
            for device in ring:
                pl.semaphore_signal(sem, device_id={"model": device}, device_id_type=MESH)

    def all_here(self):
        pl.semaphore_wait(pltpu.get_barrier_semaphore(), RING)

    def ends(self, kind, c, q, d):
        (p, s), way, other = self.place[q], 1 - PAIR * d, 1 - d
        far, near, relayed, sums, relayed2, sums2, rows = (ref.at[c, q] for ref in self.refs)
        own = sums.at[0]
        back_s, back_p = self.step(s, -way), self.step(p, -way)
        return {
            SUM_FAR: lambda: (far.at[pair(d)], relayed.at[d], relayed.at[d]),
            SUM_NEAR: lambda: (near.at[d], sums.at[d, pair(other)], sums.at[d, pair(other)]),
            SUM_RELAY: lambda: (relayed.at[d], sums.at[d, pair(d)], sums.at[d, pair(d)]),
            SUM2_FAR: lambda: (own.at[self.step(s, PAIR), d], relayed2.at[d], relayed2.at[d]),
            SUM2_NEAR: lambda: (own.at[self.step(s, way), other], sums2.at[d, other], sums2.at[d, other]),
            SUM2_RELAY: lambda: (relayed2.at[d], sums2.at[d, d], sums2.at[d, d]),
            TAKE_OWN: lambda: (rows.at[p, s, d], rows.at[p, s, d], rows.at[p, back_s, d]),
            TAKE_REST: lambda: (rows.at[p, s, other], rows.at[p, s, other], rows.at[p, back_s, other]),
            TAKE_RELAY: lambda: (rows.at[p, back_s, d], rows.at[p, back_s, d], rows.at[p, self.step(s, PAIR), d]),
            TAKE2_OWN: lambda: (rows.at[p, pair(d)], rows.at[p, pair(d)], rows.at[back_p, pair(d)]),
            TAKE2_REST: lambda: (rows.at[p, pair(other)], rows.at[p, pair(other)], rows.at[back_p, pair(other)]),
            TAKE2_RELAY: lambda: (rows.at[back_p, pair(d)], rows.at[back_p, pair(d)], rows.at[self.step(p, PAIR), pair(d)]),
        }[kind]()

    def copy(self, kind, c, q, d, src, dst):
        second_ring = kind in (SUM2_FAR, SUM2_NEAR, SUM2_RELAY, TAKE_OWN, TAKE_REST, TAKE_RELAY)
        return pltpu.make_async_remote_copy(
            src_ref=src, dst_ref=dst, send_sem=self.send_sem.at[c, q, d, kind], recv_sem=self.recv_sem.at[c, q, d, kind],
            device_id={"model": self.neighbors[q][second_ring][d]}, device_id_type=MESH)

    def send(self, c, q, d, kind):
        src, dst, _ = self.ends(kind, c, q, d)
        self.copy(kind, c, q, d, src, dst).start()

    def sent(self, c, q, *kinds):
        for kind in kinds:
            for d in BOTH:
                src, dst, _ = self.ends(kind, c, q, d)
                self.copy(kind, c, q, d, src, dst).wait_send()

    def arrived(self, c, q, d, *kinds):
        for kind in kinds:
            _, _, here = self.ends(kind, c, q, d)
            self.copy(kind, c, q, d, here, here).wait_recv()


def halves_of(ref):
    return ref[:, :COLUMNS], ref[:, COLUMNS:]


def halves(value):
    return value[:, :LANES], value[:, LANES:]


def store_block(ref, value):
    for half, part in enumerate(halves(value)):
        ref[half] = part


def add_block(ref, value):
    for half, part in enumerate(halves(value)):
        ref[half] += part


class Gather:
    def __init__(self, net):
        self.net = net

    def begin_rows(self, c, q):
        for kind in (TAKE_OWN, TAKE_REST):
            for d in BOTH:
                self.net.send(c, q, d, kind)

    def relay_rows(self, c, q):
        for d in BOTH:
            self.net.arrived(c, q, d, TAKE_OWN)
            self.net.send(c, q, d, TAKE_RELAY)

    def take_second(self, c, q):
        for d in BOTH:
            self.net.arrived(c, q, d, TAKE_REST, TAKE_RELAY)
        for kind in (TAKE2_OWN, TAKE2_REST):
            for d in BOTH:
                self.net.send(c, q, d, kind)

    def relay_last(self, c, q):
        for d in BOTH:
            self.net.arrived(c, q, d, TAKE2_OWN)
            self.net.send(c, q, d, TAKE2_RELAY)

    def complete(self, c, q):
        for d in BOTH:
            self.net.arrived(c, q, d, TAKE2_REST, TAKE2_RELAY)
        self.net.sent(c, q, TAKE_OWN, TAKE_REST, TAKE_RELAY, TAKE2_OWN, TAKE2_REST, TAKE2_RELAY)

    def middle(self):
        return [self.relay_rows, self.take_second, self.relay_last]


class Sum(Gather):
    def __init__(self, net, lhs_of, w_ref, finish):
        self.net, self.lhs_of, self.w_ref, self.finish = net, lhs_of, w_ref, finish

    def product(self, lhs, color, first, second):
        start = pl.multiple_of(block_of(color, first, second) * COLUMNS, COLUMNS)
        return jnp.dot(lhs, self.w_ref[:, pl.ds(start, COLUMNS)], preferred_element_type=F32)

    def begin(self, c, q):
        net, p, lhs = self.net, self.net.place[q][0], self.lhs_of(c, q)
        for k in range(RING):
            store_block(net.far.at[c, q, k], self.product(lhs, q, net.step(p, PAIR), k))
        for d in BOTH:
            net.send(c, q, d, SUM_FAR)
        for d in BOTH:
            for k in BOTH:
                store_block(net.near.at[c, q, d, k], self.product(lhs, q, net.step(p, 1 - PAIR * d), PAIR * (1 - d) + k))
            net.send(c, q, d, SUM_NEAR)

    def relay_sum(self, c, q):
        net, p, lhs = self.net, self.net.place[q][0], self.lhs_of(c, q)
        for d in BOTH:
            net.arrived(c, q, d, SUM_FAR)
            for k in BOTH:
                add_block(net.relayed.at[c, q, d, k], self.product(lhs, q, net.step(p, 1 - PAIR * d), PAIR * d + k))
            net.send(c, q, d, SUM_RELAY)

    def begin_second(self, c, q):
        net, lhs = self.net, self.lhs_of(c, q)
        for d in BOTH:
            net.arrived(c, q, d, SUM_NEAR, SUM_RELAY)
        for k in range(RING):
            for half, part in enumerate(halves(self.product(lhs, q, net.place[q][0], k))):
                net.sums[c, q, 0, k, half] += net.sums[c, q, 1, k, half] + part
        for kind in (SUM2_FAR, SUM2_NEAR):
            for d in BOTH:
                net.send(c, q, d, kind)
        net.sent(c, q, SUM_FAR)

    def relay_second(self, c, q):
        net = self.net
        for d in BOTH:
            net.arrived(c, q, d, SUM2_FAR)
            net.relayed2[c, q, d] += net.sums[c, q, 0, net.step(net.place[q][1], 1 - PAIR * d), d]
            net.send(c, q, d, SUM2_RELAY)

    def finish_sum(self, c, q):
        net = self.net
        net.sent(c, q, SUM_NEAR, SUM_RELAY)
        for d in BOTH:
            net.arrived(c, q, d, SUM2_NEAR, SUM2_RELAY)
        for half in BOTH:
            self.finish(c, q, half, net.sums[c, q, 0, net.place[q][1], half] + net.sums2[c, q, 0, half] + net.sums2[c, q, 1, half])
        self.begin_rows(c, q)

    def relay_rows(self, c, q):
        self.net.sent(c, q, SUM2_FAR, SUM2_NEAR, SUM2_RELAY)
        super().relay_rows(c, q)

    def middle(self):
        return [self.relay_sum, self.begin_second, self.relay_second, self.finish_sum, *super().middle()]


def normed(net, c, q, gain_ref, layer):
    rows = net.rows.shape[-PAIR]
    tile = PAIR * 8 if rows % (PAIR * 8) == 0 else 8
    spots = [(first, second, half) for first in range(RING) for second in range(RING) for half in BOTH]

    @pl.loop(0, rows // tile)
    def _(i):
        span = pl.ds(pl.multiple_of(i * tile, tile), tile)
        acts = [net.rows[(c, q) + spot + (span,)].astype(F32) for spot in spots]
        squares = functools.reduce(jnp.add, [v * v for v in acts])
        inv = lax.rsqrt(jnp.sum(squares, axis=-1, keepdims=True) / (LANES * len(acts)) + EPS)
        for spot, v in zip(spots, acts):
            column = block_of(q, *spot[:PAIR]) * COLUMNS + spot[PAIR] * LANES
            net.rows[(c, q) + spot + (span,)] = (v * inv * gain_ref[pl.ds(layer, 1), pl.ds(column, LANES)]).astype(BF16)


def rows_of(net, c, q):
    parts = []
    for upper in range(RING):
        for lower in range(RING):
            first, second = (upper, lower) if q else (lower, upper)
            parts += [net.rows[c, q, first, second, half] for half in BOTH]
    return jnp.concatenate(parts, axis=1)


def times_transposed(lhs, rhs):
    return lax.dot_general(lhs, rhs, (((1,), (1,)), ((), ())), preferred_element_type=F32)


def late_plan(width, count):
    plan, start = [], 0
    for buffer in BOTH:
        for slot in range(width // count):
            size = min(LATE_ROWS, width - start)
            if size:
                plan.append((buffer, slot * count, start, size))
            start += size
    return plan, width - start


def rope(value, cos, sin):
    return jnp.concatenate([v * cos + pltpu.roll(v, LANES // PAIR, 1) * sin for v in halves(value)], axis=1)


def put_projected(product, cos_ref, sin_ref, out_ref, span):
    for k in range(3):
        value = product(k * COLUMNS, COLUMNS)
        if k < PAIR:
            value = rope(value, cos_ref[span], sin_ref[span])
        out_ref[span, pl.ds(k * COLUMNS, COLUMNS)] = value.astype(BF16)


def statistics(product, count, target):
    top = total = picked = None
    for k in range(count // LOGITS):
        logits = product(k * LOGITS, LOGITS)
        here = jnp.max(logits, axis=-1, keepdims=True)
        ids = lax.broadcasted_iota(jnp.int32, logits.shape, 1) + k * LOGITS
        found = jnp.sum(jnp.where(ids == target, logits, 0.0), axis=-1, keepdims=True)
        if k:
            both = jnp.maximum(top, here)
            total = total * jnp.exp(top - both) + jnp.sum(jnp.exp(logits - both), axis=-1, keepdims=True)
            top, picked = both, picked + found
        else:
            top, total, picked = here, jnp.sum(jnp.exp(logits - here), axis=-1, keepdims=True), found
    lane = lax.broadcasted_iota(jnp.int32, (target.shape[0], LANES), 1)
    return jnp.where(lane == 0, top, jnp.where(lane == 1, total, picked))


def mega_kernel(chunks, layer, last, gain_ref, next_gain_ref, ids_ref, dealt_ref, old_ref, *args):
    if last:
        side_refs, args = (), args
    else:
        side_refs, args = args[:3], args[3:]
    w_out_hbm, w_gate_hbm, w_up_hbm, w_down_hbm, *args = args
    late_hbm, out_ref, *args = args
    if not last:
        new_res_ref, *args = args
    (w_out, w_gate, w_up, w_down, late_rest, res, inner, middle, stats,
     far, near, relayed, sums, relayed2, sums2, rows, w_sem, late_sem, send_sem, recv_sem, ready_sem) = args
    loads = [pltpu.make_async_copy(src.at[layer], dst, w_sem.at[i]) for i, (src, dst) in enumerate(
        ((w_out_hbm, w_out), (w_gate_hbm, w_gate), (w_up_hbm, w_up), (w_down_hbm, w_down)))]
    for load in loads:
        load.start()
    width, count = late_hbm.shape
    plan, left = late_plan(width, count)
    late = [(late_hbm.at[pl.ds(start, size)], (w_gate, w_up)[buffer].at[pl.ds(0, size), pl.ds(lane, count)]) for buffer, lane, start, size in plan]
    if left:
        late.append((late_hbm.at[pl.ds(width - left, left)], late_rest))
    late_loads = [pltpu.make_async_copy(src, dst, late_sem.at[i]) for i, (src, dst) in enumerate(late)]
    net = Torus((far, near, relayed, sums, relayed2, sums2, rows), send_sem, recv_sem)
    net.enter()
    net.all_here()

    part = rows.shape[-PAIR]

    def span_of(c, q=0, parts=1):
        return pl.ds(pl.multiple_of((PAIR * c + q) * part, 16), parts * part)

    def after_prompt(c, q=0, parts=1):
        return pl.ds(pl.multiple_of((PAIR * c + q) * part + LANES * last, 16), parts * part)

    def picked(c, ref, prompt):
        ids = ids_ref[after_prompt(c, parts=PAIR), :1]
        chosen = (ids == lax.broadcasted_iota(jnp.int32, (PAIR * part, PEERS * LANES), 1)).astype(BF16)
        value = jnp.dot(chosen, ref[...], preferred_element_type=F32)
        if prompt is not None:
            row = lax.broadcasted_iota(jnp.int32, (PAIR * part, LANES), 0) + PAIR * part * c
            chosen = (row == lax.broadcasted_iota(jnp.int32, (PAIR * part, LANES), 1)).astype(BF16)
            value += jnp.dot(chosen, prompt, preferred_element_type=F32)
        return value.astype(BF16)

    def put(ref, value, place_of):
        for q in BOTH:
            for half, columns in enumerate(halves(value)):
                ref[place_of(q) + (half,)] = columns[q * part:(q + 1) * part]

    def begin(c):
        prompts = (None, None) if last else halves_of(side_refs[PAIR])
        put(rows, picked(c, dealt_ref, prompts[0]), lambda q: (c, q) + net.place[q])
        if not last:
            put(res, picked(c, old_ref, prompts[1]), lambda q: (c, q))
        for q in BOTH:
            first.begin_rows(c, q)

    def finish(c, q, half, total):
        value = (middle[c, q, half].astype(F32) + total).astype(BF16)
        if not last:
            new_res_ref[span_of(c, q), pl.ds(half * LANES, LANES)] = value
        rows[(c, q) + net.place[q] + (half,)] = value

    first = Gather(net)
    second = Sum(net, lambda c, q: inner[c, q], w_down, finish)

    def project_out(c):
        for q in BOTH:
            first.complete(c, q)
        total = jnp.dot(jnp.concatenate([rows_of(net, c, q) for q in BOTH], axis=0), w_out[...], preferred_element_type=F32)
        for q in BOTH:
            for half, columns in enumerate(halves(total)):
                old = old_ref[after_prompt(c, q), pl.ds(half * LANES, LANES)] if last else res[c, q, half]
                value = (old.astype(F32) + columns[q * part:(q + 1) * part]).astype(BF16)
                middle[c, q, half] = value
                rows[(c, q) + net.place[q] + (half,)] = value
        for ring in net.neighbors[0]:
            for device in ring:
                pl.semaphore_signal(ready_sem.at[c], device_id={"model": device}, device_id_type=MESH)

    def begin_again(c):
        pl.semaphore_wait(ready_sem.at[c], RING)
        for q in BOTH:
            first.begin_rows(c, q)

    def hidden_of(c, stage, gain, row):
        for q in BOTH:
            stage.complete(c, q)
            normed(net, c, q, gain, row)
        return jnp.concatenate([rows_of(net, c, q) for q in BOTH], axis=0)

    def mlp(c):
        hidden = hidden_of(c, first, gain_ref, layer)
        value = (jax.nn.silu(times_transposed(hidden, w_gate[...])) * times_transposed(hidden, w_up[...])).astype(BF16)
        inner[c] = value.reshape(inner.shape[1:])
        for q in BOTH:
            second.begin(c, q)

    def after(c):
        hidden = hidden_of(c, second, next_gain_ref, 0 if last else layer + 1)

        def product(lane, size):
            parts = [jnp.dot(hidden[:, start:start + rows_here], (w_gate, w_up)[buffer][pl.ds(0, rows_here), pl.ds(at + lane, size)], preferred_element_type=F32)
                     for buffer, at, start, rows_here in plan]
            if left:
                parts.append(jnp.dot(hidden[:, width - left:], late_rest[:, pl.ds(lane, size)], preferred_element_type=F32))
            return functools.reduce(jnp.add, parts)

        if last:
            stats[span_of(c, parts=PAIR)] = statistics(product, count, ids_ref[after_prompt(c, parts=PAIR), 1:PAIR])
        else:
            put_projected(product, *side_refs[:PAIR], out_ref, span_of(c, parts=PAIR))

    def on_both(step):
        def run(c):
            for q in BOTH:
                step(c, q)
        return run

    gather = [on_both(step) for step in first.middle()]
    steps = [begin, *gather, project_out, begin_again, *gather, mlp, *map(on_both, second.middle())]
    at_mlp = steps.index(mlp)
    steps += [None] * max(0, at_mlp + chunks - len(steps)) + [after]

    @pl.loop(0, len(steps) + chunks - 1)
    def _(slot):
        @pl.when(slot == steps.index(project_out))
        def _():
            for load in loads:
                load.wait()

        @pl.when(slot == len(steps) - 1)
        def _():
            for load in late_loads:
                load.wait()

        for k, step in reversed(list(enumerate(steps))):
            if step is None:
                continue

            @pl.when(slot >= k)
            def _():
                @pl.when(slot < k + chunks)
                def _():
                    step(slot - k)

        @pl.when(slot == at_mlp + chunks - 1)
        def _():
            for load in late_loads:
                load.start()

    if last:
        out_ref[...] = jnp.zeros_like(out_ref)
        for k in range(stats.shape[0] // LANES):
            turned = stats[pl.ds(k * LANES, LANES)].T
            for i in range(3):
                out_ref[i, pl.ds(k, 1)] = turned[i:i + 1]


def mega(gain, next_gain, ids, dealt, old, sides, w_out, w_gate_t, w_up_t, w_down, late, layer, collective_id):
    last = not sides
    chunks = CHUNKS
    total = ids.shape[0] - LANES * last
    _, hidden, width = w_gate_t.shape
    rows = total // (PAIR * chunks)
    per = (chunks, PAIR)
    tile = (rows, LANES)
    count = late.shape[1]
    _, left = late_plan(width, count)

    sem = DMA(per + (PAIR, len(KINDS)))
    out = jax.ShapeDtypeStruct((3, PEERS, LANES), F32) if last else (
        jax.ShapeDtypeStruct((total, count), BF16), jax.ShapeDtypeStruct((total, COLUMNS), BF16))
    return pl.pallas_call(
        functools.partial(mega_kernel, chunks, layer, last),
        out_shape=out,
        in_specs=[VMEM] * (5 + len(sides)) + [ANY] * 5,
        out_specs=VMEM if last else (VMEM, VMEM),
        scratch_shapes=[
            pltpu.VMEM((width, COLUMNS), BF16),
            *[pltpu.VMEM((hidden, width), BF16) for _ in range(3)],
            pltpu.VMEM((left or 8, count), BF16),
            pltpu.VMEM(per + (PAIR,) + (tile if not last else (8, LANES)), BF16),
            pltpu.VMEM(per + (rows, hidden), BF16),
            pltpu.VMEM(per + (PAIR,) + tile, BF16),
            pltpu.VMEM((total if last else 8, LANES), F32),
            pltpu.VMEM(per + (RING, PAIR) + tile, F32),
            pltpu.VMEM(per + (PAIR, PAIR, PAIR) + tile, F32),
            pltpu.VMEM(per + (PAIR, PAIR, PAIR) + tile, F32),
            pltpu.VMEM(per + (PAIR, RING, PAIR) + tile, F32),
            pltpu.VMEM(per + (PAIR,) + tile, F32),
            pltpu.VMEM(per + (PAIR, PAIR) + tile, F32),
            pltpu.VMEM(per + (RING, RING, PAIR) + tile, BF16),
            DMA((RING,)), DMA((SHARDS,)), sem, sem, pltpu.SemaphoreType.REGULAR((chunks,)),
        ],
        compiler_params=pltpu.CompilerParams(collective_id=collective_id, has_side_effects=True, vmem_limit_bytes=VMEM_BYTES),
        name=f"mega{collective_id}",
    )(gain, next_gain, ids, dealt, old, *sides, w_out, w_gate_t, w_up_t, w_down, late)


TILE = 128
Q_TILE = 256
LOG2E = 1.4426950408889634
HELD = pltpu.VMEM((PEERS, PAIR, TILE, COLUMNS), BF16)
GATHER_SEMS = [DMA((PAIR, 3)), DMA((PAIR, 3)), DMA((RING,)), DMA((RING,))]


class Exchange:
    def __init__(self):
        self.me = lax.axis_index("resp")
        self.others = [(self.me + k) % PEERS for k in range(1, PEERS)]

    def enter(self, models=()):
        sem = pltpu.get_barrier_semaphore()
        for axis, devices in (("resp", self.others), ("model", models)):
            for device in devices:
                pl.semaphore_signal(sem, device_id={axis: device}, device_id_type=MESH)

    def all_here(self, models=()):
        pl.semaphore_wait(pltpu.get_barrier_semaphore(), len(self.others) + len(models))

    def copy(self, src, dst, send_sem, recv_sem, device):
        return pltpu.make_async_remote_copy(src_ref=src, dst_ref=dst, send_sem=send_sem, recv_sem=recv_sem,
                                            device_id={"resp": device}, device_id_type=MESH)

    def scatter(self, src_of, dst, send_sem, recv_sem):
        for device in self.others:
            self.copy(src_of(device), dst, send_sem.at[device], recv_sem.at[self.me], device).start()

    def collected(self, dst_of, recv_sem):
        for device in self.others:
            self.copy(dst_of(device), dst_of(device), recv_sem.at[device], recv_sem.at[device], device).wait_recv()

    def sent(self, src_of, send_sem, recv_sem):
        for device in self.others:
            self.copy(src_of(device), src_of(device), send_sem.at[device], recv_sem.at[device], device).wait_send()


class Router:
    def __init__(self, net, tiles, src_of, dst_of, sems):
        self.net, self.tiles, self.src_of, self.dst_of = net, tiles, src_of, dst_of
        self.send_sem, self.recv_sem = sems

    def send(self, t):
        self.net.scatter(lambda d: self.src_of(t, d), self.dst_of(t, self.net.me), self.send_sem.at[t], self.recv_sem.at[t])

    def collect(self, t):
        self.net.collected(lambda d: self.dst_of(t, d), self.recv_sem.at[t])

    def finish(self):
        for t in range(self.tiles):
            self.net.sent(lambda d: self.src_of(t, d), self.send_sem.at[t], self.recv_sem.at[t])


class Slices:
    def __init__(self, w_hbm, held, stage, stage_sem, send_sem, recv_sem):
        self.held, self.stage, self.send_sem, self.recv_sem = held, stage, send_sem, recv_sem
        self.me, home = lax.axis_index("model"), lax.axis_index("resp")
        self.homes = (home, (home + RING) % PEERS)
        self.others = [(self.me + k) % SHARDS for k in range(1, SHARDS)]

        self.loads = [pltpu.make_async_copy(w_hbm.at[:, pl.ds(pl.multiple_of(at * 32, 32), 32)], stage.at[which], stage_sem.at[which])
                      for which, at in enumerate(self.homes)]

    def part(self, which, device):
        return self.stage.at[which, :, :, pl.ds(pl.multiple_of(device * COLUMNS, COLUMNS), COLUMNS)]

    def copy(self, which, device, place):
        return pltpu.make_async_remote_copy(
            src_ref=self.part(which, device), dst_ref=self.held.at[self.homes[which], :, place], send_sem=self.send_sem.at[which, device],
            recv_sem=self.recv_sem.at[which, place], device_id={"model": device}, device_id_type=MESH)

    def load(self):
        for load in self.loads:
            load.start()

    def start(self):
        for which in BOTH:
            self.loads[which].wait()
            for device in self.others:
                self.copy(which, device, self.me).start()
        for which in BOTH:
            self.held[self.homes[which], :, self.me] = self.part(which, self.me)[...]

    def collect(self):
        for which in BOTH:
            for device in self.others:
                self.copy(which, device, device).wait_recv()

    def finish(self):
        for which in BOTH:
            for device in self.others:
                self.copy(which, device, self.me).wait_send()


class RespGather:
    def __init__(self, net, held, ring_send, ring_recv, near_send, near_recv):
        self.net, self.held = net, held
        self.ring_sems, self.near_sems = (ring_send, ring_recv), (near_send, near_recv)
        x, core = net.me // PAIR, net.me % PAIR
        self.at = lambda by, here: (x + by + RING) % RING * PAIR + (core if here else 1 - core)

    def ring_copy(self, d, kind, ref):
        return self.net.copy(ref, ref, self.ring_sems[0].at[d, kind], self.ring_sems[1].at[d, kind], self.at(1 - PAIR * d, True))

    def near_copy(self, kind, ref):
        return self.net.copy(ref, ref, self.near_sems[0].at[kind], self.near_sems[1].at[kind], self.at(0, False))

    def sources(self, here):
        return [self.at(by, here) for by in (0, -1, 1, PAIR)]

    def start(self):
        for d in BOTH:
            self.ring_copy(d, 0, self.held.at[self.net.me, d]).start()
        self.near_copy(0, self.held.at[self.net.me]).start()

    def start_rest(self):
        for d in BOTH:
            self.ring_copy(d, 1, self.held.at[self.net.me, 1 - d]).start()

    def relay(self):
        for d in BOTH:
            ref = self.held.at[self.at(PAIR * d - 1, True), d]
            self.ring_copy(d, 0, ref).wait_recv()
            self.ring_copy(d, PAIR, ref).start()

    def share(self):
        for d in BOTH:
            device = self.at(PAIR * d - 1, True)
            self.ring_copy(d, 1, self.held.at[device, 1 - d]).wait_recv()
            self.near_copy(1 + d, self.held.at[device]).start()
        far = self.held.at[self.at(PAIR, True)]
        for d in BOTH:
            self.ring_copy(d, PAIR, far.at[d]).wait_recv()
        self.near_copy(3, far).start()

    def collect(self):
        for kind, device in enumerate(self.sources(False)):
            self.near_copy(kind, self.held.at[device]).wait_recv()

    def finish(self):
        for kind in range(3):
            for d in BOTH:
                self.ring_copy(d, kind, self.held.at[self.net.me, d]).wait_send()
        for kind in range(RING):
            self.near_copy(kind, self.held.at[self.net.me]).wait_send()


class ColumnGather(RespGather):
    def start(self):
        for d in BOTH:
            self.ring_copy(d, 0, self.held.at[self.net.me]).start()
        for kind, device in ((0, self.net.me), (3, self.at(PAIR, True))):
            self.near_copy(kind, self.held.at[device]).start()

    def share(self):
        for d in BOTH:
            ref = self.held.at[self.at(PAIR * d - 1, True)]
            self.ring_copy(d, 0, ref).wait_recv()
            self.near_copy(1 + d, ref).start()

    def finish(self):
        for d in BOTH:
            self.ring_copy(d, 0, self.held.at[self.net.me]).wait_send()
        for kind in range(RING):
            self.near_copy(kind, self.held.at[self.net.me]).wait_send()


def deal(rows):
    out = lax.broadcasted_iota(jnp.int32, (rows, rows), 0)
    src = lax.broadcasted_iota(jnp.int32, (rows, rows), 1)
    per = rows // PEERS
    return jnp.where(src == (out % per) * PEERS + out // per, 1.0, 0.0).astype(BF16)


def undeal(rows):
    out = lax.broadcasted_iota(jnp.int32, (rows, rows), 0)
    src = lax.broadcasted_iota(jnp.int32, (rows, rows), 1)
    per = rows // PEERS
    return jnp.where(src == (out % PEERS) * per + out // PEERS, 1.0, 0.0).astype(BF16)


def split_heads(raw_ref, w_ref):
    tile = PAIR * LANES
    out = lax.broadcasted_iota(jnp.int32, (tile, tile), 0)
    src = lax.broadcasted_iota(jnp.int32, (tile, tile), 1)
    pick = jnp.where(src == (out % LANES) * PAIR + out // LANES, 1.0, 0.0).astype(BF16)

    @pl.loop(0, raw_ref.shape[1] // (RING * tile))
    def _(b):
        raws = [raw_ref[i, pl.ds(pl.multiple_of((b * RING + k) * tile, tile), tile)] for k in range(RING) for i in range(3)]
        heads = jnp.dot(pick, jnp.concatenate(raws, axis=1), preferred_element_type=F32).astype(BF16)
        for k in range(RING):
            here = pl.ds(pl.multiple_of((b * RING + k) * LANES, LANES), LANES)
            for i in range(3):
                for h in BOTH:
                    at = (k * 3 + i) * LANES
                    w_ref[here, pl.ds(i * COLUMNS + h * LANES, LANES)] = heads[h * LANES:(h + 1) * LANES, at:at + LANES]


def norm_tile(x_ref, out_ref, gain_ref):
    for i in range(x_ref.shape[0] // 16):
        v = x_ref[pl.ds(16 * i, 16), :].astype(F32)
        inv = lax.rsqrt(jnp.mean(v * v, axis=-1, keepdims=True) + EPS)
        out_ref[pl.ds(16 * i, 16), :] = (v * inv * gain_ref[pl.ds(0, 1), :]).astype(BF16)


def softmax_mix(q, pieces):
    factor = LOG2E * 128 ** -0.5
    outs = []
    for h in range(2):
        lanes = slice(128 * h, 128 * h + 128)
        scores = []
        for keys, _, mask in pieces:
            s = lax.dot_general(q[:, lanes], keys[:, lanes], (((1,), (1,)), ((), ())), preferred_element_type=F32)
            scores.append(s if mask is None else jnp.where(mask, s, -jnp.inf))
        top = functools.reduce(jnp.maximum, [jnp.max(s, axis=-1, keepdims=True) for s in scores])
        probs = [jnp.exp2((s - top) * factor) for s in scores]
        total = functools.reduce(jnp.add, [jnp.sum(p, axis=-1, keepdims=True) for p in probs])
        mixed = functools.reduce(jnp.add, [jnp.dot(p.astype(BF16), values[:, lanes], preferred_element_type=F32) for p, (_, values, _) in zip(probs, pieces)])
        outs.append(mixed / total)
    return jnp.concatenate(outs, axis=1).astype(BF16)


def prompt_rows_of(held, which):
    return held[:, which].reshape(PEERS * TILE, COLUMNS)


def attend_response(t, q, held, k_own, v_own):
    row = lax.broadcasted_iota(jnp.int32, (Q_TILE, Q_TILE), 0)
    col = lax.broadcasted_iota(jnp.int32, (Q_TILE, Q_TILE), 1)
    pieces = [(prompt_rows_of(held, 0), prompt_rows_of(held, 1), None)]
    if t:
        pieces.append((k_own[:t * Q_TILE], v_own[:t * Q_TILE], None))
    span = slice(t * Q_TILE, (t + 1) * Q_TILE)
    pieces.append((k_own[span], v_own[span], col <= row))
    return softmax_mix(q, pieces)


def deal_mixed(router, t, mixed, stage, out):
    dealt = jnp.dot(deal(Q_TILE), mixed, preferred_element_type=F32).astype(BF16)
    stage[t] = dealt.reshape(PEERS, Q_TILE // PEERS, COLUMNS)
    router.send(t)
    out[router.net.me, t] = stage[t, router.net.me]


def first_attention_kernel(xp_hbm, xr_hbm, out_hbm, wq_hbm, wk_hbm, wv_hbm, gain_ref, cos_ref, sin_ref, info_ref,
                           mixed_out, res_out, info_out, prompt_out, next_hbm, columns_hbm,
                           xs, raw, w, even, odd, q_s, k_s, v_s, held, mixed_stage, res_stage,
                           x_sem, w_sem, ring_send, ring_recv, near_send, near_recv, info_send, info_recv, spread_held, spread_sem, *routes):
    net = Exchange()
    spread_sems, slice_sems, routes = routes[:RING], routes[RING:PAIR * RING], routes[PAIR * RING:]
    slices = Slices(out_hbm, spread_held, *slice_sems)
    columns = ColumnGather(net, spread_held, *spread_sems)
    mixed_router = Router(net, RING, lambda t, d: mixed_stage.at[t, d], lambda t, d: mixed_out.at[d, t], routes[:PAIR])
    res_router = Router(net, 1, lambda t, d: res_stage.at[d], lambda t, d: res_out.at[d], routes[PAIR:])
    prompt = RespGather(net, held, ring_send, ring_recv, near_send, near_recv)
    me = net.me
    column = pl.multiple_of(lax.axis_index("model") * COLUMNS, COLUMNS)

    def load(t):
        src = xp_hbm if isinstance(t, int) and t == 0 else xr_hbm.at[pl.ds(pl.multiple_of((t - 1) * TILE, TILE), TILE)]
        return pltpu.make_async_copy(src, xs.at[t], x_sem.at[t])

    slices.load()
    load(0).start()
    weights, next_weights = ([pltpu.make_async_copy(src.at[layer], raw.at[i], w_sem.at[i]) for i, src in enumerate((wq_hbm, wk_hbm, wv_hbm))] for layer in BOTH)
    for copy in weights:
        copy.start()
    for t in range(1, 9):
        load(t).start()
    net.enter(slices.others)
    net.all_here(slices.others)
    slices.start()
    net.scatter(lambda d: info_ref.at[d], info_out.at[me], info_send, info_recv)
    info_out[me] = info_ref[me]

    def project(t, hidden):
        span = pl.ds(pl.multiple_of(t * TILE, TILE), TILE)
        qkv = jnp.dot(hidden[...], w[...], preferred_element_type=F32)
        cos, sin = cos_ref[span], sin_ref[span]
        return span, rope(qkv[:, :COLUMNS], cos, sin).astype(BF16), rope(qkv[:, COLUMNS:512], cos, sin).astype(BF16), qkv[:, 512:].astype(BF16)

    load(0).wait()
    norm_tile(xs.at[0], even, gain_ref)
    for copy in weights:
        copy.wait()
    split_heads(raw, w)
    for copy in next_weights:
        copy.start()
    load(1).wait()
    span, q, k, v = project(0, even)
    norm_tile(xs.at[1], odd, gain_ref)
    q_s[span] = q
    held[me, 0] = k
    held[me, 1] = v
    prompt.start()
    prompt.start_rest()
    for t in range(PAIR, 9):
        load(t).wait()
    spread = deal(TILE)

    @pl.loop(1, 9)
    def _(t):
        dealt = jnp.dot(spread, xs[t, :, pl.ds(column, COLUMNS)], preferred_element_type=F32).astype(BF16)
        res_stage[:, t - 1] = dealt.reshape(PEERS, TILE // PEERS, COLUMNS)

    res_out[me] = res_stage[me]

    def response_tile(t, here, there):
        span, q, k, v = project(t, here)
        norm_tile(xs.at[jnp.minimum(t + 1, 8)], there, gain_ref)
        q_s[span] = q
        own = pl.ds(pl.multiple_of((t - 1) * TILE, TILE), TILE)
        k_s[own] = k
        v_s[own] = v

    @pl.loop(0, RING)
    def _(i):
        response_tile(PAIR * i + 1, odd, even)
        response_tile(PAIR * i + PAIR, even, odd)

        @pl.when(i == 0)
        def _():
            prompt.relay()
            res_router.send(0)

        @pl.when(i == 1)
        def _():
            slices.collect()
            columns.start()

        pl.when(i == PAIR)(prompt.share)

    prompt.collect()
    for t in range(RING):
        mixed = attend_response(t, q_s[pl.ds(TILE + t * Q_TILE, Q_TILE)], held, k_s, v_s)
        deal_mixed(mixed_router, t, mixed, mixed_stage, mixed_out)
    columns.share()
    row = lax.broadcasted_iota(jnp.int32, (TILE, PEERS * TILE), 0) + me * TILE
    col = lax.broadcasted_iota(jnp.int32, (TILE, PEERS * TILE), 1)
    prompt_out[:, :COLUMNS] = softmax_mix(q_s[pl.ds(0, TILE)], [(prompt_rows_of(held, 0), prompt_rows_of(held, 1), col <= row)])
    prompt_out[:, COLUMNS:] = xs[0, :, pl.ds(column, COLUMNS)]
    for copy in next_weights:
        copy.wait()
    split_heads(raw, w)
    leave = pltpu.make_async_copy(w, next_hbm, w_sem.at[3])
    leave.start()
    columns.collect()
    out_copies = [pltpu.make_async_copy(spread_held.at[device, layer], columns_hbm.at[layer, :, device], spread_sem.at[layer, device])
                  for device in range(PEERS) for layer in BOTH]
    for copy in out_copies:
        copy.start()
    for router in (mixed_router, res_router):
        for t in range(router.tiles):
            router.collect(t)
        router.finish()
    net.collected(lambda d: info_out.at[d], info_recv)
    net.sent(lambda d: info_ref.at[d], info_send, info_recv)
    prompt.finish()
    columns.finish()
    slices.finish()
    leave.wait()
    for copy in out_copies:
        copy.wait()


def first_attention(x_prompt, x_resp, w_out, w_query, w_key, w_value, gain, cos, sin, info, collective_id):
    rows = TILE + x_resp.shape[0]
    width = x_resp.shape[1]
    return pl.pallas_call(
        first_attention_kernel,
        out_shape=(jax.ShapeDtypeStruct((PEERS, RING, 32, COLUMNS), BF16), jax.ShapeDtypeStruct((PEERS, 8, 16, COLUMNS), BF16),
                   jax.ShapeDtypeStruct((PEERS, 8, 128), jnp.int32), jax.ShapeDtypeStruct((TILE, PAIR * COLUMNS), BF16), jax.ShapeDtypeStruct((width, 3 * COLUMNS), BF16),
                   jax.ShapeDtypeStruct((PAIR, SHARDS, PEERS, 32, COLUMNS), BF16)),
        in_specs=[ANY] * 6 + [VMEM] * 4,
        out_specs=(VMEM,) * 4 + (ANY, ANY),
        scratch_shapes=[
            pltpu.VMEM((9, TILE, width), BF16), pltpu.VMEM((3, PAIR * width, LANES), BF16), pltpu.VMEM((width, 3 * COLUMNS), BF16), pltpu.VMEM((TILE, width), BF16), pltpu.VMEM((TILE, width), BF16),
            pltpu.VMEM((rows, COLUMNS), BF16), pltpu.VMEM((rows - TILE, COLUMNS), BF16), pltpu.VMEM((rows - TILE, COLUMNS), BF16),
            HELD, pltpu.VMEM((RING, PEERS, 32, COLUMNS), BF16), pltpu.VMEM((PEERS, 8, 16, COLUMNS), BF16),
            DMA((9,)), DMA((RING,)), *GATHER_SEMS, DMA((PEERS,)), DMA((PEERS,)),
            pltpu.VMEM((PEERS, PAIR, SHARDS, 32, COLUMNS), BF16), DMA((PAIR, PEERS)), *GATHER_SEMS,
            pltpu.VMEM((PAIR, PAIR, 32, width), BF16), DMA((PAIR,)), DMA((PAIR, SHARDS)), DMA((PAIR, SHARDS)),
            *[DMA((RING, PEERS)) for _ in BOTH], *[DMA((1, PEERS)) for _ in BOTH],
        ],
        compiler_params=pltpu.CompilerParams(collective_id=collective_id, has_side_effects=True, vmem_limit_bytes=VMEM_BYTES),
        name="first_attention",
    )(x_prompt, x_resp, w_out, w_query, w_key, w_value, gain, cos, sin, info)


def second_attention_kernel(qkv_ref, back_ref, mixed_out, stage, qkv_in, k_s, v_s, held, mixed_stage,
                            ring_send, ring_recv, near_send, near_recv, *routes):
    net = Exchange()
    me = net.me
    prompt = RespGather(net, held, ring_send, ring_recv, near_send, near_recv)
    router = Router(net, RING, lambda t, d: stage.at[t, d], lambda t, d: qkv_in.at[t, d], routes[:PAIR])
    mixed_router = Router(net, RING, lambda t, d: mixed_stage.at[t, d], lambda t, d: mixed_out.at[d, t], routes[PAIR:])
    for k in BOTH:
        held[me, k] = qkv_ref[pl.ds(0, TILE), pl.ds((k + 1) * COLUMNS, COLUMNS)]
    net.enter()
    count = back_ref.shape[1]

    def send_rows(t):
        place = lax.broadcasted_iota(jnp.int32, (Q_TILE, count), 0) + t * Q_TILE == back_ref[...]
        rows = jnp.dot(place.astype(BF16), qkv_ref[...], preferred_element_type=F32).astype(BF16)
        stage[t] = rows.reshape(PEERS, Q_TILE // PEERS, 3 * COLUMNS)
        if t == 0:
            net.all_here()
            prompt.start()
            prompt.start_rest()
        router.send(t)
        qkv_in[t, me] = stage[t, me]

    send_rows(0)
    prompt.relay()
    for t in range(1, RING):
        send_rows(t)
    prompt.share()
    prompt.collect()
    for t in range(RING):
        router.collect(t)
        rows = jnp.dot(undeal(Q_TILE), qkv_in[t].reshape(Q_TILE, 3 * COLUMNS), preferred_element_type=F32).astype(BF16)
        k_s[pl.ds(t * Q_TILE, Q_TILE)] = rows[:, COLUMNS:PAIR * COLUMNS]
        v_s[pl.ds(t * Q_TILE, Q_TILE)] = rows[:, PAIR * COLUMNS:]
        mixed = attend_response(t, rows[:, :COLUMNS], held, k_s, v_s)
        deal_mixed(mixed_router, t, mixed, mixed_stage, mixed_out)
    for t in range(RING):
        mixed_router.collect(t)
    for each in (router, mixed_router):
        each.finish()
    prompt.finish()


def second_attention(qkv, back, collective_id):
    rows = RING * Q_TILE
    wide = (32, 3 * COLUMNS)
    return pl.pallas_call(
        second_attention_kernel,
        out_shape=jax.ShapeDtypeStruct((PEERS, RING, 32, COLUMNS), BF16),
        in_specs=[VMEM, VMEM],
        out_specs=VMEM,
        scratch_shapes=[
            pltpu.VMEM((RING, PEERS) + wide, BF16), pltpu.VMEM((RING, PEERS) + wide, BF16),
            pltpu.VMEM((rows, COLUMNS), BF16), pltpu.VMEM((rows, COLUMNS), BF16),
            HELD, pltpu.VMEM((RING, PEERS, 32, COLUMNS), BF16), *GATHER_SEMS,
            *[DMA((RING, PEERS)) for _ in range(RING)],
        ],
        compiler_params=pltpu.CompilerParams(collective_id=collective_id, has_side_effects=True, vmem_limit_bytes=VMEM_BYTES),
        name=f"second_attention{collective_id}",
    )(qkv, back)


class Answer:
    def __init__(self, every, out_ref, stat_send, stat_recv, row_send, row_recv):
        self.every, self.out = every, out_ref
        self.stat_sems, self.row_sems = (stat_send, stat_recv), (row_send, row_recv)
        self.me, self.home = lax.axis_index("model"), lax.axis_index("resp")
        self.models = [(self.me + k) % SHARDS for k in range(1, SHARDS)]
        self.homes = [(self.home + k) % PEERS for k in range(1, PEERS)]

    def barrier(self):
        sem = pltpu.get_barrier_semaphore()
        for axis, devices in (("model", self.models), ("resp", self.homes)):
            for device in devices:
                pl.semaphore_signal(sem, device_id={axis: device}, device_id_type=MESH)
        pl.semaphore_wait(sem, len(self.models) + len(self.homes))

    def stat_copy(self, owner, device, place):
        ref = self.every.at[owner]
        return pltpu.make_async_remote_copy(
            src_ref=ref, dst_ref=ref, send_sem=self.stat_sems[0].at[device], recv_sem=self.stat_sems[1].at[place],
            device_id={"model": device}, device_id_type=MESH)

    def row_copy(self, owner, device, place):
        ref = self.out.at[owner]
        return pltpu.make_async_remote_copy(
            src_ref=ref, dst_ref=ref, send_sem=self.row_sems[0].at[device], recv_sem=self.row_sems[1].at[place],
            device_id={"resp": device}, device_id_type=MESH)

def combine_kernel(stats_ref, out_ref, every, *sems):
    net = Answer(every, out_ref, *sems)
    every[net.me] = stats_ref[...]
    net.barrier()
    for device in net.models:
        net.stat_copy(net.me, device, net.me).start()
    for device in net.models:
        net.stat_copy(device, device, device).wait_recv()
    shards = range(SHARDS)
    top = functools.reduce(jnp.maximum, [every[k, 0] for k in shards])
    total = functools.reduce(jnp.add, [every[k, 1] * jnp.exp(every[k, 0] - top) for k in shards])
    out_ref[net.home] = functools.reduce(jnp.add, [every[k, PAIR] for k in shards]) - top - jnp.log(total)
    for device in net.homes:
        net.row_copy(net.home, device, net.home).start()
    for device in net.homes:
        net.row_copy(device, device, device).wait_recv()
    for device in net.models:
        net.stat_copy(net.me, device, device).wait_send()
    for device in net.homes:
        net.row_copy(net.home, device, device).wait_send()


def combine(stats, collective_id):
    return pl.pallas_call(
        combine_kernel,
        out_shape=jax.ShapeDtypeStruct((PEERS, PEERS, LANES), F32),
        in_specs=[VMEM],
        out_specs=VMEM,
        scratch_shapes=[pltpu.VMEM((SHARDS,) + stats.shape, F32), *[DMA((SHARDS,)) for _ in BOTH], *[DMA((PEERS,)) for _ in BOTH]],
        compiler_params=pltpu.CompilerParams(collective_id=collective_id, has_side_effects=True),
        name="combine",
    )(stats)


ROPE_BASE = 10000.0
VARIANTS = (640, 768, 1024)


def rope_tables(positions):
    half = LANES // PAIR
    lane = jnp.arange(LANES)
    frequency = ROPE_BASE ** (-(lane % half).astype(F32) / half)
    angles = positions.astype(F32)[:, None] * frequency
    return jnp.cos(angles), jnp.sin(angles) * jnp.where(lane < half, -1.0, 1.0)


def solution(mesh):
    groups = mesh.shape['resp']
    row_axes = ('prompts', 'resp')
    head_spec = P(None, None, 'model', None)
    in_specs = (P(row_axes, None), P(row_axes, None, None), P(row_axes, None), P(row_axes), P(None, None), head_spec, head_spec, head_spec, P(None, 'model', None, None), P(None, None), P(None, None, 'model'), P(None, None, 'model'), P(None, 'model', None), P(None), P(None, 'model'))

    def device_step(x_prompt, x_resp, targets, resp_lens, attn_gain, w_query, w_key, w_value, w_out, mlp_gain, w_gate, w_up, w_down, final_gain, w_vocab):
        prompt_rows = x_prompt.shape[0]
        resp_len, width = x_resp.shape[1:]
        prompt_len = prompt_rows * groups
        me = lax.axis_index('model')
        home = lax.axis_index('resp')
        per = resp_len // groups
        gate_t, up_t = jnp.swapaxes(w_gate, 1, 2), jnp.swapaxes(w_up, 1, 2)
        out_flat = w_out.reshape(w_out.shape[0], COLUMNS, width)
        projections = [w.reshape(w.shape[0], PAIR * width, LANES) for w in (w_query, w_key, w_value)]
        prompt_pos = home * prompt_rows + jnp.arange(prompt_rows)

        cos, sin = rope_tables(jnp.concatenate([prompt_pos, prompt_len + jnp.arange(resp_len)]))
        info = jnp.concatenate([
            targets.reshape(per, groups).T[:, None, :],
            jnp.broadcast_to(resp_lens, (groups, groups - 1, per))], axis=1)
        mixed, res, infos, prompt, w_second, out_columns = first_attention(x_prompt, x_resp[0], out_flat, *projections, attn_gain, cos, sin, info, 0)
        lens = infos[:, 1, 0]
        need = (lens + groups - 1) // groups
        ends = jnp.sum(jnp.where(jnp.arange(groups)[:, None] >= jnp.arange(groups), need, 0), axis=1)
        starts = ends - need
        dealt = groups * per

        def finish_with(size, ident):
            def run(operands):
                mixed, res, prompt = operands
                slot = jnp.arange(prompt_rows + size) - prompt_rows
                which = jnp.sum((slot[:, None] >= ends).astype(jnp.int32), axis=1)
                row = slot - jnp.sum(jnp.where(which[:, None] == jnp.arange(groups), starts, 0), axis=1)
                real = (slot >= 0) & (slot < ends[-1])
                source = jnp.where(real, which * per + row, -1)
                chosen = source[:, None] == jnp.arange(dealt)
                wanted = jnp.sum(jnp.where(chosen, infos[:, 0, :].reshape(dealt), 0), axis=1) - me * w_vocab.shape[1]
                ids = jnp.where(jnp.arange(LANES) == 0, source[:, None], wanted[:, None])
                tables = rope_tables(jnp.where(slot < 0, home * prompt_rows + slot + prompt_rows, prompt_len + groups * row + home))
                weights = (out_columns.reshape(PAIR, width, COLUMNS), gate_t, up_t, w_down)
                qkv, new_res = mega(
                    mlp_gain, attn_gain, ids, mixed.reshape(dealt, COLUMNS), res.reshape(dealt, COLUMNS),
                    [*tables, prompt], *weights, w_second, 0, ident)
                part = per // RING
                back = jnp.where(real, (row // part) * (groups * part) + which * part + row % part, -1)
                mixed = second_attention(qkv, back[None], ident + 1)
                return mega(mlp_gain, final_gain[None], ids, mixed.reshape(dealt, COLUMNS), new_res, [], *weights, w_vocab, 1, ident + PAIR)
            return run

        smallest = sorted(VARIANTS)
        fit = sum((ends[-1] > size).astype(jnp.int32) for size in smallest[:-1])
        index = sum(jnp.where(fit == smallest.index(size), i, 0) for i, size in enumerate(VARIANTS))
        stats = lax.switch(index, [finish_with(size, 3 + 3 * i) for i, size in enumerate(VARIANTS)], (mixed, res, prompt))
        found = combine(stats, 1).reshape(groups, dealt)
        start = jnp.sum(jnp.where(jnp.arange(groups) == home, starts, 0))
        mine = lax.dynamic_slice(jnp.pad(found, ((0, 0), (0, per))), (0, start), (groups, per))
        log_probs = mine.T.reshape(resp_len)
        log_probs = jnp.where(jnp.arange(resp_len) < resp_lens[0], log_probs, 0.0)
        return log_probs[None, :]

    return jax.shard_map(device_step, mesh=mesh, in_specs=in_specs, out_specs=P(row_axes, None), check_vma=False)
```
